32 devices in a mesh: fsdp: 16 (over z, x, core), tp: 2 (over y).
Axes of the slice: x: 2, y: 2, z: 4, core: 2. Of those that a mesh axis runs over, the one named last changes fastest.
Arguments:
- block_input: bfloat16 [3072, 2304], P(('fsdp', 'tp')), may hold values from -6 to 6
- lengths: int32 [16, 9], P('fsdp'), may hold values from 1 to 96, 192 in all within a row
- attention_norm_gain: bfloat16 [2304], P('fsdp'), may hold values from 0.25 to 1.75
- attention_post_gain: bfloat16 [2304], P('fsdp'), may hold values from 0.25 to 1.75
- feedforward_norm_gain: bfloat16 [2304], P('fsdp'), may hold values from 0.25 to 1.75
- feedforward_post_gain: bfloat16 [2304], P('fsdp'), may hold values from 0.25 to 1.75
- query_weight: bfloat16 [2304, 2048], P('fsdp', 'tp'), may hold values from -0.125 to 0.125
- key_weight: bfloat16 [2304, 1024], P('fsdp', 'tp'), may hold values from -0.125 to 0.125
- value_weight: bfloat16 [2304, 1024], P('fsdp', 'tp'), may hold values from -0.125 to 0.125
- output_weight: bfloat16 [2304, 2048], P('fsdp', 'tp'), may hold values from -0.125 to 0.125
- gate_weight: bfloat16 [2304, 9216], P('fsdp', 'tp'), may hold values from -0.125 to 0.125
- up_weight: bfloat16 [2304, 9216], P('fsdp', 'tp'), may hold values from -0.125 to 0.125
- down_weight: bfloat16 [2304, 9216], P('fsdp', 'tp'), may hold values from -0.0625 to 0.0625
- output_cotangent: bfloat16 [3072, 2304], P(('fsdp', 'tp')), may hold values from -6 to 6
Outputs:
- block_output: bfloat16 [3072, 2304], P(('fsdp', 'tp'))
- input_gradient: float32 [3072, 2304], P(('fsdp', 'tp'))
- attention_norm_gain_gradient: float32 [2304], P('fsdp')
- attention_post_gain_gradient: float32 [2304], P('fsdp')
- feedforward_norm_gain_gradient: float32 [2304], P('fsdp')
- feedforward_post_gain_gradient: float32 [2304], P('fsdp')
- query_weight_gradient: float32 [2304, 2048], P('fsdp', 'tp')
- key_weight_gradient: float32 [2304, 1024], P('fsdp', 'tp')
- value_weight_gradient: float32 [2304, 1024], P('fsdp', 'tp')
- output_weight_gradient: float32 [2304, 2048], P('fsdp', 'tp')
- gate_weight_gradient: float32 [2304, 9216], P('fsdp', 'tp')
- up_weight_gradient: float32 [2304, 9216], P('fsdp', 'tp')
- down_weight_gradient: float32 [2304, 9216], P('fsdp', 'tp')
The draws below stay inside these ranges and needn't reach their ends.
Inputs may be any that keep to these rules, and one draw needn't show every extreme that they name: `lengths`: row g gives the length of group g's prompt (column 0) and of its 8 continuations; each row sums to 192, and its largest entry is 96.
All inputs are finite; a program needn't handle non-finite values.
Results may differ from the reference program's by a relative error of at most 0.017.
Values may be sent and summed in bfloat16 or wider, within the bound.
A program may use at most 512 MiB of HBM per device.

```python
import math
from functools import partial
import jax
import jax.numpy as jnp
import numpy as np
from jax import lax

D = 2304
QUERY_HEADS = 8
KEY_VALUE_HEADS = 4
HEAD_SIZE = 256
FF = 9216
NCONT = 8
TOK_GROUP = 192
MOST_LEN = 96
TOKENS = 3072
QD = 2048
KVD = 1024
N_FSDP = 16


def raised(array, key, source, target, parts, factor):
    def block_of(dim):
        return (jnp.arange(array.shape[dim]) // (array.shape[dim] // parts)).reshape((-1,) + (1,) * (array.ndim - 1 - dim))

    first = jax.random.permutation(key, parts)[block_of(target)]
    other_side = (block_of(target) + parts // 2) % parts
    return jnp.where((block_of(source) == first) | (block_of(source) == other_side), factor * array, array)


def shard_levels(key, extent, split, least, top_value):
    factor_of = 1.0
    for dim, shards_of in split:
        draws = jax.random.uniform(jax.random.fold_in(jax.random.fold_in(key, 6), dim), (shards_of,), jnp.float32, least / len(split), top_value / len(split))
        factor_of = factor_of * jnp.repeat(jnp.exp(draws), extent[dim] // shards_of).reshape((-1,) + (1,) * (len(extent) - 1 - dim))
    return factor_of


def profile(amount, total, reach, skew):
    loads = [(1 << 20) // math.isqrt(grade ** skew) + 1 for grade in range(2, amount + 1)]
    rest, counts = total - reach - (amount - 1), [1] * (amount - 1)
    while rest > 0:
        free = [i for i in range(amount - 1) if counts[i] < reach]
        whole, remaining = sum([loads[i] for i in free]), rest
        for i in free:
            addition = min(reach - counts[i], max(1, remaining * loads[i] // whole), rest)
            counts[i] = counts[i] + addition
            rest = rest - addition
    return np.array([reach] + counts)


def uneven_parts(stream_key, amount, total, reach, slope):
    if amount == 2:
        one = jax.random.randint(stream_key, (), max(1, total - reach), min(reach, total - 1) + 1)
        return jnp.stack([one, total - one])
    sizes = jnp.asarray(profile(amount, total, reach, slope), jnp.int32)
    couples = (amount - 1) // 2
    donor, taker = sizes[1:1 + 2 * couples:2], sizes[2:2 + 2 * couples:2]
    room = jnp.minimum(donor - 1, reach - taker)
    moved = jax.random.randint(jax.random.fold_in(stream_key, 1), (couples,), 0, 1 << 20) % (room + 1)
    sizes = sizes.at[1:1 + 2 * couples:2].set(donor - moved).at[2:2 + 2 * couples:2].set(taker + moved)
    return sizes[jax.random.permutation(jax.random.fold_in(stream_key, 2), amount)]


def noise(key, dims, spread, reach, shards=(), kind=jnp.bfloat16):
    entries = jax.random.normal(key, dims, jnp.float32) * spread
    if len(shards) > 0:
        entries = shard_levels(key, dims, shards, -0.22, 0.18) * entries
    return jnp.clip(entries, min=-reach, max=reach).astype(kind)


def bell_draw_with(own_key, extent, width, reach, cuts, heavy, kind=jnp.bfloat16):
    drawn = width * jax.random.normal(own_key, extent, jnp.float32)
    if cuts:
        drawn = drawn * shard_levels(own_key, extent, cuts, -0.22, 0.18)
    return jnp.clip(raised(drawn, jax.random.fold_in(own_key, 3), *heavy), -reach, reach).astype(kind)


def setup_inputs(seed: int = 0) -> dict:
    splits = jax.random.split(jax.random.key(seed), 15)
    block_input = bell_draw_with(splits[0], (TOKENS, D), 1.0, 6.0, ((0, 32),), (0, 1, 32, 2.75))
    lengths = jax.vmap(lambda own: uneven_parts(own, NCONT + 1, TOK_GROUP, MOST_LEN, 2))(jax.random.split(splits[1], N_FSDP)).reshape((N_FSDP, NCONT + 1)).astype(jnp.int32)
    attention_norm_gain = jnp.clip(1.0 + 0.15 * jax.random.normal(splits[2], (D,), jnp.float32), 0.25, 1.75).astype(jnp.bfloat16)
    attention_post_gain = jnp.clip(1.0 + 0.15 * jax.random.normal(splits[3], (D,), jnp.float32), 0.25, 1.75).astype(jnp.bfloat16)
    feedforward_norm_gain = jnp.clip(1.0 + 0.15 * jax.random.normal(splits[4], (D,), jnp.float32), 0.25, 1.75).astype(jnp.bfloat16)
    feedforward_post_gain = jnp.clip(1.0 + 0.15 * jax.random.normal(splits[5], (D,), jnp.float32), 0.25, 1.75).astype(jnp.bfloat16)
    query_weight = noise(splits[6], (D, QD), D ** -0.5, 0.125, ((0, 16), (1, 2)))
    key_weight = noise(splits[7], (D, KVD), D ** -0.5, 0.125, ((0, 16), (1, 2)))
    value_weight = noise(splits[8], (D, KVD), D ** -0.5, 0.125, ((0, 16), (1, 2)))
    output_weight = noise(splits[9], (D, QD), QD ** -0.5, 0.125, ((0, 16), (1, 2)))
    gate_weight = noise(splits[10], (D, FF), D ** -0.5, 0.125, ((0, 16), (1, 2)))
    up_weight = noise(splits[11], (D, FF), D ** -0.5, 0.125, ((0, 16), (1, 2)))
    down_weight = noise(splits[12], (D, FF), FF ** -0.5, 0.0625, ((0, 16), (1, 2)))
    output_cotangent = bell_draw_with(splits[13], (TOKENS, D), 1.0, 6.0, ((0, 32),), (0, 1, 32, 2.75))
    return {"block_input": block_input, "lengths": lengths, "attention_norm_gain": attention_norm_gain, "attention_post_gain": attention_post_gain, "feedforward_norm_gain": feedforward_norm_gain, "feedforward_post_gain": feedforward_post_gain, "query_weight": query_weight, "key_weight": key_weight, "value_weight": value_weight, "output_weight": output_weight, "gate_weight": gate_weight, "up_weight": up_weight, "down_weight": down_weight, "output_cotangent": output_cotangent}


@jax.custom_vjp
def reduced_precision(v):
    return lax.optimization_barrier(v.astype(jnp.bfloat16)).astype(jnp.float32)

@jax.custom_vjp
def low_back(v):
    return v

def low_keep(v):
    return (reduced_precision(v), None)

def low_pass(kept, grad):
    return (grad,)

def back_keep(v):
    return (v, None)

def back_low(kept, grad):
    return (reduced_precision(grad),)
reduced_precision.defvjp(low_keep, low_pass)
low_back.defvjp(back_keep, back_low)
EPSILON = 1e-06
SOFTCAP = 50.0
NEGATIVE = -1e+30
HIGHEST = lax.Precision.HIGHEST

def matmul(left_rows, right_rows):
    return jnp.dot(left_rows, right_rows, precision=HIGHEST, preferred_element_type=jnp.float32)

def normalize(value_rows, norm_gain):
    return value_rows * lax.rsqrt(lax.optimization_barrier(jnp.mean(value_rows * value_rows, axis=-1, keepdims=True)) + EPSILON) * norm_gain

def layout(lengths_row, grouped_rows):
    segment_ends = jnp.cumsum(lengths_row).astype(jnp.int32)
    segment_starts = (segment_ends - lengths_row).astype(jnp.int32)
    row_index = jnp.arange(grouped_rows, dtype=jnp.int32)
    segment = lax.optimization_barrier(jnp.sum((row_index[:, None] >= segment_ends[None, :]).astype(jnp.int32), axis=1)).astype(jnp.int32)
    onehot = segment[:, None] == jnp.arange(lengths_row.shape[0], dtype=jnp.int32)[None, :]
    segment_begin = lax.optimization_barrier(jnp.sum(jnp.where(onehot, segment_starts[None, :], 0), axis=1)).astype(jnp.int32)
    prompt_shift = jnp.where(segment > 0, lengths_row[0], 0).astype(jnp.int32)
    return (segment, (row_index - segment_begin + prompt_shift).astype(jnp.int32))

def rotary_tables(position):
    frequency = jnp.exp(jnp.arange(HEAD_SIZE // 2, dtype=jnp.float32) * (-2.0 * math.log(10000.0) / HEAD_SIZE))
    angles = position.astype(jnp.float32)[:, None] * frequency[None, :]
    return (jnp.cos(angles), jnp.sin(angles))

def apply_rotary(value_rows, cosine_lookup, sine_lookup):
    half_width = value_rows.shape[-1] // 2
    first_half = value_rows[..., :half_width]
    second_half = value_rows[..., half_width:]
    cosine_part = cosine_lookup[:, None, :]
    sine_part = sine_lookup[:, None, :]
    return jnp.concatenate([first_half * cosine_part - second_half * sine_part, second_half * cosine_part + first_half * sine_part], axis=-1)

def visible(segment):
    row_index = jnp.arange(segment.shape[0], dtype=jnp.int32)
    same_segment = (segment[:, None] == segment[None, :]) & (row_index[None, :] <= row_index[:, None])
    from_prompt = (segment[None, :] == 0) & (segment[:, None] > 0)
    return same_segment | from_prompt

def attend_group(items):
    query_input, key_rows, value_rows, cosine_lookup, sine_lookup, visible_mask = items
    grouped_rows = query_input.shape[0]
    repeat_heads = QUERY_HEADS // KEY_VALUE_HEADS
    rotated_query = reduced_precision(apply_rotary(query_input.reshape(grouped_rows, QUERY_HEADS, HEAD_SIZE), cosine_lookup, sine_lookup)).reshape(grouped_rows, KEY_VALUE_HEADS, repeat_heads, HEAD_SIZE)
    rotated_key = reduced_precision(apply_rotary(key_rows.reshape(grouped_rows, KEY_VALUE_HEADS, HEAD_SIZE), cosine_lookup, sine_lookup))
    value_reduced = reduced_precision(value_rows).reshape(grouped_rows, KEY_VALUE_HEADS, HEAD_SIZE)
    raw_scores = low_back(jnp.einsum('qgrd,kgd->grqk', rotated_query, rotated_key, precision=HIGHEST))
    capped = SOFTCAP * jnp.tanh(raw_scores * HEAD_SIZE ** (-0.5) / SOFTCAP)
    masked = jnp.where(visible_mask[None, None], capped, NEGATIVE)
    softmax_probs = reduced_precision(jax.nn.softmax(masked, axis=-1))
    mixed_heads = jnp.einsum('grqk,kgd->qgrd', softmax_probs, value_reduced, precision=HIGHEST)
    return low_back(reduced_precision(mixed_heads.reshape(grouped_rows, QUERY_HEADS * HEAD_SIZE)))

def forward(block_in, gain_one, gain_two, gain_three, gain_four, query_weight, key_weight, value_weight, output_weight, gate_weight, up_weight, down_weight, cosine_all, sine_all, visible_all):
    groups = visible_all.shape[0]
    grouped_rows = visible_all.shape[1]
    normed_one = reduced_precision(normalize(block_in, gain_one))
    query_input = low_back(matmul(normed_one, query_weight)).reshape(groups, grouped_rows, -1)
    key_rows = low_back(matmul(normed_one, key_weight)).reshape(groups, grouped_rows, -1)
    value_rows = low_back(matmul(normed_one, value_weight)).reshape(groups, grouped_rows, -1)
    attended = lax.map(jax.checkpoint(attend_group), (query_input, key_rows, value_rows, cosine_all, sine_all, visible_all))
    attended = attended.reshape(groups * grouped_rows, -1)
    branch_one = low_back(matmul(attended, output_weight.T))
    middle = block_in + normalize(branch_one, gain_two)
    normed_three = reduced_precision(normalize(middle, gain_three))
    gate_value = low_back(matmul(normed_three, gate_weight))
    up_value = low_back(matmul(normed_three, up_weight))
    hidden = reduced_precision(jax.nn.gelu(gate_value, approximate=True) * up_value)
    branch_two = low_back(matmul(hidden, down_weight.T))
    return middle + normalize(branch_two, gain_four)

def reference(block_input, lengths, attention_norm_gain, attention_post_gain, feedforward_norm_gain, feedforward_post_gain, query_weight, key_weight, value_weight, output_weight, gate_weight, up_weight, down_weight, output_cotangent):
    grouped_rows = block_input.shape[0] // lengths.shape[0]
    segment_all, position_all = jax.vmap(partial(layout, grouped_rows=grouped_rows))(lengths)
    cosine_all, sine_all = jax.vmap(rotary_tables)(position_all)
    visible_all = jax.vmap(visible)(segment_all)
    closed = partial(forward, cosine_all=cosine_all, sine_all=sine_all, visible_all=visible_all)
    block_output, pullback = jax.vjp(closed, block_input.astype(jnp.float32), attention_norm_gain.astype(jnp.float32), attention_post_gain.astype(jnp.float32), feedforward_norm_gain.astype(jnp.float32), feedforward_post_gain.astype(jnp.float32), query_weight.astype(jnp.float32), key_weight.astype(jnp.float32), value_weight.astype(jnp.float32), output_weight.astype(jnp.float32), gate_weight.astype(jnp.float32), up_weight.astype(jnp.float32), down_weight.astype(jnp.float32))
    gradients = pullback(output_cotangent.astype(jnp.float32))
    return (block_output.astype(jnp.bfloat16), gradients[0], gradients[1], gradients[2], gradients[3], gradients[4], gradients[5], gradients[6], gradients[7], gradients[8], gradients[9], gradients[10], gradients[11])
```

```python
import functools
import math

import jax
import jax.numpy as jnp
from jax import lax
from jax.experimental import pallas as pl
from jax.experimental.pallas import tpu as pltpu
from jax.sharding import PartitionSpec as P

HEAD_SIZE = 256
MESH = pl.DeviceIdType.MESH
ANY = pl.BlockSpec(memory_space=pl.ANY)
LANES = 128

EPSILON = 1e-06
SOFTCAP = 50.0
NEGATIVE = -1e30

KERNEL_FSDP = 16


def place():
    index = lax.axis_index("fsdp")
    return index // 4, (index // 2) % 2, index % 2, lax.axis_index("tp")


def fsdp_index(z, x, c):
    return (z * 2 + x) * 2 + c


def remote(source, target, send_sem, receive_sem, device):
    return pltpu.make_async_remote_copy(
        src_ref=source,
        dst_ref=target,
        send_sem=send_sem,
        recv_sem=receive_sem,
        device_id=device,
        device_id_type=MESH,
    )


def greet(devices):
    barrier = pltpu.get_barrier_semaphore()
    for device in devices:
        pl.semaphore_signal(barrier, inc=1, device_id=device, device_id_type=MESH)
    pl.semaphore_wait(barrier, len(devices))


def greet_line(z, devices, down, up):
    barrier = pltpu.get_barrier_semaphore()
    for device in devices:
        pl.semaphore_signal(barrier, inc=1, device_id=device, device_id_type=MESH)

    @pl.when(z > 0)
    def _():
        pl.semaphore_signal(barrier, inc=1, device_id=down, device_id_type=MESH)

    @pl.when(z < 3)
    def _():
        pl.semaphore_signal(barrier, inc=1, device_id=up, device_id_type=MESH)

    pl.semaphore_wait(barrier, len(devices) + (z + 2) // 3 + (5 - z) // 3)


def stage_through(source, stage, target, sems):
    inward = pltpu.make_async_copy(source, stage, sems.at[0])
    inward.start()

    def finish():
        inward.wait()
        outward = pltpu.make_async_copy(stage, target, sems.at[1])
        outward.start()
        return outward

    return finish


def gather_kernel(block_ref, out_ref, stage, send_sem, receive_sem, local_sem):
    z, x, c, t = place()
    down, up = (fsdp_index(z - 1, x, c), t), (fsdp_index(z + 1, x, c), t)
    across, other = (fsdp_index(z, 1 - x, c), t), (fsdp_index(z, x, 1 - c), t)
    greet_line(z, (across, other), down, up)
    finish_own = stage_through(block_ref, stage, out_ref.at[fsdp_index(z, x, c)], local_sem)

    def send(source, index, send_slot, device):
        return remote(source, out_ref.at[index], send_sem.at[send_slot], receive_sem.at[index], device)

    def arrived(index):
        remote(block_ref, out_ref.at[index], send_sem.at[0], receive_sem.at[index], other).wait_recv()

    own = fsdp_index(z, x, c)

    @pl.when(z < 3)
    def _():
        send(block_ref, own, 0, up).start()

    @pl.when(z > 0)
    def _():
        send(block_ref, own, 1, down).start()

    send(block_ref, own, 2, across).start()
    send(block_ref, own, 3, other).start()
    outward = finish_own()
    for d in (1, 2, 3):

        @pl.when(z >= d)
        def _():
            index = fsdp_index(z - d, x, c)
            base = 4 + 3 * (d - 1)
            arrived(index)

            @pl.when(z < 3)
            def _():
                send(out_ref.at[index], index, base, up).start()

            send(out_ref.at[index], index, base + 1, across).start()
            send(out_ref.at[index], index, base + 2, other).start()

        @pl.when(z + d <= 3)
        def _():
            index = fsdp_index(z + d, x, c)
            base = 13 + 3 * (d - 1)
            arrived(index)

            @pl.when(z > 0)
            def _():
                send(out_ref.at[index], index, base, down).start()

            send(out_ref.at[index], index, base + 1, across).start()
            send(out_ref.at[index], index, base + 2, other).start()

        if d == 1:
            index = fsdp_index(z, 1 - x, c)
            arrived(index)
            send(out_ref.at[index], index, 22, other).start()
    for d in (1, 2, 3):

        @pl.when(z >= d)
        def _():
            index = fsdp_index(z - d, 1 - x, c)
            arrived(index)
            send(out_ref.at[index], index, 22 + d, other).start()

        @pl.when(z + d <= 3)
        def _():
            index = fsdp_index(z + d, 1 - x, c)
            arrived(index)
            send(out_ref.at[index], index, 25 + d, other).start()

    for zi in range(4):
        for xi in range(2):
            arrived(fsdp_index(zi, xi, 1 - c))
    outward.wait()

    def sent(send_slot):
        send(block_ref, own, send_slot, other).wait_send()

    @pl.when(z < 3)
    def _():
        sent(0)

    @pl.when(z > 0)
    def _():
        sent(1)

    sent(2)
    sent(3)
    sent(22)
    for d in (1, 2, 3):

        @pl.when(z >= d)
        def _():
            base = 4 + 3 * (d - 1)

            @pl.when(z < 3)
            def _():
                sent(base)

            sent(base + 1)
            sent(base + 2)
            sent(22 + d)

        @pl.when(z + d <= 3)
        def _():
            base = 13 + 3 * (d - 1)

            @pl.when(z > 0)
            def _():
                sent(base)

            sent(base + 1)
            sent(base + 2)
            sent(25 + d)


def scratch_call(kernel, outputs, scratch, collective_id, *operands):
    return pl.pallas_call(
        kernel,
        out_shape=outputs,
        in_specs=[ANY] * len(operands),
        out_specs=jax.tree.map(lambda _: ANY, outputs),
        scratch_shapes=scratch,
        compiler_params=pltpu.CompilerParams(
            collective_id=collective_id, has_side_effects=True, vmem_limit_bytes=60 * 1024 * 1024
        ),
    )(*operands)


def gather_fsdp(block, collective_id):
    size = lax.axis_size("fsdp")
    if size != KERNEL_FSDP:
        return lax.all_gather(block, "fsdp", axis=0)
    return scratch_call(
        gather_kernel,
        jax.ShapeDtypeStruct((size,) + block.shape, block.dtype),
        [
            pltpu.VMEM(block.shape, block.dtype),
            pltpu.SemaphoreType.DMA((29,)),
            pltpu.SemaphoreType.DMA((size,)),
            pltpu.SemaphoreType.DMA((2,)),
        ],
        collective_id,
        block,
    )


def add_rows(rows, step, target, *sources):
    def body(i, carry):
        at = pl.ds(pl.multiple_of(i * step, step), step)
        total = sources[0][at, :].astype(jnp.float32)
        for source in sources[1:]:
            total = total + source[at, :].astype(jnp.float32)
        target[at, :] = total.astype(target.dtype)
        return carry

    lax.fori_loop(0, rows // step, body, 0)


def scatter_kernel(parts_ref, out_ref, held, from_core, from_across, from_below, from_above, total,
                   send_sem, core_sem, across_sem, below_sem, above_sem, local_sem):
    z, x, c, t = place()
    rows = out_ref.shape[0]
    down, up = (fsdp_index(z - 1, x, c), t), (fsdp_index(z + 1, x, c), t)
    across, other = (fsdp_index(z, 1 - x, c), t), (fsdp_index(z, x, 1 - c), t)
    half = z // 2
    mirrored = z + half * (3 - 2 * z)

    def target_of(i):
        if i == 3:
            return z
        base = 3 - i - (i + mirrored) // 3
        return base + half * (3 - 2 * base)

    local = []
    for k in range(8):
        owner_x = 1 - x if k < 4 else x
        copy = pltpu.make_async_copy(
            parts_ref.at[fsdp_index(target_of(k % 4), owner_x, c)], held.at[k], local_sem.at[k]
        )
        copy.start()
        local.append(copy)
    greet_line(z, (across, other), down, up)
    to_core = []
    for k in range(8):
        owner_x = 1 - x if k < 4 else x
        copy = remote(
            parts_ref.at[fsdp_index(target_of(k % 4), owner_x, 1 - c)],
            from_core.at[k],
            send_sem.at[k],
            core_sem.at[k],
            other,
        )
        copy.start()
        to_core.append(copy)
    to_across = []
    for i in range(4):
        local[i].wait()
        to_core[i].wait_recv()
        add_rows(rows, 16, held.at[i], held.at[i], from_core.at[i])
        copy = remote(held.at[i], from_across.at[i], send_sem.at[8 + i], across_sem.at[i], across)
        copy.start()
        to_across.append(copy)
    for i in range(3):
        k = 4 + i
        target = target_of(i)
        local[k].wait()
        to_core[k].wait_recv()
        to_across[i].wait_recv()

        @pl.when(target > z)
        def _():
            @pl.when(z > 0)
            def _():
                remote(held.at[k], from_below.at[target], send_sem.at[12 + i], below_sem.at[target], up).wait_recv()
                add_rows(rows, 16, held.at[k], held.at[k], from_core.at[k], from_across.at[i], from_below.at[target])

            @pl.when(z == 0)
            def _():
                add_rows(rows, 16, held.at[k], held.at[k], from_core.at[k], from_across.at[i])

            remote(held.at[k], from_below.at[target], send_sem.at[12 + i], below_sem.at[target], up).start()

        @pl.when(target < z)
        def _():
            @pl.when(z < 3)
            def _():
                remote(held.at[k], from_above.at[target], send_sem.at[12 + i], above_sem.at[target], down).wait_recv()
                add_rows(rows, 16, held.at[k], held.at[k], from_core.at[k], from_across.at[i], from_above.at[target])

            @pl.when(z == 3)
            def _():
                add_rows(rows, 16, held.at[k], held.at[k], from_core.at[k], from_across.at[i])

            remote(held.at[k], from_above.at[target], send_sem.at[12 + i], above_sem.at[target], down).start()

    local[7].wait()
    to_core[7].wait_recv()
    to_across[3].wait_recv()
    add_rows(rows, 16, total, held.at[7], from_core.at[7], from_across.at[3])

    @pl.when(z > 0)
    def _():
        remote(held.at[7], from_below.at[z], send_sem.at[12], below_sem.at[z], up).wait_recv()
        add_rows(rows, 16, total, total, from_below.at[z])

    @pl.when(z < 3)
    def _():
        remote(held.at[7], from_above.at[z], send_sem.at[12], above_sem.at[z], down).wait_recv()
        add_rows(rows, 16, total, total, from_above.at[z])

    outward = pltpu.make_async_copy(total, out_ref, local_sem.at[8])
    outward.start()
    for copy in to_core + to_across:
        copy.wait_send()
    for i in range(3):
        remote(held.at[4 + i], from_below.at[0], send_sem.at[12 + i], below_sem.at[0], other).wait_send()
    outward.wait()


def scatter_fsdp(parts, collective_id):
    size, rows, columns = parts.shape
    if size != KERNEL_FSDP:
        return lax.psum_scatter(parts, "fsdp", scatter_dimension=0, tiled=False).astype(jnp.float32)
    block = (rows, columns)
    return scratch_call(
        scatter_kernel,
        jax.ShapeDtypeStruct(block, jnp.float32),
        [
            pltpu.VMEM((8,) + block, parts.dtype),
            pltpu.VMEM((8,) + block, parts.dtype),
            pltpu.VMEM((4,) + block, parts.dtype),
            pltpu.VMEM((4,) + block, parts.dtype),
            pltpu.VMEM((4,) + block, parts.dtype),
            pltpu.VMEM(block, jnp.float32),
            pltpu.SemaphoreType.DMA((15,)),
            pltpu.SemaphoreType.DMA((8,)),
            pltpu.SemaphoreType.DMA((4,)),
            pltpu.SemaphoreType.DMA((4,)),
            pltpu.SemaphoreType.DMA((4,)),
            pltpu.SemaphoreType.DMA((9,)),
        ],
        collective_id,
        parts,
    )


def exchange_kernel(block_ref, out_ref, send_sem, receive_sem):
    index, t = lax.axis_index("fsdp"), lax.axis_index("tp")
    partner = (index, 1 - t)
    greet((partner,))
    copy = remote(block_ref, out_ref, send_sem.at[0], receive_sem.at[0], partner)
    copy.start()
    copy.wait()


def exchange_tp(block, collective_id):
    if lax.axis_size("fsdp") != KERNEL_FSDP:
        return lax.ppermute(block, "tp", [(0, 1), (1, 0)])
    return scratch_call(
        exchange_kernel,
        jax.ShapeDtypeStruct(block.shape, block.dtype),
        [pltpu.SemaphoreType.DMA((1,)), pltpu.SemaphoreType.DMA((1,))],
        collective_id,
        block,
    )


def peer(z, x, c, k):
    kz, kx, kc = k // 4, (k // 2) % 2, k % 2
    high, low = z // 2, z % 2
    high = 1 - high if kz // 2 else high
    low = 1 - low if kz % 2 else low
    return fsdp_index(high * 2 + low, 1 - x if kx else x, 1 - c if kc else c)


def resplit_kernel(parts_ref, out_ref, stage, send_sem, receive_sem, on_sem, pair_sem, local_sem):
    z, x, c, t = place()
    own = fsdp_index(z, x, c)
    partner = (own, 1 - t)
    greet([(peer(z, x, c, k), t) for k in range(1, 16)] + [partner])
    finish_own = stage_through(parts_ref.at[own], stage, out_ref.at[t, own], local_sem)
    onward = [remote(parts_ref.at[own], out_ref.at[t, own], on_sem.at[0], pair_sem.at[0], partner)]
    onward[0].start()
    direct = []
    for k in range(1, 16):
        to = peer(z, x, c, k)
        copy = remote(parts_ref.at[to], out_ref.at[t, own], send_sem.at[k], receive_sem.at[k], (to, t))
        copy.start()
        direct.append(copy)
    outward = finish_own()
    for k in range(1, 16):
        source = peer(z, x, c, k)
        direct[k - 1].wait_recv()
        copy = remote(out_ref.at[t, source], out_ref.at[t, source], on_sem.at[k], pair_sem.at[k], partner)
        copy.start()
        onward.append(copy)
    outward.wait()
    for copy in onward:
        copy.wait_recv()
    for copy in direct + onward:
        copy.wait_send()


def resplit(parts, collective_id):
    size = parts.shape[0]
    if size != KERNEL_FSDP:
        mine = lax.all_to_all(parts, "fsdp", split_axis=0, concat_axis=0, tiled=True)
        return lax.all_gather(mine, "tp", axis=0)
    return scratch_call(
        resplit_kernel,
        jax.ShapeDtypeStruct((2,) + parts.shape, parts.dtype),
        [
            pltpu.VMEM(parts.shape[1:], parts.dtype),
            pltpu.SemaphoreType.DMA((16,)),
            pltpu.SemaphoreType.DMA((16,)),
            pltpu.SemaphoreType.DMA((16,)),
            pltpu.SemaphoreType.DMA((16,)),
            pltpu.SemaphoreType.DMA((2,)),
        ],
        collective_id,
        parts,
    )


def unsplit_kernel(parts_ref, out_ref, held, received, send_sem, receive_sem, on_sem, pair_sem, local_sem):
    z, x, c, t = place()
    own = fsdp_index(z, x, c)
    rows = out_ref.shape[1]
    partner = (own, 1 - t)
    order = list(range(15, -1, -1))
    local = {}
    for k in order:
        copy = pltpu.make_async_copy(parts_ref.at[t, peer(z, x, c, k)], held.at[k], local_sem.at[k])
        copy.start()
        local[k] = copy
    greet([(peer(z, x, c, k), t) for k in range(1, 16)] + [partner])
    pair = {}
    for k in order:
        copy = remote(
            parts_ref.at[1 - t, peer(z, x, c, k)], received.at[k], on_sem.at[k], pair_sem.at[k], partner
        )
        copy.start()
        pair[k] = copy
    direct = []
    for k in order:
        local[k].wait()
        pair[k].wait_recv()
        add_rows(rows, 16, held.at[k], held.at[k], received.at[k])
        if k:
            copy = remote(held.at[k], out_ref.at[own], send_sem.at[k], receive_sem.at[k], (peer(z, x, c, k), t))
            copy.start()
            direct.append(copy)
    keep = pltpu.make_async_copy(held.at[0], out_ref.at[own], local_sem.at[16])
    keep.start()
    for copy in direct:
        copy.wait_recv()
    keep.wait()
    for copy in direct + list(pair.values()):
        copy.wait_send()


def unsplit(parts, collective_id):
    pairs, size, rows, columns = parts.shape
    if size != KERNEL_FSDP:
        mine = lax.psum_scatter(parts, "tp", scatter_dimension=0, tiled=False)
        return lax.all_to_all(mine, "fsdp", split_axis=0, concat_axis=0, tiled=True)
    return scratch_call(
        unsplit_kernel,
        jax.ShapeDtypeStruct((size, rows, columns), parts.dtype),
        [
            pltpu.VMEM((size, rows, columns), parts.dtype),
            pltpu.VMEM((size, rows, columns), parts.dtype),
            pltpu.SemaphoreType.DMA((16,)),
            pltpu.SemaphoreType.DMA((16,)),
            pltpu.SemaphoreType.DMA((16,)),
            pltpu.SemaphoreType.DMA((16,)),
            pltpu.SemaphoreType.DMA((17,)),
        ],
        collective_id,
        parts,
    )


def contract_last(left_rows, right_rows):
    return lax.dot_general(
        left_rows, right_rows, (((1,), (1,)), ((), ())), preferred_element_type=jnp.float32
    )


def contract_first(left_rows, right_rows):
    return lax.dot_general(
        left_rows, right_rows, (((0,), (0,)), ((), ())), preferred_element_type=jnp.float32
    )


def normalize_parts(value_rows):
    inverse = lax.rsqrt(jnp.mean(value_rows * value_rows, axis=-1, keepdims=True) + EPSILON)
    return (value_rows * inverse, inverse)


def norm_backward(unit_rows, inverse, norm_gain, upstream):
    scaled = upstream * norm_gain
    return inverse * (scaled - unit_rows * jnp.mean(scaled * unit_rows, axis=-1, keepdims=True))


def layout(lengths_row, row_index):
    segment_ends = jnp.cumsum(lengths_row)
    segment_starts = segment_ends - lengths_row
    segment = jnp.sum((row_index[:, None] >= segment_ends[None, :]).astype(jnp.int32), axis=1)
    onehot = segment[:, None] == jnp.arange(lengths_row.shape[0], dtype=jnp.int32)[None, :]
    segment_begin = jnp.sum(jnp.where(onehot, segment_starts[None, :], 0), axis=1)
    prompt_shift = jnp.where(segment > 0, lengths_row[0], 0)
    return (segment, row_index - segment_begin + prompt_shift)


def rotary_tables(position):
    frequency = jnp.exp(
        jnp.arange(HEAD_SIZE // 2, dtype=jnp.float32) * (-2.0 * math.log(10000.0) / HEAD_SIZE)
    )
    angles = position.astype(jnp.float32)[:, None] * frequency[None, :]
    return (jnp.cos(angles), jnp.sin(angles))


def apply_rotary(value_rows, cosine_lookup, sine_lookup):
    half_width = value_rows.shape[-1] // 2
    first_half = value_rows[..., :half_width]
    second_half = value_rows[..., half_width:]
    cosine_part = cosine_lookup[:, None, :]
    sine_part = sine_lookup[:, None, :]
    return jnp.concatenate(
        [
            first_half * cosine_part - second_half * sine_part,
            second_half * cosine_part + first_half * sine_part,
        ],
        axis=-1,
    )


def unrotate(value_rows, cosine_lookup, sine_lookup):
    half_width = value_rows.shape[-1] // 2
    first_half = value_rows[..., :half_width]
    second_half = value_rows[..., half_width:]
    cosine_part = cosine_lookup[:, None, :]
    sine_part = sine_lookup[:, None, :]
    return jnp.concatenate(
        [
            first_half * cosine_part + second_half * sine_part,
            second_half * cosine_part - first_half * sine_part,
        ],
        axis=-1,
    )


def visible(segment, row_index):
    same_segment = (segment[:, None] == segment[None, :]) & (
        row_index[None, :] <= row_index[:, None]
    )
    from_prompt = (segment[None, :] == 0) & (segment[:, None] > 0)
    return same_segment | from_prompt


def masked_scores(rotated_query, rotated_key, visible_mask):
    raw_scores = jnp.einsum(
        "qgrd,kgd->grqk", rotated_query, rotated_key, preferred_element_type=jnp.float32
    )
    tanh_value = jnp.tanh(raw_scores * HEAD_SIZE ** (-0.5) / SOFTCAP)
    return (jnp.where(visible_mask[None, None], SOFTCAP * tanh_value, NEGATIVE), tanh_value)


def gelu_product(gate_value, up_value):
    return jax.nn.gelu(gate_value, approximate=True) * up_value


def split_columns(width, size):
    main = width // size // LANES * LANES
    return main, width // size - main


def pack_units(weights, size):
    rows, width = weights[0].shape
    main, rest = split_columns(width, size)
    pieces = []
    if main:
        pieces += [
            jnp.transpose(w[:, : main * size].reshape(rows, size, main), (1, 0, 2)) for w in weights
        ]
    if rest:
        pieces += [
            jnp.transpose(w[:, main * size :].reshape(rows, size, rest), (1, 0, 2)) for w in weights
        ]
    packed = jnp.concatenate(pieces, axis=2)
    return jnp.pad(packed, ((0, 0), (0, 0), (0, -packed.shape[2] % LANES)))


def unpack_units(packed, width, amount):
    size, rows, _ = packed.shape
    main, rest = split_columns(width, size)
    arrays = []
    for i in range(amount):
        pieces = []
        if main:
            piece = packed[:, :, i * main : (i + 1) * main]
            pieces.append(jnp.transpose(piece, (1, 0, 2)).reshape(rows, size * main))
        if rest:
            start = amount * main + i * rest
            piece = packed[:, :, start : start + rest]
            pieces.append(jnp.transpose(piece, (1, 0, 2)).reshape(rows, size * rest))
        arrays.append(jnp.concatenate(pieces, axis=1))
    return arrays


def join_units(halves, width, size, amount):
    main, rest = split_columns(width, size)
    arrays = []
    for i in range(amount):
        start = amount * main + i * rest
        pieces = [half[:, i * main : (i + 1) * main] for half in halves]
        pieces += [half[:, start : start + rest] for half in halves]
        joined = jnp.concatenate(pieces, axis=1)
        arrays.append(jnp.pad(joined, ((0, 0), (0, -joined.shape[1] % LANES))))
    return arrays


def part_units(arrays, width, size, pairs):
    main, rest = split_columns(width, size)
    halves = []
    for t in range(pairs):
        pieces = [array[:, t * main : (t + 1) * main] for array in arrays]
        start = pairs * main + t * rest
        pieces += [array[:, start : start + rest] for array in arrays]
        packed = jnp.concatenate(pieces, axis=1)
        halves.append(jnp.pad(packed, ((0, 0), (0, -packed.shape[1] % LANES))))
    return jnp.stack(halves)


def shards(
    block_input,
    lengths,
    attention_norm_gain,
    attention_post_gain,
    feedforward_norm_gain,
    feedforward_post_gain,
    query_weight,
    key_weight,
    value_weight,
    output_weight,
    gate_weight,
    up_weight,
    down_weight,
    output_cotangent,
):
    low = jnp.bfloat16
    size, pairs = lax.axis_size("fsdp"), lax.axis_size("tp")
    rows_local, width = block_input.shape
    shard_rows, feed_width = gate_weight.shape
    query_width, key_width = query_weight.shape[1], key_weight.shape[1]
    output_start = query_width + 2 * key_width
    gain_start = output_start + query_width
    grouped_rows = rows_local * pairs

    gain_columns = jnp.stack(
        [attention_norm_gain, attention_post_gain, feedforward_norm_gain, feedforward_post_gain],
        axis=1,
    )
    attention_block = jnp.concatenate(
        [
            query_weight,
            key_weight,
            value_weight,
            output_weight,
            jnp.pad(gain_columns, ((0, 0), (0, LANES - 4))),
        ],
        axis=1,
    )
    attention_full = gather_fsdp(attention_block, 1).reshape(size * shard_rows, gain_start + LANES)
    gains = jnp.transpose(attention_full[:, gain_start : gain_start + 4]).astype(jnp.float32)
    gain_one, gain_two, gain_three, gain_four = gains[0], gains[1], gains[2], gains[3]
    other_input = exchange_tp(block_input, 2)

    feed_halves = resplit(pack_units((gate_weight, up_weight, down_weight), size), 3)
    feed_halves = feed_halves.reshape(pairs, size * shard_rows, feed_halves.shape[-1])
    gate_full, up_full, down_full = join_units(feed_halves, feed_width, size, 3)
    units = gate_full.shape[1]

    row_index = (
        jnp.arange(grouped_rows, dtype=jnp.int32) + lax.axis_index("tp") * rows_local
    ) % grouped_rows
    segment, position = layout(lengths[0], row_index)
    cosine_lookup, sine_lookup = rotary_tables(position)
    visible_mask = visible(segment, row_index)
    residual_both = jnp.concatenate([block_input, other_input], axis=0).astype(jnp.float32)
    unit_one_both, inverse_one_both = normalize_parts(residual_both)
    residual = residual_both[:rows_local]
    unit_one, inverse_one = unit_one_both[:rows_local], inverse_one_both[:rows_local]
    normed = (unit_one_both * gain_one).astype(low)
    projected = jnp.dot(
        normed, attention_full[:, :output_start], preferred_element_type=jnp.float32
    )
    query_raw = projected[:, :query_width]
    key_raw = projected[:, query_width : query_width + key_width]
    value_raw = projected[:, query_width + key_width :]
    heads_local = query_width // HEAD_SIZE
    kv_local = key_width // HEAD_SIZE
    repeat_heads = heads_local // kv_local
    rotated_query = apply_rotary(
        query_raw.reshape(grouped_rows, heads_local, HEAD_SIZE), cosine_lookup, sine_lookup
    ).astype(low)
    rotated_query = rotated_query.reshape(grouped_rows, kv_local, repeat_heads, HEAD_SIZE)
    rotated_key = apply_rotary(
        key_raw.reshape(grouped_rows, kv_local, HEAD_SIZE), cosine_lookup, sine_lookup
    ).astype(low)
    value_reduced = value_raw.astype(low).reshape(grouped_rows, kv_local, HEAD_SIZE)
    capped, tanh_value = masked_scores(rotated_query, rotated_key, visible_mask)
    row_peak = jnp.max(capped, axis=-1, keepdims=True)
    exponentials = jnp.exp(capped - row_peak)
    softmax_probs = exponentials / jnp.sum(exponentials, axis=-1, keepdims=True)
    probs_low = softmax_probs.astype(low)
    mixed_heads = jnp.einsum(
        "grqk,kgd->qgrd", probs_low, value_reduced, preferred_element_type=jnp.float32
    )
    attended = mixed_heads.reshape(grouped_rows, heads_local * HEAD_SIZE).astype(low)
    output_full = attention_full[:, output_start:gain_start]
    branch_parts = contract_last(attended, output_full)
    branch_one = branch_parts[:rows_local] + exchange_tp(
        branch_parts[rows_local:].astype(low), 4
    ).astype(jnp.float32)
    unit_two, inverse_two = normalize_parts(branch_one)
    middle = residual + unit_two * gain_two
    unit_three, inverse_three = normalize_parts(middle)

    feed_input = gather_fsdp((unit_three * gain_three).astype(low), 5).reshape(-1, width)
    gate_value = jnp.dot(feed_input, gate_full, preferred_element_type=jnp.float32)
    up_value = jnp.dot(feed_input, up_full, preferred_element_type=jnp.float32)
    hidden = gelu_product(gate_value, up_value).astype(low)
    branch_two = scatter_fsdp(
        contract_last(hidden, down_full).astype(low).reshape(size, rows_local, width), 6
    )
    unit_four, inverse_four = normalize_parts(branch_two)
    block_output = (middle + unit_four * gain_four).astype(low)
    upstream = output_cotangent.astype(jnp.float32)
    gain_four_grad = jnp.sum(upstream * unit_four, axis=0)
    branch_two_grad = norm_backward(unit_four, inverse_four, gain_four, upstream).astype(low)
    feed_grad_rows = gather_fsdp(branch_two_grad, 7).reshape(-1, width)
    hidden_grad = jnp.dot(feed_grad_rows, down_full, preferred_element_type=jnp.float32)
    unused_out, pullback = jax.vjp(gelu_product, gate_value, up_value)
    gate_grad, up_grad = pullback(hidden_grad)
    gate_grad, up_grad = gate_grad.astype(low), up_grad.astype(low)
    normed_three_grad = scatter_fsdp(
        (contract_last(gate_grad, gate_full) + contract_last(up_grad, up_full))
        .astype(low)
        .reshape(size, rows_local, width),
        8,
    )
    feed_grads = part_units(
        (
            contract_first(feed_input, gate_grad),
            contract_first(feed_input, up_grad),
            contract_first(feed_grad_rows, hidden),
        ),
        feed_width,
        size,
        pairs,
    ).astype(low)
    feed_grads = feed_grads.reshape(pairs, size, shard_rows, feed_grads.shape[-1])
    gate_weight_grad, up_weight_grad, down_weight_grad = unpack_units(
        unsplit(feed_grads, 9).astype(jnp.float32), feed_width, 3
    )

    gain_three_grad = jnp.sum(normed_three_grad * unit_three, axis=0)
    middle_grad = upstream + norm_backward(unit_three, inverse_three, gain_three, normed_three_grad)
    gain_two_grad = jnp.sum(middle_grad * unit_two, axis=0)
    branch_one_grad = norm_backward(unit_two, inverse_two, gain_two, middle_grad).astype(low)
    attention_grad_rows = jnp.concatenate(
        [branch_one_grad, exchange_tp(branch_one_grad, 10)], axis=0
    )
    mixed_grad = jnp.dot(
        attention_grad_rows, output_full, preferred_element_type=jnp.float32
    ).astype(low)
    mixed_grad = mixed_grad.reshape(grouped_rows, kv_local, repeat_heads, HEAD_SIZE)
    value_grad = jnp.einsum(
        "grqk,qgrd->kgd", probs_low, mixed_grad, preferred_element_type=jnp.float32
    )
    probs_grad = jnp.einsum(
        "qgrd,kgd->grqk", mixed_grad, value_reduced, preferred_element_type=jnp.float32
    )
    score_grad = softmax_probs * (
        probs_grad - jnp.sum(softmax_probs * probs_grad, axis=-1, keepdims=True)
    )
    raw_grad = (score_grad * (1.0 - tanh_value * tanh_value) * HEAD_SIZE ** (-0.5)).astype(low)
    query_grad = jnp.einsum(
        "grqk,kgd->qgrd", raw_grad, rotated_key, preferred_element_type=jnp.float32
    )
    key_grad = jnp.einsum(
        "grqk,qgrd->kgd", raw_grad, rotated_query, preferred_element_type=jnp.float32
    )
    query_grad = unrotate(
        query_grad.reshape(grouped_rows, heads_local, HEAD_SIZE), cosine_lookup, sine_lookup
    )
    key_grad = unrotate(key_grad, cosine_lookup, sine_lookup)
    projected_grad = jnp.concatenate(
        [
            query_grad.reshape(grouped_rows, heads_local * HEAD_SIZE).astype(low),
            key_grad.reshape(grouped_rows, kv_local * HEAD_SIZE).astype(low),
            value_grad.reshape(grouped_rows, kv_local * HEAD_SIZE).astype(low),
        ],
        axis=1,
    )
    input_parts = contract_last(projected_grad, attention_full[:, :output_start])

    gain_grads = jnp.stack(
        [
            jnp.sum(input_parts * unit_one_both, axis=0),
            gain_two_grad,
            gain_three_grad,
            gain_four_grad,
        ]
    )
    sent = jnp.concatenate(
        [input_parts[rows_local:].astype(low), jnp.pad(gain_grads, ((0, 12), (0, 0))).astype(low)]
    )
    received = exchange_tp(sent, 11).astype(jnp.float32)
    normed_one_grad = input_parts[:rows_local] + received[:rows_local]
    gain_grads = gain_grads + received[rows_local : rows_local + 4]
    input_gradient = middle_grad + norm_backward(unit_one, inverse_one, gain_one, normed_one_grad)

    attention_grads = jnp.concatenate(
        [
            contract_first(normed, projected_grad).astype(low),
            contract_first(attention_grad_rows, attended).astype(low),
            jnp.pad(jnp.transpose(gain_grads), ((0, 0), (0, LANES - 4))).astype(low),
        ],
        axis=1,
    )
    attention_grads = scatter_fsdp(
        attention_grads.reshape(size, shard_rows, gain_start + LANES), 12
    )
    gain_shards = jnp.transpose(attention_grads[:, gain_start : gain_start + 4])
    return (
        block_output,
        input_gradient,
        gain_shards[0],
        gain_shards[1],
        gain_shards[2],
        gain_shards[3],
        attention_grads[:, :query_width],
        attention_grads[:, query_width : query_width + key_width],
        attention_grads[:, query_width + key_width : output_start],
        attention_grads[:, output_start:gain_start],
        gate_weight_grad,
        up_weight_grad,
        down_weight_grad,
    )


def solution(mesh):
    placed = (
        P(("fsdp", "tp"), None),
        P("fsdp", None),
        P("fsdp"),
        P("fsdp"),
        P("fsdp"),
        P("fsdp"),
        P("fsdp", "tp"),
        P("fsdp", "tp"),
        P("fsdp", "tp"),
        P("fsdp", "tp"),
        P("fsdp", "tp"),
        P("fsdp", "tp"),
        P("fsdp", "tp"),
        P(("fsdp", "tp"), None),
    )
    return jax.shard_map(
        shards,
        mesh=mesh,
        in_specs=placed,
        out_specs=(
            P(("fsdp", "tp"), None),
            P(("fsdp", "tp"), None),
            P("fsdp"),
            P("fsdp"),
            P("fsdp"),
            P("fsdp"),
            P("fsdp", "tp"),
            P("fsdp", "tp"),
            P("fsdp", "tp"),
            P("fsdp", "tp"),
            P("fsdp", "tp"),
            P("fsdp", "tp"),
            P("fsdp", "tp"),
        ),
        check_vma=False,
    )
```

```python
import functools
import math

import jax
import jax.numpy as jnp
from jax import lax
from jax.experimental import pallas as pl
from jax.experimental.pallas import tpu as pltpu
from jax.sharding import PartitionSpec as P

HEAD_SIZE = 256
MESH = pl.DeviceIdType.MESH
ANY = pl.BlockSpec(memory_space=pl.ANY)
LANES = 128

EPSILON = 1e-06
SOFTCAP = 50.0
NEGATIVE = -1e30

KERNEL_FSDP = 16


def place():
    index = lax.axis_index("fsdp")
    return index // 4, (index // 2) % 2, index % 2, lax.axis_index("tp")


def fsdp_index(z, x, c):
    return (z * 2 + x) * 2 + c


def remote(source, target, send_sem, receive_sem, device):
    return pltpu.make_async_remote_copy(
        src_ref=source,
        dst_ref=target,
        send_sem=send_sem,
        recv_sem=receive_sem,
        device_id=device,
        device_id_type=MESH,
    )


def greet(devices):
    barrier = pltpu.get_barrier_semaphore()
    for device in devices:
        pl.semaphore_signal(barrier, inc=1, device_id=device, device_id_type=MESH)
    pl.semaphore_wait(barrier, len(devices))


def greet_line(z, devices, down, up):
    barrier = pltpu.get_barrier_semaphore()
    for device in devices:
        pl.semaphore_signal(barrier, inc=1, device_id=device, device_id_type=MESH)

    @pl.when(z > 0)
    def _():
        pl.semaphore_signal(barrier, inc=1, device_id=down, device_id_type=MESH)

    @pl.when(z < 3)
    def _():
        pl.semaphore_signal(barrier, inc=1, device_id=up, device_id_type=MESH)

    pl.semaphore_wait(barrier, len(devices) + (z + 2) // 3 + (5 - z) // 3)


def stage_through(source, stage, target, sems):
    inward = pltpu.make_async_copy(source, stage, sems.at[0])
    inward.start()

    def finish():
        inward.wait()
        outward = pltpu.make_async_copy(stage, target, sems.at[1])
        outward.start()
        return outward

    return finish


class Gather:
    slots = 29

    def __init__(self, block, out_ref, send_sem, receive_sem):
        self.block, self.out, self.send_sem, self.receive_sem = block, out_ref, send_sem, receive_sem
        self.z, self.x, self.c, t = place()
        z, x, c = self.z, self.x, self.c
        self.own = fsdp_index(z, x, c)
        self.down, self.up = (fsdp_index(z - 1, x, c), t), (fsdp_index(z + 1, x, c), t)
        self.across, self.other = (fsdp_index(z, 1 - x, c), t), (fsdp_index(z, x, 1 - c), t)

    def copy(self, source, index, slot, device):
        return remote(source, self.out.at[index], self.send_sem.at[slot], self.receive_sem.at[index], device)

    def relay(self, index, slot, device):
        self.copy(self.out.at[index], index, slot, device).start()

    def arrived(self, index):
        self.copy(self.block, index, 0, self.other).wait_recv()

    def sent(self, slot):
        self.copy(self.block, self.own, slot, self.other).wait_send()

    def start(self):
        @pl.when(self.z < 3)
        def _():
            self.copy(self.block, self.own, 0, self.up).start()

        @pl.when(self.z > 0)
        def _():
            self.copy(self.block, self.own, 1, self.down).start()

        self.copy(self.block, self.own, 2, self.across).start()
        self.copy(self.block, self.own, 3, self.other).start()

    def line(self, d):
        z, x, c = self.z, self.x, self.c

        @pl.when(z >= d)
        def _():
            index = fsdp_index(z - d, x, c)
            base = 4 + 3 * (d - 1)
            self.arrived(index)

            @pl.when(z < 3)
            def _():
                self.relay(index, base, self.up)

            self.relay(index, base + 1, self.across)
            self.relay(index, base + 2, self.other)

        @pl.when(z + d <= 3)
        def _():
            index = fsdp_index(z + d, x, c)
            base = 13 + 3 * (d - 1)
            self.arrived(index)

            @pl.when(z > 0)
            def _():
                self.relay(index, base, self.down)

            self.relay(index, base + 1, self.across)
            self.relay(index, base + 2, self.other)

    def side(self, d):
        z, x, c = self.z, self.x, self.c
        if d == 0:
            index = fsdp_index(z, 1 - x, c)
            self.arrived(index)
            self.relay(index, 22, self.other)
            return

        @pl.when(z >= d)
        def _():
            index = fsdp_index(z - d, 1 - x, c)
            self.arrived(index)
            self.relay(index, 22 + d, self.other)

        @pl.when(z + d <= 3)
        def _():
            index = fsdp_index(z + d, 1 - x, c)
            self.arrived(index)
            self.relay(index, 25 + d, self.other)

    def finish(self):
        z = self.z
        for zi in range(4):
            for xi in range(2):
                self.arrived(fsdp_index(zi, xi, 1 - self.c))

        @pl.when(z < 3)
        def _():
            self.sent(0)

        @pl.when(z > 0)
        def _():
            self.sent(1)

        for slot in (2, 3, 22):
            self.sent(slot)
        for d in (1, 2, 3):

            @pl.when(z >= d)
            def _():
                base = 4 + 3 * (d - 1)

                @pl.when(z < 3)
                def _():
                    self.sent(base)

                for slot in (base + 1, base + 2, 22 + d):
                    self.sent(slot)

            @pl.when(z + d <= 3)
            def _():
                base = 13 + 3 * (d - 1)

                @pl.when(z > 0)
                def _():
                    self.sent(base)

                for slot in (base + 1, base + 2, 25 + d):
                    self.sent(slot)


def gather_kernel(block_ref, out_ref, stage, send_sem, receive_sem, local_sem):
    gather = Gather(block_ref, out_ref, send_sem, receive_sem)
    greet_line(gather.z, (gather.across, gather.other), gather.down, gather.up)
    finish_own = stage_through(block_ref, stage, out_ref.at[gather.own], local_sem)
    gather.start()
    outward = finish_own()
    gather.line(1)
    gather.side(0)
    gather.line(2)
    gather.side(1)
    gather.line(3)
    gather.side(2)
    gather.side(3)
    gather.finish()
    outward.wait()


def scratch_call(kernel, outputs, scratch, collective_id, *operands):
    return pl.pallas_call(
        kernel,
        out_shape=outputs,
        in_specs=[ANY] * len(operands),
        out_specs=jax.tree.map(lambda _: ANY, outputs),
        scratch_shapes=scratch,
        compiler_params=pltpu.CompilerParams(
            collective_id=collective_id, has_side_effects=True, vmem_limit_bytes=60 * 1024 * 1024
        ),
    )(*operands)


def gather_fsdp(block, collective_id):
    size = lax.axis_size("fsdp")
    if size != KERNEL_FSDP:
        return lax.all_gather(block, "fsdp", axis=0)
    return scratch_call(
        gather_kernel,
        jax.ShapeDtypeStruct((size,) + block.shape, block.dtype),
        [
            pltpu.VMEM(block.shape, block.dtype),
            pltpu.SemaphoreType.DMA((29,)),
            pltpu.SemaphoreType.DMA((size,)),
            pltpu.SemaphoreType.DMA((2,)),
        ],
        collective_id,
        block,
    )


def add_rows(rows, step, target, *sources):
    def body(i, carry):
        at = pl.ds(pl.multiple_of(i * step, step), step)
        total = sources[0][at, :].astype(jnp.float32)
        for source in sources[1:]:
            total = total + source[at, :].astype(jnp.float32)
        target[at, :] = total.astype(target.dtype)
        return carry

    lax.fori_loop(0, rows // step, body, 0)


def scatter_kernel(amount, *refs):
    parts_refs, out_ref = refs[:amount], refs[amount]
    held, from_core, from_across, from_below, from_above, total = refs[amount + 1 : amount + 7]
    send_sem, core_send_sem, core_sem, across_sem, below_sem, above_sem, local_sem = refs[amount + 7 :]
    z, x, c, t = place()
    rows = out_ref.shape[0]
    down, up = (fsdp_index(z - 1, x, c), t), (fsdp_index(z + 1, x, c), t)
    across, other = (fsdp_index(z, 1 - x, c), t), (fsdp_index(z, x, 1 - c), t)
    half = z // 2
    mirrored = z + half * (3 - 2 * z)

    def target_of(i):
        if i == 3:
            return z
        base = 3 - i - (i + mirrored) // 3
        return base + half * (3 - 2 * base)

    columns, start = [], 0
    for ref in parts_refs:
        columns.append(pl.ds(start, ref.shape[2]))
        start += ref.shape[2]
    local = []
    for k in range(8):
        index = fsdp_index(target_of(k % 4), 1 - x if k < 4 else x, c)
        copies = [
            pltpu.make_async_copy(ref.at[index], held.at[k, :, at], local_sem.at[k * amount + i])
            for i, (ref, at) in enumerate(zip(parts_refs, columns))
        ]
        for copy in copies:
            copy.start()
        local.append(copies)
    greet_line(z, (across, other), down, up)
    to_core = []
    for k in range(8):
        index = fsdp_index(target_of(k % 4), 1 - x if k < 4 else x, 1 - c)
        copies = [
            remote(
                ref.at[index],
                from_core.at[k, :, at],
                core_send_sem.at[k * amount + i],
                core_sem.at[k * amount + i],
                other,
            )
            for i, (ref, at) in enumerate(zip(parts_refs, columns))
        ]
        for copy in copies:
            copy.start()
        to_core.append(copies)

    def both(k):
        for copy in local[k]:
            copy.wait()
        for copy in to_core[k]:
            copy.wait_recv()

    to_across = []
    for i in range(4):
        both(i)
        add_rows(rows, 16, held.at[i], held.at[i], from_core.at[i])
        copy = remote(held.at[i], from_across.at[i], send_sem.at[3 + i], across_sem.at[i], across)
        copy.start()
        to_across.append(copy)
    for i in range(3):
        k = 4 + i
        target = target_of(i)
        both(k)
        to_across[i].wait_recv()

        @pl.when(target > z)
        def _():
            @pl.when(z > 0)
            def _():
                remote(held.at[k], from_below.at[target], send_sem.at[i], below_sem.at[target], up).wait_recv()
                add_rows(rows, 16, held.at[k], held.at[k], from_core.at[k], from_across.at[i], from_below.at[target])

            @pl.when(z == 0)
            def _():
                add_rows(rows, 16, held.at[k], held.at[k], from_core.at[k], from_across.at[i])

            remote(held.at[k], from_below.at[target], send_sem.at[i], below_sem.at[target], up).start()

        @pl.when(target < z)
        def _():
            @pl.when(z < 3)
            def _():
                remote(held.at[k], from_above.at[target], send_sem.at[i], above_sem.at[target], down).wait_recv()
                add_rows(rows, 16, held.at[k], held.at[k], from_core.at[k], from_across.at[i], from_above.at[target])

            @pl.when(z == 3)
            def _():
                add_rows(rows, 16, held.at[k], held.at[k], from_core.at[k], from_across.at[i])

            remote(held.at[k], from_above.at[target], send_sem.at[i], above_sem.at[target], down).start()

    both(7)
    to_across[3].wait_recv()
    add_rows(rows, 16, total, held.at[7], from_core.at[7], from_across.at[3])

    @pl.when(z > 0)
    def _():
        remote(held.at[7], from_below.at[z], send_sem.at[0], below_sem.at[z], up).wait_recv()
        add_rows(rows, 16, total, total, from_below.at[z])

    @pl.when(z < 3)
    def _():
        remote(held.at[7], from_above.at[z], send_sem.at[0], above_sem.at[z], down).wait_recv()
        add_rows(rows, 16, total, total, from_above.at[z])

    outward = pltpu.make_async_copy(total, out_ref, local_sem.at[8 * amount])
    outward.start()
    for copy in sum(to_core, to_across):
        copy.wait_send()
    for i in range(3):
        remote(held.at[4 + i], from_below.at[0], send_sem.at[i], below_sem.at[0], other).wait_send()
    outward.wait()


def scatter_fsdp(parts, collective_id):
    size, rows, _ = parts[0].shape
    columns = sum(part.shape[2] for part in parts)
    if size != KERNEL_FSDP:
        return lax.psum_scatter(
            jnp.concatenate(parts, axis=2), "fsdp", scatter_dimension=0, tiled=False
        ).astype(jnp.float32)
    block, amount, kind = (rows, columns), len(parts), parts[0].dtype
    return scratch_call(
        functools.partial(scatter_kernel, amount),
        jax.ShapeDtypeStruct(block, jnp.float32),
        [
            pltpu.VMEM((8,) + block, kind),
            pltpu.VMEM((8,) + block, kind),
            pltpu.VMEM((4,) + block, kind),
            pltpu.VMEM((4,) + block, kind),
            pltpu.VMEM((4,) + block, kind),
            pltpu.VMEM(block, jnp.float32),
            pltpu.SemaphoreType.DMA((7,)),
            pltpu.SemaphoreType.DMA((8 * amount,)),
            pltpu.SemaphoreType.DMA((8 * amount,)),
            pltpu.SemaphoreType.DMA((4,)),
            pltpu.SemaphoreType.DMA((4,)),
            pltpu.SemaphoreType.DMA((4,)),
            pltpu.SemaphoreType.DMA((8 * amount + 1,)),
        ],
        collective_id,
        *parts,
    )


def exchange_kernel(block_ref, out_ref, send_sem, receive_sem):
    index, t = lax.axis_index("fsdp"), lax.axis_index("tp")
    partner = (index, 1 - t)
    greet((partner,))
    copy = remote(block_ref, out_ref, send_sem.at[0], receive_sem.at[0], partner)
    copy.start()
    copy.wait()


def exchange_tp(block, collective_id):
    if lax.axis_size("fsdp") != KERNEL_FSDP:
        return lax.ppermute(block, "tp", [(0, 1), (1, 0)])
    return scratch_call(
        exchange_kernel,
        jax.ShapeDtypeStruct(block.shape, block.dtype),
        [pltpu.SemaphoreType.DMA((1,)), pltpu.SemaphoreType.DMA((1,))],
        collective_id,
        block,
    )


def peer(z, x, c, k):
    kz, kx, kc = k // 4, (k // 2) % 2, k % 2
    high, low = z // 2, z % 2
    high = 1 - high if kz // 2 else high
    low = 1 - low if kz % 2 else low
    return fsdp_index(high * 2 + low, 1 - x if kx else x, 1 - c if kc else c)


MAIN = 2 * LANES
REST = LANES
FIRST_REST = KERNEL_FSDP * MAIN
UNITS = 2 * MAIN + REST


def main_of(owner):
    return pl.ds(pl.multiple_of(owner * MAIN, MAIN), MAIN)


def rest_of(z):
    return pl.ds(pl.multiple_of(FIRST_REST + z * REST, REST), REST)


def distribute_kernel(
    rows_ref, query_ref, key_ref, value_ref, output_ref, gain_ref, gate_ref, up_ref, down_ref,
    attention_ref, partner_ref, feed_ref,
    stage, feed, zeros,
    gather_send, gather_receive, local_sem, pair_rows_sem, send_sem, receive_sem, rest_send, rest_receive,
    on_send, on_receive, rest_on_send, rest_on_receive,
):
    z, x, c, t = place()
    own = fsdp_index(z, x, c)
    partner = (own, 1 - t)
    greet([(peer(z, x, c, k), t) for k in range(1, 16)] + [partner])
    rows_copy = remote(rows_ref, partner_ref, pair_rows_sem.at[0], pair_rows_sem.at[1], partner)
    rows_copy.start()
    loads, start = [], 0
    for i, ref in enumerate((query_ref, key_ref, value_ref, output_ref, gain_ref)):
        loads.append(pltpu.make_async_copy(ref, stage.at[:, pl.ds(start, ref.shape[1])], local_sem.at[i]))
        start += ref.shape[1]
    feed_loads = [
        pltpu.make_async_copy(ref, feed.at[i], local_sem.at[5 + i])
        for i, ref in enumerate((gate_ref, up_ref, down_ref))
    ]
    for copy in loads + feed_loads:
        copy.start()
    for copy in loads:
        copy.wait()
    gather = Gather(stage, attention_ref, gather_send, gather_receive)
    gather.start()
    keep = pltpu.make_async_copy(stage, attention_ref.at[own], local_sem.at[8])
    keep.start()
    for copy in feed_loads:
        copy.wait()

    def main_at(half, source):
        return feed_ref.at[:, source, :, pl.ds(pl.multiple_of(half * MAIN, MAIN), MAIN)]

    def rest_at(source):
        return feed_ref.at[:, source, :, pl.ds(2 * MAIN, REST)]

    takes_rest = (c == 0) & (x == t)

    def direct(k):
        to = peer(z, x, c, k)
        return remote(feed.at[:, :, main_of(to)], main_at(t, own), send_sem.at[k], receive_sem.at[k], (to, t))

    def rest(dz):
        to_z = peer(z, x, c, 4 * dz) // 4
        slot = 4 * dz + 2 * ((x + t) % 2) + c
        return remote(
            feed.at[:, :, rest_of(to_z)], rest_at(own), rest_send.at[dz], rest_receive.at[slot], (fsdp_index(to_z, t, 0), t)
        )

    def onward(k):
        at = main_at(t, peer(z, x, c, k))
        return remote(at if k else feed.at[:, :, main_of(own)], at, on_send.at[k], on_receive.at[k], partner)

    def rest_onward(k):
        at = rest_at(peer(z, x, c, k))
        return remote(at if k else feed.at[:, :, rest_of(z)], at, rest_on_send.at[k], rest_on_receive.at[k], partner)

    def send(dz):
        for k in range(4 * dz, 4 * dz + 4):
            if k:
                direct(k).start()
        if dz:
            rest(dz).start()
        else:

            @pl.when(jnp.logical_not(takes_rest))
            def _():
                rest(0).start()

    def pass_on(dz):
        for k in range(4 * dz, 4 * dz + 4):
            if k:
                direct(k).wait_recv()
            onward(k).start()

        @pl.when(takes_rest)
        def _():
            for k in range(4 * dz, 4 * dz + 4):
                if k:
                    remote(
                        feed.at[:, :, rest_of(0)], rest_at(own), rest_send.at[0], rest_receive.at[k], partner
                    ).wait_recv()
                rest_onward(k).start()

    send(0)
    send(1)
    keep_main = pltpu.make_async_copy(feed.at[:, :, main_of(own)], main_at(t, own), local_sem.at[9])
    keep_main.start()
    keep_rest = pltpu.make_async_copy(feed.at[:, :, rest_of(z)], rest_at(own), local_sem.at[10])

    @pl.when(takes_rest)
    def _():
        keep_rest.start()

    fills = [
        pltpu.make_async_copy(zeros, feed_ref.at[i, :, :, pl.ds(2 * MAIN, REST)], local_sem.at[11 + i])
        for i in range(3)
    ]

    @pl.when(c == 1)
    def _():
        zeros[...] = jnp.zeros_like(zeros)
        for copy in fills:
            copy.start()

    pass_on(0)
    gather.line(1)
    gather.side(0)
    send(2)
    gather.line(2)
    send(3)
    gather.side(1)
    pass_on(1)
    gather.line(3)
    gather.side(2)
    pass_on(2)
    gather.side(3)
    pass_on(3)
    gather.finish()
    rows_copy.wait()
    for k in range(16):
        onward(k).wait_recv()
        onward(k).wait_send()
        if k:
            direct(k).wait_send()

    @pl.when(jnp.logical_not(takes_rest))
    def _():
        rest(0).wait_send()

    for dz in (1, 2, 3):
        rest(dz).wait_send()

    @pl.when(takes_rest)
    def _():
        for k in range(16):
            rest_onward(k).wait_send()
        keep_rest.wait()

    @pl.when((c == 0) & (x != t))
    def _():
        for k in range(16):
            rest_onward(k).wait_recv()

    @pl.when(c == 1)
    def _():
        for copy in fills:
            copy.wait()

    keep.wait()
    keep_main.wait()


def distribute(rows, attention, gain_columns, feed, collective_id):
    size = lax.axis_size("fsdp")
    shard_rows, feed_width = feed[0].shape
    columns = sum(w.shape[1] for w in attention) + gain_columns.shape[1]
    if size != KERNEL_FSDP:
        halves = lax.all_to_all(pack_units(feed, size), "fsdp", split_axis=0, concat_axis=0, tiled=True)
        halves = lax.all_gather(halves, "tp", axis=0)
        halves = halves.reshape(halves.shape[0], size * shard_rows, halves.shape[-1])
        return (
            lax.all_gather(jnp.concatenate((*attention, gain_columns), axis=1), "fsdp", axis=0),
            lax.ppermute(rows, "tp", [(0, 1), (1, 0)]),
            jnp.stack(join_units(halves, feed_width, size, 3)),
        )
    kind = rows.dtype
    attention_full, partner_rows, feed_full = scratch_call(
        distribute_kernel,
        (
            jax.ShapeDtypeStruct((size, shard_rows, columns), kind),
            jax.ShapeDtypeStruct(rows.shape, kind),
            jax.ShapeDtypeStruct((3, size, shard_rows, UNITS), kind),
        ),
        [
            pltpu.VMEM((shard_rows, columns), kind),
            pltpu.VMEM((3, shard_rows, feed_width), kind),
            pltpu.VMEM((size, shard_rows, REST), kind),
            pltpu.SemaphoreType.DMA((Gather.slots,)),
            pltpu.SemaphoreType.DMA((size,)),
            pltpu.SemaphoreType.DMA((14,)),
            pltpu.SemaphoreType.DMA((2,)),
            pltpu.SemaphoreType.DMA((size,)),
            pltpu.SemaphoreType.DMA((size,)),
            pltpu.SemaphoreType.DMA((4,)),
            pltpu.SemaphoreType.DMA((size,)),
            pltpu.SemaphoreType.DMA((size,)),
            pltpu.SemaphoreType.DMA((size,)),
            pltpu.SemaphoreType.DMA((size,)),
            pltpu.SemaphoreType.DMA((size,)),
        ],
        collective_id,
        rows,
        *attention,
        gain_columns,
        *feed,
    )
    return attention_full, partner_rows, feed_full.reshape(3, size * shard_rows, UNITS)


def collect_kernel(
    gate_ref, up_ref, down_ref, out_ref,
    held, received, rest_held, rest_received,
    local_sem, pair_send, pair_receive, rest_pair_send, rest_pair_receive, send_sem, receive_sem, rest_send, rest_receive,
):
    z, x, c, t = place()
    own = fsdp_index(z, x, c)
    rows = out_ref.shape[1]
    partner = (own, 1 - t)
    parts = (gate_ref, up_ref, down_ref)
    order = (3, 2, 1, 0)
    takes_rest = (c == 0) & (x == t)
    gives_rest = (c == 0) & (x != t)

    def plane(dz):
        return pl.ds(peer(z, x, c, 4 * dz) // 4 * 4, 4)

    def half(which):
        return pl.ds(pl.multiple_of(which * MAIN, MAIN), MAIN)

    rest_columns = pl.ds(2 * MAIN, REST)

    def load(dz, i):
        return pltpu.make_async_copy(parts[i].at[plane(dz), :, half(t)], held.at[dz, i], local_sem.at[3 * dz + i])

    def rest_load(dz, i):
        return pltpu.make_async_copy(
            parts[i].at[plane(dz), :, rest_columns], rest_held.at[dz, i], local_sem.at[12 + 3 * dz + i]
        )

    def pair(dz, i):
        slot = 3 * dz + i
        return remote(
            parts[i].at[plane(dz), :, half(1 - t)], received.at[dz, i], pair_send.at[slot], pair_receive.at[slot], partner
        )

    def rest_pair(dz, i):
        slot = 3 * dz + i
        return remote(
            parts[i].at[plane(dz), :, rest_columns],
            rest_received.at[dz, i],
            rest_pair_send.at[slot],
            rest_pair_receive.at[slot],
            partner,
        )

    def spot(k):
        return peer(z, x, c, k) % 4

    def direct(k):
        return remote(
            held.at[k // 4, :, spot(k)], out_ref.at[:, :, main_of(own)], send_sem.at[k], receive_sem.at[k], (peer(z, x, c, k), t)
        )

    def rest_direct(k):
        return remote(
            rest_held.at[k // 4, :, spot(k)],
            out_ref.at[:, :, rest_of(z)],
            rest_send.at[k],
            rest_receive.at[z],
            (peer(z, x, c, k), t),
        )

    def add(target, source):
        def body(j, carry):
            i, at = j // 4, j % 4
            total = target[i, at].astype(jnp.float32) + source[i, at].astype(jnp.float32)
            target[i, at] = total.astype(target.dtype)
            return carry

        lax.fori_loop(0, 12, body, 0)

    for dz in order:
        for i in range(3):
            load(dz, i).start()

    @pl.when(takes_rest)
    def _():
        for dz in order:
            for i in range(3):
                rest_load(dz, i).start()

    greet([(peer(z, x, c, k), t) for k in range(1, 16)] + [partner])
    for dz in order:
        for i in range(3):
            pair(dz, i).start()

        @pl.when(gives_rest)
        def _():
            for i in range(3):
                rest_pair(dz, i).start()

    for dz in order:
        for i in range(3):
            load(dz, i).wait()
            pair(dz, i).wait_recv()
        add(held.at[dz], received.at[dz])
        for k in range(4 * dz, 4 * dz + 4):
            if k:
                direct(k).start()

        @pl.when(takes_rest)
        def _():
            for i in range(3):
                rest_load(dz, i).wait()
                rest_pair(dz, i).wait_recv()
            add(rest_held.at[dz], rest_received.at[dz])
            for k in range(4 * dz, 4 * dz + 4):
                if k:
                    rest_direct(k).start()

    keep = pltpu.make_async_copy(held.at[0, :, spot(0)], out_ref.at[:, :, main_of(own)], local_sem.at[24])
    keep.start()
    keep_rest = pltpu.make_async_copy(rest_held.at[0, :, spot(0)], out_ref.at[:, :, rest_of(z)], local_sem.at[25])

    @pl.when(takes_rest)
    def _():
        keep_rest.start()

    for k in range(1, 16):
        direct(k).wait_recv()

    for dz in range(4):
        from_z = peer(z, x, c, 4 * dz) // 4

        def arrived():
            remote(
                rest_held.at[0, :, 0], out_ref.at[:, :, rest_of(from_z)], rest_send.at[0], rest_receive.at[from_z], partner
            ).wait_recv()

        if dz:
            arrived()
        else:

            @pl.when(jnp.logical_not(takes_rest))
            def _():
                arrived()

    for k in range(1, 16):
        direct(k).wait_send()
    for dz in order:
        for i in range(3):
            pair(dz, i).wait_send()

    @pl.when(gives_rest)
    def _():
        for dz in order:
            for i in range(3):
                rest_pair(dz, i).wait_send()

    @pl.when(takes_rest)
    def _():
        for k in range(1, 16):
            rest_direct(k).wait_send()
        keep_rest.wait()

    keep.wait()


def collect(gradients, feed_width, collective_id):
    size, pairs = lax.axis_size("fsdp"), lax.axis_size("tp")
    shard_rows = gradients[0].shape[0] // size
    if size != KERNEL_FSDP:
        packed = part_units(gradients, feed_width, size, pairs)
        mine = lax.psum_scatter(packed, "tp", scatter_dimension=0, tiled=False)
        mine = mine.reshape(size, shard_rows, mine.shape[-1])
        mine = lax.all_to_all(mine, "fsdp", split_axis=0, concat_axis=0, tiled=True)
        return [g.astype(jnp.float32) for g in unpack_units(mine, feed_width, 3)]
    kind = gradients[0].dtype
    main, rest = (4, 3, 4, shard_rows, MAIN), (4, 3, 4, shard_rows, REST)
    out = scratch_call(
        collect_kernel,
        jax.ShapeDtypeStruct((3, shard_rows, feed_width), kind),
        [
            pltpu.VMEM(main, kind),
            pltpu.VMEM(main, kind),
            pltpu.VMEM(rest, kind),
            pltpu.VMEM(rest, kind),
            pltpu.SemaphoreType.DMA((26,)),
            pltpu.SemaphoreType.DMA((12,)),
            pltpu.SemaphoreType.DMA((12,)),
            pltpu.SemaphoreType.DMA((12,)),
            pltpu.SemaphoreType.DMA((12,)),
            pltpu.SemaphoreType.DMA((size,)),
            pltpu.SemaphoreType.DMA((size,)),
            pltpu.SemaphoreType.DMA((size,)),
            pltpu.SemaphoreType.DMA((4,)),
        ],
        collective_id,
        *[g.reshape(size, shard_rows, UNITS) for g in gradients],
    )
    return [out[i].astype(jnp.float32) for i in range(3)]


def contract_last(left_rows, right_rows):
    return lax.dot_general(
        left_rows, right_rows, (((1,), (1,)), ((), ())), preferred_element_type=jnp.float32
    )


def contract_first(left_rows, right_rows):
    return lax.dot_general(
        left_rows, right_rows, (((0,), (0,)), ((), ())), preferred_element_type=jnp.float32
    )


def normalize_parts(value_rows):
    inverse = lax.rsqrt(jnp.mean(value_rows * value_rows, axis=-1, keepdims=True) + EPSILON)
    return (value_rows * inverse, inverse)


def norm_backward(unit_rows, inverse, norm_gain, upstream):
    scaled = upstream * norm_gain
    return inverse * (scaled - unit_rows * jnp.mean(scaled * unit_rows, axis=-1, keepdims=True))


def layout(lengths_row, row_index):
    segment_ends = jnp.cumsum(lengths_row)
    segment_starts = segment_ends - lengths_row
    segment = jnp.sum((row_index[:, None] >= segment_ends[None, :]).astype(jnp.int32), axis=1)
    onehot = segment[:, None] == jnp.arange(lengths_row.shape[0], dtype=jnp.int32)[None, :]
    segment_begin = jnp.sum(jnp.where(onehot, segment_starts[None, :], 0), axis=1)
    prompt_shift = jnp.where(segment > 0, lengths_row[0], 0)
    return (segment, row_index - segment_begin + prompt_shift)


def rotary_tables(position):
    frequency = jnp.exp(
        jnp.arange(HEAD_SIZE // 2, dtype=jnp.float32) * (-2.0 * math.log(10000.0) / HEAD_SIZE)
    )
    angles = position.astype(jnp.float32)[:, None] * frequency[None, :]
    return (jnp.cos(angles), jnp.sin(angles))


def apply_rotary(value_rows, cosine_lookup, sine_lookup):
    half_width = value_rows.shape[-1] // 2
    first_half = value_rows[..., :half_width]
    second_half = value_rows[..., half_width:]
    cosine_part = cosine_lookup[:, None, :]
    sine_part = sine_lookup[:, None, :]
    return jnp.concatenate(
        [
            first_half * cosine_part - second_half * sine_part,
            second_half * cosine_part + first_half * sine_part,
        ],
        axis=-1,
    )


def unrotate(value_rows, cosine_lookup, sine_lookup):
    half_width = value_rows.shape[-1] // 2
    first_half = value_rows[..., :half_width]
    second_half = value_rows[..., half_width:]
    cosine_part = cosine_lookup[:, None, :]
    sine_part = sine_lookup[:, None, :]
    return jnp.concatenate(
        [
            first_half * cosine_part + second_half * sine_part,
            second_half * cosine_part - first_half * sine_part,
        ],
        axis=-1,
    )


def visible(segment, row_index):
    same_segment = (segment[:, None] == segment[None, :]) & (
        row_index[None, :] <= row_index[:, None]
    )
    from_prompt = (segment[None, :] == 0) & (segment[:, None] > 0)
    return same_segment | from_prompt


def masked_scores(rotated_query, rotated_key, visible_mask):
    raw_scores = jnp.einsum(
        "qgrd,kgd->grqk", rotated_query, rotated_key, preferred_element_type=jnp.float32
    )
    tanh_value = jnp.tanh(raw_scores * HEAD_SIZE ** (-0.5) / SOFTCAP)
    return (jnp.where(visible_mask[None, None], SOFTCAP * tanh_value, NEGATIVE), tanh_value)


def gelu_product(gate_value, up_value):
    return jax.nn.gelu(gate_value, approximate=True) * up_value


def split_columns(width, size):
    main = width // size // LANES * LANES
    return main, width // size - main


def pack_units(weights, size):
    rows, width = weights[0].shape
    main, rest = split_columns(width, size)
    pieces = []
    if main:
        pieces += [
            jnp.transpose(w[:, : main * size].reshape(rows, size, main), (1, 0, 2)) for w in weights
        ]
    if rest:
        pieces += [
            jnp.transpose(w[:, main * size :].reshape(rows, size, rest), (1, 0, 2)) for w in weights
        ]
    packed = jnp.concatenate(pieces, axis=2)
    return jnp.pad(packed, ((0, 0), (0, 0), (0, -packed.shape[2] % LANES)))


def unpack_units(packed, width, amount):
    size, rows, _ = packed.shape
    main, rest = split_columns(width, size)
    arrays = []
    for i in range(amount):
        pieces = []
        if main:
            piece = packed[:, :, i * main : (i + 1) * main]
            pieces.append(jnp.transpose(piece, (1, 0, 2)).reshape(rows, size * main))
        if rest:
            start = amount * main + i * rest
            piece = packed[:, :, start : start + rest]
            pieces.append(jnp.transpose(piece, (1, 0, 2)).reshape(rows, size * rest))
        arrays.append(jnp.concatenate(pieces, axis=1))
    return arrays


def join_units(halves, width, size, amount):
    main, rest = split_columns(width, size)
    arrays = []
    for i in range(amount):
        start = amount * main + i * rest
        pieces = [half[:, i * main : (i + 1) * main] for half in halves]
        pieces += [half[:, start : start + rest] for half in halves]
        joined = jnp.concatenate(pieces, axis=1)
        arrays.append(jnp.pad(joined, ((0, 0), (0, -joined.shape[1] % LANES))))
    return arrays


def part_units(arrays, width, size, pairs):
    main, rest = split_columns(width, size)
    halves = []
    for t in range(pairs):
        pieces = [array[:, t * main : (t + 1) * main] for array in arrays]
        start = pairs * main + t * rest
        pieces += [array[:, start : start + rest] for array in arrays]
        packed = jnp.concatenate(pieces, axis=1)
        halves.append(jnp.pad(packed, ((0, 0), (0, -packed.shape[1] % LANES))))
    return jnp.stack(halves)


def shards(
    block_input,
    lengths,
    attention_norm_gain,
    attention_post_gain,
    feedforward_norm_gain,
    feedforward_post_gain,
    query_weight,
    key_weight,
    value_weight,
    output_weight,
    gate_weight,
    up_weight,
    down_weight,
    output_cotangent,
):
    low = jnp.bfloat16
    size, pairs = lax.axis_size("fsdp"), lax.axis_size("tp")
    rows_local, width = block_input.shape
    shard_rows, feed_width = gate_weight.shape
    query_width, key_width = query_weight.shape[1], key_weight.shape[1]
    output_start = query_width + 2 * key_width
    gain_start = output_start + query_width
    grouped_rows = rows_local * pairs

    gain_columns = jnp.stack(
        [attention_norm_gain, attention_post_gain, feedforward_norm_gain, feedforward_post_gain],
        axis=1,
    )
    attention_full, other_input, feed_full = distribute(
        block_input,
        (query_weight, key_weight, value_weight, output_weight),
        jnp.pad(gain_columns, ((0, 0), (0, LANES - 4))),
        (gate_weight, up_weight, down_weight),
        1,
    )
    attention_full = attention_full.reshape(size * shard_rows, gain_start + LANES)
    gains = jnp.transpose(attention_full[:, gain_start : gain_start + 4]).astype(jnp.float32)
    gain_one, gain_two, gain_three, gain_four = gains[0], gains[1], gains[2], gains[3]
    gate_full, up_full, down_full = feed_full[0], feed_full[1], feed_full[2]

    row_index = (
        jnp.arange(grouped_rows, dtype=jnp.int32) + lax.axis_index("tp") * rows_local
    ) % grouped_rows
    segment, position = layout(lengths[0], row_index)
    cosine_lookup, sine_lookup = rotary_tables(position)
    visible_mask = visible(segment, row_index)
    residual_both = jnp.concatenate([block_input, other_input], axis=0).astype(jnp.float32)
    unit_one_both, inverse_one_both = normalize_parts(residual_both)
    residual = residual_both[:rows_local]
    unit_one, inverse_one = unit_one_both[:rows_local], inverse_one_both[:rows_local]
    normed = (unit_one_both * gain_one).astype(low)
    projected = jnp.dot(
        normed, attention_full[:, :output_start], preferred_element_type=jnp.float32
    )
    query_raw = projected[:, :query_width]
    key_raw = projected[:, query_width : query_width + key_width]
    value_raw = projected[:, query_width + key_width :]
    heads_local = query_width // HEAD_SIZE
    kv_local = key_width // HEAD_SIZE
    repeat_heads = heads_local // kv_local
    rotated_query = apply_rotary(
        query_raw.reshape(grouped_rows, heads_local, HEAD_SIZE), cosine_lookup, sine_lookup
    ).astype(low)
    rotated_query = rotated_query.reshape(grouped_rows, kv_local, repeat_heads, HEAD_SIZE)
    rotated_key = apply_rotary(
        key_raw.reshape(grouped_rows, kv_local, HEAD_SIZE), cosine_lookup, sine_lookup
    ).astype(low)
    value_reduced = value_raw.astype(low).reshape(grouped_rows, kv_local, HEAD_SIZE)
    capped, tanh_value = masked_scores(rotated_query, rotated_key, visible_mask)
    row_peak = jnp.max(capped, axis=-1, keepdims=True)
    exponentials = jnp.exp(capped - row_peak)
    softmax_probs = exponentials / jnp.sum(exponentials, axis=-1, keepdims=True)
    probs_low = softmax_probs.astype(low)
    mixed_heads = jnp.einsum(
        "grqk,kgd->qgrd", probs_low, value_reduced, preferred_element_type=jnp.float32
    )
    attended = mixed_heads.reshape(grouped_rows, heads_local * HEAD_SIZE).astype(low)
    output_full = attention_full[:, output_start:gain_start]
    branch_parts = contract_last(attended, output_full)
    branch_one = branch_parts[:rows_local] + exchange_tp(
        branch_parts[rows_local:].astype(low), 4
    ).astype(jnp.float32)
    unit_two, inverse_two = normalize_parts(branch_one)
    middle = residual + unit_two * gain_two
    unit_three, inverse_three = normalize_parts(middle)

    feed_input = gather_fsdp((unit_three * gain_three).astype(low), 5).reshape(-1, width)
    gate_value = jnp.dot(feed_input, gate_full, preferred_element_type=jnp.float32)
    up_value = jnp.dot(feed_input, up_full, preferred_element_type=jnp.float32)
    hidden = gelu_product(gate_value, up_value).astype(low)
    branch_two = scatter_fsdp(
        (contract_last(hidden, down_full).astype(low).reshape(size, rows_local, width),), 6
    )
    unit_four, inverse_four = normalize_parts(branch_two)
    block_output = (middle + unit_four * gain_four).astype(low)
    upstream = output_cotangent.astype(jnp.float32)
    gain_four_grad = jnp.sum(upstream * unit_four, axis=0)
    branch_two_grad = norm_backward(unit_four, inverse_four, gain_four, upstream).astype(low)
    feed_grad_rows = gather_fsdp(branch_two_grad, 7).reshape(-1, width)
    hidden_grad = jnp.dot(feed_grad_rows, down_full, preferred_element_type=jnp.float32)
    unused_out, pullback = jax.vjp(gelu_product, gate_value, up_value)
    gate_grad, up_grad = pullback(hidden_grad)
    gate_grad, up_grad = gate_grad.astype(low), up_grad.astype(low)
    normed_three_parts = contract_last(gate_grad, gate_full) + contract_last(up_grad, up_full)
    normed_three_grad = scatter_fsdp(
        (normed_three_parts.astype(low).reshape(size, rows_local, width),), 8
    )
    gate_weight_grad, up_weight_grad, down_weight_grad = collect(
        (
            contract_first(feed_input, gate_grad).astype(low),
            contract_first(feed_input, up_grad).astype(low),
            contract_first(feed_grad_rows, hidden).astype(low),
        ),
        feed_width,
        9,
    )

    gain_three_grad = jnp.sum(normed_three_grad * unit_three, axis=0)
    middle_grad = upstream + norm_backward(unit_three, inverse_three, gain_three, normed_three_grad)
    gain_two_grad = jnp.sum(middle_grad * unit_two, axis=0)
    branch_one_grad = norm_backward(unit_two, inverse_two, gain_two, middle_grad).astype(low)
    attention_grad_rows = jnp.concatenate(
        [branch_one_grad, exchange_tp(branch_one_grad, 10)], axis=0
    )
    mixed_grad = jnp.dot(
        attention_grad_rows, output_full, preferred_element_type=jnp.float32
    ).astype(low)
    mixed_grad = mixed_grad.reshape(grouped_rows, kv_local, repeat_heads, HEAD_SIZE)
    value_grad = jnp.einsum(
        "grqk,qgrd->kgd", probs_low, mixed_grad, preferred_element_type=jnp.float32
    )
    probs_grad = jnp.einsum(
        "qgrd,kgd->grqk", mixed_grad, value_reduced, preferred_element_type=jnp.float32
    )
    score_grad = softmax_probs * (
        probs_grad - jnp.sum(softmax_probs * probs_grad, axis=-1, keepdims=True)
    )
    raw_grad = (score_grad * (1.0 - tanh_value * tanh_value) * HEAD_SIZE ** (-0.5)).astype(low)
    query_grad = jnp.einsum(
        "grqk,kgd->qgrd", raw_grad, rotated_key, preferred_element_type=jnp.float32
    )
    key_grad = jnp.einsum(
        "grqk,qgrd->kgd", raw_grad, rotated_query, preferred_element_type=jnp.float32
    )
    query_grad = unrotate(
        query_grad.reshape(grouped_rows, heads_local, HEAD_SIZE), cosine_lookup, sine_lookup
    )
    key_grad = unrotate(key_grad, cosine_lookup, sine_lookup)
    projected_grad = jnp.concatenate(
        [
            query_grad.reshape(grouped_rows, heads_local * HEAD_SIZE).astype(low),
            key_grad.reshape(grouped_rows, kv_local * HEAD_SIZE).astype(low),
            value_grad.reshape(grouped_rows, kv_local * HEAD_SIZE).astype(low),
        ],
        axis=1,
    )
    input_parts = contract_last(projected_grad, attention_full[:, :output_start])

    gain_grads = jnp.stack(
        [
            jnp.sum(input_parts * unit_one_both, axis=0),
            gain_two_grad,
            gain_three_grad,
            gain_four_grad,
        ]
    )
    sent = jnp.concatenate(
        [input_parts[rows_local:].astype(low), jnp.pad(gain_grads, ((0, 12), (0, 0))).astype(low)]
    )
    received = exchange_tp(sent, 11).astype(jnp.float32)
    normed_one_grad = input_parts[:rows_local] + received[:rows_local]
    gain_grads = gain_grads + received[rows_local : rows_local + 4]
    input_gradient = middle_grad + norm_backward(unit_one, inverse_one, gain_one, normed_one_grad)

    attention_grads = scatter_fsdp(
        [
            part.astype(low).reshape(size, shard_rows, part.shape[1])
            for part in (
                contract_first(normed, projected_grad),
                contract_first(attention_grad_rows, attended),
                jnp.pad(jnp.transpose(gain_grads), ((0, 0), (0, LANES - 4))),
            )
        ],
        12,
    )
    gain_shards = jnp.transpose(attention_grads[:, gain_start : gain_start + 4])
    return (
        block_output,
        input_gradient,
        gain_shards[0],
        gain_shards[1],
        gain_shards[2],
        gain_shards[3],
        attention_grads[:, :query_width],
        attention_grads[:, query_width : query_width + key_width],
        attention_grads[:, query_width + key_width : output_start],
        attention_grads[:, output_start:gain_start],
        gate_weight_grad,
        up_weight_grad,
        down_weight_grad,
    )


def solution(mesh):
    placed = (
        P(("fsdp", "tp"), None),
        P("fsdp", None),
        P("fsdp"),
        P("fsdp"),
        P("fsdp"),
        P("fsdp"),
        P("fsdp", "tp"),
        P("fsdp", "tp"),
        P("fsdp", "tp"),
        P("fsdp", "tp"),
        P("fsdp", "tp"),
        P("fsdp", "tp"),
        P("fsdp", "tp"),
        P(("fsdp", "tp"), None),
    )
    return jax.shard_map(
        shards,
        mesh=mesh,
        in_specs=placed,
        out_specs=(
            P(("fsdp", "tp"), None),
            P(("fsdp", "tp"), None),
            P("fsdp"),
            P("fsdp"),
            P("fsdp"),
            P("fsdp"),
            P("fsdp", "tp"),
            P("fsdp", "tp"),
            P("fsdp", "tp"),
            P("fsdp", "tp"),
            P("fsdp", "tp"),
            P("fsdp", "tp"),
            P("fsdp", "tp"),
        ),
        check_vma=False,
    )
```

```python
import functools
import math

import jax
import jax.numpy as jnp
from jax import lax
from jax.experimental import pallas as pl
from jax.experimental.pallas import tpu as pltpu
from jax.sharding import PartitionSpec as P

HEAD_SIZE = 256
MESH = pl.DeviceIdType.MESH
ANY = pl.BlockSpec(memory_space=pl.ANY)
LANES = 128

EPSILON = 1e-06
SOFTCAP = 50.0
NEGATIVE = -1e30

KERNEL_FSDP = 16


def place():
    index = lax.axis_index("fsdp")
    return index // 4, (index // 2) % 2, index % 2, lax.axis_index("tp")


def fsdp_index(z, x, c):
    return (z * 2 + x) * 2 + c


def remote(source, target, send_sem, receive_sem, device):
    return pltpu.make_async_remote_copy(
        src_ref=source,
        dst_ref=target,
        send_sem=send_sem,
        recv_sem=receive_sem,
        device_id=device,
        device_id_type=MESH,
    )


def greet(devices):
    barrier = pltpu.get_barrier_semaphore()
    for device in devices:
        pl.semaphore_signal(barrier, inc=1, device_id=device, device_id_type=MESH)
    pl.semaphore_wait(barrier, len(devices))


def greet_line(z, devices, down, up):
    barrier = pltpu.get_barrier_semaphore()
    for device in devices:
        pl.semaphore_signal(barrier, inc=1, device_id=device, device_id_type=MESH)

    @pl.when(z > 0)
    def _():
        pl.semaphore_signal(barrier, inc=1, device_id=down, device_id_type=MESH)

    @pl.when(z < 3)
    def _():
        pl.semaphore_signal(barrier, inc=1, device_id=up, device_id_type=MESH)

    pl.semaphore_wait(barrier, len(devices) + (z + 2) // 3 + (5 - z) // 3)


def stage_through(source, stage, target, sems):
    inward = pltpu.make_async_copy(source, stage, sems.at[0])
    inward.start()

    def finish():
        inward.wait()
        outward = pltpu.make_async_copy(stage, target, sems.at[1])
        outward.start()
        return outward

    return finish


class Gather:
    slots = 29

    def __init__(self, block, out_ref, send_sem, receive_sem):
        self.block, self.out, self.send_sem, self.receive_sem = block, out_ref, send_sem, receive_sem
        self.z, self.x, self.c, t = place()
        z, x, c = self.z, self.x, self.c
        self.own = fsdp_index(z, x, c)
        self.down, self.up = (fsdp_index(z - 1, x, c), t), (fsdp_index(z + 1, x, c), t)
        self.across, self.other = (fsdp_index(z, 1 - x, c), t), (fsdp_index(z, x, 1 - c), t)

    def copy(self, source, index, slot, device):
        return remote(source, self.out.at[index], self.send_sem.at[slot], self.receive_sem.at[index], device)

    def relay(self, index, slot, device):
        self.copy(self.out.at[index], index, slot, device).start()

    def arrived(self, index):
        self.copy(self.block, index, 0, self.other).wait_recv()

    def sent(self, slot):
        self.copy(self.block, self.own, slot, self.other).wait_send()

    def start(self):
        @pl.when(self.z < 3)
        def _():
            self.copy(self.block, self.own, 0, self.up).start()

        @pl.when(self.z > 0)
        def _():
            self.copy(self.block, self.own, 1, self.down).start()

        self.copy(self.block, self.own, 2, self.across).start()
        self.copy(self.block, self.own, 3, self.other).start()

    def line(self, d):
        z, x, c = self.z, self.x, self.c

        @pl.when(z >= d)
        def _():
            index = fsdp_index(z - d, x, c)
            base = 4 + 3 * (d - 1)
            self.arrived(index)

            @pl.when(z < 3)
            def _():
                self.relay(index, base, self.up)

            self.relay(index, base + 1, self.across)
            self.relay(index, base + 2, self.other)

        @pl.when(z + d <= 3)
        def _():
            index = fsdp_index(z + d, x, c)
            base = 13 + 3 * (d - 1)
            self.arrived(index)

            @pl.when(z > 0)
            def _():
                self.relay(index, base, self.down)

            self.relay(index, base + 1, self.across)
            self.relay(index, base + 2, self.other)

    def side(self, d):
        z, x, c = self.z, self.x, self.c
        if d == 0:
            index = fsdp_index(z, 1 - x, c)
            self.arrived(index)
            self.relay(index, 22, self.other)
            return

        @pl.when(z >= d)
        def _():
            index = fsdp_index(z - d, 1 - x, c)
            self.arrived(index)
            self.relay(index, 22 + d, self.other)

        @pl.when(z + d <= 3)
        def _():
            index = fsdp_index(z + d, 1 - x, c)
            self.arrived(index)
            self.relay(index, 25 + d, self.other)

    def finish(self):
        z = self.z
        for zi in range(4):
            for xi in range(2):
                self.arrived(fsdp_index(zi, xi, 1 - self.c))

        @pl.when(z < 3)
        def _():
            self.sent(0)

        @pl.when(z > 0)
        def _():
            self.sent(1)

        for slot in (2, 3, 22):
            self.sent(slot)
        for d in (1, 2, 3):

            @pl.when(z >= d)
            def _():
                base = 4 + 3 * (d - 1)

                @pl.when(z < 3)
                def _():
                    self.sent(base)

                for slot in (base + 1, base + 2, 22 + d):
                    self.sent(slot)

            @pl.when(z + d <= 3)
            def _():
                base = 13 + 3 * (d - 1)

                @pl.when(z > 0)
                def _():
                    self.sent(base)

                for slot in (base + 1, base + 2, 25 + d):
                    self.sent(slot)


def gather_kernel(block_ref, out_ref, stage, send_sem, receive_sem, local_sem):
    gather = Gather(block_ref, out_ref, send_sem, receive_sem)
    greet_line(gather.z, (gather.across, gather.other), gather.down, gather.up)
    finish_own = stage_through(block_ref, stage, out_ref.at[gather.own], local_sem)
    gather.start()
    outward = finish_own()
    gather.line(1)
    gather.side(0)
    gather.line(2)
    gather.side(1)
    gather.line(3)
    gather.side(2)
    gather.side(3)
    gather.finish()
    outward.wait()


def scratch_call(kernel, outputs, scratch, collective_id, *operands):
    return pl.pallas_call(
        kernel,
        out_shape=outputs,
        in_specs=[ANY] * len(operands),
        out_specs=jax.tree.map(lambda _: ANY, outputs),
        scratch_shapes=scratch,
        compiler_params=pltpu.CompilerParams(
            collective_id=collective_id, has_side_effects=True, vmem_limit_bytes=60 * 1024 * 1024
        ),
    )(*operands)


def gather_fsdp(block, collective_id):
    size = lax.axis_size("fsdp")
    if size != KERNEL_FSDP:
        return lax.all_gather(block, "fsdp", axis=0)
    return scratch_call(
        gather_kernel,
        jax.ShapeDtypeStruct((size,) + block.shape, block.dtype),
        [
            pltpu.VMEM(block.shape, block.dtype),
            pltpu.SemaphoreType.DMA((29,)),
            pltpu.SemaphoreType.DMA((size,)),
            pltpu.SemaphoreType.DMA((2,)),
        ],
        collective_id,
        block,
    )


def add_rows(rows, step, target, *sources):
    def body(i, carry):
        at = pl.ds(pl.multiple_of(i * step, step), step)
        total = sources[0][at, :].astype(jnp.float32)
        for source in sources[1:]:
            total = total + source[at, :].astype(jnp.float32)
        target[at, :] = total.astype(target.dtype)
        return carry

    lax.fori_loop(0, rows // step, body, 0)


class Scatter:
    def __init__(self, buffers, semaphores):
        self.held, self.from_core, self.from_across, self.from_below, self.from_above, self.total = buffers
        self.send_sem, self.across_sem, self.below_sem, self.above_sem = semaphores
        self.z, self.x, self.c, t = place()
        z, x, c = self.z, self.x, self.c
        self.rows = self.total.shape[0]
        self.down, self.up = (fsdp_index(z - 1, x, c), t), (fsdp_index(z + 1, x, c), t)
        self.across, self.other = (fsdp_index(z, 1 - x, c), t), (fsdp_index(z, x, 1 - c), t)

    def target(self, i):
        if i == 3:
            return self.z
        half = self.z // 2
        mirrored = self.z + half * (3 - 2 * self.z)
        base = 3 - i - (i + mirrored) // 3
        return base + half * (3 - 2 * base)

    def index(self, k, core):
        return fsdp_index(self.target(k % 4), 1 - self.x if k < 4 else self.x, core)

    def add(self, target, *sources):
        add_rows(self.rows, 16, target, *sources)

    def over(self, i):
        return remote(
            self.held.at[i], self.from_across.at[i], self.send_sem.at[3 + i], self.across_sem.at[i], self.across
        )

    def going_up(self, i, target):
        return remote(
            self.held.at[4 + i], self.from_below.at[target], self.send_sem.at[i], self.below_sem.at[target], self.up
        )

    def going_down(self, i, target):
        return remote(
            self.held.at[4 + i], self.from_above.at[target], self.send_sem.at[i], self.above_sem.at[target], self.down
        )

    def side(self, i):
        self.add(self.held.at[i], self.held.at[i], self.from_core.at[i])
        self.over(i).start()

    def line(self, i):
        z, target = self.z, self.target(i)
        held = self.held.at[4 + i]
        sources = (held, self.from_core.at[4 + i], self.from_across.at[i])
        self.over(i).wait_recv()

        @pl.when(target > z)
        def _():
            @pl.when(z > 0)
            def _():
                self.going_up(i, target).wait_recv()
                self.add(held, *sources, self.from_below.at[target])

            @pl.when(z == 0)
            def _():
                self.add(held, *sources)

            self.going_up(i, target).start()

        @pl.when(target < z)
        def _():
            @pl.when(z < 3)
            def _():
                self.going_down(i, target).wait_recv()
                self.add(held, *sources, self.from_above.at[target])

            @pl.when(z == 3)
            def _():
                self.add(held, *sources)

            self.going_down(i, target).start()

    def last(self):
        z = self.z
        self.over(3).wait_recv()
        self.add(self.total, self.held.at[7], self.from_core.at[7], self.from_across.at[3])

        @pl.when(z > 0)
        def _():
            self.going_up(0, z).wait_recv()
            self.add(self.total, self.total, self.from_below.at[z])

        @pl.when(z < 3)
        def _():
            self.going_down(0, z).wait_recv()
            self.add(self.total, self.total, self.from_above.at[z])

    def finish(self):
        for i in range(4):
            self.over(i).wait_send()
        for i in range(3):
            self.going_up(i, 0).wait_send()

    @staticmethod
    def scratch(block, kind):
        return [
            *[pltpu.VMEM((amount,) + block, kind) for amount in (8, 8, 4, 4, 4)],
            pltpu.VMEM(block, jnp.float32),
            *[pltpu.SemaphoreType.DMA((amount,)) for amount in (7, 4, 4, 4)],
        ]


def scatter_kernel(amount, *refs):
    parts_refs, out_ref = refs[:amount], refs[amount]
    scatter = Scatter(refs[amount + 1 : amount + 7], refs[amount + 7 : amount + 11])
    core_send_sem, core_sem, local_sem = refs[amount + 11 :]
    columns, start = [], 0
    for ref in parts_refs:
        columns.append(pl.ds(start, ref.shape[2]))
        start += ref.shape[2]

    def local(k):
        index = scatter.index(k, scatter.c)
        return [
            pltpu.make_async_copy(ref.at[index], scatter.held.at[k, :, at], local_sem.at[k * amount + i])
            for i, (ref, at) in enumerate(zip(parts_refs, columns))
        ]

    def to_core(k):
        index = scatter.index(k, 1 - scatter.c)
        return [
            remote(
                ref.at[index],
                scatter.from_core.at[k, :, at],
                core_send_sem.at[k * amount + i],
                core_sem.at[k * amount + i],
                scatter.other,
            )
            for i, (ref, at) in enumerate(zip(parts_refs, columns))
        ]

    for k in range(8):
        for copy in local(k):
            copy.start()
    greet_line(scatter.z, (scatter.across, scatter.other), scatter.down, scatter.up)
    for k in range(8):
        for copy in to_core(k):
            copy.start()

    def both(k):
        for copy in local(k):
            copy.wait()
        for copy in to_core(k):
            copy.wait_recv()

    for i in range(4):
        both(i)
        scatter.side(i)
    for i in range(3):
        both(4 + i)
        scatter.line(i)
    both(7)
    scatter.last()
    outward = pltpu.make_async_copy(scatter.total, out_ref, local_sem.at[8 * amount])
    outward.start()
    for k in range(8):
        for copy in to_core(k):
            copy.wait_send()
    scatter.finish()
    outward.wait()


def contract(left, right, left_dim, right_dim):
    return lax.dot_general(
        left, right, (((left_dim,), (right_dim,)), ((), ())), preferred_element_type=jnp.float32
    )


def backward_kernel(
    unit_grads_ref, weights_ref, rows_ref, hidden_ref, out_ref, weight_grads_ref,
    held, from_core, from_across, from_below, from_above, total, send_sem, across_sem, below_sem, above_sem,
    core_send_sem, core_sem, local_sem, for_core, unit_grads, weights, rows, tile, tile_sem,
):
    scatter = Scatter(
        (held, from_core, from_across, from_below, from_above, total), (send_sem, across_sem, below_sem, above_sem)
    )
    block_rows, width = out_ref.shape
    blocks = rows.shape[1] // block_rows
    step = 3 * 256
    loads = [
        pltpu.make_async_copy(unit_grads_ref, unit_grads.at[pl.ds(0, 2)], local_sem.at[0]),
        pltpu.make_async_copy(weights_ref.at[pl.ds(0, 2)], weights, local_sem.at[1]),
        pltpu.make_async_copy(hidden_ref, unit_grads.at[2], local_sem.at[2]),
        pltpu.make_async_copy(rows_ref[0], rows.at[0], local_sem.at[3]),
        pltpu.make_async_copy(rows_ref[1], rows.at[1], local_sem.at[4]),
    ]
    for copy in loads:
        copy.start()
    greet_line(scatter.z, (scatter.across, scatter.other), scatter.down, scatter.up)
    loads[0].wait()
    loads[1].wait()

    def partial(j, core, target):
        spots = [pl.ds(pl.multiple_of(scatter.index(k, core) * block_rows, block_rows), block_rows) for k in (j, 4 + j)]

        def body(d, carry):
            at = pl.ds(pl.multiple_of(d * step, step), step)
            sums = None
            for i in range(2):
                left = jnp.concatenate([unit_grads[i, spot, :] for spot in spots], axis=0)
                part = contract(left, weights[i, at, :], 1, 1)
                sums = part if sums is None else sums + part
            sums = sums.astype(target.dtype)
            target[j, :, at] = sums[:block_rows]
            target[4 + j, :, at] = sums[block_rows:]
            return carry

        lax.fori_loop(0, width // step, body, 0)

    def to_core(k):
        return remote(for_core.at[k], from_core.at[k], core_send_sem.at[k], core_sem.at[k], scatter.other)

    tile_rows = tile.shape[2]

    def tile_out(u, i):
        return pltpu.make_async_copy(
            tile.at[u % 2, i], weight_grads_ref.at[i, pl.ds(u * tile_rows, tile_rows), :], tile_sem.at[u % 2, i]
        )

    def weight_tile(u):
        if u == 0:
            for copy in loads[2:]:
                copy.wait()
        if u >= 2:
            for i in range(3):
                tile_out(u - 2, i).wait()

        def body(i, carry):
            left = rows[i // 2, :, pl.ds(u * tile_rows, tile_rows)]
            tile[u % 2, i] = contract(left, unit_grads[i], 0, 0).astype(tile.dtype)
            return carry

        lax.fori_loop(0, 3, body, 0)
        for i in range(3):
            tile_out(u, i).start()

    for j in range(4):
        partial(j, 1 - scatter.c, for_core)
        to_core(j).start()
        to_core(4 + j).start()
        partial(j, scatter.c, held)
        to_core(j).wait_recv()
        scatter.side(j)
        if j == 1:
            weight_tile(0)
    weight_tile(1)
    for i in range(3):
        to_core(4 + i).wait_recv()
        scatter.line(i)
        weight_tile(2 + i)
    weight_tile(5)
    to_core(7).wait_recv()
    scatter.last()
    outward = pltpu.make_async_copy(total, out_ref, local_sem.at[5])
    outward.start()
    for k in range(8):
        to_core(k).wait_send()
    scatter.finish()
    for u in (4, 5):
        for i in range(3):
            tile_out(u, i).wait()
    outward.wait()


def scatter_fsdp(parts, collective_id):
    size, rows, _ = parts[0].shape
    columns = sum(part.shape[2] for part in parts)
    if size != KERNEL_FSDP:
        return lax.psum_scatter(
            jnp.concatenate(parts, axis=2), "fsdp", scatter_dimension=0, tiled=False
        ).astype(jnp.float32)
    block, amount = (rows, columns), len(parts)
    return scratch_call(
        functools.partial(scatter_kernel, amount),
        jax.ShapeDtypeStruct(block, jnp.float32),
        [
            *Scatter.scratch(block, parts[0].dtype),
            pltpu.SemaphoreType.DMA((8 * amount,)),
            pltpu.SemaphoreType.DMA((8 * amount,)),
            pltpu.SemaphoreType.DMA((8 * amount + 1,)),
        ],
        collective_id,
        *parts,
    )


def feed_backward(gate_grad, up_grad, feed_full, feed_input, feed_grad_rows, hidden, collective_id):
    size = lax.axis_size("fsdp")
    kind = hidden.dtype
    tokens, width = feed_input.shape
    if size != KERNEL_FSDP:
        sums = contract(gate_grad, feed_full[0], 1, 1) + contract(up_grad, feed_full[1], 1, 1)
        return (
            scatter_fsdp((sums.astype(kind).reshape(size, tokens // size, width),), collective_id),
            jnp.stack(
                [
                    contract(left, right, 0, 0).astype(kind)
                    for left, right in ((feed_input, gate_grad), (feed_input, up_grad), (feed_grad_rows, hidden))
                ]
            ),
        )
    block, units = (tokens // size, width), hidden.shape[1]
    tile_rows = width // 6

    def kernel(unit_grads_ref, weights_ref, input_ref, grad_ref, hidden_ref, *refs):
        backward_kernel(unit_grads_ref, weights_ref, (input_ref, grad_ref), hidden_ref, *refs)

    rows_grad, weight_grads = scratch_call(
        kernel,
        (jax.ShapeDtypeStruct(block, jnp.float32), jax.ShapeDtypeStruct((3, width, units), kind)),
        [
            *Scatter.scratch(block, kind),
            pltpu.SemaphoreType.DMA((8,)),
            pltpu.SemaphoreType.DMA((8,)),
            pltpu.SemaphoreType.DMA((6,)),
            pltpu.VMEM((8,) + block, kind),
            pltpu.VMEM((3, tokens, units), kind),
            pltpu.VMEM((2, width, units), kind),
            pltpu.VMEM((2, tokens, width), kind),
            pltpu.VMEM((2, 3, tile_rows, units), kind),
            pltpu.SemaphoreType.DMA((2, 3)),
        ],
        collective_id,
        jnp.stack([gate_grad, up_grad]),
        feed_full,
        feed_input,
        feed_grad_rows,
        hidden,
    )
    return rows_grad, weight_grads


def exchange_kernel(block_ref, out_ref, send_sem, receive_sem):
    index, t = lax.axis_index("fsdp"), lax.axis_index("tp")
    partner = (index, 1 - t)
    greet((partner,))
    copy = remote(block_ref, out_ref, send_sem.at[0], receive_sem.at[0], partner)
    copy.start()
    copy.wait()


def exchange_tp(block, collective_id):
    if lax.axis_size("fsdp") != KERNEL_FSDP:
        return lax.ppermute(block, "tp", [(0, 1), (1, 0)])
    return scratch_call(
        exchange_kernel,
        jax.ShapeDtypeStruct(block.shape, block.dtype),
        [pltpu.SemaphoreType.DMA((1,)), pltpu.SemaphoreType.DMA((1,))],
        collective_id,
        block,
    )


def peer(z, x, c, k):
    kz, kx, kc = k // 4, (k // 2) % 2, k % 2
    high, low = z // 2, z % 2
    high = 1 - high if kz // 2 else high
    low = 1 - low if kz % 2 else low
    return fsdp_index(high * 2 + low, 1 - x if kx else x, 1 - c if kc else c)


MAIN = 2 * LANES
REST = LANES
FIRST_REST = KERNEL_FSDP * MAIN
UNITS = 2 * MAIN + REST


def main_of(owner):
    return pl.ds(pl.multiple_of(owner * MAIN, MAIN), MAIN)


def rest_of(z):
    return pl.ds(pl.multiple_of(FIRST_REST + z * REST, REST), REST)


def distribute_kernel(
    rows_ref, query_ref, key_ref, value_ref, output_ref, gain_ref, gate_ref, up_ref, down_ref,
    attention_ref, partner_ref, feed_ref,
    stage, feed, zeros,
    gather_send, gather_receive, local_sem, pair_rows_sem, send_sem, receive_sem, rest_send, rest_receive,
    on_send, on_receive, rest_on_send, rest_on_receive,
):
    z, x, c, t = place()
    own = fsdp_index(z, x, c)
    partner = (own, 1 - t)
    greet([(peer(z, x, c, k), t) for k in range(1, 16)] + [partner])
    rows_copy = remote(rows_ref, partner_ref, pair_rows_sem.at[0], pair_rows_sem.at[1], partner)
    rows_copy.start()
    loads, start = [], 0
    for i, ref in enumerate((query_ref, key_ref, value_ref, output_ref, gain_ref)):
        loads.append(pltpu.make_async_copy(ref, stage.at[:, pl.ds(start, ref.shape[1])], local_sem.at[i]))
        start += ref.shape[1]
    feed_loads = [
        pltpu.make_async_copy(ref, feed.at[i], local_sem.at[5 + i])
        for i, ref in enumerate((gate_ref, up_ref, down_ref))
    ]
    for copy in loads + feed_loads:
        copy.start()
    for copy in loads:
        copy.wait()
    gather = Gather(stage, attention_ref, gather_send, gather_receive)
    gather.start()
    keep = pltpu.make_async_copy(stage, attention_ref.at[own], local_sem.at[8])
    keep.start()
    for copy in feed_loads:
        copy.wait()

    def main_at(half, source):
        return feed_ref.at[:, source, :, pl.ds(pl.multiple_of(half * MAIN, MAIN), MAIN)]

    def rest_at(source):
        return feed_ref.at[:, source, :, pl.ds(2 * MAIN, REST)]

    takes_rest = (c == 0) & (x == t)

    def direct(k):
        to = peer(z, x, c, k)
        return remote(feed.at[:, :, main_of(to)], main_at(t, own), send_sem.at[k], receive_sem.at[k], (to, t))

    def rest(dz):
        to_z = peer(z, x, c, 4 * dz) // 4
        slot = 4 * dz + 2 * ((x + t) % 2) + c
        return remote(
            feed.at[:, :, rest_of(to_z)], rest_at(own), rest_send.at[dz], rest_receive.at[slot], (fsdp_index(to_z, t, 0), t)
        )

    def onward(k):
        at = main_at(t, peer(z, x, c, k))
        return remote(at if k else feed.at[:, :, main_of(own)], at, on_send.at[k], on_receive.at[k], partner)

    def rest_onward(k):
        at = rest_at(peer(z, x, c, k))
        return remote(at if k else feed.at[:, :, rest_of(z)], at, rest_on_send.at[k], rest_on_receive.at[k], partner)

    def send(dz):
        for k in range(4 * dz, 4 * dz + 4):
            if k:
                direct(k).start()
        if dz:
            rest(dz).start()
        else:

            @pl.when(jnp.logical_not(takes_rest))
            def _():
                rest(0).start()

    def pass_on(dz):
        for k in range(4 * dz, 4 * dz + 4):
            if k:
                direct(k).wait_recv()
            onward(k).start()

        @pl.when(takes_rest)
        def _():
            for k in range(4 * dz, 4 * dz + 4):
                if k:
                    remote(
                        feed.at[:, :, rest_of(0)], rest_at(own), rest_send.at[0], rest_receive.at[k], partner
                    ).wait_recv()
                rest_onward(k).start()

    send(0)
    send(1)
    keep_main = pltpu.make_async_copy(feed.at[:, :, main_of(own)], main_at(t, own), local_sem.at[9])
    keep_main.start()
    keep_rest = pltpu.make_async_copy(feed.at[:, :, rest_of(z)], rest_at(own), local_sem.at[10])

    @pl.when(takes_rest)
    def _():
        keep_rest.start()

    fills = [
        pltpu.make_async_copy(zeros, feed_ref.at[i, :, :, pl.ds(2 * MAIN, REST)], local_sem.at[11 + i])
        for i in range(3)
    ]

    @pl.when(c == 1)
    def _():
        zeros[...] = jnp.zeros_like(zeros)
        for copy in fills:
            copy.start()

    send(2)
    pass_on(0)
    pass_on(1)
    gather.line(1)
    gather.side(0)
    send(3)
    gather.line(2)
    gather.side(1)
    pass_on(2)
    gather.line(3)
    gather.side(2)
    pass_on(3)
    gather.side(3)
    gather.finish()
    rows_copy.wait()
    for k in range(16):
        onward(k).wait_recv()
        onward(k).wait_send()
        if k:
            direct(k).wait_send()

    @pl.when(jnp.logical_not(takes_rest))
    def _():
        rest(0).wait_send()

    for dz in (1, 2, 3):
        rest(dz).wait_send()

    @pl.when(takes_rest)
    def _():
        for k in range(16):
            rest_onward(k).wait_send()
        keep_rest.wait()

    @pl.when((c == 0) & (x != t))
    def _():
        for k in range(16):
            rest_onward(k).wait_recv()

    @pl.when(c == 1)
    def _():
        for copy in fills:
            copy.wait()

    keep.wait()
    keep_main.wait()


def distribute(rows, attention, gain_columns, feed, collective_id):
    size = lax.axis_size("fsdp")
    shard_rows, feed_width = feed[0].shape
    columns = sum(w.shape[1] for w in attention) + gain_columns.shape[1]
    if size != KERNEL_FSDP:
        halves = lax.all_to_all(pack_units(feed, size), "fsdp", split_axis=0, concat_axis=0, tiled=True)
        halves = lax.all_gather(halves, "tp", axis=0)
        halves = halves.reshape(halves.shape[0], size * shard_rows, halves.shape[-1])
        return (
            lax.all_gather(jnp.concatenate((*attention, gain_columns), axis=1), "fsdp", axis=0),
            lax.ppermute(rows, "tp", [(0, 1), (1, 0)]),
            jnp.stack(join_units(halves, feed_width, size, 3)),
        )
    kind = rows.dtype
    attention_full, partner_rows, feed_full = scratch_call(
        distribute_kernel,
        (
            jax.ShapeDtypeStruct((size, shard_rows, columns), kind),
            jax.ShapeDtypeStruct(rows.shape, kind),
            jax.ShapeDtypeStruct((3, size, shard_rows, UNITS), kind),
        ),
        [
            pltpu.VMEM((shard_rows, columns), kind),
            pltpu.VMEM((3, shard_rows, feed_width), kind),
            pltpu.VMEM((size, shard_rows, REST), kind),
            pltpu.SemaphoreType.DMA((Gather.slots,)),
            pltpu.SemaphoreType.DMA((size,)),
            pltpu.SemaphoreType.DMA((14,)),
            pltpu.SemaphoreType.DMA((2,)),
            pltpu.SemaphoreType.DMA((size,)),
            pltpu.SemaphoreType.DMA((size,)),
            pltpu.SemaphoreType.DMA((4,)),
            pltpu.SemaphoreType.DMA((size,)),
            pltpu.SemaphoreType.DMA((size,)),
            pltpu.SemaphoreType.DMA((size,)),
            pltpu.SemaphoreType.DMA((size,)),
            pltpu.SemaphoreType.DMA((size,)),
        ],
        collective_id,
        rows,
        *attention,
        gain_columns,
        *feed,
    )
    return attention_full, partner_rows, feed_full.reshape(3, size * shard_rows, UNITS)


def collect_kernel(
    parts_ref, out_ref,
    held, received, rest_held, rest_received,
    local_sem, pair_send, pair_receive, rest_pair_send, rest_pair_receive, send_sem, receive_sem, rest_send, rest_receive,
):
    z, x, c, t = place()
    own = fsdp_index(z, x, c)
    rows = out_ref.shape[1]
    partner = (own, 1 - t)
    parts = [parts_ref.at[i] for i in range(3)]
    order = (3, 2, 1, 0)
    takes_rest = (c == 0) & (x == t)
    gives_rest = (c == 0) & (x != t)

    def plane(dz):
        return pl.ds(peer(z, x, c, 4 * dz) // 4 * 4, 4)

    def half(which):
        return pl.ds(pl.multiple_of(which * MAIN, MAIN), MAIN)

    rest_columns = pl.ds(2 * MAIN, REST)

    def load(dz, i):
        return pltpu.make_async_copy(parts[i].at[plane(dz), :, half(t)], held.at[dz, i], local_sem.at[3 * dz + i])

    def rest_load(dz, i):
        return pltpu.make_async_copy(
            parts[i].at[plane(dz), :, rest_columns], rest_held.at[dz, i], local_sem.at[12 + 3 * dz + i]
        )

    def pair(dz, i):
        slot = 3 * dz + i
        return remote(
            parts[i].at[plane(dz), :, half(1 - t)], received.at[dz, i], pair_send.at[slot], pair_receive.at[slot], partner
        )

    def rest_pair(dz, i):
        slot = 3 * dz + i
        return remote(
            parts[i].at[plane(dz), :, rest_columns],
            rest_received.at[dz, i],
            rest_pair_send.at[slot],
            rest_pair_receive.at[slot],
            partner,
        )

    def spot(k):
        return peer(z, x, c, k) % 4

    def direct(k):
        return remote(
            held.at[k // 4, :, spot(k)], out_ref.at[:, :, main_of(own)], send_sem.at[k], receive_sem.at[k], (peer(z, x, c, k), t)
        )

    def rest_direct(k):
        return remote(
            rest_held.at[k // 4, :, spot(k)],
            out_ref.at[:, :, rest_of(z)],
            rest_send.at[k],
            rest_receive.at[z],
            (peer(z, x, c, k), t),
        )

    def add(target, source):
        def body(j, carry):
            i, at = j // 4, j % 4
            total = target[i, at].astype(jnp.float32) + source[i, at].astype(jnp.float32)
            target[i, at] = total.astype(target.dtype)
            return carry

        lax.fori_loop(0, 12, body, 0)

    for dz in order:
        for i in range(3):
            load(dz, i).start()

    @pl.when(takes_rest)
    def _():
        for dz in order:
            for i in range(3):
                rest_load(dz, i).start()

    greet([(peer(z, x, c, k), t) for k in range(1, 16)] + [partner])
    for dz in order:
        for i in range(3):
            pair(dz, i).start()

        @pl.when(gives_rest)
        def _():
            for i in range(3):
                rest_pair(dz, i).start()

    for dz in order:
        for i in range(3):
            load(dz, i).wait()
            pair(dz, i).wait_recv()
        add(held.at[dz], received.at[dz])
        for k in range(4 * dz, 4 * dz + 4):
            if k:
                direct(k).start()

        @pl.when(takes_rest)
        def _():
            for i in range(3):
                rest_load(dz, i).wait()
                rest_pair(dz, i).wait_recv()
            add(rest_held.at[dz], rest_received.at[dz])
            for k in range(4 * dz, 4 * dz + 4):
                if k:
                    rest_direct(k).start()

    keep = pltpu.make_async_copy(held.at[0, :, spot(0)], out_ref.at[:, :, main_of(own)], local_sem.at[24])
    keep.start()
    keep_rest = pltpu.make_async_copy(rest_held.at[0, :, spot(0)], out_ref.at[:, :, rest_of(z)], local_sem.at[25])

    @pl.when(takes_rest)
    def _():
        keep_rest.start()

    for k in range(1, 16):
        direct(k).wait_recv()

    for dz in range(4):
        from_z = peer(z, x, c, 4 * dz) // 4

        def arrived():
            remote(
                rest_held.at[0, :, 0], out_ref.at[:, :, rest_of(from_z)], rest_send.at[0], rest_receive.at[from_z], partner
            ).wait_recv()

        if dz:
            arrived()
        else:

            @pl.when(jnp.logical_not(takes_rest))
            def _():
                arrived()

    for k in range(1, 16):
        direct(k).wait_send()
    for dz in order:
        for i in range(3):
            pair(dz, i).wait_send()

    @pl.when(gives_rest)
    def _():
        for dz in order:
            for i in range(3):
                rest_pair(dz, i).wait_send()

    @pl.when(takes_rest)
    def _():
        for k in range(1, 16):
            rest_direct(k).wait_send()
        keep_rest.wait()

    keep.wait()


def collect(gradients, feed_width, collective_id):
    size, pairs = lax.axis_size("fsdp"), lax.axis_size("tp")
    shard_rows = gradients.shape[1] // size
    if size != KERNEL_FSDP:
        packed = part_units([gradients[i] for i in range(3)], feed_width, size, pairs)
        mine = lax.psum_scatter(packed, "tp", scatter_dimension=0, tiled=False)
        mine = mine.reshape(size, shard_rows, mine.shape[-1])
        mine = lax.all_to_all(mine, "fsdp", split_axis=0, concat_axis=0, tiled=True)
        return [g.astype(jnp.float32) for g in unpack_units(mine, feed_width, 3)]
    kind = gradients.dtype
    main, rest = (4, 3, 4, shard_rows, MAIN), (4, 3, 4, shard_rows, REST)
    out = scratch_call(
        collect_kernel,
        jax.ShapeDtypeStruct((3, shard_rows, feed_width), kind),
        [
            pltpu.VMEM(main, kind),
            pltpu.VMEM(main, kind),
            pltpu.VMEM(rest, kind),
            pltpu.VMEM(rest, kind),
            pltpu.SemaphoreType.DMA((26,)),
            pltpu.SemaphoreType.DMA((12,)),
            pltpu.SemaphoreType.DMA((12,)),
            pltpu.SemaphoreType.DMA((12,)),
            pltpu.SemaphoreType.DMA((12,)),
            pltpu.SemaphoreType.DMA((size,)),
            pltpu.SemaphoreType.DMA((size,)),
            pltpu.SemaphoreType.DMA((size,)),
            pltpu.SemaphoreType.DMA((4,)),
        ],
        collective_id,
        gradients.reshape(3, size, shard_rows, UNITS),
    )
    return [out[i].astype(jnp.float32) for i in range(3)]


def contract_last(left_rows, right_rows):
    return lax.dot_general(
        left_rows, right_rows, (((1,), (1,)), ((), ())), preferred_element_type=jnp.float32
    )


def contract_first(left_rows, right_rows):
    return lax.dot_general(
        left_rows, right_rows, (((0,), (0,)), ((), ())), preferred_element_type=jnp.float32
    )


def normalize_parts(value_rows):
    inverse = lax.rsqrt(jnp.mean(value_rows * value_rows, axis=-1, keepdims=True) + EPSILON)
    return (value_rows * inverse, inverse)


def norm_backward(unit_rows, inverse, norm_gain, upstream):
    scaled = upstream * norm_gain
    return inverse * (scaled - unit_rows * jnp.mean(scaled * unit_rows, axis=-1, keepdims=True))


def layout(lengths_row, row_index):
    segment_ends = jnp.cumsum(lengths_row)
    segment_starts = segment_ends - lengths_row
    segment = jnp.sum((row_index[:, None] >= segment_ends[None, :]).astype(jnp.int32), axis=1)
    onehot = segment[:, None] == jnp.arange(lengths_row.shape[0], dtype=jnp.int32)[None, :]
    segment_begin = jnp.sum(jnp.where(onehot, segment_starts[None, :], 0), axis=1)
    prompt_shift = jnp.where(segment > 0, lengths_row[0], 0)
    return (segment, row_index - segment_begin + prompt_shift)


def rotary_tables(position):
    frequency = jnp.exp(
        jnp.arange(HEAD_SIZE // 2, dtype=jnp.float32) * (-2.0 * math.log(10000.0) / HEAD_SIZE)
    )
    angles = position.astype(jnp.float32)[:, None] * frequency[None, :]
    return (jnp.cos(angles), jnp.sin(angles))


def apply_rotary(value_rows, cosine_lookup, sine_lookup):
    half_width = value_rows.shape[-1] // 2
    first_half = value_rows[..., :half_width]
    second_half = value_rows[..., half_width:]
    cosine_part = cosine_lookup[:, None, :]
    sine_part = sine_lookup[:, None, :]
    return jnp.concatenate(
        [
            first_half * cosine_part - second_half * sine_part,
            second_half * cosine_part + first_half * sine_part,
        ],
        axis=-1,
    )


def unrotate(value_rows, cosine_lookup, sine_lookup):
    half_width = value_rows.shape[-1] // 2
    first_half = value_rows[..., :half_width]
    second_half = value_rows[..., half_width:]
    cosine_part = cosine_lookup[:, None, :]
    sine_part = sine_lookup[:, None, :]
    return jnp.concatenate(
        [
            first_half * cosine_part + second_half * sine_part,
            second_half * cosine_part - first_half * sine_part,
        ],
        axis=-1,
    )


def visible(segment, row_index):
    same_segment = (segment[:, None] == segment[None, :]) & (
        row_index[None, :] <= row_index[:, None]
    )
    from_prompt = (segment[None, :] == 0) & (segment[:, None] > 0)
    return same_segment | from_prompt


def masked_scores(rotated_query, rotated_key, visible_mask):
    raw_scores = jnp.einsum(
        "qgrd,kgd->grqk", rotated_query, rotated_key, preferred_element_type=jnp.float32
    )
    tanh_value = jnp.tanh(raw_scores * HEAD_SIZE ** (-0.5) / SOFTCAP)
    return (jnp.where(visible_mask[None, None], SOFTCAP * tanh_value, NEGATIVE), tanh_value)


def gelu_product(gate_value, up_value):
    return jax.nn.gelu(gate_value, approximate=True) * up_value


def split_columns(width, size):
    main = width // size // LANES * LANES
    return main, width // size - main


def pack_units(weights, size):
    rows, width = weights[0].shape
    main, rest = split_columns(width, size)
    pieces = []
    if main:
        pieces += [
            jnp.transpose(w[:, : main * size].reshape(rows, size, main), (1, 0, 2)) for w in weights
        ]
    if rest:
        pieces += [
            jnp.transpose(w[:, main * size :].reshape(rows, size, rest), (1, 0, 2)) for w in weights
        ]
    packed = jnp.concatenate(pieces, axis=2)
    return jnp.pad(packed, ((0, 0), (0, 0), (0, -packed.shape[2] % LANES)))


def unpack_units(packed, width, amount):
    size, rows, _ = packed.shape
    main, rest = split_columns(width, size)
    arrays = []
    for i in range(amount):
        pieces = []
        if main:
            piece = packed[:, :, i * main : (i + 1) * main]
            pieces.append(jnp.transpose(piece, (1, 0, 2)).reshape(rows, size * main))
        if rest:
            start = amount * main + i * rest
            piece = packed[:, :, start : start + rest]
            pieces.append(jnp.transpose(piece, (1, 0, 2)).reshape(rows, size * rest))
        arrays.append(jnp.concatenate(pieces, axis=1))
    return arrays


def join_units(halves, width, size, amount):
    main, rest = split_columns(width, size)
    arrays = []
    for i in range(amount):
        start = amount * main + i * rest
        pieces = [half[:, i * main : (i + 1) * main] for half in halves]
        pieces += [half[:, start : start + rest] for half in halves]
        joined = jnp.concatenate(pieces, axis=1)
        arrays.append(jnp.pad(joined, ((0, 0), (0, -joined.shape[1] % LANES))))
    return arrays


def part_units(arrays, width, size, pairs):
    main, rest = split_columns(width, size)
    halves = []
    for t in range(pairs):
        pieces = [array[:, t * main : (t + 1) * main] for array in arrays]
        start = pairs * main + t * rest
        pieces += [array[:, start : start + rest] for array in arrays]
        packed = jnp.concatenate(pieces, axis=1)
        halves.append(jnp.pad(packed, ((0, 0), (0, -packed.shape[1] % LANES))))
    return jnp.stack(halves)


def shards(
    block_input,
    lengths,
    attention_norm_gain,
    attention_post_gain,
    feedforward_norm_gain,
    feedforward_post_gain,
    query_weight,
    key_weight,
    value_weight,
    output_weight,
    gate_weight,
    up_weight,
    down_weight,
    output_cotangent,
):
    low = jnp.bfloat16
    size, pairs = lax.axis_size("fsdp"), lax.axis_size("tp")
    rows_local, width = block_input.shape
    shard_rows, feed_width = gate_weight.shape
    query_width, key_width = query_weight.shape[1], key_weight.shape[1]
    output_start = query_width + 2 * key_width
    gain_start = output_start + query_width
    grouped_rows = rows_local * pairs

    gain_columns = jnp.stack(
        [attention_norm_gain, attention_post_gain, feedforward_norm_gain, feedforward_post_gain],
        axis=1,
    )
    attention_full, other_input, feed_full = distribute(
        block_input,
        (query_weight, key_weight, value_weight, output_weight),
        jnp.pad(gain_columns, ((0, 0), (0, LANES - 4))),
        (gate_weight, up_weight, down_weight),
        1,
    )
    attention_full = attention_full.reshape(size * shard_rows, gain_start + LANES)
    gains = jnp.transpose(attention_full[:, gain_start : gain_start + 4]).astype(jnp.float32)
    gain_one, gain_two, gain_three, gain_four = gains[0], gains[1], gains[2], gains[3]
    gate_full, up_full, down_full = feed_full[0], feed_full[1], feed_full[2]

    row_index = (
        jnp.arange(grouped_rows, dtype=jnp.int32) + lax.axis_index("tp") * rows_local
    ) % grouped_rows
    segment, position = layout(lengths[0], row_index)
    cosine_lookup, sine_lookup = rotary_tables(position)
    visible_mask = visible(segment, row_index)
    residual_both = jnp.concatenate([block_input, other_input], axis=0).astype(jnp.float32)
    unit_one_both, inverse_one_both = normalize_parts(residual_both)
    residual = residual_both[:rows_local]
    unit_one, inverse_one = unit_one_both[:rows_local], inverse_one_both[:rows_local]
    normed = (unit_one_both * gain_one).astype(low)
    projected = jnp.dot(
        normed, attention_full[:, :output_start], preferred_element_type=jnp.float32
    )
    query_raw = projected[:, :query_width]
    key_raw = projected[:, query_width : query_width + key_width]
    value_raw = projected[:, query_width + key_width :]
    heads_local = query_width // HEAD_SIZE
    kv_local = key_width // HEAD_SIZE
    repeat_heads = heads_local // kv_local
    rotated_query = apply_rotary(
        query_raw.reshape(grouped_rows, heads_local, HEAD_SIZE), cosine_lookup, sine_lookup
    ).astype(low)
    rotated_query = rotated_query.reshape(grouped_rows, kv_local, repeat_heads, HEAD_SIZE)
    rotated_key = apply_rotary(
        key_raw.reshape(grouped_rows, kv_local, HEAD_SIZE), cosine_lookup, sine_lookup
    ).astype(low)
    value_reduced = value_raw.astype(low).reshape(grouped_rows, kv_local, HEAD_SIZE)
    capped, tanh_value = masked_scores(rotated_query, rotated_key, visible_mask)
    row_peak = jnp.max(capped, axis=-1, keepdims=True)
    exponentials = jnp.exp(capped - row_peak)
    softmax_probs = exponentials / jnp.sum(exponentials, axis=-1, keepdims=True)
    probs_low = softmax_probs.astype(low)
    mixed_heads = jnp.einsum(
        "grqk,kgd->qgrd", probs_low, value_reduced, preferred_element_type=jnp.float32
    )
    attended = mixed_heads.reshape(grouped_rows, heads_local * HEAD_SIZE).astype(low)
    output_full = attention_full[:, output_start:gain_start]
    branch_parts = contract_last(attended, output_full)
    branch_one = branch_parts[:rows_local] + exchange_tp(
        branch_parts[rows_local:].astype(low), 4
    ).astype(jnp.float32)
    unit_two, inverse_two = normalize_parts(branch_one)
    middle = residual + unit_two * gain_two
    unit_three, inverse_three = normalize_parts(middle)

    feed_input = gather_fsdp((unit_three * gain_three).astype(low), 5).reshape(-1, width)
    gate_value = jnp.dot(feed_input, gate_full, preferred_element_type=jnp.float32)
    up_value = jnp.dot(feed_input, up_full, preferred_element_type=jnp.float32)
    hidden = gelu_product(gate_value, up_value).astype(low)
    branch_two = scatter_fsdp(
        (contract_last(hidden, down_full).astype(low).reshape(size, rows_local, width),), 6
    )
    unit_four, inverse_four = normalize_parts(branch_two)
    block_output = (middle + unit_four * gain_four).astype(low)
    upstream = output_cotangent.astype(jnp.float32)
    gain_four_grad = jnp.sum(upstream * unit_four, axis=0)
    branch_two_grad = norm_backward(unit_four, inverse_four, gain_four, upstream).astype(low)
    feed_grad_rows = gather_fsdp(branch_two_grad, 7).reshape(-1, width)
    hidden_grad = jnp.dot(feed_grad_rows, down_full, preferred_element_type=jnp.float32)
    unused_out, pullback = jax.vjp(gelu_product, gate_value, up_value)
    gate_grad, up_grad = pullback(hidden_grad)
    gate_grad, up_grad = gate_grad.astype(low), up_grad.astype(low)
    normed_three_grad, feed_grads = feed_backward(
        gate_grad, up_grad, feed_full, feed_input, feed_grad_rows, hidden, 8
    )
    gate_weight_grad, up_weight_grad, down_weight_grad = collect(feed_grads, feed_width, 9)

    gain_three_grad = jnp.sum(normed_three_grad * unit_three, axis=0)
    middle_grad = upstream + norm_backward(unit_three, inverse_three, gain_three, normed_three_grad)
    gain_two_grad = jnp.sum(middle_grad * unit_two, axis=0)
    branch_one_grad = norm_backward(unit_two, inverse_two, gain_two, middle_grad).astype(low)
    attention_grad_rows = jnp.concatenate(
        [branch_one_grad, exchange_tp(branch_one_grad, 10)], axis=0
    )
    mixed_grad = jnp.dot(
        attention_grad_rows, output_full, preferred_element_type=jnp.float32
    ).astype(low)
    mixed_grad = mixed_grad.reshape(grouped_rows, kv_local, repeat_heads, HEAD_SIZE)
    value_grad = jnp.einsum(
        "grqk,qgrd->kgd", probs_low, mixed_grad, preferred_element_type=jnp.float32
    )
    probs_grad = jnp.einsum(
        "qgrd,kgd->grqk", mixed_grad, value_reduced, preferred_element_type=jnp.float32
    )
    score_grad = softmax_probs * (
        probs_grad - jnp.sum(softmax_probs * probs_grad, axis=-1, keepdims=True)
    )
    raw_grad = (score_grad * (1.0 - tanh_value * tanh_value) * HEAD_SIZE ** (-0.5)).astype(low)
    query_grad = jnp.einsum(
        "grqk,kgd->qgrd", raw_grad, rotated_key, preferred_element_type=jnp.float32
    )
    key_grad = jnp.einsum(
        "grqk,qgrd->kgd", raw_grad, rotated_query, preferred_element_type=jnp.float32
    )
    query_grad = unrotate(
        query_grad.reshape(grouped_rows, heads_local, HEAD_SIZE), cosine_lookup, sine_lookup
    )
    key_grad = unrotate(key_grad, cosine_lookup, sine_lookup)
    projected_grad = jnp.concatenate(
        [
            query_grad.reshape(grouped_rows, heads_local * HEAD_SIZE).astype(low),
            key_grad.reshape(grouped_rows, kv_local * HEAD_SIZE).astype(low),
            value_grad.reshape(grouped_rows, kv_local * HEAD_SIZE).astype(low),
        ],
        axis=1,
    )
    input_parts = contract_last(projected_grad, attention_full[:, :output_start])

    gain_grads = jnp.stack(
        [
            jnp.sum(input_parts * unit_one_both, axis=0),
            gain_two_grad,
            gain_three_grad,
            gain_four_grad,
        ]
    )
    sent = jnp.concatenate(
        [input_parts[rows_local:].astype(low), jnp.pad(gain_grads, ((0, 12), (0, 0))).astype(low)]
    )
    received = exchange_tp(sent, 11).astype(jnp.float32)
    normed_one_grad = input_parts[:rows_local] + received[:rows_local]
    gain_grads = gain_grads + received[rows_local : rows_local + 4]
    input_gradient = middle_grad + norm_backward(unit_one, inverse_one, gain_one, normed_one_grad)

    attention_grads = scatter_fsdp(
        [
            part.astype(low).reshape(size, shard_rows, part.shape[1])
            for part in (
                contract_first(normed, projected_grad),
                contract_first(attention_grad_rows, attended),
                jnp.pad(jnp.transpose(gain_grads), ((0, 0), (0, LANES - 4))),
            )
        ],
        12,
    )
    gain_shards = jnp.transpose(attention_grads[:, gain_start : gain_start + 4])
    return (
        block_output,
        input_gradient,
        gain_shards[0],
        gain_shards[1],
        gain_shards[2],
        gain_shards[3],
        attention_grads[:, :query_width],
        attention_grads[:, query_width : query_width + key_width],
        attention_grads[:, query_width + key_width : output_start],
        attention_grads[:, output_start:gain_start],
        gate_weight_grad,
        up_weight_grad,
        down_weight_grad,
    )


def solution(mesh):
    placed = (
        P(("fsdp", "tp"), None),
        P("fsdp", None),
        P("fsdp"),
        P("fsdp"),
        P("fsdp"),
        P("fsdp"),
        P("fsdp", "tp"),
        P("fsdp", "tp"),
        P("fsdp", "tp"),
        P("fsdp", "tp"),
        P("fsdp", "tp"),
        P("fsdp", "tp"),
        P("fsdp", "tp"),
        P(("fsdp", "tp"), None),
    )
    return jax.shard_map(
        shards,
        mesh=mesh,
        in_specs=placed,
        out_specs=(
            P(("fsdp", "tp"), None),
            P(("fsdp", "tp"), None),
            P("fsdp"),
            P("fsdp"),
            P("fsdp"),
            P("fsdp"),
            P("fsdp", "tp"),
            P("fsdp", "tp"),
            P("fsdp", "tp"),
            P("fsdp", "tp"),
            P("fsdp", "tp"),
            P("fsdp", "tp"),
            P("fsdp", "tp"),
        ),
        check_vma=False,
    )
```

```python
import functools
import math

import jax
import jax.numpy as jnp
from jax import lax
from jax.experimental import pallas as pl
from jax.experimental.pallas import tpu as pltpu
from jax.sharding import PartitionSpec as P

HEAD_SIZE = 256
MESH = pl.DeviceIdType.MESH
ANY = pl.BlockSpec(memory_space=pl.ANY)
LANES = 128

EPSILON = 1e-06
SOFTCAP = 50.0
NEGATIVE = -1e30

KERNEL_FSDP = 16


def place():
    index = lax.axis_index("fsdp")
    return index // 4, (index // 2) % 2, index % 2, lax.axis_index("tp")


def fsdp_index(z, x, c):
    return (z * 2 + x) * 2 + c


def remote(source, target, send_sem, receive_sem, device):
    return pltpu.make_async_remote_copy(
        src_ref=source,
        dst_ref=target,
        send_sem=send_sem,
        recv_sem=receive_sem,
        device_id=device,
        device_id_type=MESH,
    )


def greet(devices):
    barrier = pltpu.get_barrier_semaphore()
    for device in devices:
        pl.semaphore_signal(barrier, inc=1, device_id=device, device_id_type=MESH)
    pl.semaphore_wait(barrier, len(devices))


def greet_line(z, devices, down, up):
    barrier = pltpu.get_barrier_semaphore()
    for device in devices:
        pl.semaphore_signal(barrier, inc=1, device_id=device, device_id_type=MESH)

    @pl.when(z > 0)
    def _():
        pl.semaphore_signal(barrier, inc=1, device_id=down, device_id_type=MESH)

    @pl.when(z < 3)
    def _():
        pl.semaphore_signal(barrier, inc=1, device_id=up, device_id_type=MESH)

    pl.semaphore_wait(barrier, len(devices) + (z + 2) // 3 + (5 - z) // 3)


def stage_through(source, stage, target, sems):
    inward = pltpu.make_async_copy(source, stage, sems.at[0])
    inward.start()

    def finish():
        inward.wait()
        outward = pltpu.make_async_copy(stage, target, sems.at[1])
        outward.start()
        return outward

    return finish


class Gather:
    slots = 29

    def __init__(self, block, out_ref, send_sem, receive_sem):
        self.block, self.out, self.send_sem, self.receive_sem = block, out_ref, send_sem, receive_sem
        self.z, self.x, self.c, t = place()
        z, x, c = self.z, self.x, self.c
        self.own = fsdp_index(z, x, c)
        self.down, self.up = (fsdp_index(z - 1, x, c), t), (fsdp_index(z + 1, x, c), t)
        self.across, self.other = (fsdp_index(z, 1 - x, c), t), (fsdp_index(z, x, 1 - c), t)

    def copy(self, source, index, slot, device):
        return remote(source, self.out.at[index], self.send_sem.at[slot], self.receive_sem.at[index], device)

    def relay(self, index, slot, device):
        self.copy(self.out.at[index], index, slot, device).start()

    def arrived(self, index):
        self.copy(self.block, index, 0, self.other).wait_recv()

    def sent(self, slot):
        self.copy(self.block, self.own, slot, self.other).wait_send()

    def start(self):
        @pl.when(self.z < 3)
        def _():
            self.copy(self.block, self.own, 0, self.up).start()

        @pl.when(self.z > 0)
        def _():
            self.copy(self.block, self.own, 1, self.down).start()

        self.copy(self.block, self.own, 2, self.across).start()
        self.copy(self.block, self.own, 3, self.other).start()

    def line(self, d):
        z, x, c = self.z, self.x, self.c

        @pl.when(z >= d)
        def _():
            index = fsdp_index(z - d, x, c)
            base = 4 + 3 * (d - 1)
            self.arrived(index)

            @pl.when(z < 3)
            def _():
                self.relay(index, base, self.up)

            self.relay(index, base + 1, self.across)
            self.relay(index, base + 2, self.other)

        @pl.when(z + d <= 3)
        def _():
            index = fsdp_index(z + d, x, c)
            base = 13 + 3 * (d - 1)
            self.arrived(index)

            @pl.when(z > 0)
            def _():
                self.relay(index, base, self.down)

            self.relay(index, base + 1, self.across)
            self.relay(index, base + 2, self.other)

    def side(self, d):
        z, x, c = self.z, self.x, self.c
        if d == 0:
            index = fsdp_index(z, 1 - x, c)
            self.arrived(index)
            self.relay(index, 22, self.other)
            return

        @pl.when(z >= d)
        def _():
            index = fsdp_index(z - d, 1 - x, c)
            self.arrived(index)
            self.relay(index, 22 + d, self.other)

        @pl.when(z + d <= 3)
        def _():
            index = fsdp_index(z + d, 1 - x, c)
            self.arrived(index)
            self.relay(index, 25 + d, self.other)

    def finish(self):
        z = self.z
        for zi in range(4):
            for xi in range(2):
                self.arrived(fsdp_index(zi, xi, 1 - self.c))

        @pl.when(z < 3)
        def _():
            self.sent(0)

        @pl.when(z > 0)
        def _():
            self.sent(1)

        for slot in (2, 3, 22):
            self.sent(slot)
        for d in (1, 2, 3):

            @pl.when(z >= d)
            def _():
                base = 4 + 3 * (d - 1)

                @pl.when(z < 3)
                def _():
                    self.sent(base)

                for slot in (base + 1, base + 2, 22 + d):
                    self.sent(slot)

            @pl.when(z + d <= 3)
            def _():
                base = 13 + 3 * (d - 1)

                @pl.when(z > 0)
                def _():
                    self.sent(base)

                for slot in (base + 1, base + 2, 25 + d):
                    self.sent(slot)


def gather_kernel(block_ref, out_ref, stage, send_sem, receive_sem, local_sem):
    gather = Gather(block_ref, out_ref, send_sem, receive_sem)
    greet_line(gather.z, (gather.across, gather.other), gather.down, gather.up)
    finish_own = stage_through(block_ref, stage, out_ref.at[gather.own], local_sem)
    gather.start()
    outward = finish_own()
    gather.line(1)
    gather.side(0)
    gather.line(2)
    gather.side(1)
    gather.line(3)
    gather.side(2)
    gather.side(3)
    gather.finish()
    outward.wait()


def scratch_call(kernel, outputs, scratch, collective_id, *operands):
    return pl.pallas_call(
        kernel,
        out_shape=outputs,
        in_specs=[ANY] * len(operands),
        out_specs=jax.tree.map(lambda _: ANY, outputs),
        scratch_shapes=scratch,
        compiler_params=pltpu.CompilerParams(
            collective_id=collective_id, has_side_effects=True, vmem_limit_bytes=60 * 1024 * 1024
        ),
    )(*operands)


def gather_fsdp(block, collective_id):
    size = lax.axis_size("fsdp")
    if size != KERNEL_FSDP:
        return lax.all_gather(block, "fsdp", axis=0)
    return scratch_call(
        gather_kernel,
        jax.ShapeDtypeStruct((size,) + block.shape, block.dtype),
        [
            pltpu.VMEM(block.shape, block.dtype),
            pltpu.SemaphoreType.DMA((29,)),
            pltpu.SemaphoreType.DMA((size,)),
            pltpu.SemaphoreType.DMA((2,)),
        ],
        collective_id,
        block,
    )


def add_rows(rows, step, target, *sources):
    def body(i, carry):
        at = pl.ds(pl.multiple_of(i * step, step), step)
        total = sources[0][at, :].astype(jnp.float32)
        for source in sources[1:]:
            total = total + source[at, :].astype(jnp.float32)
        target[at, :] = total.astype(target.dtype)
        return carry

    lax.fori_loop(0, rows // step, body, 0)


class Scatter:
    def __init__(self, buffers, semaphores):
        self.held, self.from_core, self.from_across, self.from_below, self.from_above, self.total = buffers
        self.send_sem, self.across_sem, self.below_sem, self.above_sem = semaphores
        self.z, self.x, self.c, t = place()
        z, x, c = self.z, self.x, self.c
        self.rows = self.total.shape[0]
        self.down, self.up = (fsdp_index(z - 1, x, c), t), (fsdp_index(z + 1, x, c), t)
        self.across, self.other = (fsdp_index(z, 1 - x, c), t), (fsdp_index(z, x, 1 - c), t)

    def target(self, i):
        if i == 3:
            return self.z
        half = self.z // 2
        mirrored = self.z + half * (3 - 2 * self.z)
        base = 3 - i - (i + mirrored) // 3
        return base + half * (3 - 2 * base)

    def index(self, k, core):
        return fsdp_index(self.target(k % 4), 1 - self.x if k < 4 else self.x, core)

    def add(self, target, *sources):
        add_rows(self.rows, 16, target, *sources)

    def over(self, i):
        return remote(
            self.held.at[i], self.from_across.at[i], self.send_sem.at[3 + i], self.across_sem.at[i], self.across
        )

    def going_up(self, i, target):
        return remote(
            self.held.at[4 + i], self.from_below.at[target], self.send_sem.at[i], self.below_sem.at[target], self.up
        )

    def going_down(self, i, target):
        return remote(
            self.held.at[4 + i], self.from_above.at[target], self.send_sem.at[i], self.above_sem.at[target], self.down
        )

    def side(self, i):
        self.add(self.held.at[i], self.held.at[i], self.from_core.at[i])
        self.over(i).start()

    def line(self, i):
        z, target = self.z, self.target(i)
        held = self.held.at[4 + i]
        sources = (held, self.from_core.at[4 + i], self.from_across.at[i])
        self.over(i).wait_recv()

        @pl.when(target > z)
        def _():
            @pl.when(z > 0)
            def _():
                self.going_up(i, target).wait_recv()
                self.add(held, *sources, self.from_below.at[target])

            @pl.when(z == 0)
            def _():
                self.add(held, *sources)

            self.going_up(i, target).start()

        @pl.when(target < z)
        def _():
            @pl.when(z < 3)
            def _():
                self.going_down(i, target).wait_recv()
                self.add(held, *sources, self.from_above.at[target])

            @pl.when(z == 3)
            def _():
                self.add(held, *sources)

            self.going_down(i, target).start()

    def last(self):
        z = self.z
        self.over(3).wait_recv()
        self.add(self.total, self.held.at[7], self.from_core.at[7], self.from_across.at[3])

        @pl.when(z > 0)
        def _():
            self.going_up(0, z).wait_recv()
            self.add(self.total, self.total, self.from_below.at[z])

        @pl.when(z < 3)
        def _():
            self.going_down(0, z).wait_recv()
            self.add(self.total, self.total, self.from_above.at[z])

    def finish(self):
        for i in range(4):
            self.over(i).wait_send()
        for i in range(3):
            self.going_up(i, 0).wait_send()

    @staticmethod
    def scratch(block, kind):
        return [
            *[pltpu.VMEM((amount,) + block, kind) for amount in (8, 8, 4, 4, 4)],
            pltpu.VMEM(block, jnp.float32),
            *[pltpu.SemaphoreType.DMA((amount,)) for amount in (7, 4, 4, 4)],
        ]


class Blocks:
    def __init__(self, scatter, parts_refs, core_send_sem, core_sem, local_sem):
        self.scatter, self.parts = scatter, []
        self.core_send_sem, self.core_sem, self.local_sem = core_send_sem, core_sem, local_sem
        start = 0
        for ref in parts_refs:
            self.parts.append((ref, pl.ds(start, ref.shape[2])))
            start += ref.shape[2]

    def local(self, k):
        index = self.scatter.index(k, self.scatter.c)
        return [
            pltpu.make_async_copy(
                ref.at[index], self.scatter.held.at[k, :, at], self.local_sem.at[k * len(self.parts) + i]
            )
            for i, (ref, at) in enumerate(self.parts)
        ]

    def to_core(self, k):
        index = self.scatter.index(k, 1 - self.scatter.c)
        return [
            remote(
                ref.at[index],
                self.scatter.from_core.at[k, :, at],
                self.core_send_sem.at[k * len(self.parts) + i],
                self.core_sem.at[k * len(self.parts) + i],
                self.scatter.other,
            )
            for i, (ref, at) in enumerate(self.parts)
        ]

    def load(self):
        for k in range(8):
            for copy in self.local(k):
                copy.start()

    def send(self):
        for k in range(8):
            for copy in self.to_core(k):
                copy.start()

    def both(self, k):
        for copy in self.local(k):
            copy.wait()
        for copy in self.to_core(k):
            copy.wait_recv()

    def finish(self):
        for k in range(8):
            for copy in self.to_core(k):
                copy.wait_send()


def scatter_kernel(amount, *refs):
    out_ref = refs[amount]
    scatter = Scatter(refs[amount + 1 : amount + 7], refs[amount + 7 : amount + 11])
    blocks = Blocks(scatter, refs[:amount], *refs[amount + 11 : amount + 14])
    (out_sem,) = refs[amount + 14 :]
    blocks.load()
    greet_line(scatter.z, (scatter.across, scatter.other), scatter.down, scatter.up)
    blocks.send()
    for i in range(4):
        blocks.both(i)
        scatter.side(i)
    for i in range(3):
        blocks.both(4 + i)
        scatter.line(i)
    blocks.both(7)
    scatter.last()
    outward = pltpu.make_async_copy(scatter.total, out_ref, out_sem.at[0])
    outward.start()
    blocks.finish()
    scatter.finish()
    outward.wait()


def contract(left, right, left_dim, right_dim):
    return lax.dot_general(
        left, right, (((left_dim,), (right_dim,)), ((), ())), preferred_element_type=jnp.float32
    )


def backward_kernel(
    unit_grads_ref, weights_ref, rows_ref, hidden_ref, out_ref, weight_grads_ref,
    held, from_core, from_across, from_below, from_above, total, send_sem, across_sem, below_sem, above_sem,
    core_send_sem, core_sem, local_sem, for_core, unit_grads, weights, rows, tile, tile_sem,
):
    scatter = Scatter(
        (held, from_core, from_across, from_below, from_above, total), (send_sem, across_sem, below_sem, above_sem)
    )
    block_rows, width = out_ref.shape
    blocks = rows.shape[1] // block_rows
    step = 3 * 256
    loads = [
        pltpu.make_async_copy(unit_grads_ref, unit_grads.at[pl.ds(0, 2)], local_sem.at[0]),
        pltpu.make_async_copy(weights_ref.at[pl.ds(0, 2)], weights, local_sem.at[1]),
        pltpu.make_async_copy(hidden_ref, unit_grads.at[2], local_sem.at[2]),
        pltpu.make_async_copy(rows_ref[0], rows.at[0], local_sem.at[3]),
        pltpu.make_async_copy(rows_ref[1], rows.at[1], local_sem.at[4]),
    ]
    for copy in loads:
        copy.start()
    greet_line(scatter.z, (scatter.across, scatter.other), scatter.down, scatter.up)
    loads[0].wait()
    loads[1].wait()

    def partial(j, core, target):
        spots = [pl.ds(pl.multiple_of(scatter.index(k, core) * block_rows, block_rows), block_rows) for k in (j, 4 + j)]

        def body(d, carry):
            at = pl.ds(pl.multiple_of(d * step, step), step)
            sums = None
            for i in range(2):
                left = jnp.concatenate([unit_grads[i, spot, :] for spot in spots], axis=0)
                part = contract(left, weights[i, at, :], 1, 1)
                sums = part if sums is None else sums + part
            sums = sums.astype(target.dtype)
            target[j, :, at] = sums[:block_rows]
            target[4 + j, :, at] = sums[block_rows:]
            return carry

        lax.fori_loop(0, width // step, body, 0)

    def to_core(k):
        return remote(for_core.at[k], from_core.at[k], core_send_sem.at[k], core_sem.at[k], scatter.other)

    tile_rows = tile.shape[2]

    def tile_out(u, i):
        return pltpu.make_async_copy(
            tile.at[u % 2, i], weight_grads_ref.at[i, pl.ds(u * tile_rows, tile_rows), :], tile_sem.at[u % 2, i]
        )

    def weight_tile(u):
        if u == 0:
            for copy in loads[2:]:
                copy.wait()
        if u >= 2:
            for i in range(3):
                tile_out(u - 2, i).wait()

        def body(i, carry):
            left = rows[i // 2, :, pl.ds(u * tile_rows, tile_rows)]
            tile[u % 2, i] = contract(left, unit_grads[i], 0, 0).astype(tile.dtype)
            return carry

        lax.fori_loop(0, 3, body, 0)
        for i in range(3):
            tile_out(u, i).start()

    for j in range(4):
        partial(j, 1 - scatter.c, for_core)
        to_core(j).start()
        to_core(4 + j).start()
        partial(j, scatter.c, held)
        to_core(j).wait_recv()
        scatter.side(j)
        if j == 1:
            weight_tile(0)
    weight_tile(1)
    for i in range(3):
        to_core(4 + i).wait_recv()
        scatter.line(i)
        weight_tile(2 + i)
    weight_tile(5)
    to_core(7).wait_recv()
    scatter.last()
    outward = pltpu.make_async_copy(total, out_ref, local_sem.at[5])
    outward.start()
    for k in range(8):
        to_core(k).wait_send()
    scatter.finish()
    for u in (4, 5):
        for i in range(3):
            tile_out(u, i).wait()
    outward.wait()


def scatter_fsdp(parts, collective_id):
    size, rows, _ = parts[0].shape
    columns = sum(part.shape[2] for part in parts)
    if size != KERNEL_FSDP:
        return lax.psum_scatter(
            jnp.concatenate(parts, axis=2), "fsdp", scatter_dimension=0, tiled=False
        ).astype(jnp.float32)
    block, amount = (rows, columns), len(parts)
    return scratch_call(
        functools.partial(scatter_kernel, amount),
        jax.ShapeDtypeStruct(block, jnp.float32),
        [
            *Scatter.scratch(block, parts[0].dtype),
            *[pltpu.SemaphoreType.DMA((8 * amount,)) for _ in range(3)],
            pltpu.SemaphoreType.DMA((1,)),
        ],
        collective_id,
        *parts,
    )


def feed_backward(gate_grad, up_grad, feed_full, feed_input, feed_grad_rows, hidden, collective_id):
    size = lax.axis_size("fsdp")
    kind = hidden.dtype
    tokens, width = feed_input.shape
    if size != KERNEL_FSDP:
        sums = contract(gate_grad, feed_full[0], 1, 1) + contract(up_grad, feed_full[1], 1, 1)
        return (
            scatter_fsdp((sums.astype(kind).reshape(size, tokens // size, width),), collective_id),
            jnp.stack(
                [
                    contract(left, right, 0, 0).astype(kind)
                    for left, right in ((feed_input, gate_grad), (feed_input, up_grad), (feed_grad_rows, hidden))
                ]
            ),
        )
    block, units = (tokens // size, width), hidden.shape[1]
    tile_rows = width // 6

    def kernel(unit_grads_ref, weights_ref, input_ref, grad_ref, hidden_ref, *refs):
        backward_kernel(unit_grads_ref, weights_ref, (input_ref, grad_ref), hidden_ref, *refs)

    rows_grad, weight_grads = scratch_call(
        kernel,
        (jax.ShapeDtypeStruct(block, jnp.float32), jax.ShapeDtypeStruct((3, width, units), kind)),
        [
            *Scatter.scratch(block, kind),
            pltpu.SemaphoreType.DMA((8,)),
            pltpu.SemaphoreType.DMA((8,)),
            pltpu.SemaphoreType.DMA((6,)),
            pltpu.VMEM((8,) + block, kind),
            pltpu.VMEM((3, tokens, units), kind),
            pltpu.VMEM((2, width, units), kind),
            pltpu.VMEM((2, tokens, width), kind),
            pltpu.VMEM((2, 3, tile_rows, units), kind),
            pltpu.SemaphoreType.DMA((2, 3)),
        ],
        collective_id,
        jnp.stack([gate_grad, up_grad]),
        feed_full,
        feed_input,
        feed_grad_rows,
        hidden,
    )
    return rows_grad, weight_grads


def exchange_kernel(block_ref, out_ref, send_sem, receive_sem):
    index, t = lax.axis_index("fsdp"), lax.axis_index("tp")
    partner = (index, 1 - t)
    greet((partner,))
    copy = remote(block_ref, out_ref, send_sem.at[0], receive_sem.at[0], partner)
    copy.start()
    copy.wait()


def exchange_tp(block, collective_id):
    if lax.axis_size("fsdp") != KERNEL_FSDP:
        return lax.ppermute(block, "tp", [(0, 1), (1, 0)])
    return scratch_call(
        exchange_kernel,
        jax.ShapeDtypeStruct(block.shape, block.dtype),
        [pltpu.SemaphoreType.DMA((1,)), pltpu.SemaphoreType.DMA((1,))],
        collective_id,
        block,
    )


def peer(z, x, c, k):
    kz, kx, kc = k // 4, (k // 2) % 2, k % 2
    high, low = z // 2, z % 2
    high = 1 - high if kz // 2 else high
    low = 1 - low if kz % 2 else low
    return fsdp_index(high * 2 + low, 1 - x if kx else x, 1 - c if kc else c)


MAIN = 2 * LANES
REST = LANES
FIRST_REST = KERNEL_FSDP * MAIN
UNITS = 2 * MAIN + REST


def main_of(owner):
    return pl.ds(pl.multiple_of(owner * MAIN, MAIN), MAIN)


def rest_of(z):
    return pl.ds(pl.multiple_of(FIRST_REST + z * REST, REST), REST)


def distribute_kernel(
    rows_ref, query_ref, key_ref, value_ref, output_ref, gain_ref, gate_ref, up_ref, down_ref,
    attention_ref, partner_ref, feed_ref,
    stage, feed, zeros,
    gather_send, gather_receive, local_sem, pair_rows_sem, send_sem, receive_sem, rest_send, rest_receive,
    on_send, on_receive, rest_on_send, rest_on_receive,
):
    z, x, c, t = place()
    own = fsdp_index(z, x, c)
    partner = (own, 1 - t)
    greet([(peer(z, x, c, k), t) for k in range(1, 16)] + [partner])
    rows_copy = remote(rows_ref, partner_ref, pair_rows_sem.at[0], pair_rows_sem.at[1], partner)
    rows_copy.start()
    loads, start = [], 0
    for i, ref in enumerate((query_ref, key_ref, value_ref, output_ref, gain_ref)):
        loads.append(pltpu.make_async_copy(ref, stage.at[:, pl.ds(start, ref.shape[1])], local_sem.at[i]))
        start += ref.shape[1]
    feed_loads = [
        pltpu.make_async_copy(ref, feed.at[i], local_sem.at[5 + i])
        for i, ref in enumerate((gate_ref, up_ref, down_ref))
    ]
    for copy in loads + feed_loads:
        copy.start()
    for copy in loads:
        copy.wait()
    gather = Gather(stage, attention_ref, gather_send, gather_receive)
    gather.start()
    keep = pltpu.make_async_copy(stage, attention_ref.at[own], local_sem.at[8])
    keep.start()
    for copy in feed_loads:
        copy.wait()

    def main_at(half, source):
        return feed_ref.at[:, source, :, pl.ds(pl.multiple_of(half * MAIN, MAIN), MAIN)]

    def rest_at(source):
        return feed_ref.at[:, source, :, pl.ds(2 * MAIN, REST)]

    takes_rest = (c == 0) & (x == t)

    def direct(k):
        to = peer(z, x, c, k)
        return remote(feed.at[:, :, main_of(to)], main_at(t, own), send_sem.at[k], receive_sem.at[k], (to, t))

    def rest(dz):
        to_z = peer(z, x, c, 4 * dz) // 4
        slot = 4 * dz + 2 * ((x + t) % 2) + c
        return remote(
            feed.at[:, :, rest_of(to_z)], rest_at(own), rest_send.at[dz], rest_receive.at[slot], (fsdp_index(to_z, t, 0), t)
        )

    def onward(k):
        at = main_at(t, peer(z, x, c, k))
        return remote(at if k else feed.at[:, :, main_of(own)], at, on_send.at[k], on_receive.at[k], partner)

    def rest_onward(k):
        at = rest_at(peer(z, x, c, k))
        return remote(at if k else feed.at[:, :, rest_of(z)], at, rest_on_send.at[k], rest_on_receive.at[k], partner)

    def send(dz):
        for k in range(4 * dz, 4 * dz + 4):
            if k:
                direct(k).start()
        if dz:
            rest(dz).start()
        else:

            @pl.when(jnp.logical_not(takes_rest))
            def _():
                rest(0).start()

    def pass_on(dz):
        for k in range(4 * dz, 4 * dz + 4):
            if k:
                direct(k).wait_recv()
            onward(k).start()

        @pl.when(takes_rest)
        def _():
            for k in range(4 * dz, 4 * dz + 4):
                if k:
                    remote(
                        feed.at[:, :, rest_of(0)], rest_at(own), rest_send.at[0], rest_receive.at[k], partner
                    ).wait_recv()
                rest_onward(k).start()

    send(0)
    send(1)
    keep_main = pltpu.make_async_copy(feed.at[:, :, main_of(own)], main_at(t, own), local_sem.at[9])
    keep_main.start()
    keep_rest = pltpu.make_async_copy(feed.at[:, :, rest_of(z)], rest_at(own), local_sem.at[10])

    @pl.when(takes_rest)
    def _():
        keep_rest.start()

    fills = [
        pltpu.make_async_copy(zeros, feed_ref.at[i, :, :, pl.ds(2 * MAIN, REST)], local_sem.at[11 + i])
        for i in range(3)
    ]

    @pl.when(c == 1)
    def _():
        zeros[...] = jnp.zeros_like(zeros)
        for copy in fills:
            copy.start()

    send(2)
    pass_on(0)
    pass_on(1)
    gather.line(1)
    gather.side(0)
    send(3)
    gather.line(2)
    gather.side(1)
    pass_on(2)
    gather.line(3)
    gather.side(2)
    pass_on(3)
    gather.side(3)
    gather.finish()
    rows_copy.wait()
    for k in range(16):
        onward(k).wait_recv()
        onward(k).wait_send()
        if k:
            direct(k).wait_send()

    @pl.when(jnp.logical_not(takes_rest))
    def _():
        rest(0).wait_send()

    for dz in (1, 2, 3):
        rest(dz).wait_send()

    @pl.when(takes_rest)
    def _():
        for k in range(16):
            rest_onward(k).wait_send()
        keep_rest.wait()

    @pl.when((c == 0) & (x != t))
    def _():
        for k in range(16):
            rest_onward(k).wait_recv()

    @pl.when(c == 1)
    def _():
        for copy in fills:
            copy.wait()

    keep.wait()
    keep_main.wait()


def distribute(rows, attention, gain_columns, feed, collective_id):
    size = lax.axis_size("fsdp")
    shard_rows, feed_width = feed[0].shape
    columns = sum(w.shape[1] for w in attention) + gain_columns.shape[1]
    if size != KERNEL_FSDP:
        halves = lax.all_to_all(pack_units(feed, size), "fsdp", split_axis=0, concat_axis=0, tiled=True)
        halves = lax.all_gather(halves, "tp", axis=0)
        halves = halves.reshape(halves.shape[0], size * shard_rows, halves.shape[-1])
        return (
            lax.all_gather(jnp.concatenate((*attention, gain_columns), axis=1), "fsdp", axis=0),
            lax.ppermute(rows, "tp", [(0, 1), (1, 0)]),
            jnp.stack(join_units(halves, feed_width, size, 3)),
        )
    kind = rows.dtype
    attention_full, partner_rows, feed_full = scratch_call(
        distribute_kernel,
        (
            jax.ShapeDtypeStruct((size, shard_rows, columns), kind),
            jax.ShapeDtypeStruct(rows.shape, kind),
            jax.ShapeDtypeStruct((3, size, shard_rows, UNITS), kind),
        ),
        [
            pltpu.VMEM((shard_rows, columns), kind),
            pltpu.VMEM((3, shard_rows, feed_width), kind),
            pltpu.VMEM((size, shard_rows, REST), kind),
            pltpu.SemaphoreType.DMA((Gather.slots,)),
            pltpu.SemaphoreType.DMA((size,)),
            pltpu.SemaphoreType.DMA((14,)),
            pltpu.SemaphoreType.DMA((2,)),
            pltpu.SemaphoreType.DMA((size,)),
            pltpu.SemaphoreType.DMA((size,)),
            pltpu.SemaphoreType.DMA((4,)),
            pltpu.SemaphoreType.DMA((size,)),
            pltpu.SemaphoreType.DMA((size,)),
            pltpu.SemaphoreType.DMA((size,)),
            pltpu.SemaphoreType.DMA((size,)),
            pltpu.SemaphoreType.DMA((size,)),
        ],
        collective_id,
        rows,
        *attention,
        gain_columns,
        *feed,
    )
    return attention_full, partner_rows, feed_full.reshape(3, size * shard_rows, UNITS)


def collect_kernel(
    parts_ref, projected_ref, output_ref, gain_ref, out_ref, attention_ref,
    held, received, rest_held, rest_received,
    local_sem, pair_send, pair_receive, rest_pair_send, rest_pair_receive, send_sem, receive_sem, rest_send, rest_receive,
    *scatter_refs,
):
    scatter = Scatter(scatter_refs[:6], scatter_refs[6:10])
    blocks = Blocks(scatter, (projected_ref, output_ref, gain_ref), *scatter_refs[10:13])
    blocks.load()
    z, x, c, t = place()
    own = fsdp_index(z, x, c)
    rows = out_ref.shape[1]
    partner = (own, 1 - t)
    parts = [parts_ref.at[i] for i in range(3)]
    order = (3, 2, 1, 0)
    takes_rest = (c == 0) & (x == t)
    gives_rest = (c == 0) & (x != t)

    def plane(dz):
        return pl.ds(peer(z, x, c, 4 * dz) // 4 * 4, 4)

    def half(which):
        return pl.ds(pl.multiple_of(which * MAIN, MAIN), MAIN)

    rest_columns = pl.ds(2 * MAIN, REST)

    def load(dz, i):
        return pltpu.make_async_copy(parts[i].at[plane(dz), :, half(t)], held.at[dz, i], local_sem.at[3 * dz + i])

    def rest_load(dz, i):
        return pltpu.make_async_copy(
            parts[i].at[plane(dz), :, rest_columns], rest_held.at[dz, i], local_sem.at[12 + 3 * dz + i]
        )

    def pair(dz, i):
        slot = 3 * dz + i
        return remote(
            parts[i].at[plane(dz), :, half(1 - t)], received.at[dz, i], pair_send.at[slot], pair_receive.at[slot], partner
        )

    def rest_pair(dz, i):
        slot = 3 * dz + i
        return remote(
            parts[i].at[plane(dz), :, rest_columns],
            rest_received.at[dz, i],
            rest_pair_send.at[slot],
            rest_pair_receive.at[slot],
            partner,
        )

    def spot(k):
        return peer(z, x, c, k) % 4

    def direct(k):
        return remote(
            held.at[k // 4, :, spot(k)], out_ref.at[:, :, main_of(own)], send_sem.at[k], receive_sem.at[k], (peer(z, x, c, k), t)
        )

    def rest_direct(k):
        return remote(
            rest_held.at[k // 4, :, spot(k)],
            out_ref.at[:, :, rest_of(z)],
            rest_send.at[k],
            rest_receive.at[z],
            (peer(z, x, c, k), t),
        )

    def add(target, source):
        def body(j, carry):
            i, at = j // 4, j % 4
            total = target[i, at].astype(jnp.float32) + source[i, at].astype(jnp.float32)
            target[i, at] = total.astype(target.dtype)
            return carry

        lax.fori_loop(0, 12, body, 0)

    for dz in order:
        for i in range(3):
            load(dz, i).start()

    @pl.when(takes_rest)
    def _():
        for dz in order:
            for i in range(3):
                rest_load(dz, i).start()

    greet([(peer(z, x, c, k), t) for k in range(1, 16)] + [partner])
    blocks.send()
    for dz in order:
        for i in range(3):
            pair(dz, i).start()

        @pl.when(gives_rest)
        def _():
            for i in range(3):
                rest_pair(dz, i).start()

    def pass_on(dz):
        for i in range(3):
            load(dz, i).wait()
            pair(dz, i).wait_recv()
        add(held.at[dz], received.at[dz])
        for k in range(4 * dz, 4 * dz + 4):
            if k:
                direct(k).start()

        @pl.when(takes_rest)
        def _():
            for i in range(3):
                rest_load(dz, i).wait()
                rest_pair(dz, i).wait_recv()
            add(rest_held.at[dz], rest_received.at[dz])
            for k in range(4 * dz, 4 * dz + 4):
                if k:
                    rest_direct(k).start()

    def line(i):
        blocks.both(4 + i)
        scatter.line(i)

    for i in range(4):
        blocks.both(i)
        scatter.side(i)
    pass_on(3)
    line(0)
    pass_on(2)
    line(1)
    pass_on(1)
    line(2)
    pass_on(0)
    blocks.both(7)
    scatter.last()
    outward = pltpu.make_async_copy(scatter.total, attention_ref, local_sem.at[26])
    outward.start()
    keep = pltpu.make_async_copy(held.at[0, :, spot(0)], out_ref.at[:, :, main_of(own)], local_sem.at[24])
    keep.start()
    keep_rest = pltpu.make_async_copy(rest_held.at[0, :, spot(0)], out_ref.at[:, :, rest_of(z)], local_sem.at[25])

    @pl.when(takes_rest)
    def _():
        keep_rest.start()

    for k in range(1, 16):
        direct(k).wait_recv()

    for dz in range(4):
        from_z = peer(z, x, c, 4 * dz) // 4

        def arrived():
            remote(
                rest_held.at[0, :, 0], out_ref.at[:, :, rest_of(from_z)], rest_send.at[0], rest_receive.at[from_z], partner
            ).wait_recv()

        if dz:
            arrived()
        else:

            @pl.when(jnp.logical_not(takes_rest))
            def _():
                arrived()

    for k in range(1, 16):
        direct(k).wait_send()
    for dz in order:
        for i in range(3):
            pair(dz, i).wait_send()

    @pl.when(gives_rest)
    def _():
        for dz in order:
            for i in range(3):
                rest_pair(dz, i).wait_send()

    @pl.when(takes_rest)
    def _():
        for k in range(1, 16):
            rest_direct(k).wait_send()
        keep_rest.wait()

    blocks.finish()
    scatter.finish()
    keep.wait()
    outward.wait()


def collect(gradients, feed_width, attention_parts, collective_id):
    size, pairs = lax.axis_size("fsdp"), lax.axis_size("tp")
    shard_rows = gradients.shape[1] // size
    if size != KERNEL_FSDP:
        packed = part_units([gradients[i] for i in range(3)], feed_width, size, pairs)
        mine = lax.psum_scatter(packed, "tp", scatter_dimension=0, tiled=False)
        mine = mine.reshape(size, shard_rows, mine.shape[-1])
        mine = lax.all_to_all(mine, "fsdp", split_axis=0, concat_axis=0, tiled=True)
        feed = [g.astype(jnp.float32) for g in unpack_units(mine, feed_width, 3)]
        return feed, scatter_fsdp(attention_parts, collective_id)
    kind = gradients.dtype
    main, rest = (4, 3, 4, shard_rows, MAIN), (4, 3, 4, shard_rows, REST)
    block = (shard_rows, sum(part.shape[2] for part in attention_parts))
    out, attention = scratch_call(
        collect_kernel,
        (
            jax.ShapeDtypeStruct((3, shard_rows, feed_width), kind),
            jax.ShapeDtypeStruct(block, jnp.float32),
        ),
        [
            pltpu.VMEM(main, kind),
            pltpu.VMEM(main, kind),
            pltpu.VMEM(rest, kind),
            pltpu.VMEM(rest, kind),
            pltpu.SemaphoreType.DMA((27,)),
            pltpu.SemaphoreType.DMA((12,)),
            pltpu.SemaphoreType.DMA((12,)),
            pltpu.SemaphoreType.DMA((12,)),
            pltpu.SemaphoreType.DMA((12,)),
            pltpu.SemaphoreType.DMA((size,)),
            pltpu.SemaphoreType.DMA((size,)),
            pltpu.SemaphoreType.DMA((size,)),
            pltpu.SemaphoreType.DMA((4,)),
            *Scatter.scratch(block, kind),
            *[pltpu.SemaphoreType.DMA((24,)) for _ in range(3)],
        ],
        collective_id,
        gradients.reshape(3, size, shard_rows, UNITS),
        *attention_parts,
    )
    return [out[i].astype(jnp.float32) for i in range(3)], attention


def contract_last(left_rows, right_rows):
    return lax.dot_general(
        left_rows, right_rows, (((1,), (1,)), ((), ())), preferred_element_type=jnp.float32
    )


def contract_first(left_rows, right_rows):
    return lax.dot_general(
        left_rows, right_rows, (((0,), (0,)), ((), ())), preferred_element_type=jnp.float32
    )


def normalize_parts(value_rows):
    inverse = lax.rsqrt(jnp.mean(value_rows * value_rows, axis=-1, keepdims=True) + EPSILON)
    return (value_rows * inverse, inverse)


def norm_backward(unit_rows, inverse, norm_gain, upstream):
    scaled = upstream * norm_gain
    return inverse * (scaled - unit_rows * jnp.mean(scaled * unit_rows, axis=-1, keepdims=True))


def layout(lengths_row, row_index):
    segment_ends = jnp.cumsum(lengths_row)
    segment_starts = segment_ends - lengths_row
    segment = jnp.sum((row_index[:, None] >= segment_ends[None, :]).astype(jnp.int32), axis=1)
    onehot = segment[:, None] == jnp.arange(lengths_row.shape[0], dtype=jnp.int32)[None, :]
    segment_begin = jnp.sum(jnp.where(onehot, segment_starts[None, :], 0), axis=1)
    prompt_shift = jnp.where(segment > 0, lengths_row[0], 0)
    return (segment, row_index - segment_begin + prompt_shift)


def rotary_tables(position):
    frequency = jnp.exp(
        jnp.arange(HEAD_SIZE // 2, dtype=jnp.float32) * (-2.0 * math.log(10000.0) / HEAD_SIZE)
    )
    angles = position.astype(jnp.float32)[:, None] * frequency[None, :]
    return (jnp.cos(angles), jnp.sin(angles))


def apply_rotary(value_rows, cosine_lookup, sine_lookup):
    half_width = value_rows.shape[-1] // 2
    first_half = value_rows[..., :half_width]
    second_half = value_rows[..., half_width:]
    cosine_part = cosine_lookup[:, None, :]
    sine_part = sine_lookup[:, None, :]
    return jnp.concatenate(
        [
            first_half * cosine_part - second_half * sine_part,
            second_half * cosine_part + first_half * sine_part,
        ],
        axis=-1,
    )


def unrotate(value_rows, cosine_lookup, sine_lookup):
    half_width = value_rows.shape[-1] // 2
    first_half = value_rows[..., :half_width]
    second_half = value_rows[..., half_width:]
    cosine_part = cosine_lookup[:, None, :]
    sine_part = sine_lookup[:, None, :]
    return jnp.concatenate(
        [
            first_half * cosine_part + second_half * sine_part,
            second_half * cosine_part - first_half * sine_part,
        ],
        axis=-1,
    )


def visible(segment, row_index):
    same_segment = (segment[:, None] == segment[None, :]) & (
        row_index[None, :] <= row_index[:, None]
    )
    from_prompt = (segment[None, :] == 0) & (segment[:, None] > 0)
    return same_segment | from_prompt


def masked_scores(rotated_query, rotated_key, visible_mask):
    raw_scores = jnp.einsum(
        "qgrd,kgd->grqk", rotated_query, rotated_key, preferred_element_type=jnp.float32
    )
    tanh_value = jnp.tanh(raw_scores * HEAD_SIZE ** (-0.5) / SOFTCAP)
    return (jnp.where(visible_mask[None, None], SOFTCAP * tanh_value, NEGATIVE), tanh_value)


def gelu_product(gate_value, up_value):
    return jax.nn.gelu(gate_value, approximate=True) * up_value


def split_columns(width, size):
    main = width // size // LANES * LANES
    return main, width // size - main


def pack_units(weights, size):
    rows, width = weights[0].shape
    main, rest = split_columns(width, size)
    pieces = []
    if main:
        pieces += [
            jnp.transpose(w[:, : main * size].reshape(rows, size, main), (1, 0, 2)) for w in weights
        ]
    if rest:
        pieces += [
            jnp.transpose(w[:, main * size :].reshape(rows, size, rest), (1, 0, 2)) for w in weights
        ]
    packed = jnp.concatenate(pieces, axis=2)
    return jnp.pad(packed, ((0, 0), (0, 0), (0, -packed.shape[2] % LANES)))


def unpack_units(packed, width, amount):
    size, rows, _ = packed.shape
    main, rest = split_columns(width, size)
    arrays = []
    for i in range(amount):
        pieces = []
        if main:
            piece = packed[:, :, i * main : (i + 1) * main]
            pieces.append(jnp.transpose(piece, (1, 0, 2)).reshape(rows, size * main))
        if rest:
            start = amount * main + i * rest
            piece = packed[:, :, start : start + rest]
            pieces.append(jnp.transpose(piece, (1, 0, 2)).reshape(rows, size * rest))
        arrays.append(jnp.concatenate(pieces, axis=1))
    return arrays


def join_units(halves, width, size, amount):
    main, rest = split_columns(width, size)
    arrays = []
    for i in range(amount):
        start = amount * main + i * rest
        pieces = [half[:, i * main : (i + 1) * main] for half in halves]
        pieces += [half[:, start : start + rest] for half in halves]
        joined = jnp.concatenate(pieces, axis=1)
        arrays.append(jnp.pad(joined, ((0, 0), (0, -joined.shape[1] % LANES))))
    return arrays


def part_units(arrays, width, size, pairs):
    main, rest = split_columns(width, size)
    halves = []
    for t in range(pairs):
        pieces = [array[:, t * main : (t + 1) * main] for array in arrays]
        start = pairs * main + t * rest
        pieces += [array[:, start : start + rest] for array in arrays]
        packed = jnp.concatenate(pieces, axis=1)
        halves.append(jnp.pad(packed, ((0, 0), (0, -packed.shape[1] % LANES))))
    return jnp.stack(halves)


def shards(
    block_input,
    lengths,
    attention_norm_gain,
    attention_post_gain,
    feedforward_norm_gain,
    feedforward_post_gain,
    query_weight,
    key_weight,
    value_weight,
    output_weight,
    gate_weight,
    up_weight,
    down_weight,
    output_cotangent,
):
    low = jnp.bfloat16
    size, pairs = lax.axis_size("fsdp"), lax.axis_size("tp")
    rows_local, width = block_input.shape
    shard_rows, feed_width = gate_weight.shape
    query_width, key_width = query_weight.shape[1], key_weight.shape[1]
    output_start = query_width + 2 * key_width
    gain_start = output_start + query_width
    grouped_rows = rows_local * pairs

    gain_columns = jnp.stack(
        [attention_norm_gain, attention_post_gain, feedforward_norm_gain, feedforward_post_gain],
        axis=1,
    )
    attention_full, other_input, feed_full = distribute(
        block_input,
        (query_weight, key_weight, value_weight, output_weight),
        jnp.pad(gain_columns, ((0, 0), (0, LANES - 4))),
        (gate_weight, up_weight, down_weight),
        1,
    )
    attention_full = attention_full.reshape(size * shard_rows, gain_start + LANES)
    gains = jnp.transpose(attention_full[:, gain_start : gain_start + 4]).astype(jnp.float32)
    gain_one, gain_two, gain_three, gain_four = gains[0], gains[1], gains[2], gains[3]
    gate_full, up_full, down_full = feed_full[0], feed_full[1], feed_full[2]

    row_index = (
        jnp.arange(grouped_rows, dtype=jnp.int32) + lax.axis_index("tp") * rows_local
    ) % grouped_rows
    segment, position = layout(lengths[0], row_index)
    cosine_lookup, sine_lookup = rotary_tables(position)
    visible_mask = visible(segment, row_index)
    residual_both = jnp.concatenate([block_input, other_input], axis=0).astype(jnp.float32)
    unit_one_both, inverse_one_both = normalize_parts(residual_both)
    residual = residual_both[:rows_local]
    unit_one, inverse_one = unit_one_both[:rows_local], inverse_one_both[:rows_local]
    normed = (unit_one_both * gain_one).astype(low)
    projected = jnp.dot(
        normed, attention_full[:, :output_start], preferred_element_type=jnp.float32
    )
    query_raw = projected[:, :query_width]
    key_raw = projected[:, query_width : query_width + key_width]
    value_raw = projected[:, query_width + key_width :]
    heads_local = query_width // HEAD_SIZE
    kv_local = key_width // HEAD_SIZE
    repeat_heads = heads_local // kv_local
    rotated_query = apply_rotary(
        query_raw.reshape(grouped_rows, heads_local, HEAD_SIZE), cosine_lookup, sine_lookup
    ).astype(low)
    rotated_query = rotated_query.reshape(grouped_rows, kv_local, repeat_heads, HEAD_SIZE)
    rotated_key = apply_rotary(
        key_raw.reshape(grouped_rows, kv_local, HEAD_SIZE), cosine_lookup, sine_lookup
    ).astype(low)
    value_reduced = value_raw.astype(low).reshape(grouped_rows, kv_local, HEAD_SIZE)
    capped, tanh_value = masked_scores(rotated_query, rotated_key, visible_mask)
    row_peak = jnp.max(capped, axis=-1, keepdims=True)
    exponentials = jnp.exp(capped - row_peak)
    softmax_probs = exponentials / jnp.sum(exponentials, axis=-1, keepdims=True)
    probs_low = softmax_probs.astype(low)
    mixed_heads = jnp.einsum(
        "grqk,kgd->qgrd", probs_low, value_reduced, preferred_element_type=jnp.float32
    )
    attended = mixed_heads.reshape(grouped_rows, heads_local * HEAD_SIZE).astype(low)
    output_full = attention_full[:, output_start:gain_start]
    branch_parts = contract_last(attended, output_full)
    branch_one = branch_parts[:rows_local] + exchange_tp(
        branch_parts[rows_local:].astype(low), 4
    ).astype(jnp.float32)
    unit_two, inverse_two = normalize_parts(branch_one)
    middle = residual + unit_two * gain_two
    unit_three, inverse_three = normalize_parts(middle)

    feed_input = gather_fsdp((unit_three * gain_three).astype(low), 5).reshape(-1, width)
    gate_value = jnp.dot(feed_input, gate_full, preferred_element_type=jnp.float32)
    up_value = jnp.dot(feed_input, up_full, preferred_element_type=jnp.float32)
    hidden = gelu_product(gate_value, up_value).astype(low)
    branch_two = scatter_fsdp(
        (contract_last(hidden, down_full).astype(low).reshape(size, rows_local, width),), 6
    )
    unit_four, inverse_four = normalize_parts(branch_two)
    block_output = (middle + unit_four * gain_four).astype(low)
    upstream = output_cotangent.astype(jnp.float32)
    gain_four_grad = jnp.sum(upstream * unit_four, axis=0)
    branch_two_grad = norm_backward(unit_four, inverse_four, gain_four, upstream).astype(low)
    feed_grad_rows = gather_fsdp(branch_two_grad, 7).reshape(-1, width)
    hidden_grad = jnp.dot(feed_grad_rows, down_full, preferred_element_type=jnp.float32)
    unused_out, pullback = jax.vjp(gelu_product, gate_value, up_value)
    gate_grad, up_grad = pullback(hidden_grad)
    gate_grad, up_grad = gate_grad.astype(low), up_grad.astype(low)
    normed_three_grad, feed_grads = feed_backward(
        gate_grad, up_grad, feed_full, feed_input, feed_grad_rows, hidden, 8
    )
    gain_three_grad = jnp.sum(normed_three_grad * unit_three, axis=0)
    middle_grad = upstream + norm_backward(unit_three, inverse_three, gain_three, normed_three_grad)
    gain_two_grad = jnp.sum(middle_grad * unit_two, axis=0)
    branch_one_grad = norm_backward(unit_two, inverse_two, gain_two, middle_grad).astype(low)
    attention_grad_rows = jnp.concatenate(
        [branch_one_grad, exchange_tp(branch_one_grad, 10)], axis=0
    )
    mixed_grad = jnp.dot(
        attention_grad_rows, output_full, preferred_element_type=jnp.float32
    ).astype(low)
    mixed_grad = mixed_grad.reshape(grouped_rows, kv_local, repeat_heads, HEAD_SIZE)
    value_grad = jnp.einsum(
        "grqk,qgrd->kgd", probs_low, mixed_grad, preferred_element_type=jnp.float32
    )
    probs_grad = jnp.einsum(
        "qgrd,kgd->grqk", mixed_grad, value_reduced, preferred_element_type=jnp.float32
    )
    score_grad = softmax_probs * (
        probs_grad - jnp.sum(softmax_probs * probs_grad, axis=-1, keepdims=True)
    )
    raw_grad = (score_grad * (1.0 - tanh_value * tanh_value) * HEAD_SIZE ** (-0.5)).astype(low)
    query_grad = jnp.einsum(
        "grqk,kgd->qgrd", raw_grad, rotated_key, preferred_element_type=jnp.float32
    )
    key_grad = jnp.einsum(
        "grqk,qgrd->kgd", raw_grad, rotated_query, preferred_element_type=jnp.float32
    )
    query_grad = unrotate(
        query_grad.reshape(grouped_rows, heads_local, HEAD_SIZE), cosine_lookup, sine_lookup
    )
    key_grad = unrotate(key_grad, cosine_lookup, sine_lookup)
    projected_grad = jnp.concatenate(
        [
            query_grad.reshape(grouped_rows, heads_local * HEAD_SIZE).astype(low),
            key_grad.reshape(grouped_rows, kv_local * HEAD_SIZE).astype(low),
            value_grad.reshape(grouped_rows, kv_local * HEAD_SIZE).astype(low),
        ],
        axis=1,
    )
    input_parts = contract_last(projected_grad, attention_full[:, :output_start])

    gain_grads = jnp.stack(
        [
            jnp.sum(input_parts * unit_one_both, axis=0),
            gain_two_grad,
            gain_three_grad,
            gain_four_grad,
        ]
    )
    sent = jnp.concatenate(
        [input_parts[rows_local:].astype(low), jnp.pad(gain_grads, ((0, 12), (0, 0))).astype(low)]
    )
    received = exchange_tp(sent, 11).astype(jnp.float32)
    normed_one_grad = input_parts[:rows_local] + received[:rows_local]
    gain_grads = gain_grads + received[rows_local : rows_local + 4]
    input_gradient = middle_grad + norm_backward(unit_one, inverse_one, gain_one, normed_one_grad)

    (gate_weight_grad, up_weight_grad, down_weight_grad), attention_grads = collect(
        feed_grads,
        feed_width,
        [
            part.astype(low).reshape(size, shard_rows, part.shape[1])
            for part in (
                contract_first(normed, projected_grad),
                contract_first(attention_grad_rows, attended),
                jnp.pad(jnp.transpose(gain_grads), ((0, 0), (0, LANES - 4))),
            )
        ],
        9,
    )
    gain_shards = jnp.transpose(attention_grads[:, gain_start : gain_start + 4])
    return (
        block_output,
        input_gradient,
        gain_shards[0],
        gain_shards[1],
        gain_shards[2],
        gain_shards[3],
        attention_grads[:, :query_width],
        attention_grads[:, query_width : query_width + key_width],
        attention_grads[:, query_width + key_width : output_start],
        attention_grads[:, output_start:gain_start],
        gate_weight_grad,
        up_weight_grad,
        down_weight_grad,
    )


def solution(mesh):
    placed = (
        P(("fsdp", "tp"), None),
        P("fsdp", None),
        P("fsdp"),
        P("fsdp"),
        P("fsdp"),
        P("fsdp"),
        P("fsdp", "tp"),
        P("fsdp", "tp"),
        P("fsdp", "tp"),
        P("fsdp", "tp"),
        P("fsdp", "tp"),
        P("fsdp", "tp"),
        P("fsdp", "tp"),
        P(("fsdp", "tp"), None),
    )
    return jax.shard_map(
        shards,
        mesh=mesh,
        in_specs=placed,
        out_specs=(
            P(("fsdp", "tp"), None),
            P(("fsdp", "tp"), None),
            P("fsdp"),
            P("fsdp"),
            P("fsdp"),
            P("fsdp"),
            P("fsdp", "tp"),
            P("fsdp", "tp"),
            P("fsdp", "tp"),
            P("fsdp", "tp"),
            P("fsdp", "tp"),
            P("fsdp", "tp"),
            P("fsdp", "tp"),
        ),
        check_vma=False,
    )
```

```python
import functools
import math

import jax
import jax.numpy as jnp
from jax import lax
from jax.experimental import pallas as pl
from jax.experimental.pallas import tpu as pltpu
from jax.sharding import PartitionSpec as P

HEAD_SIZE = 256
MESH = pl.DeviceIdType.MESH
ANY = pl.BlockSpec(memory_space=pl.ANY)
LANES = 128

EPSILON = 1e-06
SOFTCAP = 50.0
NEGATIVE = -1e30

KERNEL_FSDP = 16


def place():
    index = lax.axis_index("fsdp")
    return index // 4, (index // 2) % 2, index % 2, lax.axis_index("tp")


def fsdp_index(z, x, c):
    return (z * 2 + x) * 2 + c


def remote(source, target, send_sem, receive_sem, device):
    return pltpu.make_async_remote_copy(
        src_ref=source,
        dst_ref=target,
        send_sem=send_sem,
        recv_sem=receive_sem,
        device_id=device,
        device_id_type=MESH,
    )


def greet(devices):
    barrier = pltpu.get_barrier_semaphore()
    for device in devices:
        pl.semaphore_signal(barrier, inc=1, device_id=device, device_id_type=MESH)
    pl.semaphore_wait(barrier, len(devices))


def greet_line(z, devices, down, up):
    barrier = pltpu.get_barrier_semaphore()
    for device in devices:
        pl.semaphore_signal(barrier, inc=1, device_id=device, device_id_type=MESH)

    @pl.when(z > 0)
    def _():
        pl.semaphore_signal(barrier, inc=1, device_id=down, device_id_type=MESH)

    @pl.when(z < 3)
    def _():
        pl.semaphore_signal(barrier, inc=1, device_id=up, device_id_type=MESH)

    pl.semaphore_wait(barrier, len(devices) + (z + 2) // 3 + (5 - z) // 3)


def stage_through(source, stage, target, sems):
    inward = pltpu.make_async_copy(source, stage, sems.at[0])
    inward.start()

    def finish():
        inward.wait()
        outward = pltpu.make_async_copy(stage, target, sems.at[1])
        outward.start()
        return outward

    return finish


class Gather:
    slots = 29

    def __init__(self, block, out_ref, send_sem, receive_sem):
        self.block, self.out, self.send_sem, self.receive_sem = block, out_ref, send_sem, receive_sem
        self.z, self.x, self.c, t = place()
        z, x, c = self.z, self.x, self.c
        self.own = fsdp_index(z, x, c)
        self.down, self.up = (fsdp_index(z - 1, x, c), t), (fsdp_index(z + 1, x, c), t)
        self.across, self.other = (fsdp_index(z, 1 - x, c), t), (fsdp_index(z, x, 1 - c), t)

    def copy(self, source, index, slot, device):
        return remote(source, self.out.at[index], self.send_sem.at[slot], self.receive_sem.at[index], device)

    def relay(self, index, slot, device):
        self.copy(self.out.at[index], index, slot, device).start()

    def arrived(self, index):
        self.copy(self.block, index, 0, self.other).wait_recv()

    def sent(self, slot):
        self.copy(self.block, self.own, slot, self.other).wait_send()

    def start(self):
        @pl.when(self.z < 3)
        def _():
            self.copy(self.block, self.own, 0, self.up).start()

        @pl.when(self.z > 0)
        def _():
            self.copy(self.block, self.own, 1, self.down).start()

        self.copy(self.block, self.own, 2, self.across).start()
        self.copy(self.block, self.own, 3, self.other).start()

    def line(self, d):
        z, x, c = self.z, self.x, self.c

        @pl.when(z >= d)
        def _():
            index = fsdp_index(z - d, x, c)
            base = 4 + 3 * (d - 1)
            self.arrived(index)

            @pl.when(z < 3)
            def _():
                self.relay(index, base, self.up)

            self.relay(index, base + 1, self.across)
            self.relay(index, base + 2, self.other)

        @pl.when(z + d <= 3)
        def _():
            index = fsdp_index(z + d, x, c)
            base = 13 + 3 * (d - 1)
            self.arrived(index)

            @pl.when(z > 0)
            def _():
                self.relay(index, base, self.down)

            self.relay(index, base + 1, self.across)
            self.relay(index, base + 2, self.other)

    def side(self, d):
        z, x, c = self.z, self.x, self.c
        if d == 0:
            index = fsdp_index(z, 1 - x, c)
            self.arrived(index)
            self.relay(index, 22, self.other)
            return

        @pl.when(z >= d)
        def _():
            index = fsdp_index(z - d, 1 - x, c)
            self.arrived(index)
            self.relay(index, 22 + d, self.other)

        @pl.when(z + d <= 3)
        def _():
            index = fsdp_index(z + d, 1 - x, c)
            self.arrived(index)
            self.relay(index, 25 + d, self.other)

    def finish(self, waits=True):
        z = self.z
        if waits:
            for zi in range(4):
                for xi in range(2):
                    self.arrived(fsdp_index(zi, xi, 1 - self.c))

        @pl.when(z < 3)
        def _():
            self.sent(0)

        @pl.when(z > 0)
        def _():
            self.sent(1)

        for slot in (2, 3, 22):
            self.sent(slot)
        for d in (1, 2, 3):

            @pl.when(z >= d)
            def _():
                base = 4 + 3 * (d - 1)

                @pl.when(z < 3)
                def _():
                    self.sent(base)

                for slot in (base + 1, base + 2, 22 + d):
                    self.sent(slot)

            @pl.when(z + d <= 3)
            def _():
                base = 13 + 3 * (d - 1)

                @pl.when(z > 0)
                def _():
                    self.sent(base)

                for slot in (base + 1, base + 2, 25 + d):
                    self.sent(slot)


def gather_kernel(block_ref, out_ref, stage, send_sem, receive_sem, local_sem):
    gather = Gather(block_ref, out_ref, send_sem, receive_sem)
    greet_line(gather.z, (gather.across, gather.other), gather.down, gather.up)
    finish_own = stage_through(block_ref, stage, out_ref.at[gather.own], local_sem)
    gather.start()
    outward = finish_own()
    gather.line(1)
    gather.side(0)
    gather.line(2)
    gather.side(1)
    gather.line(3)
    gather.side(2)
    gather.side(3)
    gather.finish()
    outward.wait()


def scratch_call(kernel, outputs, scratch, collective_id, *operands):
    return pl.pallas_call(
        kernel,
        out_shape=outputs,
        in_specs=[ANY] * len(operands),
        out_specs=jax.tree.map(lambda _: ANY, outputs),
        scratch_shapes=scratch,
        compiler_params=pltpu.CompilerParams(
            collective_id=collective_id, has_side_effects=True, vmem_limit_bytes=60 * 1024 * 1024
        ),
    )(*operands)


def gather_fsdp(block, collective_id):
    size = lax.axis_size("fsdp")
    if size != KERNEL_FSDP:
        return lax.all_gather(block, "fsdp", axis=0)
    return scratch_call(
        gather_kernel,
        jax.ShapeDtypeStruct((size,) + block.shape, block.dtype),
        [
            pltpu.VMEM(block.shape, block.dtype),
            pltpu.SemaphoreType.DMA((29,)),
            pltpu.SemaphoreType.DMA((size,)),
            pltpu.SemaphoreType.DMA((2,)),
        ],
        collective_id,
        block,
    )


def add_rows(rows, step, target, *sources):
    def body(i, carry):
        at = pl.ds(pl.multiple_of(i * step, step), step)
        total = sources[0][at, :].astype(jnp.float32)
        for source in sources[1:]:
            total = total + source[at, :].astype(jnp.float32)
        target[at, :] = total.astype(target.dtype)
        return carry

    lax.fori_loop(0, rows // step, body, 0)


class Scatter:
    def __init__(self, buffers, semaphores):
        self.held, self.from_core, self.from_across, self.from_below, self.from_above, self.total = buffers
        self.send_sem, self.across_sem, self.below_sem, self.above_sem = semaphores
        self.z, self.x, self.c, t = place()
        z, x, c = self.z, self.x, self.c
        self.rows = self.total.shape[0]
        self.down, self.up = (fsdp_index(z - 1, x, c), t), (fsdp_index(z + 1, x, c), t)
        self.across, self.other = (fsdp_index(z, 1 - x, c), t), (fsdp_index(z, x, 1 - c), t)

    def target(self, i):
        if i == 3:
            return self.z
        half = self.z // 2
        mirrored = self.z + half * (3 - 2 * self.z)
        base = 3 - i - (i + mirrored) // 3
        return base + half * (3 - 2 * base)

    def index(self, k, core):
        return fsdp_index(self.target(k % 4), 1 - self.x if k < 4 else self.x, core)

    def add(self, target, *sources):
        add_rows(self.rows, 16, target, *sources)

    def over(self, i):
        return remote(
            self.held.at[i], self.from_across.at[i], self.send_sem.at[3 + i], self.across_sem.at[i], self.across
        )

    def going_up(self, i, target):
        return remote(
            self.held.at[4 + i], self.from_below.at[target], self.send_sem.at[i], self.below_sem.at[target], self.up
        )

    def going_down(self, i, target):
        return remote(
            self.held.at[4 + i], self.from_above.at[target], self.send_sem.at[i], self.above_sem.at[target], self.down
        )

    def side(self, i):
        self.add(self.held.at[i], self.held.at[i], self.from_core.at[i])
        self.over(i).start()

    def line(self, i):
        z, target = self.z, self.target(i)
        held = self.held.at[4 + i]
        sources = (held, self.from_core.at[4 + i], self.from_across.at[i])
        self.over(i).wait_recv()

        @pl.when(target > z)
        def _():
            @pl.when(z > 0)
            def _():
                self.going_up(i, target).wait_recv()
                self.add(held, *sources, self.from_below.at[target])

            @pl.when(z == 0)
            def _():
                self.add(held, *sources)

            self.going_up(i, target).start()

        @pl.when(target < z)
        def _():
            @pl.when(z < 3)
            def _():
                self.going_down(i, target).wait_recv()
                self.add(held, *sources, self.from_above.at[target])

            @pl.when(z == 3)
            def _():
                self.add(held, *sources)

            self.going_down(i, target).start()

    def last(self):
        z = self.z
        self.over(3).wait_recv()
        self.add(self.total, self.held.at[7], self.from_core.at[7], self.from_across.at[3])

        @pl.when(z > 0)
        def _():
            self.going_up(0, z).wait_recv()
            self.add(self.total, self.total, self.from_below.at[z])

        @pl.when(z < 3)
        def _():
            self.going_down(0, z).wait_recv()
            self.add(self.total, self.total, self.from_above.at[z])

    def finish(self):
        for i in range(4):
            self.over(i).wait_send()
        for i in range(3):
            self.going_up(i, 0).wait_send()

    @staticmethod
    def scratch(block, kind):
        return [
            *[pltpu.VMEM((amount,) + block, kind) for amount in (8, 8, 4, 4, 4)],
            pltpu.VMEM(block, jnp.float32),
            *[pltpu.SemaphoreType.DMA((amount,)) for amount in (7, 4, 4, 4)],
        ]


class Blocks:
    def __init__(self, scatter, parts_refs, core_send_sem, core_sem, local_sem):
        self.scatter, self.parts = scatter, []
        self.core_send_sem, self.core_sem, self.local_sem = core_send_sem, core_sem, local_sem
        start = 0
        for ref in parts_refs:
            self.parts.append((ref, pl.ds(start, ref.shape[2])))
            start += ref.shape[2]

    def local(self, k):
        index = self.scatter.index(k, self.scatter.c)
        return [
            pltpu.make_async_copy(
                ref.at[index], self.scatter.held.at[k, :, at], self.local_sem.at[k * len(self.parts) + i]
            )
            for i, (ref, at) in enumerate(self.parts)
        ]

    def to_core(self, k):
        index = self.scatter.index(k, 1 - self.scatter.c)
        return [
            remote(
                ref.at[index],
                self.scatter.from_core.at[k, :, at],
                self.core_send_sem.at[k * len(self.parts) + i],
                self.core_sem.at[k * len(self.parts) + i],
                self.scatter.other,
            )
            for i, (ref, at) in enumerate(self.parts)
        ]

    def load(self):
        for k in range(8):
            for copy in self.local(k):
                copy.start()

    def send(self):
        for k in range(8):
            for copy in self.to_core(k):
                copy.start()

    def both(self, k):
        for copy in self.local(k):
            copy.wait()
        for copy in self.to_core(k):
            copy.wait_recv()

    def finish(self):
        for k in range(8):
            for copy in self.to_core(k):
                copy.wait_send()


def scatter_kernel(amount, *refs):
    out_ref = refs[amount]
    scatter = Scatter(refs[amount + 1 : amount + 7], refs[amount + 7 : amount + 11])
    blocks = Blocks(scatter, refs[:amount], *refs[amount + 11 : amount + 14])
    (out_sem,) = refs[amount + 14 :]
    blocks.load()
    greet_line(scatter.z, (scatter.across, scatter.other), scatter.down, scatter.up)
    blocks.send()
    for i in range(4):
        blocks.both(i)
        scatter.side(i)
    for i in range(3):
        blocks.both(4 + i)
        scatter.line(i)
    blocks.both(7)
    scatter.last()
    outward = pltpu.make_async_copy(scatter.total, out_ref, out_sem.at[0])
    outward.start()
    blocks.finish()
    scatter.finish()
    outward.wait()


def contract(left, right, left_dim, right_dim):
    return lax.dot_general(
        left, right, (((left_dim,), (right_dim,)), ((), ())), preferred_element_type=jnp.float32
    )


def backward_kernel(
    unit_grads_ref, weights_ref, rows_ref, hidden_ref, out_ref, weight_grads_ref,
    held, from_core, from_across, from_below, from_above, total, send_sem, across_sem, below_sem, above_sem,
    core_send_sem, core_sem, local_sem, for_core, unit_grads, weights, rows, tile, tile_sem,
):
    scatter = Scatter(
        (held, from_core, from_across, from_below, from_above, total), (send_sem, across_sem, below_sem, above_sem)
    )
    block_rows, width = out_ref.shape
    loads = [
        pltpu.make_async_copy(unit_grads_ref, unit_grads.at[pl.ds(0, 2)], local_sem.at[0]),
        pltpu.make_async_copy(weights_ref.at[pl.ds(0, 2)], weights, local_sem.at[1]),
        pltpu.make_async_copy(hidden_ref, unit_grads.at[2], local_sem.at[2]),
        pltpu.make_async_copy(rows_ref[0], rows.at[0], local_sem.at[3]),
        pltpu.make_async_copy(rows_ref[1], rows.at[1], local_sem.at[4]),
    ]
    for copy in loads:
        copy.start()
    greet_line(scatter.z, (scatter.across, scatter.other), scatter.down, scatter.up)
    loads[0].wait()
    loads[1].wait()

    def to_core(k):
        return remote(for_core.at[k], from_core.at[k], core_send_sem.at[k], core_sem.at[k], scatter.other)

    tile_rows = tile.shape[2]

    def tile_out(u, i):
        return pltpu.make_async_copy(
            tile.at[u % 2, i], weight_grads_ref.at[i, pl.ds(u * tile_rows, tile_rows), :], tile_sem.at[u % 2, i]
        )

    def weight_tile(u):
        if u == 0:
            for copy in loads[2:]:
                copy.wait()
        if u >= 2:
            for i in range(3):
                tile_out(u - 2, i).wait()

        def body(i, carry):
            left = rows[i // 2, :, pl.ds(u * tile_rows, tile_rows)]
            tile[u % 2, i] = contract(left, unit_grads[i], 0, 0).astype(tile.dtype)
            return carry

        lax.fori_loop(0, 3, body, 0)
        for i in range(3):
            tile_out(u, i).start()

    for j in range(4):
        partial_pair(scatter, unit_grads, weights, block_rows, j, 1 - scatter.c, for_core)
        to_core(j).start()
        to_core(4 + j).start()
        partial_pair(scatter, unit_grads, weights, block_rows, j, scatter.c, held)
        to_core(j).wait_recv()
        scatter.side(j)
        if j == 1:
            weight_tile(0)
    weight_tile(1)
    for i in range(3):
        to_core(4 + i).wait_recv()
        scatter.line(i)
        weight_tile(2 + i)
    weight_tile(5)
    to_core(7).wait_recv()
    scatter.last()
    outward = pltpu.make_async_copy(total, out_ref, local_sem.at[5])
    outward.start()
    for k in range(8):
        to_core(k).wait_send()
    scatter.finish()
    for u in (4, 5):
        for i in range(3):
            tile_out(u, i).wait()
    outward.wait()


def scatter_fsdp(parts, collective_id):
    size, rows, _ = parts[0].shape
    columns = sum(part.shape[2] for part in parts)
    if size != KERNEL_FSDP:
        return lax.psum_scatter(
            jnp.concatenate(parts, axis=2), "fsdp", scatter_dimension=0, tiled=False
        ).astype(jnp.float32)
    block, amount = (rows, columns), len(parts)
    return scratch_call(
        functools.partial(scatter_kernel, amount),
        jax.ShapeDtypeStruct(block, jnp.float32),
        [
            *Scatter.scratch(block, parts[0].dtype),
            *[pltpu.SemaphoreType.DMA((8 * amount,)) for _ in range(3)],
            pltpu.SemaphoreType.DMA((1,)),
        ],
        collective_id,
        *parts,
    )


def gather_through(block_ref, gathered, gathered_ref, send_sem, receive_sem, out_sem, prepare, compute):
    gather = Gather(block_ref, gathered, send_sem, receive_sem)
    z, x, c = gather.z, gather.x, gather.c
    _, block_rows, width = gathered.shape
    own = pltpu.make_async_copy(block_ref, gathered.at[gather.own], out_sem.at[8])
    own.start()
    greet_line(z, (gather.across, gather.other), gather.down, gather.up)
    gather.start()

    def out(number):
        at = pl.ds(number * 2, 2)
        return pltpu.make_async_copy(gathered.at[at], gathered_ref.at[at], out_sem.at[number])

    def pairs(first, side):
        def body(i, carry):
            dz = first + i
            zi = (z // 2 + dz // 2) % 2 * 2 + (z + dz) % 2
            number = zi * 2 + side
            gather.arrived(fsdp_index(zi, side, 1 - c))
            out(number).start()
            left = gathered[pl.ds(number * 2, 2)].reshape(2 * block_rows, width)
            compute(number, pl.ds(pl.multiple_of(number * 2 * block_rows, 2 * block_rows), 2 * block_rows), left)
            return carry

        lax.fori_loop(0, 2, body, 0)

    gather.line(1)
    gather.side(0)
    own.wait()
    prepare()
    pairs(0, x)
    gather.line(2)
    gather.side(1)
    pairs(0, 1 - x)
    gather.line(3)
    gather.side(2)
    pairs(2, x)
    gather.side(3)
    pairs(2, 1 - x)
    gather.finish(waits=False)
    for number in range(8):
        out(number).wait()


GELU_SCALE = math.sqrt(2.0 / math.pi)
GELU_CUBE = 0.044715


def feed_first_kernel(
    block_ref, weights_ref, gathered_ref, gate_up_ref, hidden_ref,
    gathered, send_sem, receive_sem, out_sem, weights, gate_up, hidden, load_sem, gate_up_sem, hidden_sem,
):
    load = pltpu.make_async_copy(weights_ref.at[pl.ds(0, 2)], weights, load_sem.at[0])
    load.start()

    def outs(number, rows):
        return (
            pltpu.make_async_copy(gate_up.at[:, rows, :], gate_up_ref.at[:, rows, :], gate_up_sem.at[number]),
            pltpu.make_async_copy(hidden.at[rows, :], hidden_ref.at[rows, :], hidden_sem.at[number]),
        )

    def compute(number, rows, left):
        gate = contract(left, weights[0], 1, 0)
        gate_up[0, rows, :] = gate
        up = contract(left, weights[1], 1, 0)
        gate_up[1, rows, :] = up
        gate = gate_up[0, rows, :]
        curve = jnp.tanh(GELU_SCALE * (gate + GELU_CUBE * (gate * gate * gate)))
        hidden[rows, :] = (0.5 * gate * (1.0 + curve) * up).astype(hidden.dtype)
        for copy in outs(number, rows):
            copy.start()

    gather_through(block_ref, gathered, gathered_ref, send_sem, receive_sem, out_sem, load.wait, compute)
    pair_rows = hidden.shape[0] // 8
    for number in range(8):
        for copy in outs(number, pl.ds(number * pair_rows, pair_rows)):
            copy.wait()


def hidden_back_kernel(
    block_ref, weights_ref, gate_up_ref, gathered_ref, unit_grads_ref,
    gathered, send_sem, receive_sem, out_sem, weights, gate_up, unit_grads, load_sem, grads_sem,
):
    loads = [
        pltpu.make_async_copy(weights_ref.at[2], weights, load_sem.at[0]),
        pltpu.make_async_copy(gate_up_ref, gate_up, load_sem.at[1]),
    ]
    for copy in loads:
        copy.start()

    def prepare():
        for copy in loads:
            copy.wait()

    def out(number, rows):
        return pltpu.make_async_copy(unit_grads.at[:, rows, :], unit_grads_ref.at[:, rows, :], grads_sem.at[number])

    def compute(number, rows, left):
        hidden_grad = contract(left, weights[...], 1, 0)
        gate, up = gate_up[0, rows, :], gate_up[1, rows, :]
        square = gate * gate
        curve = jnp.tanh(GELU_SCALE * (gate + GELU_CUBE * (square * gate)))
        inner = GELU_SCALE * (1.0 + 3.0 * GELU_CUBE * square)
        slope = 0.5 * (1.0 + curve) + 0.5 * gate * (1.0 - curve * curve) * inner
        unit_grads[0, rows, :] = (hidden_grad * up * slope).astype(unit_grads.dtype)
        unit_grads[1, rows, :] = (hidden_grad * (0.5 * gate * (1.0 + curve))).astype(unit_grads.dtype)
        out(number, rows).start()

    gather_through(block_ref, gathered, gathered_ref, send_sem, receive_sem, out_sem, prepare, compute)
    pair_rows = unit_grads.shape[1] // 8
    for number in range(8):
        out(number, pl.ds(number * pair_rows, pair_rows)).wait()


def gather_scratch(size, block, kind):
    return [
        pltpu.VMEM((size,) + block, kind),
        pltpu.SemaphoreType.DMA((Gather.slots,)),
        pltpu.SemaphoreType.DMA((size,)),
        pltpu.SemaphoreType.DMA((9,)),
    ]


def feed_first(block, feed_full, collective_id):
    size = lax.axis_size("fsdp")
    tokens, width, units, kind = size * block.shape[0], block.shape[1], feed_full.shape[2], block.dtype
    if size != KERNEL_FSDP:
        rows = lax.all_gather(block, "fsdp", axis=0, tiled=True)
        gate, up = contract(rows, feed_full[0], 1, 0), contract(rows, feed_full[1], 1, 0)
        return rows, jnp.stack([gate, up]), gelu_product(gate, up).astype(kind)
    rows, gate_up, hidden = scratch_call(
        feed_first_kernel,
        (
            jax.ShapeDtypeStruct((size,) + block.shape, kind),
            jax.ShapeDtypeStruct((2, tokens, units), jnp.float32),
            jax.ShapeDtypeStruct((tokens, units), kind),
        ),
        [
            *gather_scratch(size, block.shape, kind),
            pltpu.VMEM((2, width, units), kind),
            pltpu.VMEM((2, tokens, units), jnp.float32),
            pltpu.VMEM((tokens, units), kind),
            pltpu.SemaphoreType.DMA((1,)),
            pltpu.SemaphoreType.DMA((8,)),
            pltpu.SemaphoreType.DMA((8,)),
        ],
        collective_id,
        block,
        feed_full,
    )
    return rows.reshape(tokens, width), gate_up, hidden


def hidden_back(block, feed_full, gate_up, collective_id):
    size = lax.axis_size("fsdp")
    tokens, width, units, kind = size * block.shape[0], block.shape[1], feed_full.shape[2], block.dtype
    if size != KERNEL_FSDP:
        rows = lax.all_gather(block, "fsdp", axis=0, tiled=True)
        unused_out, pullback = jax.vjp(gelu_product, gate_up[0], gate_up[1])
        gradients = pullback(contract(rows, feed_full[2], 1, 0))
        return rows, jnp.stack(gradients).astype(kind)
    rows, unit_grads = scratch_call(
        hidden_back_kernel,
        (
            jax.ShapeDtypeStruct((size,) + block.shape, kind),
            jax.ShapeDtypeStruct((2, tokens, units), kind),
        ),
        [
            *gather_scratch(size, block.shape, kind),
            pltpu.VMEM((width, units), kind),
            pltpu.VMEM((2, tokens, units), jnp.float32),
            pltpu.VMEM((2, tokens, units), kind),
            pltpu.SemaphoreType.DMA((2,)),
            pltpu.SemaphoreType.DMA((8,)),
        ],
        collective_id,
        block,
        feed_full,
        gate_up,
    )
    return rows.reshape(tokens, width), unit_grads


def partial_pair(scatter, units, weights, block_rows, j, core, target):
    amount, width, _ = weights.shape
    step = 3 * 256
    spots = [pl.ds(pl.multiple_of(scatter.index(k, core) * block_rows, block_rows), block_rows) for k in (j, 4 + j)]

    def body(d, carry):
        at = pl.ds(pl.multiple_of(d * step, step), step)
        sums = None
        for i in range(amount):
            left = jnp.concatenate([units[i, spot, :] for spot in spots], axis=0)
            part = contract(left, weights[i, at, :], 1, 1)
            sums = part if sums is None else sums + part
        sums = sums.astype(target.dtype)
        target[j, :, at] = sums[:block_rows]
        target[4 + j, :, at] = sums[block_rows:]
        return carry

    lax.fori_loop(0, width // step, body, 0)


def feed_last_kernel(
    hidden_ref, weights_ref, out_ref,
    held, from_core, from_across, from_below, from_above, total, send_sem, across_sem, below_sem, above_sem,
    core_send_sem, core_sem, local_sem, for_core, hidden, weights,
):
    scatter = Scatter(
        (held, from_core, from_across, from_below, from_above, total), (send_sem, across_sem, below_sem, above_sem)
    )
    loads = [
        pltpu.make_async_copy(hidden_ref, hidden.at[0], local_sem.at[0]),
        pltpu.make_async_copy(weights_ref.at[pl.ds(2, 1)], weights, local_sem.at[1]),
    ]
    for copy in loads:
        copy.start()
    greet_line(scatter.z, (scatter.across, scatter.other), scatter.down, scatter.up)
    for copy in loads:
        copy.wait()

    def to_core(k):
        return remote(for_core.at[k], from_core.at[k], core_send_sem.at[k], core_sem.at[k], scatter.other)

    for j in range(4):
        partial_pair(scatter, hidden, weights, out_ref.shape[0], j, 1 - scatter.c, for_core)
        to_core(j).start()
        to_core(4 + j).start()
        partial_pair(scatter, hidden, weights, out_ref.shape[0], j, scatter.c, held)
        to_core(j).wait_recv()
        scatter.side(j)
    for i in range(3):
        to_core(4 + i).wait_recv()
        scatter.line(i)
    to_core(7).wait_recv()
    scatter.last()
    outward = pltpu.make_async_copy(total, out_ref, local_sem.at[2])
    outward.start()
    for k in range(8):
        to_core(k).wait_send()
    scatter.finish()
    outward.wait()


def feed_last(hidden, feed_full, collective_id):
    size = lax.axis_size("fsdp")
    tokens, width, kind = hidden.shape[0], feed_full.shape[1], hidden.dtype
    block = (tokens // size, width)
    if size != KERNEL_FSDP:
        sums = contract(hidden, feed_full[2], 1, 1).astype(kind)
        return scatter_fsdp((sums.reshape((size,) + block),), collective_id)
    return scratch_call(
        feed_last_kernel,
        jax.ShapeDtypeStruct(block, jnp.float32),
        [
            *Scatter.scratch(block, kind),
            pltpu.SemaphoreType.DMA((8,)),
            pltpu.SemaphoreType.DMA((8,)),
            pltpu.SemaphoreType.DMA((3,)),
            pltpu.VMEM((8,) + block, kind),
            pltpu.VMEM((1,) + hidden.shape, kind),
            pltpu.VMEM((1,) + feed_full.shape[1:], kind),
        ],
        collective_id,
        hidden,
        feed_full,
    )


def feed_backward(unit_grads, feed_full, feed_input, feed_grad_rows, hidden, collective_id):
    size = lax.axis_size("fsdp")
    kind = hidden.dtype
    tokens, width = feed_input.shape
    if size != KERNEL_FSDP:
        gate_grad, up_grad = unit_grads[0], unit_grads[1]
        sums = contract(gate_grad, feed_full[0], 1, 1) + contract(up_grad, feed_full[1], 1, 1)
        return (
            scatter_fsdp((sums.astype(kind).reshape(size, tokens // size, width),), collective_id),
            jnp.stack(
                [
                    contract(left, right, 0, 0).astype(kind)
                    for left, right in ((feed_input, gate_grad), (feed_input, up_grad), (feed_grad_rows, hidden))
                ]
            ),
        )
    block, units = (tokens // size, width), hidden.shape[1]
    tile_rows = width // 6

    def kernel(unit_grads_ref, weights_ref, input_ref, grad_ref, hidden_ref, *refs):
        backward_kernel(unit_grads_ref, weights_ref, (input_ref, grad_ref), hidden_ref, *refs)

    rows_grad, weight_grads = scratch_call(
        kernel,
        (jax.ShapeDtypeStruct(block, jnp.float32), jax.ShapeDtypeStruct((3, width, units), kind)),
        [
            *Scatter.scratch(block, kind),
            pltpu.SemaphoreType.DMA((8,)),
            pltpu.SemaphoreType.DMA((8,)),
            pltpu.SemaphoreType.DMA((6,)),
            pltpu.VMEM((8,) + block, kind),
            pltpu.VMEM((3, tokens, units), kind),
            pltpu.VMEM((2, width, units), kind),
            pltpu.VMEM((2, tokens, width), kind),
            pltpu.VMEM((2, 3, tile_rows, units), kind),
            pltpu.SemaphoreType.DMA((2, 3)),
        ],
        collective_id,
        unit_grads,
        feed_full,
        feed_input,
        feed_grad_rows,
        hidden,
    )
    return rows_grad, weight_grads


def exchange_kernel(block_ref, out_ref, send_sem, receive_sem):
    index, t = lax.axis_index("fsdp"), lax.axis_index("tp")
    partner = (index, 1 - t)
    greet((partner,))
    copy = remote(block_ref, out_ref, send_sem.at[0], receive_sem.at[0], partner)
    copy.start()
    copy.wait()


def exchange_tp(block, collective_id):
    if lax.axis_size("fsdp") != KERNEL_FSDP:
        return lax.ppermute(block, "tp", [(0, 1), (1, 0)])
    return scratch_call(
        exchange_kernel,
        jax.ShapeDtypeStruct(block.shape, block.dtype),
        [pltpu.SemaphoreType.DMA((1,)), pltpu.SemaphoreType.DMA((1,))],
        collective_id,
        block,
    )


def peer(z, x, c, k):
    kz, kx, kc = k // 4, (k // 2) % 2, k % 2
    high, low = z // 2, z % 2
    high = 1 - high if kz // 2 else high
    low = 1 - low if kz % 2 else low
    return fsdp_index(high * 2 + low, 1 - x if kx else x, 1 - c if kc else c)


MAIN = 2 * LANES
REST = LANES
FIRST_REST = KERNEL_FSDP * MAIN
UNITS = 2 * MAIN + REST


def main_of(owner):
    return pl.ds(pl.multiple_of(owner * MAIN, MAIN), MAIN)


def rest_of(z):
    return pl.ds(pl.multiple_of(FIRST_REST + z * REST, REST), REST)


def distribute_kernel(
    rows_ref, query_ref, key_ref, value_ref, output_ref, gain_ref, gate_ref, up_ref, down_ref,
    attention_ref, partner_ref, feed_ref,
    stage, feed, zeros,
    gather_send, gather_receive, local_sem, pair_rows_sem, send_sem, receive_sem, rest_send, rest_receive,
    on_send, on_receive, rest_on_send, rest_on_receive,
):
    z, x, c, t = place()
    own = fsdp_index(z, x, c)
    partner = (own, 1 - t)
    greet([(peer(z, x, c, k), t) for k in range(1, 16)] + [partner])
    rows_copy = remote(rows_ref, partner_ref, pair_rows_sem.at[0], pair_rows_sem.at[1], partner)
    rows_copy.start()
    loads, start = [], 0
    for i, ref in enumerate((query_ref, key_ref, value_ref, output_ref, gain_ref)):
        loads.append(pltpu.make_async_copy(ref, stage.at[:, pl.ds(start, ref.shape[1])], local_sem.at[i]))
        start += ref.shape[1]
    feed_loads = [
        pltpu.make_async_copy(ref, feed.at[i], local_sem.at[5 + i])
        for i, ref in enumerate((gate_ref, up_ref, down_ref))
    ]
    for copy in loads + feed_loads:
        copy.start()
    for copy in loads:
        copy.wait()
    gather = Gather(stage, attention_ref, gather_send, gather_receive)
    gather.start()
    keep = pltpu.make_async_copy(stage, attention_ref.at[own], local_sem.at[8])
    keep.start()
    for copy in feed_loads:
        copy.wait()

    def main_at(half, source):
        return feed_ref.at[:, source, :, pl.ds(pl.multiple_of(half * MAIN, MAIN), MAIN)]

    def rest_at(source):
        return feed_ref.at[:, source, :, pl.ds(2 * MAIN, REST)]

    takes_rest = (c == 0) & (x == t)

    def direct(k):
        to = peer(z, x, c, k)
        return remote(feed.at[:, :, main_of(to)], main_at(t, own), send_sem.at[k], receive_sem.at[k], (to, t))

    def rest(dz):
        to_z = peer(z, x, c, 4 * dz) // 4
        slot = 4 * dz + 2 * ((x + t) % 2) + c
        return remote(
            feed.at[:, :, rest_of(to_z)], rest_at(own), rest_send.at[dz], rest_receive.at[slot], (fsdp_index(to_z, t, 0), t)
        )

    def onward(k):
        at = main_at(t, peer(z, x, c, k))
        return remote(at if k else feed.at[:, :, main_of(own)], at, on_send.at[k], on_receive.at[k], partner)

    def rest_onward(k):
        at = rest_at(peer(z, x, c, k))
        return remote(at if k else feed.at[:, :, rest_of(z)], at, rest_on_send.at[k], rest_on_receive.at[k], partner)

    def send(dz):
        for k in range(4 * dz, 4 * dz + 4):
            if k:
                direct(k).start()
        if dz:
            rest(dz).start()
        else:

            @pl.when(jnp.logical_not(takes_rest))
            def _():
                rest(0).start()

    def pass_on(dz):
        for k in range(4 * dz, 4 * dz + 4):
            if k:
                direct(k).wait_recv()
            onward(k).start()

        @pl.when(takes_rest)
        def _():
            for k in range(4 * dz, 4 * dz + 4):
                if k:
                    remote(
                        feed.at[:, :, rest_of(0)], rest_at(own), rest_send.at[0], rest_receive.at[k], partner
                    ).wait_recv()
                rest_onward(k).start()

    send(0)
    send(1)
    keep_main = pltpu.make_async_copy(feed.at[:, :, main_of(own)], main_at(t, own), local_sem.at[9])
    keep_main.start()
    keep_rest = pltpu.make_async_copy(feed.at[:, :, rest_of(z)], rest_at(own), local_sem.at[10])

    @pl.when(takes_rest)
    def _():
        keep_rest.start()

    fills = [
        pltpu.make_async_copy(zeros, feed_ref.at[i, :, :, pl.ds(2 * MAIN, REST)], local_sem.at[11 + i])
        for i in range(3)
    ]

    @pl.when(c == 1)
    def _():
        zeros[...] = jnp.zeros_like(zeros)
        for copy in fills:
            copy.start()

    send(2)
    pass_on(0)
    pass_on(1)
    gather.line(1)
    gather.side(0)
    send(3)
    gather.line(2)
    gather.side(1)
    pass_on(2)
    gather.line(3)
    gather.side(2)
    pass_on(3)
    gather.side(3)
    gather.finish()
    rows_copy.wait()
    for k in range(16):
        onward(k).wait_recv()
        onward(k).wait_send()
        if k:
            direct(k).wait_send()

    @pl.when(jnp.logical_not(takes_rest))
    def _():
        rest(0).wait_send()

    for dz in (1, 2, 3):
        rest(dz).wait_send()

    @pl.when(takes_rest)
    def _():
        for k in range(16):
            rest_onward(k).wait_send()
        keep_rest.wait()

    @pl.when((c == 0) & (x != t))
    def _():
        for k in range(16):
            rest_onward(k).wait_recv()

    @pl.when(c == 1)
    def _():
        for copy in fills:
            copy.wait()

    keep.wait()
    keep_main.wait()


def distribute(rows, attention, gain_columns, feed, collective_id):
    size = lax.axis_size("fsdp")
    shard_rows, feed_width = feed[0].shape
    columns = sum(w.shape[1] for w in attention) + gain_columns.shape[1]
    if size != KERNEL_FSDP:
        halves = lax.all_to_all(pack_units(feed, size), "fsdp", split_axis=0, concat_axis=0, tiled=True)
        halves = lax.all_gather(halves, "tp", axis=0)
        halves = halves.reshape(halves.shape[0], size * shard_rows, halves.shape[-1])
        return (
            lax.all_gather(jnp.concatenate((*attention, gain_columns), axis=1), "fsdp", axis=0),
            lax.ppermute(rows, "tp", [(0, 1), (1, 0)]),
            jnp.stack(join_units(halves, feed_width, size, 3)),
        )
    kind = rows.dtype
    attention_full, partner_rows, feed_full = scratch_call(
        distribute_kernel,
        (
            jax.ShapeDtypeStruct((size, shard_rows, columns), kind),
            jax.ShapeDtypeStruct(rows.shape, kind),
            jax.ShapeDtypeStruct((3, size, shard_rows, UNITS), kind),
        ),
        [
            pltpu.VMEM((shard_rows, columns), kind),
            pltpu.VMEM((3, shard_rows, feed_width), kind),
            pltpu.VMEM((size, shard_rows, REST), kind),
            pltpu.SemaphoreType.DMA((Gather.slots,)),
            pltpu.SemaphoreType.DMA((size,)),
            pltpu.SemaphoreType.DMA((14,)),
            pltpu.SemaphoreType.DMA((2,)),
            pltpu.SemaphoreType.DMA((size,)),
            pltpu.SemaphoreType.DMA((size,)),
            pltpu.SemaphoreType.DMA((4,)),
            pltpu.SemaphoreType.DMA((size,)),
            pltpu.SemaphoreType.DMA((size,)),
            pltpu.SemaphoreType.DMA((size,)),
            pltpu.SemaphoreType.DMA((size,)),
            pltpu.SemaphoreType.DMA((size,)),
        ],
        collective_id,
        rows,
        *attention,
        gain_columns,
        *feed,
    )
    return attention_full, partner_rows, feed_full.reshape(3, size * shard_rows, UNITS)


def collect_kernel(
    parts_ref, projected_ref, output_ref, gain_ref, out_ref, attention_ref,
    held, received, rest_held, rest_received,
    local_sem, pair_send, pair_receive, rest_pair_send, rest_pair_receive, send_sem, receive_sem, rest_send, rest_receive,
    *scatter_refs,
):
    scatter = Scatter(scatter_refs[:6], scatter_refs[6:10])
    blocks = Blocks(scatter, (projected_ref, output_ref, gain_ref), *scatter_refs[10:13])
    blocks.load()
    z, x, c, t = place()
    own = fsdp_index(z, x, c)
    rows = out_ref.shape[1]
    partner = (own, 1 - t)
    parts = [parts_ref.at[i] for i in range(3)]
    order = (3, 2, 1, 0)
    takes_rest = (c == 0) & (x == t)
    gives_rest = (c == 0) & (x != t)

    def plane(dz):
        return pl.ds(peer(z, x, c, 4 * dz) // 4 * 4, 4)

    def half(which):
        return pl.ds(pl.multiple_of(which * MAIN, MAIN), MAIN)

    rest_columns = pl.ds(2 * MAIN, REST)

    def load(dz, i):
        return pltpu.make_async_copy(parts[i].at[plane(dz), :, half(t)], held.at[dz, i], local_sem.at[3 * dz + i])

    def rest_load(dz, i):
        return pltpu.make_async_copy(
            parts[i].at[plane(dz), :, rest_columns], rest_held.at[dz, i], local_sem.at[12 + 3 * dz + i]
        )

    def pair(dz, i):
        slot = 3 * dz + i
        return remote(
            parts[i].at[plane(dz), :, half(1 - t)], received.at[dz, i], pair_send.at[slot], pair_receive.at[slot], partner
        )

    def rest_pair(dz, i):
        slot = 3 * dz + i
        return remote(
            parts[i].at[plane(dz), :, rest_columns],
            rest_received.at[dz, i],
            rest_pair_send.at[slot],
            rest_pair_receive.at[slot],
            partner,
        )

    def spot(k):
        return peer(z, x, c, k) % 4

    def direct(k):
        return remote(
            held.at[k // 4, :, spot(k)], out_ref.at[:, :, main_of(own)], send_sem.at[k], receive_sem.at[k], (peer(z, x, c, k), t)
        )

    def rest_direct(k):
        return remote(
            rest_held.at[k // 4, :, spot(k)],
            out_ref.at[:, :, rest_of(z)],
            rest_send.at[k],
            rest_receive.at[z],
            (peer(z, x, c, k), t),
        )

    def add(target, source):
        def body(j, carry):
            i, at = j // 4, j % 4
            total = target[i, at].astype(jnp.float32) + source[i, at].astype(jnp.float32)
            target[i, at] = total.astype(target.dtype)
            return carry

        lax.fori_loop(0, 12, body, 0)

    for dz in order:
        for i in range(3):
            load(dz, i).start()

    @pl.when(takes_rest)
    def _():
        for dz in order:
            for i in range(3):
                rest_load(dz, i).start()

    greet([(peer(z, x, c, k), t) for k in range(1, 16)] + [partner])
    blocks.send()
    for dz in order:
        for i in range(3):
            pair(dz, i).start()

        @pl.when(gives_rest)
        def _():
            for i in range(3):
                rest_pair(dz, i).start()

    def pass_on(dz):
        for i in range(3):
            load(dz, i).wait()
            pair(dz, i).wait_recv()
        add(held.at[dz], received.at[dz])
        for k in range(4 * dz, 4 * dz + 4):
            if k:
                direct(k).start()

        @pl.when(takes_rest)
        def _():
            for i in range(3):
                rest_load(dz, i).wait()
                rest_pair(dz, i).wait_recv()
            add(rest_held.at[dz], rest_received.at[dz])
            for k in range(4 * dz, 4 * dz + 4):
                if k:
                    rest_direct(k).start()

    def line(i):
        blocks.both(4 + i)
        scatter.line(i)

    for i in range(4):
        blocks.both(i)
        scatter.side(i)
    pass_on(3)
    line(0)
    pass_on(2)
    line(1)
    pass_on(1)
    line(2)
    pass_on(0)
    blocks.both(7)
    scatter.last()
    outward = pltpu.make_async_copy(scatter.total, attention_ref, local_sem.at[26])
    outward.start()
    keep = pltpu.make_async_copy(held.at[0, :, spot(0)], out_ref.at[:, :, main_of(own)], local_sem.at[24])
    keep.start()
    keep_rest = pltpu.make_async_copy(rest_held.at[0, :, spot(0)], out_ref.at[:, :, rest_of(z)], local_sem.at[25])

    @pl.when(takes_rest)
    def _():
        keep_rest.start()

    for k in range(1, 16):
        direct(k).wait_recv()

    for dz in range(4):
        from_z = peer(z, x, c, 4 * dz) // 4

        def arrived():
            remote(
                rest_held.at[0, :, 0], out_ref.at[:, :, rest_of(from_z)], rest_send.at[0], rest_receive.at[from_z], partner
            ).wait_recv()

        if dz:
            arrived()
        else:

            @pl.when(jnp.logical_not(takes_rest))
            def _():
                arrived()

    for k in range(1, 16):
        direct(k).wait_send()
    for dz in order:
        for i in range(3):
            pair(dz, i).wait_send()

    @pl.when(gives_rest)
    def _():
        for dz in order:
            for i in range(3):
                rest_pair(dz, i).wait_send()

    @pl.when(takes_rest)
    def _():
        for k in range(1, 16):
            rest_direct(k).wait_send()
        keep_rest.wait()

    blocks.finish()
    scatter.finish()
    keep.wait()
    outward.wait()


def collect(gradients, feed_width, attention_parts, collective_id):
    size, pairs = lax.axis_size("fsdp"), lax.axis_size("tp")
    shard_rows = gradients.shape[1] // size
    if size != KERNEL_FSDP:
        packed = part_units([gradients[i] for i in range(3)], feed_width, size, pairs)
        mine = lax.psum_scatter(packed, "tp", scatter_dimension=0, tiled=False)
        mine = mine.reshape(size, shard_rows, mine.shape[-1])
        mine = lax.all_to_all(mine, "fsdp", split_axis=0, concat_axis=0, tiled=True)
        feed = [g.astype(jnp.float32) for g in unpack_units(mine, feed_width, 3)]
        return feed, scatter_fsdp(attention_parts, collective_id)
    kind = gradients.dtype
    main, rest = (4, 3, 4, shard_rows, MAIN), (4, 3, 4, shard_rows, REST)
    block = (shard_rows, sum(part.shape[2] for part in attention_parts))
    out, attention = scratch_call(
        collect_kernel,
        (
            jax.ShapeDtypeStruct((3, shard_rows, feed_width), kind),
            jax.ShapeDtypeStruct(block, jnp.float32),
        ),
        [
            pltpu.VMEM(main, kind),
            pltpu.VMEM(main, kind),
            pltpu.VMEM(rest, kind),
            pltpu.VMEM(rest, kind),
            pltpu.SemaphoreType.DMA((27,)),
            pltpu.SemaphoreType.DMA((12,)),
            pltpu.SemaphoreType.DMA((12,)),
            pltpu.SemaphoreType.DMA((12,)),
            pltpu.SemaphoreType.DMA((12,)),
            pltpu.SemaphoreType.DMA((size,)),
            pltpu.SemaphoreType.DMA((size,)),
            pltpu.SemaphoreType.DMA((size,)),
            pltpu.SemaphoreType.DMA((4,)),
            *Scatter.scratch(block, kind),
            *[pltpu.SemaphoreType.DMA((24,)) for _ in range(3)],
        ],
        collective_id,
        gradients.reshape(3, size, shard_rows, UNITS),
        *attention_parts,
    )
    return [out[i].astype(jnp.float32) for i in range(3)], attention


def contract_last(left_rows, right_rows):
    return lax.dot_general(
        left_rows, right_rows, (((1,), (1,)), ((), ())), preferred_element_type=jnp.float32
    )


def contract_first(left_rows, right_rows):
    return lax.dot_general(
        left_rows, right_rows, (((0,), (0,)), ((), ())), preferred_element_type=jnp.float32
    )


def normalize_parts(value_rows):
    inverse = lax.rsqrt(jnp.mean(value_rows * value_rows, axis=-1, keepdims=True) + EPSILON)
    return (value_rows * inverse, inverse)


def norm_backward(unit_rows, inverse, norm_gain, upstream):
    scaled = upstream * norm_gain
    return inverse * (scaled - unit_rows * jnp.mean(scaled * unit_rows, axis=-1, keepdims=True))


def layout(lengths_row, row_index):
    segment_ends = jnp.cumsum(lengths_row)
    segment_starts = segment_ends - lengths_row
    segment = jnp.sum((row_index[:, None] >= segment_ends[None, :]).astype(jnp.int32), axis=1)
    onehot = segment[:, None] == jnp.arange(lengths_row.shape[0], dtype=jnp.int32)[None, :]
    segment_begin = jnp.sum(jnp.where(onehot, segment_starts[None, :], 0), axis=1)
    prompt_shift = jnp.where(segment > 0, lengths_row[0], 0)
    return (segment, row_index - segment_begin + prompt_shift)


def rotary_tables(position):
    frequency = jnp.exp(
        jnp.arange(HEAD_SIZE // 2, dtype=jnp.float32) * (-2.0 * math.log(10000.0) / HEAD_SIZE)
    )
    angles = position.astype(jnp.float32)[:, None] * frequency[None, :]
    return (jnp.cos(angles), jnp.sin(angles))


def apply_rotary(value_rows, cosine_lookup, sine_lookup):
    half_width = value_rows.shape[-1] // 2
    first_half = value_rows[..., :half_width]
    second_half = value_rows[..., half_width:]
    cosine_part = cosine_lookup[:, None, :]
    sine_part = sine_lookup[:, None, :]
    return jnp.concatenate(
        [
            first_half * cosine_part - second_half * sine_part,
            second_half * cosine_part + first_half * sine_part,
        ],
        axis=-1,
    )


def unrotate(value_rows, cosine_lookup, sine_lookup):
    half_width = value_rows.shape[-1] // 2
    first_half = value_rows[..., :half_width]
    second_half = value_rows[..., half_width:]
    cosine_part = cosine_lookup[:, None, :]
    sine_part = sine_lookup[:, None, :]
    return jnp.concatenate(
        [
            first_half * cosine_part + second_half * sine_part,
            second_half * cosine_part - first_half * sine_part,
        ],
        axis=-1,
    )


def visible(segment, row_index):
    same_segment = (segment[:, None] == segment[None, :]) & (
        row_index[None, :] <= row_index[:, None]
    )
    from_prompt = (segment[None, :] == 0) & (segment[:, None] > 0)
    return same_segment | from_prompt


def masked_scores(rotated_query, rotated_key, visible_mask):
    raw_scores = jnp.einsum(
        "qgrd,kgd->grqk", rotated_query, rotated_key, preferred_element_type=jnp.float32
    )
    tanh_value = jnp.tanh(raw_scores * HEAD_SIZE ** (-0.5) / SOFTCAP)
    return (jnp.where(visible_mask[None, None], SOFTCAP * tanh_value, NEGATIVE), tanh_value)


def gelu_product(gate_value, up_value):
    return jax.nn.gelu(gate_value, approximate=True) * up_value


def split_columns(width, size):
    main = width // size // LANES * LANES
    return main, width // size - main


def pack_units(weights, size):
    rows, width = weights[0].shape
    main, rest = split_columns(width, size)
    pieces = []
    if main:
        pieces += [
            jnp.transpose(w[:, : main * size].reshape(rows, size, main), (1, 0, 2)) for w in weights
        ]
    if rest:
        pieces += [
            jnp.transpose(w[:, main * size :].reshape(rows, size, rest), (1, 0, 2)) for w in weights
        ]
    packed = jnp.concatenate(pieces, axis=2)
    return jnp.pad(packed, ((0, 0), (0, 0), (0, -packed.shape[2] % LANES)))


def unpack_units(packed, width, amount):
    size, rows, _ = packed.shape
    main, rest = split_columns(width, size)
    arrays = []
    for i in range(amount):
        pieces = []
        if main:
            piece = packed[:, :, i * main : (i + 1) * main]
            pieces.append(jnp.transpose(piece, (1, 0, 2)).reshape(rows, size * main))
        if rest:
            start = amount * main + i * rest
            piece = packed[:, :, start : start + rest]
            pieces.append(jnp.transpose(piece, (1, 0, 2)).reshape(rows, size * rest))
        arrays.append(jnp.concatenate(pieces, axis=1))
    return arrays


def join_units(halves, width, size, amount):
    main, rest = split_columns(width, size)
    arrays = []
    for i in range(amount):
        start = amount * main + i * rest
        pieces = [half[:, i * main : (i + 1) * main] for half in halves]
        pieces += [half[:, start : start + rest] for half in halves]
        joined = jnp.concatenate(pieces, axis=1)
        arrays.append(jnp.pad(joined, ((0, 0), (0, -joined.shape[1] % LANES))))
    return arrays


def part_units(arrays, width, size, pairs):
    main, rest = split_columns(width, size)
    halves = []
    for t in range(pairs):
        pieces = [array[:, t * main : (t + 1) * main] for array in arrays]
        start = pairs * main + t * rest
        pieces += [array[:, start : start + rest] for array in arrays]
        packed = jnp.concatenate(pieces, axis=1)
        halves.append(jnp.pad(packed, ((0, 0), (0, -packed.shape[1] % LANES))))
    return jnp.stack(halves)


def shards(
    block_input,
    lengths,
    attention_norm_gain,
    attention_post_gain,
    feedforward_norm_gain,
    feedforward_post_gain,
    query_weight,
    key_weight,
    value_weight,
    output_weight,
    gate_weight,
    up_weight,
    down_weight,
    output_cotangent,
):
    low = jnp.bfloat16
    size, pairs = lax.axis_size("fsdp"), lax.axis_size("tp")
    rows_local, width = block_input.shape
    shard_rows, feed_width = gate_weight.shape
    query_width, key_width = query_weight.shape[1], key_weight.shape[1]
    output_start = query_width + 2 * key_width
    gain_start = output_start + query_width
    grouped_rows = rows_local * pairs

    gain_columns = jnp.stack(
        [attention_norm_gain, attention_post_gain, feedforward_norm_gain, feedforward_post_gain],
        axis=1,
    )
    attention_full, other_input, feed_full = distribute(
        block_input,
        (query_weight, key_weight, value_weight, output_weight),
        jnp.pad(gain_columns, ((0, 0), (0, LANES - 4))),
        (gate_weight, up_weight, down_weight),
        1,
    )
    attention_full = attention_full.reshape(size * shard_rows, gain_start + LANES)
    gains = jnp.transpose(attention_full[:, gain_start : gain_start + 4]).astype(jnp.float32)
    gain_one, gain_two, gain_three, gain_four = gains[0], gains[1], gains[2], gains[3]

    row_index = (
        jnp.arange(grouped_rows, dtype=jnp.int32) + lax.axis_index("tp") * rows_local
    ) % grouped_rows
    segment, position = layout(lengths[0], row_index)
    cosine_lookup, sine_lookup = rotary_tables(position)
    visible_mask = visible(segment, row_index)
    residual_both = jnp.concatenate([block_input, other_input], axis=0).astype(jnp.float32)
    unit_one_both, inverse_one_both = normalize_parts(residual_both)
    residual = residual_both[:rows_local]
    unit_one, inverse_one = unit_one_both[:rows_local], inverse_one_both[:rows_local]
    normed = (unit_one_both * gain_one).astype(low)
    projected = jnp.dot(
        normed, attention_full[:, :output_start], preferred_element_type=jnp.float32
    )
    query_raw = projected[:, :query_width]
    key_raw = projected[:, query_width : query_width + key_width]
    value_raw = projected[:, query_width + key_width :]
    heads_local = query_width // HEAD_SIZE
    kv_local = key_width // HEAD_SIZE
    repeat_heads = heads_local // kv_local
    rotated_query = apply_rotary(
        query_raw.reshape(grouped_rows, heads_local, HEAD_SIZE), cosine_lookup, sine_lookup
    ).astype(low)
    rotated_query = rotated_query.reshape(grouped_rows, kv_local, repeat_heads, HEAD_SIZE)
    rotated_key = apply_rotary(
        key_raw.reshape(grouped_rows, kv_local, HEAD_SIZE), cosine_lookup, sine_lookup
    ).astype(low)
    value_reduced = value_raw.astype(low).reshape(grouped_rows, kv_local, HEAD_SIZE)
    capped, tanh_value = masked_scores(rotated_query, rotated_key, visible_mask)
    row_peak = jnp.max(capped, axis=-1, keepdims=True)
    exponentials = jnp.exp(capped - row_peak)
    softmax_probs = exponentials / jnp.sum(exponentials, axis=-1, keepdims=True)
    probs_low = softmax_probs.astype(low)
    mixed_heads = jnp.einsum(
        "grqk,kgd->qgrd", probs_low, value_reduced, preferred_element_type=jnp.float32
    )
    attended = mixed_heads.reshape(grouped_rows, heads_local * HEAD_SIZE).astype(low)
    output_full = attention_full[:, output_start:gain_start]
    branch_parts = contract_last(attended, output_full)
    branch_one = branch_parts[:rows_local] + exchange_tp(
        branch_parts[rows_local:].astype(low), 4
    ).astype(jnp.float32)
    unit_two, inverse_two = normalize_parts(branch_one)
    middle = residual + unit_two * gain_two
    unit_three, inverse_three = normalize_parts(middle)

    feed_input, gate_up, hidden = feed_first((unit_three * gain_three).astype(low), feed_full, 5)
    branch_two = feed_last(hidden, feed_full, 6)
    unit_four, inverse_four = normalize_parts(branch_two)
    block_output = (middle + unit_four * gain_four).astype(low)
    upstream = output_cotangent.astype(jnp.float32)
    gain_four_grad = jnp.sum(upstream * unit_four, axis=0)
    branch_two_grad = norm_backward(unit_four, inverse_four, gain_four, upstream).astype(low)
    feed_grad_rows, unit_grads = hidden_back(branch_two_grad, feed_full, gate_up, 7)
    normed_three_grad, feed_grads = feed_backward(
        unit_grads, feed_full, feed_input, feed_grad_rows, hidden, 8
    )
    gain_three_grad = jnp.sum(normed_three_grad * unit_three, axis=0)
    middle_grad = upstream + norm_backward(unit_three, inverse_three, gain_three, normed_three_grad)
    gain_two_grad = jnp.sum(middle_grad * unit_two, axis=0)
    branch_one_grad = norm_backward(unit_two, inverse_two, gain_two, middle_grad).astype(low)
    attention_grad_rows = jnp.concatenate(
        [branch_one_grad, exchange_tp(branch_one_grad, 10)], axis=0
    )
    mixed_grad = jnp.dot(
        attention_grad_rows, output_full, preferred_element_type=jnp.float32
    ).astype(low)
    mixed_grad = mixed_grad.reshape(grouped_rows, kv_local, repeat_heads, HEAD_SIZE)
    value_grad = jnp.einsum(
        "grqk,qgrd->kgd", probs_low, mixed_grad, preferred_element_type=jnp.float32
    )
    probs_grad = jnp.einsum(
        "qgrd,kgd->grqk", mixed_grad, value_reduced, preferred_element_type=jnp.float32
    )
    score_grad = softmax_probs * (
        probs_grad - jnp.sum(softmax_probs * probs_grad, axis=-1, keepdims=True)
    )
    raw_grad = (score_grad * (1.0 - tanh_value * tanh_value) * HEAD_SIZE ** (-0.5)).astype(low)
    query_grad = jnp.einsum(
        "grqk,kgd->qgrd", raw_grad, rotated_key, preferred_element_type=jnp.float32
    )
    key_grad = jnp.einsum(
        "grqk,qgrd->kgd", raw_grad, rotated_query, preferred_element_type=jnp.float32
    )
    query_grad = unrotate(
        query_grad.reshape(grouped_rows, heads_local, HEAD_SIZE), cosine_lookup, sine_lookup
    )
    key_grad = unrotate(key_grad, cosine_lookup, sine_lookup)
    projected_grad = jnp.concatenate(
        [
            query_grad.reshape(grouped_rows, heads_local * HEAD_SIZE).astype(low),
            key_grad.reshape(grouped_rows, kv_local * HEAD_SIZE).astype(low),
            value_grad.reshape(grouped_rows, kv_local * HEAD_SIZE).astype(low),
        ],
        axis=1,
    )
    input_parts = contract_last(projected_grad, attention_full[:, :output_start])

    gain_grads = jnp.stack(
        [
            jnp.sum(input_parts * unit_one_both, axis=0),
            gain_two_grad,
            gain_three_grad,
            gain_four_grad,
        ]
    )
    sent = jnp.concatenate(
        [input_parts[rows_local:].astype(low), jnp.pad(gain_grads, ((0, 12), (0, 0))).astype(low)]
    )
    received = exchange_tp(sent, 11).astype(jnp.float32)
    normed_one_grad = input_parts[:rows_local] + received[:rows_local]
    gain_grads = gain_grads + received[rows_local : rows_local + 4]
    input_gradient = middle_grad + norm_backward(unit_one, inverse_one, gain_one, normed_one_grad)

    (gate_weight_grad, up_weight_grad, down_weight_grad), attention_grads = collect(
        feed_grads,
        feed_width,
        [
            part.astype(low).reshape(size, shard_rows, part.shape[1])
            for part in (
                contract_first(normed, projected_grad),
                contract_first(attention_grad_rows, attended),
                jnp.pad(jnp.transpose(gain_grads), ((0, 0), (0, LANES - 4))),
            )
        ],
        9,
    )
    gain_shards = jnp.transpose(attention_grads[:, gain_start : gain_start + 4])
    return (
        block_output,
        input_gradient,
        gain_shards[0],
        gain_shards[1],
        gain_shards[2],
        gain_shards[3],
        attention_grads[:, :query_width],
        attention_grads[:, query_width : query_width + key_width],
        attention_grads[:, query_width + key_width : output_start],
        attention_grads[:, output_start:gain_start],
        gate_weight_grad,
        up_weight_grad,
        down_weight_grad,
    )


def solution(mesh):
    placed = (
        P(("fsdp", "tp"), None),
        P("fsdp", None),
        P("fsdp"),
        P("fsdp"),
        P("fsdp"),
        P("fsdp"),
        P("fsdp", "tp"),
        P("fsdp", "tp"),
        P("fsdp", "tp"),
        P("fsdp", "tp"),
        P("fsdp", "tp"),
        P("fsdp", "tp"),
        P("fsdp", "tp"),
        P(("fsdp", "tp"), None),
    )
    return jax.shard_map(
        shards,
        mesh=mesh,
        in_specs=placed,
        out_specs=(
            P(("fsdp", "tp"), None),
            P(("fsdp", "tp"), None),
            P("fsdp"),
            P("fsdp"),
            P("fsdp"),
            P("fsdp"),
            P("fsdp", "tp"),
            P("fsdp", "tp"),
            P("fsdp", "tp"),
            P("fsdp", "tp"),
            P("fsdp", "tp"),
            P("fsdp", "tp"),
            P("fsdp", "tp"),
        ),
        check_vma=False,
    )
```

```python
import functools
import math

import jax
import jax.numpy as jnp
from jax import lax
from jax.experimental import pallas as pl
from jax.experimental.pallas import tpu as pltpu
from jax.sharding import PartitionSpec as P

HEAD_SIZE = 256
MESH = pl.DeviceIdType.MESH
ANY = pl.BlockSpec(memory_space=pl.ANY)
LANES = 128

EPSILON = 1e-06
SOFTCAP = 50.0
NEGATIVE = -1e30

KERNEL_FSDP = 16


def place():
    index = lax.axis_index("fsdp")
    return index // 4, (index // 2) % 2, index % 2, lax.axis_index("tp")


def fsdp_index(z, x, c):
    return (z * 2 + x) * 2 + c


def remote(source, target, send_sem, receive_sem, device):
    return pltpu.make_async_remote_copy(
        src_ref=source,
        dst_ref=target,
        send_sem=send_sem,
        recv_sem=receive_sem,
        device_id=device,
        device_id_type=MESH,
    )


def greet(devices):
    barrier = pltpu.get_barrier_semaphore()
    for device in devices:
        pl.semaphore_signal(barrier, inc=1, device_id=device, device_id_type=MESH)
    pl.semaphore_wait(barrier, len(devices))


def greet_line(z, devices, down, up):
    barrier = pltpu.get_barrier_semaphore()
    for device in devices:
        pl.semaphore_signal(barrier, inc=1, device_id=device, device_id_type=MESH)

    @pl.when(z > 0)
    def _():
        pl.semaphore_signal(barrier, inc=1, device_id=down, device_id_type=MESH)

    @pl.when(z < 3)
    def _():
        pl.semaphore_signal(barrier, inc=1, device_id=up, device_id_type=MESH)

    pl.semaphore_wait(barrier, len(devices) + (z + 2) // 3 + (5 - z) // 3)


class Gather:
    slots = 29

    def __init__(self, block, out_ref, send_sem, receive_sem):
        self.block, self.out, self.send_sem, self.receive_sem = block, out_ref, send_sem, receive_sem
        self.z, self.x, self.c, t = place()
        z, x, c = self.z, self.x, self.c
        self.own = fsdp_index(z, x, c)
        self.down, self.up = (fsdp_index(z - 1, x, c), t), (fsdp_index(z + 1, x, c), t)
        self.across, self.other = (fsdp_index(z, 1 - x, c), t), (fsdp_index(z, x, 1 - c), t)

    def copy(self, source, index, slot, device):
        return remote(source, self.out.at[index], self.send_sem.at[slot], self.receive_sem.at[index], device)

    def relay(self, index, slot, device):
        self.copy(self.out.at[index], index, slot, device).start()

    def arrived(self, index):
        self.copy(self.block, index, 0, self.other).wait_recv()

    def sent(self, slot):
        self.copy(self.block, self.own, slot, self.other).wait_send()

    def start(self):
        @pl.when(self.z < 3)
        def _():
            self.copy(self.block, self.own, 0, self.up).start()

        @pl.when(self.z > 0)
        def _():
            self.copy(self.block, self.own, 1, self.down).start()

        self.copy(self.block, self.own, 2, self.across).start()
        self.copy(self.block, self.own, 3, self.other).start()

    def line(self, d):
        z, x, c = self.z, self.x, self.c

        @pl.when(z >= d)
        def _():
            index = fsdp_index(z - d, x, c)
            base = 4 + 3 * (d - 1)
            self.arrived(index)

            @pl.when(z < 3)
            def _():
                self.relay(index, base, self.up)

            self.relay(index, base + 1, self.across)
            self.relay(index, base + 2, self.other)

        @pl.when(z + d <= 3)
        def _():
            index = fsdp_index(z + d, x, c)
            base = 13 + 3 * (d - 1)
            self.arrived(index)

            @pl.when(z > 0)
            def _():
                self.relay(index, base, self.down)

            self.relay(index, base + 1, self.across)
            self.relay(index, base + 2, self.other)

    def side(self, d):
        z, x, c = self.z, self.x, self.c
        if d == 0:
            index = fsdp_index(z, 1 - x, c)
            self.arrived(index)
            self.relay(index, 22, self.other)
            return

        @pl.when(z >= d)
        def _():
            index = fsdp_index(z - d, 1 - x, c)
            self.arrived(index)
            self.relay(index, 22 + d, self.other)

        @pl.when(z + d <= 3)
        def _():
            index = fsdp_index(z + d, 1 - x, c)
            self.arrived(index)
            self.relay(index, 25 + d, self.other)

    def finish(self, waits=True):
        z = self.z
        if waits:
            for zi in range(4):
                for xi in range(2):
                    self.arrived(fsdp_index(zi, xi, 1 - self.c))

        @pl.when(z < 3)
        def _():
            self.sent(0)

        @pl.when(z > 0)
        def _():
            self.sent(1)

        for slot in (2, 3, 22):
            self.sent(slot)
        for d in (1, 2, 3):

            @pl.when(z >= d)
            def _():
                base = 4 + 3 * (d - 1)

                @pl.when(z < 3)
                def _():
                    self.sent(base)

                for slot in (base + 1, base + 2, 22 + d):
                    self.sent(slot)

            @pl.when(z + d <= 3)
            def _():
                base = 13 + 3 * (d - 1)

                @pl.when(z > 0)
                def _():
                    self.sent(base)

                for slot in (base + 1, base + 2, 25 + d):
                    self.sent(slot)


def scratch_call(kernel, outputs, scratch, collective_id, *operands):
    return pl.pallas_call(
        kernel,
        out_shape=outputs,
        in_specs=[ANY] * len(operands),
        out_specs=jax.tree.map(lambda _: ANY, outputs),
        scratch_shapes=scratch,
        compiler_params=pltpu.CompilerParams(
            collective_id=collective_id, has_side_effects=True, vmem_limit_bytes=60 * 1024 * 1024
        ),
    )(*operands)


def add_rows(rows, step, target, *sources):
    def body(i, carry):
        at = pl.ds(pl.multiple_of(i * step, step), step)
        total = sources[0][at, :].astype(jnp.float32)
        for source in sources[1:]:
            total = total + source[at, :].astype(jnp.float32)
        target[at, :] = total.astype(target.dtype)
        return carry

    lax.fori_loop(0, rows // step, body, 0)


class Scatter:
    def __init__(self, buffers, semaphores):
        self.held, self.from_core, self.from_across, self.from_below, self.from_above, self.total = buffers
        self.send_sem, self.across_sem, self.below_sem, self.above_sem = semaphores
        self.z, self.x, self.c, t = place()
        z, x, c = self.z, self.x, self.c
        self.rows = self.total.shape[0]
        self.down, self.up = (fsdp_index(z - 1, x, c), t), (fsdp_index(z + 1, x, c), t)
        self.across, self.other = (fsdp_index(z, 1 - x, c), t), (fsdp_index(z, x, 1 - c), t)

    def target(self, i):
        half = self.z // 2
        mirrored = self.z + half * (3 - 2 * self.z)
        base = 3 - i + mirrored * (i // 2) * (2 * (i % 2) - 1)
        return base + half * (3 - 2 * base)

    def index(self, k, core):
        return fsdp_index(self.target(k % 4), (self.x + 1 - k // 4) % 2, core)

    def add(self, target, *sources):
        add_rows(self.rows, 16, target, *sources)

    def over(self, i):
        return remote(
            self.held.at[i], self.from_across.at[i], self.send_sem.at[3 + i], self.across_sem.at[i], self.across
        )

    def going_up(self, i, target):
        return remote(
            self.held.at[4 + i], self.from_below.at[target], self.send_sem.at[i], self.below_sem.at[target], self.up
        )

    def going_down(self, i, target):
        return remote(
            self.held.at[4 + i], self.from_above.at[target], self.send_sem.at[i], self.above_sem.at[target], self.down
        )

    def side(self, i):
        self.add(self.held.at[i], self.held.at[i], self.from_core.at[i])
        self.over(i).start()

    def line(self, i):
        z, target = self.z, self.target(i)
        held = self.held.at[4 + i]
        sources = (held, self.from_core.at[4 + i], self.from_across.at[i])
        self.over(i).wait_recv()

        @pl.when(target > z)
        def _():
            @pl.when(z > 0)
            def _():
                self.going_up(i, target).wait_recv()
                self.add(held, *sources, self.from_below.at[target])

            @pl.when(z == 0)
            def _():
                self.add(held, *sources)

            self.going_up(i, target).start()

        @pl.when(target < z)
        def _():
            @pl.when(z < 3)
            def _():
                self.going_down(i, target).wait_recv()
                self.add(held, *sources, self.from_above.at[target])

            @pl.when(z == 3)
            def _():
                self.add(held, *sources)

            self.going_down(i, target).start()

    def last(self):
        z = self.z
        self.over(3).wait_recv()
        self.add(self.total, self.held.at[7], self.from_core.at[7], self.from_across.at[3])

        @pl.when(z > 0)
        def _():
            self.going_up(0, z).wait_recv()
            self.add(self.total, self.total, self.from_below.at[z])

        @pl.when(z < 3)
        def _():
            self.going_down(0, z).wait_recv()
            self.add(self.total, self.total, self.from_above.at[z])

    def finish(self):
        for i in range(4):
            self.over(i).wait_send()
        for i in range(3):
            self.going_up(i, 0).wait_send()

    @staticmethod
    def scratch(block, kind):
        return [
            *[pltpu.VMEM((amount,) + block, kind) for amount in (8, 8, 4, 4, 4)],
            pltpu.VMEM(block, jnp.float32),
            *[pltpu.SemaphoreType.DMA((amount,)) for amount in (7, 4, 4, 4)],
        ]


class Blocks:
    def __init__(self, scatter, parts_refs, core_send_sem, core_sem, local_sem):
        self.scatter, self.parts = scatter, []
        self.core_send_sem, self.core_sem, self.local_sem = core_send_sem, core_sem, local_sem
        start = 0
        for ref in parts_refs:
            self.parts.append((ref, pl.ds(start, ref.shape[2])))
            start += ref.shape[2]

    def local(self, k):
        index = self.scatter.index(k, self.scatter.c)
        return [
            pltpu.make_async_copy(
                ref.at[index], self.scatter.held.at[k, :, at], self.local_sem.at[k * len(self.parts) + i]
            )
            for i, (ref, at) in enumerate(self.parts)
        ]

    def to_core(self, k):
        index = self.scatter.index(k, 1 - self.scatter.c)
        return [
            remote(
                ref.at[index],
                self.scatter.from_core.at[k, :, at],
                self.core_send_sem.at[k * len(self.parts) + i],
                self.core_sem.at[k * len(self.parts) + i],
                self.scatter.other,
            )
            for i, (ref, at) in enumerate(self.parts)
        ]

    def load(self):
        for k in range(8):
            for copy in self.local(k):
                copy.start()

    def send(self):
        for k in range(8):
            for copy in self.to_core(k):
                copy.start()

    def both(self, k):
        for copy in self.local(k):
            copy.wait()
        for copy in self.to_core(k):
            copy.wait_recv()

    def finish(self):
        for k in range(8):
            for copy in self.to_core(k):
                copy.wait_send()


def contract(left, right, left_dim, right_dim):
    return lax.dot_general(
        left, right, (((left_dim,), (right_dim,)), ((), ())), preferred_element_type=jnp.float32
    )


def backward_kernel(
    unit_grads_ref, weights_ref, rows_ref, hidden_ref, out_ref, weight_grads_ref,
    held, from_core, from_across, from_below, from_above, total, send_sem, across_sem, below_sem, above_sem,
    core_send_sem, core_sem, local_sem, for_core, unit_grads, weights, rows, tile, tile_sem,
):
    scatter = Scatter(
        (held, from_core, from_across, from_below, from_above, total), (send_sem, across_sem, below_sem, above_sem)
    )
    block_rows, width = out_ref.shape
    loads = [
        pltpu.make_async_copy(unit_grads_ref, unit_grads.at[pl.ds(0, 2)], local_sem.at[0]),
        pltpu.make_async_copy(weights_ref.at[pl.ds(0, 2)], weights, local_sem.at[1]),
        pltpu.make_async_copy(hidden_ref, unit_grads.at[2], local_sem.at[2]),
        pltpu.make_async_copy(rows_ref[0], rows.at[0], local_sem.at[3]),
        pltpu.make_async_copy(rows_ref[1], rows.at[1], local_sem.at[4]),
    ]
    for copy in loads:
        copy.start()
    greet_line(scatter.z, (scatter.across, scatter.other), scatter.down, scatter.up)
    loads[0].wait()
    loads[1].wait()

    def to_core(k):
        return remote(for_core.at[k], from_core.at[k], core_send_sem.at[k], core_sem.at[k], scatter.other)

    tile_rows = tile.shape[2]

    def tile_out(u, i):
        at = pl.ds(pl.multiple_of(u * tile_rows, tile_rows), tile_rows)
        return pltpu.make_async_copy(tile.at[u % 2, i], weight_grads_ref.at[i, at, :], tile_sem.at[u % 2, i])

    def weight_tile(u):
        @pl.when(u == 0)
        def _():
            for copy in loads[2:]:
                copy.wait()

        @pl.when(u >= 2)
        def _():
            for i in range(3):
                tile_out(u - 2, i).wait()

        def body(i, carry):
            left = rows[i // 2, :, pl.ds(pl.multiple_of(u * tile_rows, tile_rows), tile_rows)]
            tile[u % 2, i] = contract(left, unit_grads[i], 0, 0).astype(tile.dtype)
            return carry

        lax.fori_loop(0, 3, body, 0)
        for i in range(3):
            tile_out(u, i).start()

    def step(n, carry):
        @pl.when(n < 4)
        def _():
            partial_pair(scatter, unit_grads, weights, block_rows, n, 1 - scatter.c, for_core)
            to_core(n).start()
            to_core(4 + n).start()
            partial_pair(scatter, unit_grads, weights, block_rows, n, scatter.c, held)
            to_core(n).wait_recv()
            scatter.side(n)

        @pl.when((n >= 4) & (n < 7))
        def _():
            to_core(n).wait_recv()
            scatter.line(n - 4)

        late = n // 4

        @pl.when((n % 2 == 1) | (n >= 4))
        def _():
            weight_tile((1 - late) * (n // 2) + late * (n - 2))

        return carry

    lax.fori_loop(0, 8, step, 0)
    to_core(7).wait_recv()
    scatter.last()
    outward = pltpu.make_async_copy(total, out_ref, local_sem.at[5])
    outward.start()
    for k in range(8):
        to_core(k).wait_send()
    scatter.finish()
    for u in (4, 5):
        for i in range(3):
            tile_out(u, i).wait()
    outward.wait()


def scatter_fsdp(parts):
    return lax.psum_scatter(jnp.concatenate(parts, axis=2), "fsdp", scatter_dimension=0, tiled=False).astype(jnp.float32)


def gather_through(block_ref, gathered, gathered_ref, send_sem, receive_sem, out_sem, prepare, compute):
    gather = Gather(block_ref, gathered, send_sem, receive_sem)
    z, x, c = gather.z, gather.x, gather.c
    _, block_rows, width = gathered.shape
    own = pltpu.make_async_copy(block_ref, gathered.at[gather.own], out_sem.at[8])
    own.start()
    greet_line(z, (gather.across, gather.other), gather.down, gather.up)
    gather.start()

    def out(number):
        at = pl.ds(number * 2, 2)
        return pltpu.make_async_copy(gathered.at[at], gathered_ref.at[at], out_sem.at[number])

    def step(n, carry):
        @pl.when(n == 2)
        def _():
            gather.line(2)
            gather.side(1)

        @pl.when(n == 4)
        def _():
            gather.line(3)
            gather.side(2)

        @pl.when(n == 6)
        def _():
            gather.side(3)

        dz = n // 4 * 2 + n % 2
        side = (x + n // 2) % 2
        zi = (z // 2 + dz // 2) % 2 * 2 + (z + dz) % 2
        number = zi * 2 + side
        gather.arrived(fsdp_index(zi, side, 1 - c))
        out(number).start()
        left = gathered[pl.ds(number * 2, 2)].reshape(2 * block_rows, width)
        compute(number, pl.ds(pl.multiple_of(number * 2 * block_rows, 2 * block_rows), 2 * block_rows), left)
        return carry

    gather.line(1)
    gather.side(0)
    own.wait()
    prepare()
    lax.fori_loop(0, 8, step, 0)
    gather.finish(waits=False)
    for number in range(8):
        out(number).wait()


GELU_SCALE = math.sqrt(2.0 / math.pi)
GELU_CUBE = 0.044715


def feed_first_kernel(
    block_ref, weights_ref, gathered_ref, gate_up_ref, hidden_ref,
    gathered, send_sem, receive_sem, out_sem, weights, gate_up, hidden, load_sem, gate_up_sem, hidden_sem,
):
    load = pltpu.make_async_copy(weights_ref.at[pl.ds(0, 2)], weights, load_sem.at[0])
    load.start()

    def outs(number, rows):
        return (
            pltpu.make_async_copy(gate_up.at[:, rows, :], gate_up_ref.at[:, rows, :], gate_up_sem.at[number]),
            pltpu.make_async_copy(hidden.at[rows, :], hidden_ref.at[rows, :], hidden_sem.at[number]),
        )

    def compute(number, rows, left):
        gate = contract(left, weights[0], 1, 0)
        gate_up[0, rows, :] = gate
        up = contract(left, weights[1], 1, 0)
        gate_up[1, rows, :] = up
        gate = gate_up[0, rows, :]
        curve = jnp.tanh(GELU_SCALE * (gate + GELU_CUBE * (gate * gate * gate)))
        hidden[rows, :] = (0.5 * gate * (1.0 + curve) * up).astype(hidden.dtype)
        for copy in outs(number, rows):
            copy.start()

    gather_through(block_ref, gathered, gathered_ref, send_sem, receive_sem, out_sem, load.wait, compute)
    pair_rows = hidden.shape[0] // 8
    for number in range(8):
        for copy in outs(number, pl.ds(number * pair_rows, pair_rows)):
            copy.wait()


def hidden_back_kernel(
    block_ref, weights_ref, gate_up_ref, gathered_ref, unit_grads_ref,
    gathered, send_sem, receive_sem, out_sem, weights, gate_up, unit_grads, load_sem, grads_sem,
):
    loads = [
        pltpu.make_async_copy(weights_ref.at[2], weights, load_sem.at[0]),
        pltpu.make_async_copy(gate_up_ref, gate_up, load_sem.at[1]),
    ]
    for copy in loads:
        copy.start()

    def prepare():
        for copy in loads:
            copy.wait()

    def out(number, rows):
        return pltpu.make_async_copy(unit_grads.at[:, rows, :], unit_grads_ref.at[:, rows, :], grads_sem.at[number])

    def compute(number, rows, left):
        hidden_grad = contract(left, weights[...], 1, 0)
        gate, up = gate_up[0, rows, :], gate_up[1, rows, :]
        square = gate * gate
        curve = jnp.tanh(GELU_SCALE * (gate + GELU_CUBE * (square * gate)))
        inner = GELU_SCALE * (1.0 + 3.0 * GELU_CUBE * square)
        slope = 0.5 * (1.0 + curve) + 0.5 * gate * (1.0 - curve * curve) * inner
        unit_grads[0, rows, :] = (hidden_grad * up * slope).astype(unit_grads.dtype)
        unit_grads[1, rows, :] = (hidden_grad * (0.5 * gate * (1.0 + curve))).astype(unit_grads.dtype)
        out(number, rows).start()

    gather_through(block_ref, gathered, gathered_ref, send_sem, receive_sem, out_sem, prepare, compute)
    pair_rows = unit_grads.shape[1] // 8
    for number in range(8):
        out(number, pl.ds(number * pair_rows, pair_rows)).wait()


def gather_scratch(size, block, kind):
    return [
        pltpu.VMEM((size,) + block, kind),
        pltpu.SemaphoreType.DMA((Gather.slots,)),
        pltpu.SemaphoreType.DMA((size,)),
        pltpu.SemaphoreType.DMA((9,)),
    ]


def feed_first(block, feed_full, collective_id):
    size = lax.axis_size("fsdp")
    tokens, width, units, kind = size * block.shape[0], block.shape[1], feed_full.shape[2], block.dtype
    if size != KERNEL_FSDP:
        rows = lax.all_gather(block, "fsdp", axis=0, tiled=True)
        gate, up = contract(rows, feed_full[0], 1, 0), contract(rows, feed_full[1], 1, 0)
        return rows, jnp.stack([gate, up]), gelu_product(gate, up).astype(kind)
    rows, gate_up, hidden = scratch_call(
        feed_first_kernel,
        (
            jax.ShapeDtypeStruct((size,) + block.shape, kind),
            jax.ShapeDtypeStruct((2, tokens, units), jnp.float32),
            jax.ShapeDtypeStruct((tokens, units), kind),
        ),
        [
            *gather_scratch(size, block.shape, kind),
            pltpu.VMEM((2, width, units), kind),
            pltpu.VMEM((2, tokens, units), jnp.float32),
            pltpu.VMEM((tokens, units), kind),
            pltpu.SemaphoreType.DMA((1,)),
            pltpu.SemaphoreType.DMA((8,)),
            pltpu.SemaphoreType.DMA((8,)),
        ],
        collective_id,
        block,
        feed_full,
    )
    return rows.reshape(tokens, width), gate_up, hidden


def hidden_back(block, feed_full, gate_up, collective_id):
    size = lax.axis_size("fsdp")
    tokens, width, units, kind = size * block.shape[0], block.shape[1], feed_full.shape[2], block.dtype
    if size != KERNEL_FSDP:
        rows = lax.all_gather(block, "fsdp", axis=0, tiled=True)
        unused_out, pullback = jax.vjp(gelu_product, gate_up[0], gate_up[1])
        gradients = pullback(contract(rows, feed_full[2], 1, 0))
        return rows, jnp.stack(gradients).astype(kind)
    rows, unit_grads = scratch_call(
        hidden_back_kernel,
        (
            jax.ShapeDtypeStruct((size,) + block.shape, kind),
            jax.ShapeDtypeStruct((2, tokens, units), kind),
        ),
        [
            *gather_scratch(size, block.shape, kind),
            pltpu.VMEM((width, units), kind),
            pltpu.VMEM((2, tokens, units), jnp.float32),
            pltpu.VMEM((2, tokens, units), kind),
            pltpu.SemaphoreType.DMA((2,)),
            pltpu.SemaphoreType.DMA((8,)),
        ],
        collective_id,
        block,
        feed_full,
        gate_up,
    )
    return rows.reshape(tokens, width), unit_grads


def partial_pair(scatter, units, weights, block_rows, j, core, target):
    amount, width, _ = weights.shape
    step = 3 * 256
    spots = [pl.ds(pl.multiple_of(scatter.index(k, core) * block_rows, block_rows), block_rows) for k in (j, 4 + j)]

    def body(d, carry):
        at = pl.ds(pl.multiple_of(d * step, step), step)
        sums = None
        for i in range(amount):
            left = jnp.concatenate([units[i, spot, :] for spot in spots], axis=0)
            part = contract(left, weights[i, at, :], 1, 1)
            sums = part if sums is None else sums + part
        sums = sums.astype(target.dtype)
        target[j, :, at] = sums[:block_rows]
        target[4 + j, :, at] = sums[block_rows:]
        return carry

    lax.fori_loop(0, width // step, body, 0)


def feed_last_kernel(
    hidden_ref, weights_ref, out_ref,
    held, from_core, from_across, from_below, from_above, total, send_sem, across_sem, below_sem, above_sem,
    core_send_sem, core_sem, local_sem, for_core, hidden, weights,
):
    scatter = Scatter(
        (held, from_core, from_across, from_below, from_above, total), (send_sem, across_sem, below_sem, above_sem)
    )
    loads = [
        pltpu.make_async_copy(hidden_ref, hidden.at[0], local_sem.at[0]),
        pltpu.make_async_copy(weights_ref.at[pl.ds(2, 1)], weights, local_sem.at[1]),
    ]
    for copy in loads:
        copy.start()
    greet_line(scatter.z, (scatter.across, scatter.other), scatter.down, scatter.up)
    for copy in loads:
        copy.wait()

    def to_core(k):
        return remote(for_core.at[k], from_core.at[k], core_send_sem.at[k], core_sem.at[k], scatter.other)

    def share(j, carry):
        partial_pair(scatter, hidden, weights, out_ref.shape[0], j, 1 - scatter.c, for_core)
        to_core(j).start()
        to_core(4 + j).start()
        partial_pair(scatter, hidden, weights, out_ref.shape[0], j, scatter.c, held)
        to_core(j).wait_recv()
        scatter.side(j)
        return carry

    def along(i, carry):
        to_core(4 + i).wait_recv()
        scatter.line(i)
        return carry

    lax.fori_loop(0, 4, share, 0)
    lax.fori_loop(0, 3, along, 0)
    to_core(7).wait_recv()
    scatter.last()
    outward = pltpu.make_async_copy(total, out_ref, local_sem.at[2])
    outward.start()
    for k in range(8):
        to_core(k).wait_send()
    scatter.finish()
    outward.wait()


def feed_last(hidden, feed_full, collective_id):
    size = lax.axis_size("fsdp")
    tokens, width, kind = hidden.shape[0], feed_full.shape[1], hidden.dtype
    block = (tokens // size, width)
    if size != KERNEL_FSDP:
        sums = contract(hidden, feed_full[2], 1, 1).astype(kind)
        return scatter_fsdp((sums.reshape((size,) + block),))
    return scratch_call(
        feed_last_kernel,
        jax.ShapeDtypeStruct(block, jnp.float32),
        [
            *Scatter.scratch(block, kind),
            pltpu.SemaphoreType.DMA((8,)),
            pltpu.SemaphoreType.DMA((8,)),
            pltpu.SemaphoreType.DMA((3,)),
            pltpu.VMEM((8,) + block, kind),
            pltpu.VMEM((1,) + hidden.shape, kind),
            pltpu.VMEM((1,) + feed_full.shape[1:], kind),
        ],
        collective_id,
        hidden,
        feed_full,
    )


def feed_backward(unit_grads, feed_full, feed_input, feed_grad_rows, hidden, collective_id):
    size = lax.axis_size("fsdp")
    kind = hidden.dtype
    tokens, width = feed_input.shape
    if size != KERNEL_FSDP:
        gate_grad, up_grad = unit_grads[0], unit_grads[1]
        sums = contract(gate_grad, feed_full[0], 1, 1) + contract(up_grad, feed_full[1], 1, 1)
        return (
            scatter_fsdp((sums.astype(kind).reshape(size, tokens // size, width),)),
            jnp.stack(
                [
                    contract(left, right, 0, 0).astype(kind)
                    for left, right in ((feed_input, gate_grad), (feed_input, up_grad), (feed_grad_rows, hidden))
                ]
            ),
        )
    block, units = (tokens // size, width), hidden.shape[1]
    tile_rows = width // 6

    def kernel(unit_grads_ref, weights_ref, input_ref, grad_ref, hidden_ref, *refs):
        backward_kernel(unit_grads_ref, weights_ref, (input_ref, grad_ref), hidden_ref, *refs)

    rows_grad, weight_grads = scratch_call(
        kernel,
        (jax.ShapeDtypeStruct(block, jnp.float32), jax.ShapeDtypeStruct((3, width, units), kind)),
        [
            *Scatter.scratch(block, kind),
            pltpu.SemaphoreType.DMA((8,)),
            pltpu.SemaphoreType.DMA((8,)),
            pltpu.SemaphoreType.DMA((6,)),
            pltpu.VMEM((8,) + block, kind),
            pltpu.VMEM((3, tokens, units), kind),
            pltpu.VMEM((2, width, units), kind),
            pltpu.VMEM((2, tokens, width), kind),
            pltpu.VMEM((2, 3, tile_rows, units), kind),
            pltpu.SemaphoreType.DMA((2, 3)),
        ],
        collective_id,
        unit_grads,
        feed_full,
        feed_input,
        feed_grad_rows,
        hidden,
    )
    return rows_grad, weight_grads


def exchange_kernel(block_ref, out_ref, send_sem, receive_sem):
    index, t = lax.axis_index("fsdp"), lax.axis_index("tp")
    partner = (index, 1 - t)
    greet((partner,))
    copy = remote(block_ref, out_ref, send_sem.at[0], receive_sem.at[0], partner)
    copy.start()
    copy.wait()


def exchange_tp(block, collective_id):
    if lax.axis_size("fsdp") != KERNEL_FSDP:
        return lax.ppermute(block, "tp", [(0, 1), (1, 0)])
    return scratch_call(
        exchange_kernel,
        jax.ShapeDtypeStruct(block.shape, block.dtype),
        [pltpu.SemaphoreType.DMA((1,)), pltpu.SemaphoreType.DMA((1,))],
        collective_id,
        block,
    )


def peer(z, x, c, k):
    kz, kx, kc = k // 4, (k // 2) % 2, k % 2
    high, low = z // 2, z % 2
    high = 1 - high if kz // 2 else high
    low = 1 - low if kz % 2 else low
    return fsdp_index(high * 2 + low, 1 - x if kx else x, 1 - c if kc else c)


MAIN = 2 * LANES
REST = LANES
FIRST_REST = KERNEL_FSDP * MAIN
UNITS = 2 * MAIN + REST


def main_of(owner):
    return pl.ds(pl.multiple_of(owner * MAIN, MAIN), MAIN)


def rest_of(z):
    return pl.ds(pl.multiple_of(FIRST_REST + z * REST, REST), REST)


def distribute_kernel(
    rows_ref, query_ref, key_ref, value_ref, output_ref, gain_ref, gate_ref, up_ref, down_ref,
    attention_ref, partner_ref, feed_ref,
    stage, feed, zeros,
    gather_send, gather_receive, local_sem, pair_rows_sem, send_sem, receive_sem, rest_send, rest_receive,
    on_send, on_receive, rest_on_send, rest_on_receive,
):
    z, x, c, t = place()
    own = fsdp_index(z, x, c)
    partner = (own, 1 - t)
    greet([(peer(z, x, c, k), t) for k in range(1, 16)] + [partner])
    rows_copy = remote(rows_ref, partner_ref, pair_rows_sem.at[0], pair_rows_sem.at[1], partner)
    rows_copy.start()
    loads, start = [], 0
    for i, ref in enumerate((query_ref, key_ref, value_ref, output_ref, gain_ref)):
        loads.append(pltpu.make_async_copy(ref, stage.at[:, pl.ds(start, ref.shape[1])], local_sem.at[i]))
        start += ref.shape[1]
    feed_loads = [
        pltpu.make_async_copy(ref, feed.at[i], local_sem.at[5 + i])
        for i, ref in enumerate((gate_ref, up_ref, down_ref))
    ]
    for copy in loads + feed_loads:
        copy.start()
    for copy in loads:
        copy.wait()
    gather = Gather(stage, attention_ref, gather_send, gather_receive)
    gather.start()
    keep = pltpu.make_async_copy(stage, attention_ref.at[own], local_sem.at[8])
    keep.start()
    for copy in feed_loads:
        copy.wait()

    def main_at(half, source):
        return feed_ref.at[:, source, :, pl.ds(pl.multiple_of(half * MAIN, MAIN), MAIN)]

    def rest_at(source):
        return feed_ref.at[:, source, :, pl.ds(2 * MAIN, REST)]

    takes_rest = (c == 0) & (x == t)

    def direct(k):
        to = peer(z, x, c, k)
        return remote(feed.at[:, :, main_of(to)], main_at(t, own), send_sem.at[k], receive_sem.at[k], (to, t))

    def rest(dz):
        to_z = peer(z, x, c, 4 * dz) // 4
        slot = 4 * dz + 2 * ((x + t) % 2) + c
        return remote(
            feed.at[:, :, rest_of(to_z)], rest_at(own), rest_send.at[dz], rest_receive.at[slot], (fsdp_index(to_z, t, 0), t)
        )

    def onward(k):
        at = main_at(t, peer(z, x, c, k))
        return remote(at if k else feed.at[:, :, main_of(own)], at, on_send.at[k], on_receive.at[k], partner)

    def rest_onward(k):
        at = rest_at(peer(z, x, c, k))
        return remote(at if k else feed.at[:, :, rest_of(z)], at, rest_on_send.at[k], rest_on_receive.at[k], partner)

    def send(dz):
        for k in range(4 * dz, 4 * dz + 4):
            if k:
                direct(k).start()
        if dz:
            rest(dz).start()
        else:

            @pl.when(jnp.logical_not(takes_rest))
            def _():
                rest(0).start()

    def pass_on(dz):
        for k in range(4 * dz, 4 * dz + 4):
            if k:
                direct(k).wait_recv()
            onward(k).start()

        @pl.when(takes_rest)
        def _():
            for k in range(4 * dz, 4 * dz + 4):
                if k:
                    remote(
                        feed.at[:, :, rest_of(0)], rest_at(own), rest_send.at[0], rest_receive.at[k], partner
                    ).wait_recv()
                rest_onward(k).start()

    send(0)
    send(1)
    keep_main = pltpu.make_async_copy(feed.at[:, :, main_of(own)], main_at(t, own), local_sem.at[9])
    keep_main.start()
    keep_rest = pltpu.make_async_copy(feed.at[:, :, rest_of(z)], rest_at(own), local_sem.at[10])

    @pl.when(takes_rest)
    def _():
        keep_rest.start()

    fills = [
        pltpu.make_async_copy(zeros, feed_ref.at[i, :, :, pl.ds(2 * MAIN, REST)], local_sem.at[11 + i])
        for i in range(3)
    ]

    @pl.when(c == 1)
    def _():
        zeros[...] = jnp.zeros_like(zeros)
        for copy in fills:
            copy.start()

    send(2)
    pass_on(0)
    pass_on(1)
    gather.line(1)
    gather.side(0)
    send(3)
    gather.line(2)
    gather.side(1)
    pass_on(2)
    gather.line(3)
    gather.side(2)
    pass_on(3)
    gather.side(3)
    gather.finish()
    rows_copy.wait()
    for k in range(16):
        onward(k).wait_recv()
        onward(k).wait_send()
        if k:
            direct(k).wait_send()

    @pl.when(jnp.logical_not(takes_rest))
    def _():
        rest(0).wait_send()

    for dz in (1, 2, 3):
        rest(dz).wait_send()

    @pl.when(takes_rest)
    def _():
        for k in range(16):
            rest_onward(k).wait_send()
        keep_rest.wait()

    @pl.when((c == 0) & (x != t))
    def _():
        for k in range(16):
            rest_onward(k).wait_recv()

    @pl.when(c == 1)
    def _():
        for copy in fills:
            copy.wait()

    keep.wait()
    keep_main.wait()


def distribute(rows, attention, gain_columns, feed, collective_id):
    size = lax.axis_size("fsdp")
    shard_rows, feed_width = feed[0].shape
    columns = sum(w.shape[1] for w in attention) + gain_columns.shape[1]
    if size != KERNEL_FSDP:
        halves = lax.all_to_all(pack_units(feed, size), "fsdp", split_axis=0, concat_axis=0, tiled=True)
        halves = lax.all_gather(halves, "tp", axis=0)
        halves = halves.reshape(halves.shape[0], size * shard_rows, halves.shape[-1])
        return (
            lax.all_gather(jnp.concatenate((*attention, gain_columns), axis=1), "fsdp", axis=0),
            lax.ppermute(rows, "tp", [(0, 1), (1, 0)]),
            jnp.stack(join_units(halves, feed_width, size, 3)),
        )
    kind = rows.dtype
    attention_full, partner_rows, feed_full = scratch_call(
        distribute_kernel,
        (
            jax.ShapeDtypeStruct((size, shard_rows, columns), kind),
            jax.ShapeDtypeStruct(rows.shape, kind),
            jax.ShapeDtypeStruct((3, size, shard_rows, UNITS), kind),
        ),
        [
            pltpu.VMEM((shard_rows, columns), kind),
            pltpu.VMEM((3, shard_rows, feed_width), kind),
            pltpu.VMEM((size, shard_rows, REST), kind),
            pltpu.SemaphoreType.DMA((Gather.slots,)),
            pltpu.SemaphoreType.DMA((size,)),
            pltpu.SemaphoreType.DMA((14,)),
            pltpu.SemaphoreType.DMA((2,)),
            pltpu.SemaphoreType.DMA((size,)),
            pltpu.SemaphoreType.DMA((size,)),
            pltpu.SemaphoreType.DMA((4,)),
            pltpu.SemaphoreType.DMA((size,)),
            pltpu.SemaphoreType.DMA((size,)),
            pltpu.SemaphoreType.DMA((size,)),
            pltpu.SemaphoreType.DMA((size,)),
            pltpu.SemaphoreType.DMA((size,)),
        ],
        collective_id,
        rows,
        *attention,
        gain_columns,
        *feed,
    )
    return attention_full, partner_rows, feed_full.reshape(3, size * shard_rows, UNITS)


def collect_kernel(
    parts_ref, projected_ref, output_ref, gain_ref, out_ref, attention_ref,
    held, received, rest_held, rest_received,
    local_sem, pair_send, pair_receive, rest_pair_send, rest_pair_receive, send_sem, receive_sem, rest_send, rest_receive,
    *scatter_refs,
):
    scatter = Scatter(scatter_refs[:6], scatter_refs[6:10])
    blocks = Blocks(scatter, (projected_ref, output_ref, gain_ref), *scatter_refs[10:13])
    blocks.load()
    z, x, c, t = place()
    own = fsdp_index(z, x, c)
    rows = out_ref.shape[1]
    partner = (own, 1 - t)
    parts = [parts_ref.at[i] for i in range(3)]
    order = (3, 2, 1, 0)
    takes_rest = (c == 0) & (x == t)
    gives_rest = (c == 0) & (x != t)

    def plane(dz):
        return pl.ds(peer(z, x, c, 4 * dz) // 4 * 4, 4)

    def half(which):
        return pl.ds(pl.multiple_of(which * MAIN, MAIN), MAIN)

    rest_columns = pl.ds(2 * MAIN, REST)

    def load(dz, i):
        return pltpu.make_async_copy(parts[i].at[plane(dz), :, half(t)], held.at[dz, i], local_sem.at[3 * dz + i])

    def rest_load(dz, i):
        return pltpu.make_async_copy(
            parts[i].at[plane(dz), :, rest_columns], rest_held.at[dz, i], local_sem.at[12 + 3 * dz + i]
        )

    def pair(dz, i):
        slot = 3 * dz + i
        return remote(
            parts[i].at[plane(dz), :, half(1 - t)], received.at[dz, i], pair_send.at[slot], pair_receive.at[slot], partner
        )

    def rest_pair(dz, i):
        slot = 3 * dz + i
        return remote(
            parts[i].at[plane(dz), :, rest_columns],
            rest_received.at[dz, i],
            rest_pair_send.at[slot],
            rest_pair_receive.at[slot],
            partner,
        )

    def spot(k):
        return peer(z, x, c, k) % 4

    def direct(k):
        return remote(
            held.at[k // 4, :, spot(k)], out_ref.at[:, :, main_of(own)], send_sem.at[k], receive_sem.at[k], (peer(z, x, c, k), t)
        )

    def rest_direct(k):
        return remote(
            rest_held.at[k // 4, :, spot(k)],
            out_ref.at[:, :, rest_of(z)],
            rest_send.at[k],
            rest_receive.at[z],
            (peer(z, x, c, k), t),
        )

    def add(target, source):
        def body(j, carry):
            i, at = j // 4, j % 4
            total = target[i, at].astype(jnp.float32) + source[i, at].astype(jnp.float32)
            target[i, at] = total.astype(target.dtype)
            return carry

        lax.fori_loop(0, 12, body, 0)

    for dz in order:
        for i in range(3):
            load(dz, i).start()

    @pl.when(takes_rest)
    def _():
        for dz in order:
            for i in range(3):
                rest_load(dz, i).start()

    greet([(peer(z, x, c, k), t) for k in range(1, 16)] + [partner])
    blocks.send()
    for dz in order:
        for i in range(3):
            pair(dz, i).start()

        @pl.when(gives_rest)
        def _():
            for i in range(3):
                rest_pair(dz, i).start()

    def pass_on(dz):
        for i in range(3):
            load(dz, i).wait()
            pair(dz, i).wait_recv()
        add(held.at[dz], received.at[dz])
        for k in range(4 * dz, 4 * dz + 4):
            if k:
                direct(k).start()

        @pl.when(takes_rest)
        def _():
            for i in range(3):
                rest_load(dz, i).wait()
                rest_pair(dz, i).wait_recv()
            add(rest_held.at[dz], rest_received.at[dz])
            for k in range(4 * dz, 4 * dz + 4):
                if k:
                    rest_direct(k).start()

    def line(i):
        blocks.both(4 + i)
        scatter.line(i)

    def share(i, carry):
        blocks.both(i)
        scatter.side(i)
        return carry

    lax.fori_loop(0, 4, share, 0)
    pass_on(3)
    line(0)
    pass_on(2)
    line(1)
    pass_on(1)
    line(2)
    pass_on(0)
    blocks.both(7)
    scatter.last()
    outward = pltpu.make_async_copy(scatter.total, attention_ref, local_sem.at[26])
    outward.start()
    keep = pltpu.make_async_copy(held.at[0, :, spot(0)], out_ref.at[:, :, main_of(own)], local_sem.at[24])
    keep.start()
    keep_rest = pltpu.make_async_copy(rest_held.at[0, :, spot(0)], out_ref.at[:, :, rest_of(z)], local_sem.at[25])

    @pl.when(takes_rest)
    def _():
        keep_rest.start()

    for k in range(1, 16):
        direct(k).wait_recv()

    for dz in range(4):
        from_z = peer(z, x, c, 4 * dz) // 4

        def arrived():
            remote(
                rest_held.at[0, :, 0], out_ref.at[:, :, rest_of(from_z)], rest_send.at[0], rest_receive.at[from_z], partner
            ).wait_recv()

        if dz:
            arrived()
        else:

            @pl.when(jnp.logical_not(takes_rest))
            def _():
                arrived()

    for k in range(1, 16):
        direct(k).wait_send()
    for dz in order:
        for i in range(3):
            pair(dz, i).wait_send()

    @pl.when(gives_rest)
    def _():
        for dz in order:
            for i in range(3):
                rest_pair(dz, i).wait_send()

    @pl.when(takes_rest)
    def _():
        for k in range(1, 16):
            rest_direct(k).wait_send()
        keep_rest.wait()

    blocks.finish()
    scatter.finish()
    keep.wait()
    outward.wait()


def collect(gradients, feed_width, attention_parts, collective_id):
    size, pairs = lax.axis_size("fsdp"), lax.axis_size("tp")
    shard_rows = gradients.shape[1] // size
    if size != KERNEL_FSDP:
        packed = part_units([gradients[i] for i in range(3)], feed_width, size, pairs)
        mine = lax.psum_scatter(packed, "tp", scatter_dimension=0, tiled=False)
        mine = mine.reshape(size, shard_rows, mine.shape[-1])
        mine = lax.all_to_all(mine, "fsdp", split_axis=0, concat_axis=0, tiled=True)
        feed = [g.astype(jnp.float32) for g in unpack_units(mine, feed_width, 3)]
        return feed, scatter_fsdp(attention_parts)
    kind = gradients.dtype
    main, rest = (4, 3, 4, shard_rows, MAIN), (4, 3, 4, shard_rows, REST)
    block = (shard_rows, sum(part.shape[2] for part in attention_parts))
    out, attention = scratch_call(
        collect_kernel,
        (
            jax.ShapeDtypeStruct((3, shard_rows, feed_width), kind),
            jax.ShapeDtypeStruct(block, jnp.float32),
        ),
        [
            pltpu.VMEM(main, kind),
            pltpu.VMEM(main, kind),
            pltpu.VMEM(rest, kind),
            pltpu.VMEM(rest, kind),
            pltpu.SemaphoreType.DMA((27,)),
            pltpu.SemaphoreType.DMA((12,)),
            pltpu.SemaphoreType.DMA((12,)),
            pltpu.SemaphoreType.DMA((12,)),
            pltpu.SemaphoreType.DMA((12,)),
            pltpu.SemaphoreType.DMA((size,)),
            pltpu.SemaphoreType.DMA((size,)),
            pltpu.SemaphoreType.DMA((size,)),
            pltpu.SemaphoreType.DMA((4,)),
            *Scatter.scratch(block, kind),
            *[pltpu.SemaphoreType.DMA((24,)) for _ in range(3)],
        ],
        collective_id,
        gradients.reshape(3, size, shard_rows, UNITS),
        *attention_parts,
    )
    return [out[i].astype(jnp.float32) for i in range(3)], attention


def contract_last(left_rows, right_rows):
    return lax.dot_general(
        left_rows, right_rows, (((1,), (1,)), ((), ())), preferred_element_type=jnp.float32
    )


def contract_first(left_rows, right_rows):
    return lax.dot_general(
        left_rows, right_rows, (((0,), (0,)), ((), ())), preferred_element_type=jnp.float32
    )


def normalize_parts(value_rows):
    inverse = lax.rsqrt(jnp.mean(value_rows * value_rows, axis=-1, keepdims=True) + EPSILON)
    return (value_rows * inverse, inverse)


def norm_backward(unit_rows, inverse, norm_gain, upstream):
    scaled = upstream * norm_gain
    return inverse * (scaled - unit_rows * jnp.mean(scaled * unit_rows, axis=-1, keepdims=True))


def layout(lengths_row, row_index):
    segment_ends = jnp.cumsum(lengths_row)
    segment_starts = segment_ends - lengths_row
    segment = jnp.sum((row_index[:, None] >= segment_ends[None, :]).astype(jnp.int32), axis=1)
    onehot = segment[:, None] == jnp.arange(lengths_row.shape[0], dtype=jnp.int32)[None, :]
    segment_begin = jnp.sum(jnp.where(onehot, segment_starts[None, :], 0), axis=1)
    prompt_shift = jnp.where(segment > 0, lengths_row[0], 0)
    return (segment, row_index - segment_begin + prompt_shift)


def rotary_tables(position):
    frequency = jnp.exp(
        jnp.arange(HEAD_SIZE // 2, dtype=jnp.float32) * (-2.0 * math.log(10000.0) / HEAD_SIZE)
    )
    angles = position.astype(jnp.float32)[:, None] * frequency[None, :]
    return (jnp.cos(angles), jnp.sin(angles))


def apply_rotary(value_rows, cosine_lookup, sine_lookup):
    half_width = value_rows.shape[-1] // 2
    first_half = value_rows[..., :half_width]
    second_half = value_rows[..., half_width:]
    cosine_part = cosine_lookup[:, None, :]
    sine_part = sine_lookup[:, None, :]
    return jnp.concatenate(
        [
            first_half * cosine_part - second_half * sine_part,
            second_half * cosine_part + first_half * sine_part,
        ],
        axis=-1,
    )


def unrotate(value_rows, cosine_lookup, sine_lookup):
    half_width = value_rows.shape[-1] // 2
    first_half = value_rows[..., :half_width]
    second_half = value_rows[..., half_width:]
    cosine_part = cosine_lookup[:, None, :]
    sine_part = sine_lookup[:, None, :]
    return jnp.concatenate(
        [
            first_half * cosine_part + second_half * sine_part,
            second_half * cosine_part - first_half * sine_part,
        ],
        axis=-1,
    )


def visible(segment, row_index):
    same_segment = (segment[:, None] == segment[None, :]) & (
        row_index[None, :] <= row_index[:, None]
    )
    from_prompt = (segment[None, :] == 0) & (segment[:, None] > 0)
    return same_segment | from_prompt


def masked_scores(rotated_query, rotated_key, visible_mask):
    raw_scores = jnp.einsum(
        "qgrd,kgd->grqk", rotated_query, rotated_key, preferred_element_type=jnp.float32
    )
    tanh_value = jnp.tanh(raw_scores * HEAD_SIZE ** (-0.5) / SOFTCAP)
    return (jnp.where(visible_mask[None, None], SOFTCAP * tanh_value, NEGATIVE), tanh_value)


def gelu_product(gate_value, up_value):
    return jax.nn.gelu(gate_value, approximate=True) * up_value


def split_columns(width, size):
    main = width // size // LANES * LANES
    return main, width // size - main


def pack_units(weights, size):
    rows, width = weights[0].shape
    main, rest = split_columns(width, size)
    pieces = []
    if main:
        pieces += [
            jnp.transpose(w[:, : main * size].reshape(rows, size, main), (1, 0, 2)) for w in weights
        ]
    if rest:
        pieces += [
            jnp.transpose(w[:, main * size :].reshape(rows, size, rest), (1, 0, 2)) for w in weights
        ]
    packed = jnp.concatenate(pieces, axis=2)
    return jnp.pad(packed, ((0, 0), (0, 0), (0, -packed.shape[2] % LANES)))


def unpack_units(packed, width, amount):
    size, rows, _ = packed.shape
    main, rest = split_columns(width, size)
    arrays = []
    for i in range(amount):
        pieces = []
        if main:
            piece = packed[:, :, i * main : (i + 1) * main]
            pieces.append(jnp.transpose(piece, (1, 0, 2)).reshape(rows, size * main))
        if rest:
            start = amount * main + i * rest
            piece = packed[:, :, start : start + rest]
            pieces.append(jnp.transpose(piece, (1, 0, 2)).reshape(rows, size * rest))
        arrays.append(jnp.concatenate(pieces, axis=1))
    return arrays


def join_units(halves, width, size, amount):
    main, rest = split_columns(width, size)
    arrays = []
    for i in range(amount):
        start = amount * main + i * rest
        pieces = [half[:, i * main : (i + 1) * main] for half in halves]
        pieces += [half[:, start : start + rest] for half in halves]
        joined = jnp.concatenate(pieces, axis=1)
        arrays.append(jnp.pad(joined, ((0, 0), (0, -joined.shape[1] % LANES))))
    return arrays


def part_units(arrays, width, size, pairs):
    main, rest = split_columns(width, size)
    halves = []
    for t in range(pairs):
        pieces = [array[:, t * main : (t + 1) * main] for array in arrays]
        start = pairs * main + t * rest
        pieces += [array[:, start : start + rest] for array in arrays]
        packed = jnp.concatenate(pieces, axis=1)
        halves.append(jnp.pad(packed, ((0, 0), (0, -packed.shape[1] % LANES))))
    return jnp.stack(halves)


def shards(
    block_input,
    lengths,
    attention_norm_gain,
    attention_post_gain,
    feedforward_norm_gain,
    feedforward_post_gain,
    query_weight,
    key_weight,
    value_weight,
    output_weight,
    gate_weight,
    up_weight,
    down_weight,
    output_cotangent,
):
    low = jnp.bfloat16
    size, pairs = lax.axis_size("fsdp"), lax.axis_size("tp")
    rows_local, width = block_input.shape
    shard_rows, feed_width = gate_weight.shape
    query_width, key_width = query_weight.shape[1], key_weight.shape[1]
    output_start = query_width + 2 * key_width
    gain_start = output_start + query_width
    grouped_rows = rows_local * pairs

    gain_columns = jnp.stack(
        [attention_norm_gain, attention_post_gain, feedforward_norm_gain, feedforward_post_gain],
        axis=1,
    )
    attention_full, other_input, feed_full = distribute(
        block_input,
        (query_weight, key_weight, value_weight, output_weight),
        jnp.pad(gain_columns, ((0, 0), (0, LANES - 4))),
        (gate_weight, up_weight, down_weight),
        1,
    )
    attention_full = attention_full.reshape(size * shard_rows, gain_start + LANES)
    gains = jnp.transpose(attention_full[:, gain_start : gain_start + 4]).astype(jnp.float32)
    gain_one, gain_two, gain_three, gain_four = gains[0], gains[1], gains[2], gains[3]

    row_index = (
        jnp.arange(grouped_rows, dtype=jnp.int32) + lax.axis_index("tp") * rows_local
    ) % grouped_rows
    segment, position = layout(lengths[0], row_index)
    cosine_lookup, sine_lookup = rotary_tables(position)
    visible_mask = visible(segment, row_index)
    residual_both = jnp.concatenate([block_input, other_input], axis=0).astype(jnp.float32)
    unit_one_both, inverse_one_both = normalize_parts(residual_both)
    residual = residual_both[:rows_local]
    unit_one, inverse_one = unit_one_both[:rows_local], inverse_one_both[:rows_local]
    normed = (unit_one_both * gain_one).astype(low)
    projected = jnp.dot(
        normed, attention_full[:, :output_start], preferred_element_type=jnp.float32
    )
    query_raw = projected[:, :query_width]
    key_raw = projected[:, query_width : query_width + key_width]
    value_raw = projected[:, query_width + key_width :]
    heads_local = query_width // HEAD_SIZE
    kv_local = key_width // HEAD_SIZE
    repeat_heads = heads_local // kv_local
    rotated_query = apply_rotary(
        query_raw.reshape(grouped_rows, heads_local, HEAD_SIZE), cosine_lookup, sine_lookup
    ).astype(low)
    rotated_query = rotated_query.reshape(grouped_rows, kv_local, repeat_heads, HEAD_SIZE)
    rotated_key = apply_rotary(
        key_raw.reshape(grouped_rows, kv_local, HEAD_SIZE), cosine_lookup, sine_lookup
    ).astype(low)
    value_reduced = value_raw.astype(low).reshape(grouped_rows, kv_local, HEAD_SIZE)
    capped, tanh_value = masked_scores(rotated_query, rotated_key, visible_mask)
    row_peak = jnp.max(capped, axis=-1, keepdims=True)
    exponentials = jnp.exp(capped - row_peak)
    softmax_probs = exponentials / jnp.sum(exponentials, axis=-1, keepdims=True)
    probs_low = softmax_probs.astype(low)
    mixed_heads = jnp.einsum(
        "grqk,kgd->qgrd", probs_low, value_reduced, preferred_element_type=jnp.float32
    )
    attended = mixed_heads.reshape(grouped_rows, heads_local * HEAD_SIZE).astype(low)
    output_full = attention_full[:, output_start:gain_start]
    branch_parts = contract_last(attended, output_full)
    branch_one = branch_parts[:rows_local] + exchange_tp(
        branch_parts[rows_local:].astype(low), 4
    ).astype(jnp.float32)
    unit_two, inverse_two = normalize_parts(branch_one)
    middle = residual + unit_two * gain_two
    unit_three, inverse_three = normalize_parts(middle)

    feed_input, gate_up, hidden = feed_first((unit_three * gain_three).astype(low), feed_full, 5)
    branch_two = feed_last(hidden, feed_full, 6)
    unit_four, inverse_four = normalize_parts(branch_two)
    block_output = (middle + unit_four * gain_four).astype(low)
    upstream = output_cotangent.astype(jnp.float32)
    gain_four_grad = jnp.sum(upstream * unit_four, axis=0)
    branch_two_grad = norm_backward(unit_four, inverse_four, gain_four, upstream).astype(low)
    feed_grad_rows, unit_grads = hidden_back(branch_two_grad, feed_full, gate_up, 7)
    normed_three_grad, feed_grads = feed_backward(
        unit_grads, feed_full, feed_input, feed_grad_rows, hidden, 8
    )
    gain_three_grad = jnp.sum(normed_three_grad * unit_three, axis=0)
    middle_grad = upstream + norm_backward(unit_three, inverse_three, gain_three, normed_three_grad)
    gain_two_grad = jnp.sum(middle_grad * unit_two, axis=0)
    branch_one_grad = norm_backward(unit_two, inverse_two, gain_two, middle_grad).astype(low)
    attention_grad_rows = jnp.concatenate(
        [branch_one_grad, exchange_tp(branch_one_grad, 10)], axis=0
    )
    mixed_grad = jnp.dot(
        attention_grad_rows, output_full, preferred_element_type=jnp.float32
    ).astype(low)
    mixed_grad = mixed_grad.reshape(grouped_rows, kv_local, repeat_heads, HEAD_SIZE)
    value_grad = jnp.einsum(
        "grqk,qgrd->kgd", probs_low, mixed_grad, preferred_element_type=jnp.float32
    )
    probs_grad = jnp.einsum(
        "qgrd,kgd->grqk", mixed_grad, value_reduced, preferred_element_type=jnp.float32
    )
    score_grad = softmax_probs * (
        probs_grad - jnp.sum(softmax_probs * probs_grad, axis=-1, keepdims=True)
    )
    raw_grad = (score_grad * (1.0 - tanh_value * tanh_value) * HEAD_SIZE ** (-0.5)).astype(low)
    query_grad = jnp.einsum(
        "grqk,kgd->qgrd", raw_grad, rotated_key, preferred_element_type=jnp.float32
    )
    key_grad = jnp.einsum(
        "grqk,qgrd->kgd", raw_grad, rotated_query, preferred_element_type=jnp.float32
    )
    query_grad = unrotate(
        query_grad.reshape(grouped_rows, heads_local, HEAD_SIZE), cosine_lookup, sine_lookup
    )
    key_grad = unrotate(key_grad, cosine_lookup, sine_lookup)
    projected_grad = jnp.concatenate(
        [
            query_grad.reshape(grouped_rows, heads_local * HEAD_SIZE).astype(low),
            key_grad.reshape(grouped_rows, kv_local * HEAD_SIZE).astype(low),
            value_grad.reshape(grouped_rows, kv_local * HEAD_SIZE).astype(low),
        ],
        axis=1,
    )
    input_parts = contract_last(projected_grad, attention_full[:, :output_start])

    gain_grads = jnp.stack(
        [
            jnp.sum(input_parts * unit_one_both, axis=0),
            gain_two_grad,
            gain_three_grad,
            gain_four_grad,
        ]
    )
    sent = jnp.concatenate(
        [input_parts[rows_local:].astype(low), jnp.pad(gain_grads, ((0, 12), (0, 0))).astype(low)]
    )
    received = exchange_tp(sent, 11).astype(jnp.float32)
    normed_one_grad = input_parts[:rows_local] + received[:rows_local]
    gain_grads = gain_grads + received[rows_local : rows_local + 4]
    input_gradient = middle_grad + norm_backward(unit_one, inverse_one, gain_one, normed_one_grad)

    (gate_weight_grad, up_weight_grad, down_weight_grad), attention_grads = collect(
        feed_grads,
        feed_width,
        [
            part.astype(low).reshape(size, shard_rows, part.shape[1])
            for part in (
                contract_first(normed, projected_grad),
                contract_first(attention_grad_rows, attended),
                jnp.pad(jnp.transpose(gain_grads), ((0, 0), (0, LANES - 4))),
            )
        ],
        9,
    )
    gain_shards = jnp.transpose(attention_grads[:, gain_start : gain_start + 4])
    return (
        block_output,
        input_gradient,
        gain_shards[0],
        gain_shards[1],
        gain_shards[2],
        gain_shards[3],
        attention_grads[:, :query_width],
        attention_grads[:, query_width : query_width + key_width],
        attention_grads[:, query_width + key_width : output_start],
        attention_grads[:, output_start:gain_start],
        gate_weight_grad,
        up_weight_grad,
        down_weight_grad,
    )


def solution(mesh):
    placed = (
        P(("fsdp", "tp"), None),
        P("fsdp", None),
        P("fsdp"),
        P("fsdp"),
        P("fsdp"),
        P("fsdp"),
        P("fsdp", "tp"),
        P("fsdp", "tp"),
        P("fsdp", "tp"),
        P("fsdp", "tp"),
        P("fsdp", "tp"),
        P("fsdp", "tp"),
        P("fsdp", "tp"),
        P(("fsdp", "tp"), None),
    )
    return jax.shard_map(
        shards,
        mesh=mesh,
        in_specs=placed,
        out_specs=(
            P(("fsdp", "tp"), None),
            P(("fsdp", "tp"), None),
            P("fsdp"),
            P("fsdp"),
            P("fsdp"),
            P("fsdp"),
            P("fsdp", "tp"),
            P("fsdp", "tp"),
            P("fsdp", "tp"),
            P("fsdp", "tp"),
            P("fsdp", "tp"),
            P("fsdp", "tp"),
            P("fsdp", "tp"),
        ),
        check_vma=False,
    )
```

```python
import functools
import math

import jax
import jax.numpy as jnp
from jax import lax
from jax.experimental import pallas as pl
from jax.experimental.pallas import tpu as pltpu
from jax.sharding import PartitionSpec as P

HEAD_SIZE = 256
MESH = pl.DeviceIdType.MESH
ANY = pl.BlockSpec(memory_space=pl.ANY)
LANES = 128

EPSILON = 1e-06
SOFTCAP = 50.0
NEGATIVE = -1e30

KERNEL_FSDP = 16


def place():
    index = lax.axis_index("fsdp")
    return index // 4, (index // 2) % 2, index % 2, lax.axis_index("tp")


def fsdp_index(z, x, c):
    return (z * 2 + x) * 2 + c


def remote(source, target, send_sem, receive_sem, device):
    return pltpu.make_async_remote_copy(
        src_ref=source,
        dst_ref=target,
        send_sem=send_sem,
        recv_sem=receive_sem,
        device_id=device,
        device_id_type=MESH,
    )


def greet(devices):
    barrier = pltpu.get_barrier_semaphore()
    for device in devices:
        pl.semaphore_signal(barrier, inc=1, device_id=device, device_id_type=MESH)
    pl.semaphore_wait(barrier, len(devices))


def greet_line(z, devices, down, up):
    barrier = pltpu.get_barrier_semaphore()
    for device in devices:
        pl.semaphore_signal(barrier, inc=1, device_id=device, device_id_type=MESH)

    @pl.when(z > 0)
    def _():
        pl.semaphore_signal(barrier, inc=1, device_id=down, device_id_type=MESH)

    @pl.when(z < 3)
    def _():
        pl.semaphore_signal(barrier, inc=1, device_id=up, device_id_type=MESH)

    pl.semaphore_wait(barrier, len(devices) + (z + 2) // 3 + (5 - z) // 3)


class Gather:
    slots = 29

    def __init__(self, block, out_ref, send_sem, receive_sem):
        self.block, self.out, self.send_sem, self.receive_sem = block, out_ref, send_sem, receive_sem
        self.z, self.x, self.c, t = place()
        z, x, c = self.z, self.x, self.c
        self.own = fsdp_index(z, x, c)
        self.down, self.up = (fsdp_index(z - 1, x, c), t), (fsdp_index(z + 1, x, c), t)
        self.across, self.other = (fsdp_index(z, 1 - x, c), t), (fsdp_index(z, x, 1 - c), t)

    def copy(self, source, index, slot, device):
        return remote(source, self.out.at[index], self.send_sem.at[slot], self.receive_sem.at[index], device)

    def relay(self, index, slot, device):
        self.copy(self.out.at[index], index, slot, device).start()

    def arrived(self, index):
        self.copy(self.block, index, 0, self.other).wait_recv()

    def sent(self, slot):
        self.copy(self.block, self.own, slot, self.other).wait_send()

    def start(self):
        @pl.when(self.z < 3)
        def _():
            self.copy(self.block, self.own, 0, self.up).start()

        @pl.when(self.z > 0)
        def _():
            self.copy(self.block, self.own, 1, self.down).start()

        self.copy(self.block, self.own, 2, self.across).start()
        self.copy(self.block, self.own, 3, self.other).start()

    def line(self, d):
        z, x, c = self.z, self.x, self.c

        @pl.when(z >= d)
        def _():
            index = fsdp_index(z - d, x, c)
            base = 4 + 3 * (d - 1)
            self.arrived(index)

            @pl.when(z < 3)
            def _():
                self.relay(index, base, self.up)

            self.relay(index, base + 1, self.across)
            self.relay(index, base + 2, self.other)

        @pl.when(z + d <= 3)
        def _():
            index = fsdp_index(z + d, x, c)
            base = 13 + 3 * (d - 1)
            self.arrived(index)

            @pl.when(z > 0)
            def _():
                self.relay(index, base, self.down)

            self.relay(index, base + 1, self.across)
            self.relay(index, base + 2, self.other)

    def side(self, d):
        z, x, c = self.z, self.x, self.c
        if d == 0:
            index = fsdp_index(z, 1 - x, c)
            self.arrived(index)
            self.relay(index, 22, self.other)
            return

        @pl.when(z >= d)
        def _():
            index = fsdp_index(z - d, 1 - x, c)
            self.arrived(index)
            self.relay(index, 22 + d, self.other)

        @pl.when(z + d <= 3)
        def _():
            index = fsdp_index(z + d, 1 - x, c)
            self.arrived(index)
            self.relay(index, 25 + d, self.other)

    def finish(self, waits=True):
        z = self.z
        if waits:
            for zi in range(4):
                for xi in range(2):
                    self.arrived(fsdp_index(zi, xi, 1 - self.c))

        @pl.when(z < 3)
        def _():
            self.sent(0)

        @pl.when(z > 0)
        def _():
            self.sent(1)

        for slot in (2, 3, 22):
            self.sent(slot)
        for d in (1, 2, 3):

            @pl.when(z >= d)
            def _():
                base = 4 + 3 * (d - 1)

                @pl.when(z < 3)
                def _():
                    self.sent(base)

                for slot in (base + 1, base + 2, 22 + d):
                    self.sent(slot)

            @pl.when(z + d <= 3)
            def _():
                base = 13 + 3 * (d - 1)

                @pl.when(z > 0)
                def _():
                    self.sent(base)

                for slot in (base + 1, base + 2, 25 + d):
                    self.sent(slot)


def scratch_call(kernel, outputs, scratch, collective_id, *operands):
    return pl.pallas_call(
        kernel,
        out_shape=outputs,
        in_specs=[ANY] * len(operands),
        out_specs=jax.tree.map(lambda _: ANY, outputs),
        scratch_shapes=scratch,
        compiler_params=pltpu.CompilerParams(
            collective_id=collective_id, has_side_effects=True, vmem_limit_bytes=60 * 1024 * 1024
        ),
    )(*operands)


def add_rows(rows, step, target, *sources):
    def body(i, carry):
        at = pl.ds(pl.multiple_of(i * step, step), step)
        total = sources[0][at, :].astype(jnp.float32)
        for source in sources[1:]:
            total = total + source[at, :].astype(jnp.float32)
        target[at, :] = total.astype(target.dtype)
        return carry

    lax.fori_loop(0, rows // step, body, 0)


class Scatter:
    def __init__(self, buffers, semaphores):
        self.held, self.from_core, self.from_across, self.from_below, self.from_above, self.total = buffers
        self.send_sem, self.across_sem, self.below_sem, self.above_sem = semaphores
        self.z, self.x, self.c, t = place()
        z, x, c = self.z, self.x, self.c
        self.rows = self.total.shape[0]
        self.down, self.up = (fsdp_index(z - 1, x, c), t), (fsdp_index(z + 1, x, c), t)
        self.across, self.other = (fsdp_index(z, 1 - x, c), t), (fsdp_index(z, x, 1 - c), t)

    def target(self, i):
        half = self.z // 2
        mirrored = self.z + half * (3 - 2 * self.z)
        base = 3 - i + mirrored * (i // 2) * (2 * (i % 2) - 1)
        return base + half * (3 - 2 * base)

    def index(self, k, core):
        return fsdp_index(self.target(k % 4), (self.x + 1 - k // 4) % 2, core)

    def add(self, target, *sources):
        add_rows(self.rows, 16, target, *sources)

    def over(self, i):
        return remote(
            self.held.at[i], self.from_across.at[i], self.send_sem.at[3 + i], self.across_sem.at[i], self.across
        )

    def going_up(self, i, target):
        return remote(
            self.held.at[4 + i], self.from_below.at[target], self.send_sem.at[i], self.below_sem.at[target], self.up
        )

    def going_down(self, i, target):
        return remote(
            self.held.at[4 + i], self.from_above.at[target], self.send_sem.at[i], self.above_sem.at[target], self.down
        )

    def side(self, i):
        self.add(self.held.at[i], self.held.at[i], self.from_core.at[i])
        self.over(i).start()

    def line(self, i):
        z, target = self.z, self.target(i)
        held = self.held.at[4 + i]
        sources = (held, self.from_core.at[4 + i], self.from_across.at[i])
        self.over(i).wait_recv()

        @pl.when(target > z)
        def _():
            @pl.when(z > 0)
            def _():
                self.going_up(i, target).wait_recv()
                self.add(held, *sources, self.from_below.at[target])

            @pl.when(z == 0)
            def _():
                self.add(held, *sources)

            self.going_up(i, target).start()

        @pl.when(target < z)
        def _():
            @pl.when(z < 3)
            def _():
                self.going_down(i, target).wait_recv()
                self.add(held, *sources, self.from_above.at[target])

            @pl.when(z == 3)
            def _():
                self.add(held, *sources)

            self.going_down(i, target).start()

    def last(self):
        z = self.z
        self.over(3).wait_recv()
        self.add(self.total, self.held.at[7], self.from_core.at[7], self.from_across.at[3])

        @pl.when(z > 0)
        def _():
            self.going_up(0, z).wait_recv()
            self.add(self.total, self.total, self.from_below.at[z])

        @pl.when(z < 3)
        def _():
            self.going_down(0, z).wait_recv()
            self.add(self.total, self.total, self.from_above.at[z])

    def finish(self):
        for i in range(4):
            self.over(i).wait_send()
        for i in range(3):
            self.going_up(i, 0).wait_send()

    @staticmethod
    def scratch(block, kind):
        return [
            *[pltpu.VMEM((amount,) + block, kind) for amount in (8, 8, 4, 4, 4)],
            pltpu.VMEM(block, jnp.float32),
            *[pltpu.SemaphoreType.DMA((amount,)) for amount in (7, 4, 4, 4)],
        ]


class Blocks:
    def __init__(self, scatter, parts_refs, core_send_sem, core_sem, local_sem):
        self.scatter, self.parts = scatter, []
        self.core_send_sem, self.core_sem, self.local_sem = core_send_sem, core_sem, local_sem
        start = 0
        for ref in parts_refs:
            self.parts.append((ref, pl.ds(start, ref.shape[2])))
            start += ref.shape[2]

    def local(self, k):
        index = self.scatter.index(k, self.scatter.c)
        return [
            pltpu.make_async_copy(
                ref.at[index], self.scatter.held.at[k, :, at], self.local_sem.at[k * len(self.parts) + i]
            )
            for i, (ref, at) in enumerate(self.parts)
        ]

    def to_core(self, k):
        index = self.scatter.index(k, 1 - self.scatter.c)
        return [
            remote(
                ref.at[index],
                self.scatter.from_core.at[k, :, at],
                self.core_send_sem.at[k * len(self.parts) + i],
                self.core_sem.at[k * len(self.parts) + i],
                self.scatter.other,
            )
            for i, (ref, at) in enumerate(self.parts)
        ]

    def load(self):
        for k in range(8):
            for copy in self.local(k):
                copy.start()

    def send(self):
        for k in range(8):
            for copy in self.to_core(k):
                copy.start()

    def both(self, k):
        for copy in self.local(k):
            copy.wait()
        for copy in self.to_core(k):
            copy.wait_recv()

    def finish(self):
        for k in range(8):
            for copy in self.to_core(k):
                copy.wait_send()


def contract(left, right, left_dim, right_dim):
    return lax.dot_general(
        left, right, (((left_dim,), (right_dim,)), ((), ())), preferred_element_type=jnp.float32
    )


def backward_kernel(
    unit_grads_ref, weights_ref, rows_ref, hidden_ref, out_ref, weight_grads_ref,
    held, from_core, from_across, from_below, from_above, total, send_sem, across_sem, below_sem, above_sem,
    core_send_sem, core_sem, local_sem, for_core, unit_grads, weights, rows, tile, tile_sem,
):
    scatter = Scatter(
        (held, from_core, from_across, from_below, from_above, total), (send_sem, across_sem, below_sem, above_sem)
    )
    block_rows, width = out_ref.shape
    loads = [
        pltpu.make_async_copy(unit_grads_ref, unit_grads.at[pl.ds(0, 2)], local_sem.at[0]),
        pltpu.make_async_copy(weights_ref.at[pl.ds(0, 2)], weights, local_sem.at[1]),
        pltpu.make_async_copy(hidden_ref, unit_grads.at[2], local_sem.at[2]),
        pltpu.make_async_copy(rows_ref[0], rows.at[0], local_sem.at[3]),
        pltpu.make_async_copy(rows_ref[1], rows.at[1], local_sem.at[4]),
    ]
    for copy in loads:
        copy.start()
    greet_line(scatter.z, (scatter.across, scatter.other), scatter.down, scatter.up)
    loads[0].wait()
    loads[1].wait()

    def to_core(k):
        return remote(for_core.at[k], from_core.at[k], core_send_sem.at[k], core_sem.at[k], scatter.other)

    tile_rows = tile.shape[2]

    def tile_out(u, i):
        at = pl.ds(pl.multiple_of(u * tile_rows, tile_rows), tile_rows)
        return pltpu.make_async_copy(tile.at[u % 2, i], weight_grads_ref.at[i, at, :], tile_sem.at[u % 2, i])

    def weight_tile(u):
        @pl.when(u == 0)
        def _():
            for copy in loads[2:]:
                copy.wait()

        @pl.when(u >= 2)
        def _():
            for i in range(3):
                tile_out(u - 2, i).wait()

        def body(i, carry):
            left = rows[i // 2, :, pl.ds(pl.multiple_of(u * tile_rows, tile_rows), tile_rows)]
            tile[u % 2, i] = contract(left, unit_grads[i], 0, 0).astype(tile.dtype)
            return carry

        lax.fori_loop(0, 3, body, 0)
        for i in range(3):
            tile_out(u, i).start()

    def step(n, carry):
        @pl.when(n < 4)
        def _():
            partial_pair(scatter, unit_grads, weights, block_rows, n, 1 - scatter.c, for_core)
            to_core(n).start()
            to_core(4 + n).start()
            partial_pair(scatter, unit_grads, weights, block_rows, n, scatter.c, held)
            to_core(n).wait_recv()
            scatter.side(n)

        @pl.when((n >= 4) & (n < 7))
        def _():
            to_core(n).wait_recv()
            scatter.line(n - 4)

        late = n // 4

        @pl.when((n % 2 == 1) | (n >= 4))
        def _():
            weight_tile((1 - late) * (n // 2) + late * (n - 2))

        return carry

    lax.fori_loop(0, 8, step, 0)
    to_core(7).wait_recv()
    scatter.last()
    outward = pltpu.make_async_copy(total, out_ref, local_sem.at[5])
    outward.start()
    for k in range(8):
        to_core(k).wait_send()
    scatter.finish()
    for u in (4, 5):
        for i in range(3):
            tile_out(u, i).wait()
    outward.wait()


def scatter_fsdp(parts):
    return lax.psum_scatter(jnp.concatenate(parts, axis=2), "fsdp", scatter_dimension=0, tiled=False).astype(jnp.float32)


def gather_through(block_ref, gathered, gathered_ref, send_sem, receive_sem, out_sem, prepare, compute):
    gather = Gather(block_ref, gathered, send_sem, receive_sem)
    z, x, c = gather.z, gather.x, gather.c
    _, block_rows, width = gathered.shape
    own = pltpu.make_async_copy(block_ref, gathered.at[gather.own], out_sem.at[8])
    own.start()
    greet_line(z, (gather.across, gather.other), gather.down, gather.up)
    gather.start()

    def out(number):
        at = pl.ds(number * 2, 2)
        return pltpu.make_async_copy(gathered.at[at], gathered_ref.at[at], out_sem.at[number])

    def step(n, carry):
        @pl.when(n == 2)
        def _():
            gather.line(2)
            gather.side(1)

        @pl.when(n == 4)
        def _():
            gather.line(3)
            gather.side(2)

        @pl.when(n == 6)
        def _():
            gather.side(3)

        dz = n // 4 * 2 + n % 2
        side = (x + n // 2) % 2
        zi = (z // 2 + dz // 2) % 2 * 2 + (z + dz) % 2
        number = zi * 2 + side
        gather.arrived(fsdp_index(zi, side, 1 - c))
        out(number).start()
        left = gathered[pl.ds(number * 2, 2)].reshape(2 * block_rows, width)
        compute(number, pl.ds(pl.multiple_of(number * 2 * block_rows, 2 * block_rows), 2 * block_rows), left)
        return carry

    gather.line(1)
    gather.side(0)
    own.wait()
    prepare()
    lax.fori_loop(0, 8, step, 0)
    gather.finish(waits=False)
    for number in range(8):
        out(number).wait()


GELU_SCALE = math.sqrt(2.0 / math.pi)
GELU_CUBE = 0.044715


def feed_first_kernel(
    block_ref, weights_ref, gathered_ref, gate_up_ref, hidden_ref,
    gathered, send_sem, receive_sem, out_sem, weights, gate_up, hidden, load_sem, gate_up_sem, hidden_sem,
):
    load = pltpu.make_async_copy(weights_ref.at[pl.ds(0, 2)], weights, load_sem.at[0])
    load.start()

    def outs(number, rows):
        return (
            pltpu.make_async_copy(gate_up.at[:, rows, :], gate_up_ref.at[:, rows, :], gate_up_sem.at[number]),
            pltpu.make_async_copy(hidden.at[rows, :], hidden_ref.at[rows, :], hidden_sem.at[number]),
        )

    def compute(number, rows, left):
        gate = contract(left, weights[0], 1, 0)
        gate_up[0, rows, :] = gate
        up = contract(left, weights[1], 1, 0)
        gate_up[1, rows, :] = up
        gate = gate_up[0, rows, :]
        curve = jnp.tanh(GELU_SCALE * (gate + GELU_CUBE * (gate * gate * gate)))
        hidden[rows, :] = (0.5 * gate * (1.0 + curve) * up).astype(hidden.dtype)
        for copy in outs(number, rows):
            copy.start()

    gather_through(block_ref, gathered, gathered_ref, send_sem, receive_sem, out_sem, load.wait, compute)
    pair_rows = hidden.shape[0] // 8
    for number in range(8):
        for copy in outs(number, pl.ds(number * pair_rows, pair_rows)):
            copy.wait()


def hidden_back_kernel(
    block_ref, weights_ref, gate_up_ref, gathered_ref, unit_grads_ref,
    gathered, send_sem, receive_sem, out_sem, weights, gate_up, unit_grads, load_sem, grads_sem,
):
    loads = [
        pltpu.make_async_copy(weights_ref.at[2], weights, load_sem.at[0]),
        pltpu.make_async_copy(gate_up_ref, gate_up, load_sem.at[1]),
    ]
    for copy in loads:
        copy.start()

    def prepare():
        for copy in loads:
            copy.wait()

    def out(number, rows):
        return pltpu.make_async_copy(unit_grads.at[:, rows, :], unit_grads_ref.at[:, rows, :], grads_sem.at[number])

    def compute(number, rows, left):
        hidden_grad = contract(left, weights[...], 1, 0)
        gate, up = gate_up[0, rows, :], gate_up[1, rows, :]
        square = gate * gate
        curve = jnp.tanh(GELU_SCALE * (gate + GELU_CUBE * (square * gate)))
        inner = GELU_SCALE * (1.0 + 3.0 * GELU_CUBE * square)
        slope = 0.5 * (1.0 + curve) + 0.5 * gate * (1.0 - curve * curve) * inner
        unit_grads[0, rows, :] = (hidden_grad * up * slope).astype(unit_grads.dtype)
        unit_grads[1, rows, :] = (hidden_grad * (0.5 * gate * (1.0 + curve))).astype(unit_grads.dtype)
        out(number, rows).start()

    gather_through(block_ref, gathered, gathered_ref, send_sem, receive_sem, out_sem, prepare, compute)
    pair_rows = unit_grads.shape[1] // 8
    for number in range(8):
        out(number, pl.ds(number * pair_rows, pair_rows)).wait()


def gather_scratch(size, block, kind):
    return [
        pltpu.VMEM((size,) + block, kind),
        pltpu.SemaphoreType.DMA((Gather.slots,)),
        pltpu.SemaphoreType.DMA((size,)),
        pltpu.SemaphoreType.DMA((9,)),
    ]


def feed_first(block, feed_full, collective_id):
    size = lax.axis_size("fsdp")
    tokens, width, units, kind = size * block.shape[0], block.shape[1], feed_full.shape[2], block.dtype
    if size != KERNEL_FSDP:
        rows = lax.all_gather(block, "fsdp", axis=0, tiled=True)
        gate, up = contract(rows, feed_full[0], 1, 0), contract(rows, feed_full[1], 1, 0)
        return rows, jnp.stack([gate, up]), gelu_product(gate, up).astype(kind)
    rows, gate_up, hidden = scratch_call(
        feed_first_kernel,
        (
            jax.ShapeDtypeStruct((size,) + block.shape, kind),
            jax.ShapeDtypeStruct((2, tokens, units), jnp.float32),
            jax.ShapeDtypeStruct((tokens, units), kind),
        ),
        [
            *gather_scratch(size, block.shape, kind),
            pltpu.VMEM((2, width, units), kind),
            pltpu.VMEM((2, tokens, units), jnp.float32),
            pltpu.VMEM((tokens, units), kind),
            pltpu.SemaphoreType.DMA((1,)),
            pltpu.SemaphoreType.DMA((8,)),
            pltpu.SemaphoreType.DMA((8,)),
        ],
        collective_id,
        block,
        feed_full,
    )
    return rows.reshape(tokens, width), gate_up, hidden


def hidden_back(block, feed_full, gate_up, collective_id):
    size = lax.axis_size("fsdp")
    tokens, width, units, kind = size * block.shape[0], block.shape[1], feed_full.shape[2], block.dtype
    if size != KERNEL_FSDP:
        rows = lax.all_gather(block, "fsdp", axis=0, tiled=True)
        unused_out, pullback = jax.vjp(gelu_product, gate_up[0], gate_up[1])
        gradients = pullback(contract(rows, feed_full[2], 1, 0))
        return rows, jnp.stack(gradients).astype(kind)
    rows, unit_grads = scratch_call(
        hidden_back_kernel,
        (
            jax.ShapeDtypeStruct((size,) + block.shape, kind),
            jax.ShapeDtypeStruct((2, tokens, units), kind),
        ),
        [
            *gather_scratch(size, block.shape, kind),
            pltpu.VMEM((width, units), kind),
            pltpu.VMEM((2, tokens, units), jnp.float32),
            pltpu.VMEM((2, tokens, units), kind),
            pltpu.SemaphoreType.DMA((2,)),
            pltpu.SemaphoreType.DMA((8,)),
        ],
        collective_id,
        block,
        feed_full,
        gate_up,
    )
    return rows.reshape(tokens, width), unit_grads


def partial_pair(scatter, units, weights, block_rows, j, core, target):
    amount, width, _ = weights.shape
    step = 3 * 256
    spots = [pl.ds(pl.multiple_of(scatter.index(k, core) * block_rows, block_rows), block_rows) for k in (j, 4 + j)]

    def body(d, carry):
        at = pl.ds(pl.multiple_of(d * step, step), step)
        sums = None
        for i in range(amount):
            left = jnp.concatenate([units[i, spot, :] for spot in spots], axis=0)
            part = contract(left, weights[i, at, :], 1, 1)
            sums = part if sums is None else sums + part
        sums = sums.astype(target.dtype)
        target[j, :, at] = sums[:block_rows]
        target[4 + j, :, at] = sums[block_rows:]
        return carry

    lax.fori_loop(0, width // step, body, 0)


def feed_last_kernel(
    hidden_ref, weights_ref, out_ref,
    held, from_core, from_across, from_below, from_above, total, send_sem, across_sem, below_sem, above_sem,
    core_send_sem, core_sem, local_sem, for_core, hidden, weights,
):
    scatter = Scatter(
        (held, from_core, from_across, from_below, from_above, total), (send_sem, across_sem, below_sem, above_sem)
    )
    loads = [
        pltpu.make_async_copy(hidden_ref, hidden.at[0], local_sem.at[0]),
        pltpu.make_async_copy(weights_ref.at[pl.ds(2, 1)], weights, local_sem.at[1]),
    ]
    for copy in loads:
        copy.start()
    greet_line(scatter.z, (scatter.across, scatter.other), scatter.down, scatter.up)
    for copy in loads:
        copy.wait()

    def to_core(k):
        return remote(for_core.at[k], from_core.at[k], core_send_sem.at[k], core_sem.at[k], scatter.other)

    def share(j, carry):
        partial_pair(scatter, hidden, weights, out_ref.shape[0], j, 1 - scatter.c, for_core)
        to_core(j).start()
        to_core(4 + j).start()
        partial_pair(scatter, hidden, weights, out_ref.shape[0], j, scatter.c, held)
        to_core(j).wait_recv()
        scatter.side(j)
        return carry

    def along(i, carry):
        to_core(4 + i).wait_recv()
        scatter.line(i)
        return carry

    lax.fori_loop(0, 4, share, 0)
    lax.fori_loop(0, 3, along, 0)
    to_core(7).wait_recv()
    scatter.last()
    outward = pltpu.make_async_copy(total, out_ref, local_sem.at[2])
    outward.start()
    for k in range(8):
        to_core(k).wait_send()
    scatter.finish()
    outward.wait()


def feed_last(hidden, feed_full, collective_id):
    size = lax.axis_size("fsdp")
    tokens, width, kind = hidden.shape[0], feed_full.shape[1], hidden.dtype
    block = (tokens // size, width)
    if size != KERNEL_FSDP:
        sums = contract(hidden, feed_full[2], 1, 1).astype(kind)
        return scatter_fsdp((sums.reshape((size,) + block),))
    return scratch_call(
        feed_last_kernel,
        jax.ShapeDtypeStruct(block, jnp.float32),
        [
            *Scatter.scratch(block, kind),
            pltpu.SemaphoreType.DMA((8,)),
            pltpu.SemaphoreType.DMA((8,)),
            pltpu.SemaphoreType.DMA((3,)),
            pltpu.VMEM((8,) + block, kind),
            pltpu.VMEM((1,) + hidden.shape, kind),
            pltpu.VMEM((1,) + feed_full.shape[1:], kind),
        ],
        collective_id,
        hidden,
        feed_full,
    )


def feed_backward(unit_grads, feed_full, feed_input, feed_grad_rows, hidden, collective_id):
    size = lax.axis_size("fsdp")
    kind = hidden.dtype
    tokens, width = feed_input.shape
    if size != KERNEL_FSDP:
        gate_grad, up_grad = unit_grads[0], unit_grads[1]
        sums = contract(gate_grad, feed_full[0], 1, 1) + contract(up_grad, feed_full[1], 1, 1)
        return (
            scatter_fsdp((sums.astype(kind).reshape(size, tokens // size, width),)),
            jnp.stack(
                [
                    contract(left, right, 0, 0).astype(kind)
                    for left, right in ((feed_input, gate_grad), (feed_input, up_grad), (feed_grad_rows, hidden))
                ]
            ),
        )
    block, units = (tokens // size, width), hidden.shape[1]
    tile_rows = width // 6

    def kernel(unit_grads_ref, weights_ref, input_ref, grad_ref, hidden_ref, *refs):
        backward_kernel(unit_grads_ref, weights_ref, (input_ref, grad_ref), hidden_ref, *refs)

    rows_grad, weight_grads = scratch_call(
        kernel,
        (jax.ShapeDtypeStruct(block, jnp.float32), jax.ShapeDtypeStruct((3, width, units), kind)),
        [
            *Scatter.scratch(block, kind),
            pltpu.SemaphoreType.DMA((8,)),
            pltpu.SemaphoreType.DMA((8,)),
            pltpu.SemaphoreType.DMA((6,)),
            pltpu.VMEM((8,) + block, kind),
            pltpu.VMEM((3, tokens, units), kind),
            pltpu.VMEM((2, width, units), kind),
            pltpu.VMEM((2, tokens, width), kind),
            pltpu.VMEM((2, 3, tile_rows, units), kind),
            pltpu.SemaphoreType.DMA((2, 3)),
        ],
        collective_id,
        unit_grads,
        feed_full,
        feed_input,
        feed_grad_rows,
        hidden,
    )
    return rows_grad, weight_grads


def exchange_kernel(block_ref, out_ref, send_sem, receive_sem):
    index, t = lax.axis_index("fsdp"), lax.axis_index("tp")
    partner = (index, 1 - t)
    greet((partner,))
    copy = remote(block_ref, out_ref, send_sem.at[0], receive_sem.at[0], partner)
    copy.start()
    copy.wait()


def exchange_tp(block, collective_id):
    if lax.axis_size("fsdp") != KERNEL_FSDP:
        return lax.ppermute(block, "tp", [(0, 1), (1, 0)])
    return scratch_call(
        exchange_kernel,
        jax.ShapeDtypeStruct(block.shape, block.dtype),
        [pltpu.SemaphoreType.DMA((1,)), pltpu.SemaphoreType.DMA((1,))],
        collective_id,
        block,
    )


def peer(z, x, c, k):
    kz, kx, kc = k // 4, (k // 2) % 2, k % 2
    high, low = z // 2, z % 2
    high = 1 - high if kz // 2 else high
    low = 1 - low if kz % 2 else low
    return fsdp_index(high * 2 + low, 1 - x if kx else x, 1 - c if kc else c)


MAIN = 2 * LANES
REST = LANES
FIRST_REST = KERNEL_FSDP * MAIN
UNITS = 2 * MAIN + REST


def main_of(owner):
    return pl.ds(pl.multiple_of(owner * MAIN, MAIN), MAIN)


def rest_of(z):
    return pl.ds(pl.multiple_of(FIRST_REST + z * REST, REST), REST)


def distribute_kernel(
    rows_ref, query_ref, key_ref, value_ref, output_ref, gain_ref, gate_ref, up_ref, down_ref,
    attention_ref, partner_ref, feed_ref,
    stage, feed, zeros,
    gather_send, gather_receive, local_sem, pair_rows_sem, send_sem, receive_sem, rest_send, rest_receive,
    on_send, on_receive, rest_on_send, rest_on_receive,
):
    z, x, c, t = place()
    own = fsdp_index(z, x, c)
    partner = (own, 1 - t)
    greet([(peer(z, x, c, k), t) for k in range(1, 16)] + [partner])
    rows_copy = remote(rows_ref, partner_ref, pair_rows_sem.at[0], pair_rows_sem.at[1], partner)
    rows_copy.start()
    loads, start = [], 0
    for i, ref in enumerate((query_ref, key_ref, value_ref, output_ref, gain_ref)):
        loads.append(pltpu.make_async_copy(ref, stage.at[:, pl.ds(start, ref.shape[1])], local_sem.at[i]))
        start += ref.shape[1]
    feed_loads = [
        pltpu.make_async_copy(ref, feed.at[i], local_sem.at[5 + i])
        for i, ref in enumerate((gate_ref, up_ref, down_ref))
    ]
    for copy in loads + feed_loads:
        copy.start()
    for copy in loads:
        copy.wait()
    gather = Gather(stage, attention_ref, gather_send, gather_receive)
    gather.start()
    keep = pltpu.make_async_copy(stage, attention_ref.at[own], local_sem.at[8])
    keep.start()
    for copy in feed_loads:
        copy.wait()

    def main_at(half, source):
        return feed_ref.at[:, source, :, pl.ds(pl.multiple_of(half * MAIN, MAIN), MAIN)]

    def rest_at(source):
        return feed_ref.at[:, source, :, pl.ds(2 * MAIN, REST)]

    takes_rest = (c == 0) & (x == t)

    def direct(k):
        to = peer(z, x, c, k)
        return remote(feed.at[:, :, main_of(to)], main_at(t, own), send_sem.at[k], receive_sem.at[k], (to, t))

    def rest(dz):
        to_z = peer(z, x, c, 4 * dz) // 4
        slot = 4 * dz + 2 * ((x + t) % 2) + c
        return remote(
            feed.at[:, :, rest_of(to_z)], rest_at(own), rest_send.at[dz], rest_receive.at[slot], (fsdp_index(to_z, t, 0), t)
        )

    def onward(k):
        at = main_at(t, peer(z, x, c, k))
        return remote(at if k else feed.at[:, :, main_of(own)], at, on_send.at[k], on_receive.at[k], partner)

    def rest_onward(k):
        at = rest_at(peer(z, x, c, k))
        return remote(at if k else feed.at[:, :, rest_of(z)], at, rest_on_send.at[k], rest_on_receive.at[k], partner)

    def send(dz):
        for k in range(4 * dz, 4 * dz + 4):
            if k:
                direct(k).start()
        if dz:
            rest(dz).start()
        else:

            @pl.when(jnp.logical_not(takes_rest))
            def _():
                rest(0).start()

    def pass_on(dz):
        for k in range(4 * dz, 4 * dz + 4):
            if k:
                direct(k).wait_recv()
            onward(k).start()

        @pl.when(takes_rest)
        def _():
            for k in range(4 * dz, 4 * dz + 4):
                if k:
                    remote(
                        feed.at[:, :, rest_of(0)], rest_at(own), rest_send.at[0], rest_receive.at[k], partner
                    ).wait_recv()
                rest_onward(k).start()

    send(0)
    send(1)
    keep_main = pltpu.make_async_copy(feed.at[:, :, main_of(own)], main_at(t, own), local_sem.at[9])
    keep_main.start()
    keep_rest = pltpu.make_async_copy(feed.at[:, :, rest_of(z)], rest_at(own), local_sem.at[10])

    @pl.when(takes_rest)
    def _():
        keep_rest.start()

    fills = [
        pltpu.make_async_copy(zeros, feed_ref.at[i, :, :, pl.ds(2 * MAIN, REST)], local_sem.at[11 + i])
        for i in range(3)
    ]

    @pl.when(c == 1)
    def _():
        zeros[...] = jnp.zeros_like(zeros)
        for copy in fills:
            copy.start()

    send(2)
    pass_on(0)
    pass_on(1)
    gather.line(1)
    gather.side(0)
    send(3)
    gather.line(2)
    gather.side(1)
    pass_on(2)
    gather.line(3)
    pass_on(3)
    gather.side(2)
    gather.side(3)
    gather.finish()
    rows_copy.wait()
    for k in range(16):
        onward(k).wait_recv()
        onward(k).wait_send()
        if k:
            direct(k).wait_send()

    @pl.when(jnp.logical_not(takes_rest))
    def _():
        rest(0).wait_send()

    for dz in (1, 2, 3):
        rest(dz).wait_send()

    @pl.when(takes_rest)
    def _():
        for k in range(16):
            rest_onward(k).wait_send()
        keep_rest.wait()

    @pl.when((c == 0) & (x != t))
    def _():
        for k in range(16):
            rest_onward(k).wait_recv()

    @pl.when(c == 1)
    def _():
        for copy in fills:
            copy.wait()

    keep.wait()
    keep_main.wait()


def distribute(rows, attention, gain_columns, feed, collective_id):
    size = lax.axis_size("fsdp")
    shard_rows, feed_width = feed[0].shape
    columns = sum(w.shape[1] for w in attention) + gain_columns.shape[1]
    if size != KERNEL_FSDP:
        halves = lax.all_to_all(pack_units(feed, size), "fsdp", split_axis=0, concat_axis=0, tiled=True)
        halves = lax.all_gather(halves, "tp", axis=0)
        halves = halves.reshape(halves.shape[0], size * shard_rows, halves.shape[-1])
        return (
            lax.all_gather(jnp.concatenate((*attention, gain_columns), axis=1), "fsdp", axis=0),
            lax.ppermute(rows, "tp", [(0, 1), (1, 0)]),
            jnp.stack(join_units(halves, feed_width, size, 3)),
        )
    kind = rows.dtype
    attention_full, partner_rows, feed_full = scratch_call(
        distribute_kernel,
        (
            jax.ShapeDtypeStruct((size, shard_rows, columns), kind),
            jax.ShapeDtypeStruct(rows.shape, kind),
            jax.ShapeDtypeStruct((3, size, shard_rows, UNITS), kind),
        ),
        [
            pltpu.VMEM((shard_rows, columns), kind),
            pltpu.VMEM((3, shard_rows, feed_width), kind),
            pltpu.VMEM((size, shard_rows, REST), kind),
            pltpu.SemaphoreType.DMA((Gather.slots,)),
            pltpu.SemaphoreType.DMA((size,)),
            pltpu.SemaphoreType.DMA((14,)),
            pltpu.SemaphoreType.DMA((2,)),
            pltpu.SemaphoreType.DMA((size,)),
            pltpu.SemaphoreType.DMA((size,)),
            pltpu.SemaphoreType.DMA((4,)),
            pltpu.SemaphoreType.DMA((size,)),
            pltpu.SemaphoreType.DMA((size,)),
            pltpu.SemaphoreType.DMA((size,)),
            pltpu.SemaphoreType.DMA((size,)),
            pltpu.SemaphoreType.DMA((size,)),
        ],
        collective_id,
        rows,
        *attention,
        gain_columns,
        *feed,
    )
    return attention_full, partner_rows, feed_full.reshape(3, size * shard_rows, UNITS)


def collect_kernel(
    parts_ref, projected_ref, output_ref, gain_ref, out_ref, attention_ref,
    held, received, rest_held, rest_received,
    local_sem, pair_send, pair_receive, rest_pair_send, rest_pair_receive, send_sem, receive_sem, rest_send, rest_receive,
    *scatter_refs,
):
    scatter = Scatter(scatter_refs[:6], scatter_refs[6:10])
    blocks = Blocks(scatter, (projected_ref, output_ref, gain_ref), *scatter_refs[10:13])
    blocks.load()
    z, x, c, t = place()
    own = fsdp_index(z, x, c)
    rows = out_ref.shape[1]
    partner = (own, 1 - t)
    parts = [parts_ref.at[i] for i in range(3)]
    order = (2, 3, 1, 0)
    takes_rest = (c == 0) & (x == t)
    gives_rest = (c == 0) & (x != t)

    def plane(dz):
        return pl.ds(peer(z, x, c, 4 * dz) // 4 * 4, 4)

    def half(which):
        return pl.ds(pl.multiple_of(which * MAIN, MAIN), MAIN)

    rest_columns = pl.ds(2 * MAIN, REST)

    def load(dz, i):
        return pltpu.make_async_copy(parts[i].at[plane(dz), :, half(t)], held.at[dz, i], local_sem.at[3 * dz + i])

    def rest_load(dz, i):
        return pltpu.make_async_copy(
            parts[i].at[plane(dz), :, rest_columns], rest_held.at[dz, i], local_sem.at[12 + 3 * dz + i]
        )

    def pair(dz, i):
        slot = 3 * dz + i
        return remote(
            parts[i].at[plane(dz), :, half(1 - t)], received.at[dz, i], pair_send.at[slot], pair_receive.at[slot], partner
        )

    def rest_pair(dz, i):
        slot = 3 * dz + i
        return remote(
            parts[i].at[plane(dz), :, rest_columns],
            rest_received.at[dz, i],
            rest_pair_send.at[slot],
            rest_pair_receive.at[slot],
            partner,
        )

    def spot(k):
        return peer(z, x, c, k) % 4

    def direct(k):
        return remote(
            held.at[k // 4, :, spot(k)], out_ref.at[:, :, main_of(own)], send_sem.at[k], receive_sem.at[k], (peer(z, x, c, k), t)
        )

    def rest_direct(k):
        return remote(
            rest_held.at[k // 4, :, spot(k)],
            out_ref.at[:, :, rest_of(z)],
            rest_send.at[k],
            rest_receive.at[z],
            (peer(z, x, c, k), t),
        )

    def add(target, source):
        def body(j, carry):
            i, at = j // 4, j % 4
            total = target[i, at].astype(jnp.float32) + source[i, at].astype(jnp.float32)
            target[i, at] = total.astype(target.dtype)
            return carry

        lax.fori_loop(0, 12, body, 0)

    for dz in order:
        for i in range(3):
            load(dz, i).start()

    @pl.when(takes_rest)
    def _():
        for dz in order:
            for i in range(3):
                rest_load(dz, i).start()

    greet([(peer(z, x, c, k), t) for k in range(1, 16)] + [partner])
    blocks.send()
    for dz in order:
        for i in range(3):
            pair(dz, i).start()

        @pl.when(gives_rest)
        def _():
            for i in range(3):
                rest_pair(dz, i).start()

    def pass_on(dz):
        for i in range(3):
            load(dz, i).wait()
            pair(dz, i).wait_recv()
        add(held.at[dz], received.at[dz])
        for k in range(4 * dz, 4 * dz + 4):
            if k:
                direct(k).start()

        @pl.when(takes_rest)
        def _():
            for i in range(3):
                rest_load(dz, i).wait()
                rest_pair(dz, i).wait_recv()
            add(rest_held.at[dz], rest_received.at[dz])
            for k in range(4 * dz, 4 * dz + 4):
                if k:
                    rest_direct(k).start()

    def line(i):
        blocks.both(4 + i)
        scatter.line(i)

    def share(i, carry):
        blocks.both(i)
        scatter.side(i)
        return carry

    lax.fori_loop(0, 4, share, 0)
    pass_on(2)
    line(0)
    pass_on(3)
    line(1)
    pass_on(1)
    line(2)
    pass_on(0)
    blocks.both(7)
    scatter.last()
    outward = pltpu.make_async_copy(scatter.total, attention_ref, local_sem.at[26])
    outward.start()
    keep = pltpu.make_async_copy(held.at[0, :, spot(0)], out_ref.at[:, :, main_of(own)], local_sem.at[24])
    keep.start()
    keep_rest = pltpu.make_async_copy(rest_held.at[0, :, spot(0)], out_ref.at[:, :, rest_of(z)], local_sem.at[25])

    @pl.when(takes_rest)
    def _():
        keep_rest.start()

    for k in range(1, 16):
        direct(k).wait_recv()

    for dz in range(4):
        from_z = peer(z, x, c, 4 * dz) // 4

        def arrived():
            remote(
                rest_held.at[0, :, 0], out_ref.at[:, :, rest_of(from_z)], rest_send.at[0], rest_receive.at[from_z], partner
            ).wait_recv()

        if dz:
            arrived()
        else:

            @pl.when(jnp.logical_not(takes_rest))
            def _():
                arrived()

    for k in range(1, 16):
        direct(k).wait_send()
    for dz in order:
        for i in range(3):
            pair(dz, i).wait_send()

    @pl.when(gives_rest)
    def _():
        for dz in order:
            for i in range(3):
                rest_pair(dz, i).wait_send()

    @pl.when(takes_rest)
    def _():
        for k in range(1, 16):
            rest_direct(k).wait_send()
        keep_rest.wait()

    blocks.finish()
    scatter.finish()
    keep.wait()
    outward.wait()


def collect(gradients, feed_width, attention_parts, collective_id):
    size, pairs = lax.axis_size("fsdp"), lax.axis_size("tp")
    shard_rows = gradients.shape[1] // size
    if size != KERNEL_FSDP:
        packed = part_units([gradients[i] for i in range(3)], feed_width, size, pairs)
        mine = lax.psum_scatter(packed, "tp", scatter_dimension=0, tiled=False)
        mine = mine.reshape(size, shard_rows, mine.shape[-1])
        mine = lax.all_to_all(mine, "fsdp", split_axis=0, concat_axis=0, tiled=True)
        feed = [g.astype(jnp.float32) for g in unpack_units(mine, feed_width, 3)]
        return feed, scatter_fsdp(attention_parts)
    kind = gradients.dtype
    main, rest = (4, 3, 4, shard_rows, MAIN), (4, 3, 4, shard_rows, REST)
    block = (shard_rows, sum(part.shape[2] for part in attention_parts))
    out, attention = scratch_call(
        collect_kernel,
        (
            jax.ShapeDtypeStruct((3, shard_rows, feed_width), kind),
            jax.ShapeDtypeStruct(block, jnp.float32),
        ),
        [
            pltpu.VMEM(main, kind),
            pltpu.VMEM(main, kind),
            pltpu.VMEM(rest, kind),
            pltpu.VMEM(rest, kind),
            pltpu.SemaphoreType.DMA((27,)),
            pltpu.SemaphoreType.DMA((12,)),
            pltpu.SemaphoreType.DMA((12,)),
            pltpu.SemaphoreType.DMA((12,)),
            pltpu.SemaphoreType.DMA((12,)),
            pltpu.SemaphoreType.DMA((size,)),
            pltpu.SemaphoreType.DMA((size,)),
            pltpu.SemaphoreType.DMA((size,)),
            pltpu.SemaphoreType.DMA((4,)),
            *Scatter.scratch(block, kind),
            *[pltpu.SemaphoreType.DMA((24,)) for _ in range(3)],
        ],
        collective_id,
        gradients.reshape(3, size, shard_rows, UNITS),
        *attention_parts,
    )
    return [out[i].astype(jnp.float32) for i in range(3)], attention


def contract_last(left_rows, right_rows):
    return lax.dot_general(
        left_rows, right_rows, (((1,), (1,)), ((), ())), preferred_element_type=jnp.float32
    )


def contract_first(left_rows, right_rows):
    return lax.dot_general(
        left_rows, right_rows, (((0,), (0,)), ((), ())), preferred_element_type=jnp.float32
    )


def normalize_parts(value_rows):
    inverse = lax.rsqrt(jnp.mean(value_rows * value_rows, axis=-1, keepdims=True) + EPSILON)
    return (value_rows * inverse, inverse)


def norm_backward(unit_rows, inverse, norm_gain, upstream):
    scaled = upstream * norm_gain
    return inverse * (scaled - unit_rows * jnp.mean(scaled * unit_rows, axis=-1, keepdims=True))


def layout(lengths_row, row_index):
    segment_ends = jnp.cumsum(lengths_row)
    segment_starts = segment_ends - lengths_row
    segment = jnp.sum((row_index[:, None] >= segment_ends[None, :]).astype(jnp.int32), axis=1)
    onehot = segment[:, None] == jnp.arange(lengths_row.shape[0], dtype=jnp.int32)[None, :]
    segment_begin = jnp.sum(jnp.where(onehot, segment_starts[None, :], 0), axis=1)
    prompt_shift = jnp.where(segment > 0, lengths_row[0], 0)
    return (segment, row_index - segment_begin + prompt_shift)


def rotary_tables(position):
    frequency = jnp.exp(
        jnp.arange(HEAD_SIZE // 2, dtype=jnp.float32) * (-2.0 * math.log(10000.0) / HEAD_SIZE)
    )
    angles = position.astype(jnp.float32)[:, None] * frequency[None, :]
    return (jnp.cos(angles), jnp.sin(angles))


def apply_rotary(value_rows, cosine_lookup, sine_lookup):
    half_width = value_rows.shape[-1] // 2
    first_half = value_rows[..., :half_width]
    second_half = value_rows[..., half_width:]
    cosine_part = cosine_lookup[:, None, :]
    sine_part = sine_lookup[:, None, :]
    return jnp.concatenate(
        [
            first_half * cosine_part - second_half * sine_part,
            second_half * cosine_part + first_half * sine_part,
        ],
        axis=-1,
    )


def unrotate(value_rows, cosine_lookup, sine_lookup):
    half_width = value_rows.shape[-1] // 2
    first_half = value_rows[..., :half_width]
    second_half = value_rows[..., half_width:]
    cosine_part = cosine_lookup[:, None, :]
    sine_part = sine_lookup[:, None, :]
    return jnp.concatenate(
        [
            first_half * cosine_part + second_half * sine_part,
            second_half * cosine_part - first_half * sine_part,
        ],
        axis=-1,
    )


def visible(segment, row_index):
    same_segment = (segment[:, None] == segment[None, :]) & (
        row_index[None, :] <= row_index[:, None]
    )
    from_prompt = (segment[None, :] == 0) & (segment[:, None] > 0)
    return same_segment | from_prompt


def masked_scores(rotated_query, rotated_key, visible_mask):
    raw_scores = jnp.einsum(
        "qgrd,kgd->grqk", rotated_query, rotated_key, preferred_element_type=jnp.float32
    )
    tanh_value = jnp.tanh(raw_scores * HEAD_SIZE ** (-0.5) / SOFTCAP)
    return (jnp.where(visible_mask[None, None], SOFTCAP * tanh_value, NEGATIVE), tanh_value)


def gelu_product(gate_value, up_value):
    return jax.nn.gelu(gate_value, approximate=True) * up_value


def split_columns(width, size):
    main = width // size // LANES * LANES
    return main, width // size - main


def pack_units(weights, size):
    rows, width = weights[0].shape
    main, rest = split_columns(width, size)
    pieces = []
    if main:
        pieces += [
            jnp.transpose(w[:, : main * size].reshape(rows, size, main), (1, 0, 2)) for w in weights
        ]
    if rest:
        pieces += [
            jnp.transpose(w[:, main * size :].reshape(rows, size, rest), (1, 0, 2)) for w in weights
        ]
    packed = jnp.concatenate(pieces, axis=2)
    return jnp.pad(packed, ((0, 0), (0, 0), (0, -packed.shape[2] % LANES)))


def unpack_units(packed, width, amount):
    size, rows, _ = packed.shape
    main, rest = split_columns(width, size)
    arrays = []
    for i in range(amount):
        pieces = []
        if main:
            piece = packed[:, :, i * main : (i + 1) * main]
            pieces.append(jnp.transpose(piece, (1, 0, 2)).reshape(rows, size * main))
        if rest:
            start = amount * main + i * rest
            piece = packed[:, :, start : start + rest]
            pieces.append(jnp.transpose(piece, (1, 0, 2)).reshape(rows, size * rest))
        arrays.append(jnp.concatenate(pieces, axis=1))
    return arrays


def join_units(halves, width, size, amount):
    main, rest = split_columns(width, size)
    arrays = []
    for i in range(amount):
        start = amount * main + i * rest
        pieces = [half[:, i * main : (i + 1) * main] for half in halves]
        pieces += [half[:, start : start + rest] for half in halves]
        joined = jnp.concatenate(pieces, axis=1)
        arrays.append(jnp.pad(joined, ((0, 0), (0, -joined.shape[1] % LANES))))
    return arrays


def part_units(arrays, width, size, pairs):
    main, rest = split_columns(width, size)
    halves = []
    for t in range(pairs):
        pieces = [array[:, t * main : (t + 1) * main] for array in arrays]
        start = pairs * main + t * rest
        pieces += [array[:, start : start + rest] for array in arrays]
        packed = jnp.concatenate(pieces, axis=1)
        halves.append(jnp.pad(packed, ((0, 0), (0, -packed.shape[1] % LANES))))
    return jnp.stack(halves)


def shards(
    block_input,
    lengths,
    attention_norm_gain,
    attention_post_gain,
    feedforward_norm_gain,
    feedforward_post_gain,
    query_weight,
    key_weight,
    value_weight,
    output_weight,
    gate_weight,
    up_weight,
    down_weight,
    output_cotangent,
):
    low = jnp.bfloat16
    size, pairs = lax.axis_size("fsdp"), lax.axis_size("tp")
    rows_local, width = block_input.shape
    shard_rows, feed_width = gate_weight.shape
    query_width, key_width = query_weight.shape[1], key_weight.shape[1]
    output_start = query_width + 2 * key_width
    gain_start = output_start + query_width
    grouped_rows = rows_local * pairs

    gain_columns = jnp.stack(
        [attention_norm_gain, attention_post_gain, feedforward_norm_gain, feedforward_post_gain],
        axis=1,
    )
    attention_full, other_input, feed_full = distribute(
        block_input,
        (query_weight, key_weight, value_weight, output_weight),
        jnp.pad(gain_columns, ((0, 0), (0, LANES - 4))),
        (gate_weight, up_weight, down_weight),
        1,
    )
    attention_full = attention_full.reshape(size * shard_rows, gain_start + LANES)
    gains = jnp.transpose(attention_full[:, gain_start : gain_start + 4]).astype(jnp.float32)
    gain_one, gain_two, gain_three, gain_four = gains[0], gains[1], gains[2], gains[3]

    row_index = (
        jnp.arange(grouped_rows, dtype=jnp.int32) + lax.axis_index("tp") * rows_local
    ) % grouped_rows
    segment, position = layout(lengths[0], row_index)
    cosine_lookup, sine_lookup = rotary_tables(position)
    visible_mask = visible(segment, row_index)
    residual_both = jnp.concatenate([block_input, other_input], axis=0).astype(jnp.float32)
    unit_one_both, inverse_one_both = normalize_parts(residual_both)
    residual = residual_both[:rows_local]
    unit_one, inverse_one = unit_one_both[:rows_local], inverse_one_both[:rows_local]
    normed = (unit_one_both * gain_one).astype(low)
    projected = jnp.dot(
        normed, attention_full[:, :output_start], preferred_element_type=jnp.float32
    )
    query_raw = projected[:, :query_width]
    key_raw = projected[:, query_width : query_width + key_width]
    value_raw = projected[:, query_width + key_width :]
    heads_local = query_width // HEAD_SIZE
    kv_local = key_width // HEAD_SIZE
    repeat_heads = heads_local // kv_local
    rotated_query = apply_rotary(
        query_raw.reshape(grouped_rows, heads_local, HEAD_SIZE), cosine_lookup, sine_lookup
    ).astype(low)
    rotated_query = rotated_query.reshape(grouped_rows, kv_local, repeat_heads, HEAD_SIZE)
    rotated_key = apply_rotary(
        key_raw.reshape(grouped_rows, kv_local, HEAD_SIZE), cosine_lookup, sine_lookup
    ).astype(low)
    value_reduced = value_raw.astype(low).reshape(grouped_rows, kv_local, HEAD_SIZE)
    capped, tanh_value = masked_scores(rotated_query, rotated_key, visible_mask)
    row_peak = jnp.max(capped, axis=-1, keepdims=True)
    exponentials = jnp.exp(capped - row_peak)
    softmax_probs = exponentials / jnp.sum(exponentials, axis=-1, keepdims=True)
    probs_low = softmax_probs.astype(low)
    mixed_heads = jnp.einsum(
        "grqk,kgd->qgrd", probs_low, value_reduced, preferred_element_type=jnp.float32
    )
    attended = mixed_heads.reshape(grouped_rows, heads_local * HEAD_SIZE).astype(low)
    output_full = attention_full[:, output_start:gain_start]
    branch_parts = contract_last(attended, output_full)
    branch_one = branch_parts[:rows_local] + exchange_tp(
        branch_parts[rows_local:].astype(low), 4
    ).astype(jnp.float32)
    unit_two, inverse_two = normalize_parts(branch_one)
    middle = residual + unit_two * gain_two
    unit_three, inverse_three = normalize_parts(middle)

    feed_input, gate_up, hidden = feed_first((unit_three * gain_three).astype(low), feed_full, 5)
    branch_two = feed_last(hidden, feed_full, 6)
    unit_four, inverse_four = normalize_parts(branch_two)
    block_output = (middle + unit_four * gain_four).astype(low)
    upstream = output_cotangent.astype(jnp.float32)
    gain_four_grad = jnp.sum(upstream * unit_four, axis=0)
    branch_two_grad = norm_backward(unit_four, inverse_four, gain_four, upstream).astype(low)
    feed_grad_rows, unit_grads = hidden_back(branch_two_grad, feed_full, gate_up, 7)
    normed_three_grad, feed_grads = feed_backward(
        unit_grads, feed_full, feed_input, feed_grad_rows, hidden, 8
    )
    gain_three_grad = jnp.sum(normed_three_grad * unit_three, axis=0)
    middle_grad = upstream + norm_backward(unit_three, inverse_three, gain_three, normed_three_grad)
    gain_two_grad = jnp.sum(middle_grad * unit_two, axis=0)
    branch_one_grad = norm_backward(unit_two, inverse_two, gain_two, middle_grad).astype(low)
    attention_grad_rows = jnp.concatenate(
        [branch_one_grad, exchange_tp(branch_one_grad, 10)], axis=0
    )
    mixed_grad = jnp.dot(
        attention_grad_rows, output_full, preferred_element_type=jnp.float32
    ).astype(low)
    mixed_grad = mixed_grad.reshape(grouped_rows, kv_local, repeat_heads, HEAD_SIZE)
    value_grad = jnp.einsum(
        "grqk,qgrd->kgd", probs_low, mixed_grad, preferred_element_type=jnp.float32
    )
    probs_grad = jnp.einsum(
        "qgrd,kgd->grqk", mixed_grad, value_reduced, preferred_element_type=jnp.float32
    )
    score_grad = softmax_probs * (
        probs_grad - jnp.sum(softmax_probs * probs_grad, axis=-1, keepdims=True)
    )
    raw_grad = (score_grad * (1.0 - tanh_value * tanh_value) * HEAD_SIZE ** (-0.5)).astype(low)
    query_grad = jnp.einsum(
        "grqk,kgd->qgrd", raw_grad, rotated_key, preferred_element_type=jnp.float32
    )
    key_grad = jnp.einsum(
        "grqk,qgrd->kgd", raw_grad, rotated_query, preferred_element_type=jnp.float32
    )
    query_grad = unrotate(
        query_grad.reshape(grouped_rows, heads_local, HEAD_SIZE), cosine_lookup, sine_lookup
    )
    key_grad = unrotate(key_grad, cosine_lookup, sine_lookup)
    projected_grad = jnp.concatenate(
        [
            query_grad.reshape(grouped_rows, heads_local * HEAD_SIZE).astype(low),
            key_grad.reshape(grouped_rows, kv_local * HEAD_SIZE).astype(low),
            value_grad.reshape(grouped_rows, kv_local * HEAD_SIZE).astype(low),
        ],
        axis=1,
    )
    input_parts = contract_last(projected_grad, attention_full[:, :output_start])

    gain_grads = jnp.stack(
        [
            jnp.sum(input_parts * unit_one_both, axis=0),
            gain_two_grad,
            gain_three_grad,
            gain_four_grad,
        ]
    )
    sent = jnp.concatenate(
        [input_parts[rows_local:].astype(low), jnp.pad(gain_grads, ((0, 12), (0, 0))).astype(low)]
    )
    received = exchange_tp(sent, 11).astype(jnp.float32)
    normed_one_grad = input_parts[:rows_local] + received[:rows_local]
    gain_grads = gain_grads + received[rows_local : rows_local + 4]
    input_gradient = middle_grad + norm_backward(unit_one, inverse_one, gain_one, normed_one_grad)

    (gate_weight_grad, up_weight_grad, down_weight_grad), attention_grads = collect(
        feed_grads,
        feed_width,
        [
            part.astype(low).reshape(size, shard_rows, part.shape[1])
            for part in (
                contract_first(normed, projected_grad),
                contract_first(attention_grad_rows, attended),
                jnp.pad(jnp.transpose(gain_grads), ((0, 0), (0, LANES - 4))),
            )
        ],
        9,
    )
    gain_shards = jnp.transpose(attention_grads[:, gain_start : gain_start + 4])
    return (
        block_output,
        input_gradient,
        gain_shards[0],
        gain_shards[1],
        gain_shards[2],
        gain_shards[3],
        attention_grads[:, :query_width],
        attention_grads[:, query_width : query_width + key_width],
        attention_grads[:, query_width + key_width : output_start],
        attention_grads[:, output_start:gain_start],
        gate_weight_grad,
        up_weight_grad,
        down_weight_grad,
    )


def solution(mesh):
    placed = (
        P(("fsdp", "tp"), None),
        P("fsdp", None),
        P("fsdp"),
        P("fsdp"),
        P("fsdp"),
        P("fsdp"),
        P("fsdp", "tp"),
        P("fsdp", "tp"),
        P("fsdp", "tp"),
        P("fsdp", "tp"),
        P("fsdp", "tp"),
        P("fsdp", "tp"),
        P("fsdp", "tp"),
        P(("fsdp", "tp"), None),
    )
    return jax.shard_map(
        shards,
        mesh=mesh,
        in_specs=placed,
        out_specs=(
            P(("fsdp", "tp"), None),
            P(("fsdp", "tp"), None),
            P("fsdp"),
            P("fsdp"),
            P("fsdp"),
            P("fsdp"),
            P("fsdp", "tp"),
            P("fsdp", "tp"),
            P("fsdp", "tp"),
            P("fsdp", "tp"),
            P("fsdp", "tp"),
            P("fsdp", "tp"),
            P("fsdp", "tp"),
        ),
        check_vma=False,
    )
```

```python
import functools
import math

import jax
import jax.numpy as jnp
from jax import lax
from jax.experimental import pallas as pl
from jax.experimental.pallas import tpu as pltpu
from jax.sharding import PartitionSpec as P

HEAD_SIZE = 256
MESH = pl.DeviceIdType.MESH
ANY = pl.BlockSpec(memory_space=pl.ANY)
LANES = 128

EPSILON = 1e-06
SOFTCAP = 50.0
NEGATIVE = -1e30

KERNEL_FSDP = 16


def place():
    index = lax.axis_index("fsdp")
    return index // 4, (index // 2) % 2, index % 2, lax.axis_index("tp")


def fsdp_index(z, x, c):
    return (z * 2 + x) * 2 + c


def remote(source, target, send_sem, receive_sem, device):
    return pltpu.make_async_remote_copy(
        src_ref=source,
        dst_ref=target,
        send_sem=send_sem,
        recv_sem=receive_sem,
        device_id=device,
        device_id_type=MESH,
    )


def greet(devices):
    barrier = pltpu.get_barrier_semaphore()
    for device in devices:
        pl.semaphore_signal(barrier, inc=1, device_id=device, device_id_type=MESH)
    pl.semaphore_wait(barrier, len(devices))


def greet_line(z, devices, down, up):
    barrier = pltpu.get_barrier_semaphore()
    for device in devices:
        pl.semaphore_signal(barrier, inc=1, device_id=device, device_id_type=MESH)

    @pl.when(z > 0)
    def _():
        pl.semaphore_signal(barrier, inc=1, device_id=down, device_id_type=MESH)

    @pl.when(z < 3)
    def _():
        pl.semaphore_signal(barrier, inc=1, device_id=up, device_id_type=MESH)

    pl.semaphore_wait(barrier, len(devices) + (z + 2) // 3 + (5 - z) // 3)


class Gather:
    slots = 29

    def __init__(self, block, out_ref, send_sem, receive_sem):
        self.block, self.out, self.send_sem, self.receive_sem = block, out_ref, send_sem, receive_sem
        self.z, self.x, self.c, t = place()
        z, x, c = self.z, self.x, self.c
        self.own = fsdp_index(z, x, c)
        self.down, self.up = (fsdp_index(z - 1, x, c), t), (fsdp_index(z + 1, x, c), t)
        self.across, self.other = (fsdp_index(z, 1 - x, c), t), (fsdp_index(z, x, 1 - c), t)

    def copy(self, source, index, slot, device):
        return remote(source, self.out.at[index], self.send_sem.at[slot], self.receive_sem.at[index], device)

    def relay(self, index, slot, device):
        self.copy(self.out.at[index], index, slot, device).start()

    def arrived(self, index):
        self.copy(self.block, index, 0, self.other).wait_recv()

    def sent(self, slot):
        self.copy(self.block, self.own, slot, self.other).wait_send()

    def start(self):
        @pl.when(self.z < 3)
        def _():
            self.copy(self.block, self.own, 0, self.up).start()

        @pl.when(self.z > 0)
        def _():
            self.copy(self.block, self.own, 1, self.down).start()

        self.copy(self.block, self.own, 2, self.across).start()
        self.copy(self.block, self.own, 3, self.other).start()

    def line(self, d):
        z, x, c = self.z, self.x, self.c

        @pl.when(z >= d)
        def _():
            index = fsdp_index(z - d, x, c)
            base = 4 + 3 * (d - 1)
            self.arrived(index)

            @pl.when(z < 3)
            def _():
                self.relay(index, base, self.up)

            self.relay(index, base + 1, self.across)
            self.relay(index, base + 2, self.other)

        @pl.when(z + d <= 3)
        def _():
            index = fsdp_index(z + d, x, c)
            base = 13 + 3 * (d - 1)
            self.arrived(index)

            @pl.when(z > 0)
            def _():
                self.relay(index, base, self.down)

            self.relay(index, base + 1, self.across)
            self.relay(index, base + 2, self.other)

    def side(self, d):
        z, x, c = self.z, self.x, self.c
        if d == 0:
            index = fsdp_index(z, 1 - x, c)
            self.arrived(index)
            self.relay(index, 22, self.other)
            return

        @pl.when(z >= d)
        def _():
            index = fsdp_index(z - d, 1 - x, c)
            self.arrived(index)
            self.relay(index, 22 + d, self.other)

        @pl.when(z + d <= 3)
        def _():
            index = fsdp_index(z + d, 1 - x, c)
            self.arrived(index)
            self.relay(index, 25 + d, self.other)

    def finish(self, waits=True):
        z = self.z
        if waits:
            for zi in range(4):
                for xi in range(2):
                    self.arrived(fsdp_index(zi, xi, 1 - self.c))

        @pl.when(z < 3)
        def _():
            self.sent(0)

        @pl.when(z > 0)
        def _():
            self.sent(1)

        for slot in (2, 3, 22):
            self.sent(slot)
        for d in (1, 2, 3):

            @pl.when(z >= d)
            def _():
                base = 4 + 3 * (d - 1)

                @pl.when(z < 3)
                def _():
                    self.sent(base)

                for slot in (base + 1, base + 2, 22 + d):
                    self.sent(slot)

            @pl.when(z + d <= 3)
            def _():
                base = 13 + 3 * (d - 1)

                @pl.when(z > 0)
                def _():
                    self.sent(base)

                for slot in (base + 1, base + 2, 25 + d):
                    self.sent(slot)


def scratch_call(kernel, outputs, scratch, collective_id, *operands):
    return pl.pallas_call(
        kernel,
        out_shape=outputs,
        in_specs=[ANY] * len(operands),
        out_specs=jax.tree.map(lambda _: ANY, outputs),
        scratch_shapes=scratch,
        compiler_params=pltpu.CompilerParams(
            collective_id=collective_id, has_side_effects=True, vmem_limit_bytes=60 * 1024 * 1024
        ),
    )(*operands)


def add_rows(rows, step, target, *sources):
    def body(i, carry):
        at = pl.ds(pl.multiple_of(i * step, step), step)
        total = sources[0][at, :].astype(jnp.float32)
        for source in sources[1:]:
            total = total + source[at, :].astype(jnp.float32)
        target[at, :] = total.astype(target.dtype)
        return carry

    lax.fori_loop(0, rows // step, body, 0)


class Scatter:
    def __init__(self, buffers, semaphores):
        self.held, self.from_core, self.from_across, self.from_below, self.from_above, self.total = buffers
        self.send_sem, self.across_sem, self.below_sem, self.above_sem = semaphores
        self.z, self.x, self.c, t = place()
        z, x, c = self.z, self.x, self.c
        self.rows = self.total.shape[0]
        self.down, self.up = (fsdp_index(z - 1, x, c), t), (fsdp_index(z + 1, x, c), t)
        self.across, self.other = (fsdp_index(z, 1 - x, c), t), (fsdp_index(z, x, 1 - c), t)

    def target(self, i):
        half = self.z // 2
        mirrored = self.z + half * (3 - 2 * self.z)
        base = 3 - i + mirrored * (i // 2) * (2 * (i % 2) - 1)
        return base + half * (3 - 2 * base)

    def index(self, k, core):
        return fsdp_index(self.target(k % 4), (self.x + 1 - k // 4) % 2, core)

    def add(self, target, *sources):
        add_rows(self.rows, 16, target, *sources)

    def over(self, i):
        return remote(
            self.held.at[i], self.from_across.at[i], self.send_sem.at[3 + i], self.across_sem.at[i], self.across
        )

    def going_up(self, i, target):
        return remote(
            self.held.at[4 + i], self.from_below.at[target], self.send_sem.at[i], self.below_sem.at[target], self.up
        )

    def going_down(self, i, target):
        return remote(
            self.held.at[4 + i], self.from_above.at[target], self.send_sem.at[i], self.above_sem.at[target], self.down
        )

    def side(self, i):
        self.add(self.held.at[i], self.held.at[i], self.from_core.at[i])
        self.over(i).start()

    def line(self, i):
        z, target = self.z, self.target(i)
        held = self.held.at[4 + i]
        sources = (held, self.from_core.at[4 + i], self.from_across.at[i])
        self.over(i).wait_recv()

        @pl.when(target > z)
        def _():
            @pl.when(z > 0)
            def _():
                self.going_up(i, target).wait_recv()
                self.add(held, *sources, self.from_below.at[target])

            @pl.when(z == 0)
            def _():
                self.add(held, *sources)

            self.going_up(i, target).start()

        @pl.when(target < z)
        def _():
            @pl.when(z < 3)
            def _():
                self.going_down(i, target).wait_recv()
                self.add(held, *sources, self.from_above.at[target])

            @pl.when(z == 3)
            def _():
                self.add(held, *sources)

            self.going_down(i, target).start()

    def last(self):
        z = self.z
        self.over(3).wait_recv()
        self.add(self.total, self.held.at[7], self.from_core.at[7], self.from_across.at[3])

        @pl.when(z > 0)
        def _():
            self.going_up(0, z).wait_recv()
            self.add(self.total, self.total, self.from_below.at[z])

        @pl.when(z < 3)
        def _():
            self.going_down(0, z).wait_recv()
            self.add(self.total, self.total, self.from_above.at[z])

    def finish(self):
        for i in range(4):
            self.over(i).wait_send()
        for i in range(3):
            self.going_up(i, 0).wait_send()

    @staticmethod
    def scratch(block, kind):
        return [
            *[pltpu.VMEM((amount,) + block, kind) for amount in (8, 8, 4, 4, 4)],
            pltpu.VMEM(block, jnp.float32),
            *[pltpu.SemaphoreType.DMA((amount,)) for amount in (7, 4, 4, 4)],
        ]


class Blocks:
    def __init__(self, scatter, parts_refs, core_send_sem, core_sem, local_sem):
        self.scatter, self.parts = scatter, []
        self.core_send_sem, self.core_sem, self.local_sem = core_send_sem, core_sem, local_sem
        start = 0
        for ref in parts_refs:
            self.parts.append((ref, pl.ds(start, ref.shape[2])))
            start += ref.shape[2]

    def local(self, k):
        index = self.scatter.index(k, self.scatter.c)
        return [
            pltpu.make_async_copy(
                ref.at[index], self.scatter.held.at[k, :, at], self.local_sem.at[k * len(self.parts) + i]
            )
            for i, (ref, at) in enumerate(self.parts)
        ]

    def to_core(self, k):
        index = self.scatter.index(k, 1 - self.scatter.c)
        return [
            remote(
                ref.at[index],
                self.scatter.from_core.at[k, :, at],
                self.core_send_sem.at[k * len(self.parts) + i],
                self.core_sem.at[k * len(self.parts) + i],
                self.scatter.other,
            )
            for i, (ref, at) in enumerate(self.parts)
        ]

    def load(self):
        for k in range(8):
            for copy in self.local(k):
                copy.start()

    def send(self):
        for k in range(8):
            for copy in self.to_core(k):
                copy.start()

    def both(self, k):
        for copy in self.local(k):
            copy.wait()
        for copy in self.to_core(k):
            copy.wait_recv()

    def finish(self):
        for k in range(8):
            for copy in self.to_core(k):
                copy.wait_send()


def contract(left, right, left_dim, right_dim):
    return lax.dot_general(
        left, right, (((left_dim,), (right_dim,)), ((), ())), preferred_element_type=jnp.float32
    )


def backward_kernel(
    unit_grads_ref, weights_ref, rows_ref, hidden_ref, out_ref, weight_grads_ref,
    held, from_core, from_across, from_below, from_above, total, send_sem, across_sem, below_sem, above_sem,
    core_send_sem, core_sem, local_sem, for_core, unit_grads, weights, rows, tile, tile_sem,
):
    scatter = Scatter(
        (held, from_core, from_across, from_below, from_above, total), (send_sem, across_sem, below_sem, above_sem)
    )
    block_rows, width = out_ref.shape
    loads = [
        pltpu.make_async_copy(unit_grads_ref, unit_grads.at[pl.ds(0, 2)], local_sem.at[0]),
        pltpu.make_async_copy(weights_ref.at[pl.ds(0, 2)], weights, local_sem.at[1]),
        pltpu.make_async_copy(hidden_ref, unit_grads.at[2], local_sem.at[2]),
        pltpu.make_async_copy(rows_ref[0], rows.at[0], local_sem.at[3]),
        pltpu.make_async_copy(rows_ref[1], rows.at[1], local_sem.at[4]),
    ]
    for copy in loads:
        copy.start()
    greet_line(scatter.z, (scatter.across, scatter.other), scatter.down, scatter.up)
    loads[0].wait()
    loads[1].wait()

    def to_core(k):
        return remote(for_core.at[k], from_core.at[k], core_send_sem.at[k], core_sem.at[k], scatter.other)

    tile_rows = tile.shape[2]

    def tile_out(u, i):
        at = pl.ds(pl.multiple_of(u * tile_rows, tile_rows), tile_rows)
        return pltpu.make_async_copy(tile.at[u % 2, i], weight_grads_ref.at[i, at, :], tile_sem.at[u % 2, i])

    def weight_tile(u):
        @pl.when(u == 0)
        def _():
            for copy in loads[2:]:
                copy.wait()

        @pl.when(u >= 2)
        def _():
            for i in range(3):
                tile_out(u - 2, i).wait()

        def body(i, carry):
            left = rows[i // 2, :, pl.ds(pl.multiple_of(u * tile_rows, tile_rows), tile_rows)]
            tile[u % 2, i] = contract(left, unit_grads[i], 0, 0).astype(tile.dtype)
            return carry

        lax.fori_loop(0, 3, body, 0)
        for i in range(3):
            tile_out(u, i).start()

    def step(n, carry):
        @pl.when(n < 4)
        def _():
            partial_pair(scatter, unit_grads, weights, block_rows, n, 1 - scatter.c, for_core)
            to_core(n).start()
            to_core(4 + n).start()
            partial_pair(scatter, unit_grads, weights, block_rows, n, scatter.c, held)
            to_core(n).wait_recv()
            scatter.side(n)

        @pl.when(n >= 4)
        def _():
            to_core(n).wait_recv()
            scatter.line(n - 4)

        @pl.when(n >= 4)
        def _():
            weight_tile(2 * n - 8)
            weight_tile(2 * n - 7)

        return carry

    lax.fori_loop(0, 7, step, 0)
    to_core(7).wait_recv()
    scatter.last()
    outward = pltpu.make_async_copy(total, out_ref, local_sem.at[5])
    outward.start()
    for k in range(8):
        to_core(k).wait_send()
    scatter.finish()
    for u in (4, 5):
        for i in range(3):
            tile_out(u, i).wait()
    outward.wait()


def scatter_fsdp(parts):
    return lax.psum_scatter(jnp.concatenate(parts, axis=2), "fsdp", scatter_dimension=0, tiled=False).astype(jnp.float32)


def gather_through(block_ref, gathered, gathered_ref, send_sem, receive_sem, out_sem, prepare, compute):
    gather = Gather(block_ref, gathered, send_sem, receive_sem)
    z, x, c = gather.z, gather.x, gather.c
    _, block_rows, width = gathered.shape
    own = pltpu.make_async_copy(block_ref, gathered.at[gather.own], out_sem.at[8])
    own.start()
    greet_line(z, (gather.across, gather.other), gather.down, gather.up)
    gather.start()

    def out(number):
        at = pl.ds(number * 2, 2)
        return pltpu.make_async_copy(gathered.at[at], gathered_ref.at[at], out_sem.at[number])

    def step(n, carry):
        @pl.when(n == 2)
        def _():
            gather.line(2)
            gather.side(1)

        @pl.when(n == 4)
        def _():
            gather.line(3)
            gather.side(2)

        @pl.when(n == 6)
        def _():
            gather.side(3)

        dz = n // 4 * 2 + n % 2
        side = (x + n // 2) % 2
        zi = (z // 2 + dz // 2) % 2 * 2 + (z + dz) % 2
        number = zi * 2 + side
        gather.arrived(fsdp_index(zi, side, 1 - c))
        out(number).start()
        left = gathered[pl.ds(number * 2, 2)].reshape(2 * block_rows, width)
        compute(number, pl.ds(pl.multiple_of(number * 2 * block_rows, 2 * block_rows), 2 * block_rows), left)
        return carry

    gather.line(1)
    gather.side(0)
    own.wait()
    prepare()
    lax.fori_loop(0, 8, step, 0)
    gather.finish(waits=False)
    for number in range(8):
        out(number).wait()


GELU_SCALE = math.sqrt(2.0 / math.pi)
GELU_CUBE = 0.044715


def feed_first_kernel(
    block_ref, weights_ref, gathered_ref, gate_up_ref, hidden_ref,
    gathered, send_sem, receive_sem, out_sem, weights, gate_up, hidden, load_sem, gate_up_sem, hidden_sem,
):
    load = pltpu.make_async_copy(weights_ref.at[pl.ds(0, 2)], weights, load_sem.at[0])
    load.start()

    def outs(number, rows):
        return (
            pltpu.make_async_copy(gate_up.at[:, rows, :], gate_up_ref.at[:, rows, :], gate_up_sem.at[number]),
            pltpu.make_async_copy(hidden.at[rows, :], hidden_ref.at[rows, :], hidden_sem.at[number]),
        )

    def compute(number, rows, left):
        gate = contract(left, weights[0], 1, 0)
        gate_up[0, rows, :] = gate
        up = contract(left, weights[1], 1, 0)
        gate_up[1, rows, :] = up
        gate = gate_up[0, rows, :]
        curve = jnp.tanh(GELU_SCALE * (gate + GELU_CUBE * (gate * gate * gate)))
        hidden[rows, :] = (0.5 * gate * (1.0 + curve) * up).astype(hidden.dtype)
        for copy in outs(number, rows):
            copy.start()

    gather_through(block_ref, gathered, gathered_ref, send_sem, receive_sem, out_sem, load.wait, compute)
    pair_rows = hidden.shape[0] // 8
    for number in range(8):
        for copy in outs(number, pl.ds(number * pair_rows, pair_rows)):
            copy.wait()


def hidden_back_kernel(
    block_ref, weights_ref, gate_up_ref, gathered_ref, unit_grads_ref,
    gathered, send_sem, receive_sem, out_sem, weights, gate_up, unit_grads, load_sem, grads_sem,
):
    loads = [
        pltpu.make_async_copy(weights_ref.at[2], weights, load_sem.at[0]),
        pltpu.make_async_copy(gate_up_ref, gate_up, load_sem.at[1]),
    ]
    for copy in loads:
        copy.start()

    def prepare():
        for copy in loads:
            copy.wait()

    def out(number, rows):
        return pltpu.make_async_copy(unit_grads.at[:, rows, :], unit_grads_ref.at[:, rows, :], grads_sem.at[number])

    def compute(number, rows, left):
        hidden_grad = contract(left, weights[...], 1, 0)
        gate, up = gate_up[0, rows, :], gate_up[1, rows, :]
        square = gate * gate
        curve = jnp.tanh(GELU_SCALE * (gate + GELU_CUBE * (square * gate)))
        inner = GELU_SCALE * (1.0 + 3.0 * GELU_CUBE * square)
        slope = 0.5 * (1.0 + curve) + 0.5 * gate * (1.0 - curve * curve) * inner
        unit_grads[0, rows, :] = (hidden_grad * up * slope).astype(unit_grads.dtype)
        unit_grads[1, rows, :] = (hidden_grad * (0.5 * gate * (1.0 + curve))).astype(unit_grads.dtype)
        out(number, rows).start()

    gather_through(block_ref, gathered, gathered_ref, send_sem, receive_sem, out_sem, prepare, compute)
    pair_rows = unit_grads.shape[1] // 8
    for number in range(8):
        out(number, pl.ds(number * pair_rows, pair_rows)).wait()


def gather_scratch(size, block, kind):
    return [
        pltpu.VMEM((size,) + block, kind),
        pltpu.SemaphoreType.DMA((Gather.slots,)),
        pltpu.SemaphoreType.DMA((size,)),
        pltpu.SemaphoreType.DMA((9,)),
    ]


def feed_first(block, feed_full, collective_id):
    size = lax.axis_size("fsdp")
    tokens, width, units, kind = size * block.shape[0], block.shape[1], feed_full.shape[2], block.dtype
    if size != KERNEL_FSDP:
        rows = lax.all_gather(block, "fsdp", axis=0, tiled=True)
        gate, up = contract(rows, feed_full[0], 1, 0), contract(rows, feed_full[1], 1, 0)
        return rows, jnp.stack([gate, up]), gelu_product(gate, up).astype(kind)
    rows, gate_up, hidden = scratch_call(
        feed_first_kernel,
        (
            jax.ShapeDtypeStruct((size,) + block.shape, kind),
            jax.ShapeDtypeStruct((2, tokens, units), jnp.float32),
            jax.ShapeDtypeStruct((tokens, units), kind),
        ),
        [
            *gather_scratch(size, block.shape, kind),
            pltpu.VMEM((2, width, units), kind),
            pltpu.VMEM((2, tokens, units), jnp.float32),
            pltpu.VMEM((tokens, units), kind),
            pltpu.SemaphoreType.DMA((1,)),
            pltpu.SemaphoreType.DMA((8,)),
            pltpu.SemaphoreType.DMA((8,)),
        ],
        collective_id,
        block,
        feed_full,
    )
    return rows.reshape(tokens, width), gate_up, hidden


def hidden_back(block, feed_full, gate_up, collective_id):
    size = lax.axis_size("fsdp")
    tokens, width, units, kind = size * block.shape[0], block.shape[1], feed_full.shape[2], block.dtype
    if size != KERNEL_FSDP:
        rows = lax.all_gather(block, "fsdp", axis=0, tiled=True)
        unused_out, pullback = jax.vjp(gelu_product, gate_up[0], gate_up[1])
        gradients = pullback(contract(rows, feed_full[2], 1, 0))
        return rows, jnp.stack(gradients).astype(kind)
    rows, unit_grads = scratch_call(
        hidden_back_kernel,
        (
            jax.ShapeDtypeStruct((size,) + block.shape, kind),
            jax.ShapeDtypeStruct((2, tokens, units), kind),
        ),
        [
            *gather_scratch(size, block.shape, kind),
            pltpu.VMEM((width, units), kind),
            pltpu.VMEM((2, tokens, units), jnp.float32),
            pltpu.VMEM((2, tokens, units), kind),
            pltpu.SemaphoreType.DMA((2,)),
            pltpu.SemaphoreType.DMA((8,)),
        ],
        collective_id,
        block,
        feed_full,
        gate_up,
    )
    return rows.reshape(tokens, width), unit_grads


def partial_pair(scatter, units, weights, block_rows, j, core, target):
    amount, width, _ = weights.shape
    step = 3 * 256
    spots = [pl.ds(pl.multiple_of(scatter.index(k, core) * block_rows, block_rows), block_rows) for k in (j, 4 + j)]

    def body(d, carry):
        at = pl.ds(pl.multiple_of(d * step, step), step)
        sums = None
        for i in range(amount):
            left = jnp.concatenate([units[i, spot, :] for spot in spots], axis=0)
            part = contract(left, weights[i, at, :], 1, 1)
            sums = part if sums is None else sums + part
        sums = sums.astype(target.dtype)
        target[j, :, at] = sums[:block_rows]
        target[4 + j, :, at] = sums[block_rows:]
        return carry

    lax.fori_loop(0, width // step, body, 0)


def feed_last_kernel(
    hidden_ref, weights_ref, out_ref,
    held, from_core, from_across, from_below, from_above, total, send_sem, across_sem, below_sem, above_sem,
    core_send_sem, core_sem, local_sem, for_core, hidden, weights,
):
    scatter = Scatter(
        (held, from_core, from_across, from_below, from_above, total), (send_sem, across_sem, below_sem, above_sem)
    )
    loads = [
        pltpu.make_async_copy(hidden_ref, hidden.at[0], local_sem.at[0]),
        pltpu.make_async_copy(weights_ref.at[pl.ds(2, 1)], weights, local_sem.at[1]),
    ]
    for copy in loads:
        copy.start()
    greet_line(scatter.z, (scatter.across, scatter.other), scatter.down, scatter.up)
    for copy in loads:
        copy.wait()

    def to_core(k):
        return remote(for_core.at[k], from_core.at[k], core_send_sem.at[k], core_sem.at[k], scatter.other)

    def share(j, carry):
        partial_pair(scatter, hidden, weights, out_ref.shape[0], j, 1 - scatter.c, for_core)
        to_core(j).start()
        to_core(4 + j).start()
        partial_pair(scatter, hidden, weights, out_ref.shape[0], j, scatter.c, held)
        to_core(j).wait_recv()
        scatter.side(j)
        return carry

    def along(i, carry):
        to_core(4 + i).wait_recv()
        scatter.line(i)
        return carry

    lax.fori_loop(0, 4, share, 0)
    lax.fori_loop(0, 3, along, 0)
    to_core(7).wait_recv()
    scatter.last()
    outward = pltpu.make_async_copy(total, out_ref, local_sem.at[2])
    outward.start()
    for k in range(8):
        to_core(k).wait_send()
    scatter.finish()
    outward.wait()


def feed_last(hidden, feed_full, collective_id):
    size = lax.axis_size("fsdp")
    tokens, width, kind = hidden.shape[0], feed_full.shape[1], hidden.dtype
    block = (tokens // size, width)
    if size != KERNEL_FSDP:
        sums = contract(hidden, feed_full[2], 1, 1).astype(kind)
        return scatter_fsdp((sums.reshape((size,) + block),))
    return scratch_call(
        feed_last_kernel,
        jax.ShapeDtypeStruct(block, jnp.float32),
        [
            *Scatter.scratch(block, kind),
            pltpu.SemaphoreType.DMA((8,)),
            pltpu.SemaphoreType.DMA((8,)),
            pltpu.SemaphoreType.DMA((3,)),
            pltpu.VMEM((8,) + block, kind),
            pltpu.VMEM((1,) + hidden.shape, kind),
            pltpu.VMEM((1,) + feed_full.shape[1:], kind),
        ],
        collective_id,
        hidden,
        feed_full,
    )


def feed_backward(unit_grads, feed_full, feed_input, feed_grad_rows, hidden, collective_id):
    size = lax.axis_size("fsdp")
    kind = hidden.dtype
    tokens, width = feed_input.shape
    if size != KERNEL_FSDP:
        gate_grad, up_grad = unit_grads[0], unit_grads[1]
        sums = contract(gate_grad, feed_full[0], 1, 1) + contract(up_grad, feed_full[1], 1, 1)
        return (
            scatter_fsdp((sums.astype(kind).reshape(size, tokens // size, width),)),
            jnp.stack(
                [
                    contract(left, right, 0, 0).astype(kind)
                    for left, right in ((feed_input, gate_grad), (feed_input, up_grad), (feed_grad_rows, hidden))
                ]
            ),
        )
    block, units = (tokens // size, width), hidden.shape[1]
    tile_rows = width // 6

    def kernel(unit_grads_ref, weights_ref, input_ref, grad_ref, hidden_ref, *refs):
        backward_kernel(unit_grads_ref, weights_ref, (input_ref, grad_ref), hidden_ref, *refs)

    rows_grad, weight_grads = scratch_call(
        kernel,
        (jax.ShapeDtypeStruct(block, jnp.float32), jax.ShapeDtypeStruct((3, width, units), kind)),
        [
            *Scatter.scratch(block, kind),
            pltpu.SemaphoreType.DMA((8,)),
            pltpu.SemaphoreType.DMA((8,)),
            pltpu.SemaphoreType.DMA((6,)),
            pltpu.VMEM((8,) + block, kind),
            pltpu.VMEM((3, tokens, units), kind),
            pltpu.VMEM((2, width, units), kind),
            pltpu.VMEM((2, tokens, width), kind),
            pltpu.VMEM((2, 3, tile_rows, units), kind),
            pltpu.SemaphoreType.DMA((2, 3)),
        ],
        collective_id,
        unit_grads,
        feed_full,
        feed_input,
        feed_grad_rows,
        hidden,
    )
    return rows_grad, weight_grads


def exchange_kernel(block_ref, out_ref, send_sem, receive_sem):
    index, t = lax.axis_index("fsdp"), lax.axis_index("tp")
    partner = (index, 1 - t)
    greet((partner,))
    copy = remote(block_ref, out_ref, send_sem.at[0], receive_sem.at[0], partner)
    copy.start()
    copy.wait()


def exchange_tp(block, collective_id):
    if lax.axis_size("fsdp") != KERNEL_FSDP:
        return lax.ppermute(block, "tp", [(0, 1), (1, 0)])
    return scratch_call(
        exchange_kernel,
        jax.ShapeDtypeStruct(block.shape, block.dtype),
        [pltpu.SemaphoreType.DMA((1,)), pltpu.SemaphoreType.DMA((1,))],
        collective_id,
        block,
    )


def peer(z, x, c, k):
    kz, kx, kc = k // 4, (k // 2) % 2, k % 2
    high, low = z // 2, z % 2
    high = 1 - high if kz // 2 else high
    low = 1 - low if kz % 2 else low
    return fsdp_index(high * 2 + low, 1 - x if kx else x, 1 - c if kc else c)


MAIN = 2 * LANES
REST = LANES
FIRST_REST = KERNEL_FSDP * MAIN
UNITS = 2 * MAIN + REST


def main_of(owner):
    return pl.ds(pl.multiple_of(owner * MAIN, MAIN), MAIN)


def rest_of(z):
    return pl.ds(pl.multiple_of(FIRST_REST + z * REST, REST), REST)


def distribute_kernel(
    rows_ref, query_ref, key_ref, value_ref, output_ref, gain_ref, gate_ref, up_ref, down_ref,
    attention_ref, partner_ref, feed_ref,
    stage, feed, zeros,
    gather_send, gather_receive, local_sem, pair_rows_sem, send_sem, receive_sem, rest_send, rest_receive,
    on_send, on_receive, rest_on_send, rest_on_receive,
):
    z, x, c, t = place()
    own = fsdp_index(z, x, c)
    partner = (own, 1 - t)
    greet([(peer(z, x, c, k), t) for k in range(1, 16)] + [partner])
    rows_copy = remote(rows_ref, partner_ref, pair_rows_sem.at[0], pair_rows_sem.at[1], partner)
    rows_copy.start()
    loads, start = [], 0
    for i, ref in enumerate((query_ref, key_ref, value_ref, output_ref, gain_ref)):
        loads.append(pltpu.make_async_copy(ref, stage.at[:, pl.ds(start, ref.shape[1])], local_sem.at[i]))
        start += ref.shape[1]
    feed_loads = [
        pltpu.make_async_copy(ref, feed.at[i], local_sem.at[5 + i])
        for i, ref in enumerate((gate_ref, up_ref, down_ref))
    ]
    for copy in loads + feed_loads:
        copy.start()
    for copy in loads:
        copy.wait()
    gather = Gather(stage, attention_ref, gather_send, gather_receive)
    gather.start()
    keep = pltpu.make_async_copy(stage, attention_ref.at[own], local_sem.at[8])
    keep.start()
    for copy in feed_loads:
        copy.wait()

    def main_at(half, source):
        return feed_ref.at[:, source, :, pl.ds(pl.multiple_of(half * MAIN, MAIN), MAIN)]

    def rest_at(source):
        return feed_ref.at[:, source, :, pl.ds(2 * MAIN, REST)]

    takes_rest = (c == 0) & (x == t)

    def direct(k):
        to = peer(z, x, c, k)
        return remote(feed.at[:, :, main_of(to)], main_at(t, own), send_sem.at[k], receive_sem.at[k], (to, t))

    def rest(dz):
        to_z = peer(z, x, c, 4 * dz) // 4
        slot = 4 * dz + 2 * ((x + t) % 2) + c
        return remote(
            feed.at[:, :, rest_of(to_z)], rest_at(own), rest_send.at[dz], rest_receive.at[slot], (fsdp_index(to_z, t, 0), t)
        )

    def onward(k):
        at = main_at(t, peer(z, x, c, k))
        return remote(at if k else feed.at[:, :, main_of(own)], at, on_send.at[k], on_receive.at[k], partner)

    def rest_onward(k):
        at = rest_at(peer(z, x, c, k))
        return remote(at if k else feed.at[:, :, rest_of(z)], at, rest_on_send.at[k], rest_on_receive.at[k], partner)

    def send(dz):
        for k in range(4 * dz, 4 * dz + 4):
            if k:
                direct(k).start()
        if dz:
            rest(dz).start()
        else:

            @pl.when(jnp.logical_not(takes_rest))
            def _():
                rest(0).start()

    def pass_on(dz):
        for k in range(4 * dz, 4 * dz + 4):
            if k:
                direct(k).wait_recv()
            onward(k).start()

        @pl.when(takes_rest)
        def _():
            for k in range(4 * dz, 4 * dz + 4):
                if k:
                    remote(
                        feed.at[:, :, rest_of(0)], rest_at(own), rest_send.at[0], rest_receive.at[k], partner
                    ).wait_recv()
                rest_onward(k).start()

    send(0)
    send(1)
    keep_main = pltpu.make_async_copy(feed.at[:, :, main_of(own)], main_at(t, own), local_sem.at[9])
    keep_main.start()
    keep_rest = pltpu.make_async_copy(feed.at[:, :, rest_of(z)], rest_at(own), local_sem.at[10])

    @pl.when(takes_rest)
    def _():
        keep_rest.start()

    fills = [
        pltpu.make_async_copy(zeros, feed_ref.at[i, :, :, pl.ds(2 * MAIN, REST)], local_sem.at[11 + i])
        for i in range(3)
    ]

    @pl.when(c == 1)
    def _():
        zeros[...] = jnp.zeros_like(zeros)
        for copy in fills:
            copy.start()

    send(2)
    pass_on(0)
    pass_on(1)
    gather.line(1)
    gather.side(0)
    send(3)
    gather.line(2)
    gather.side(1)
    pass_on(2)
    gather.line(3)
    pass_on(3)
    gather.side(2)
    gather.side(3)
    gather.finish()
    rows_copy.wait()
    for k in range(16):
        onward(k).wait_recv()
        onward(k).wait_send()
        if k:
            direct(k).wait_send()

    @pl.when(jnp.logical_not(takes_rest))
    def _():
        rest(0).wait_send()

    for dz in (1, 2, 3):
        rest(dz).wait_send()

    @pl.when(takes_rest)
    def _():
        for k in range(16):
            rest_onward(k).wait_send()
        keep_rest.wait()

    @pl.when((c == 0) & (x != t))
    def _():
        for k in range(16):
            rest_onward(k).wait_recv()

    @pl.when(c == 1)
    def _():
        for copy in fills:
            copy.wait()

    keep.wait()
    keep_main.wait()


def distribute(rows, attention, gain_columns, feed, collective_id):
    size = lax.axis_size("fsdp")
    shard_rows, feed_width = feed[0].shape
    columns = sum(w.shape[1] for w in attention) + gain_columns.shape[1]
    if size != KERNEL_FSDP:
        halves = lax.all_to_all(pack_units(feed, size), "fsdp", split_axis=0, concat_axis=0, tiled=True)
        halves = lax.all_gather(halves, "tp", axis=0)
        halves = halves.reshape(halves.shape[0], size * shard_rows, halves.shape[-1])
        return (
            lax.all_gather(jnp.concatenate((*attention, gain_columns), axis=1), "fsdp", axis=0),
            lax.ppermute(rows, "tp", [(0, 1), (1, 0)]),
            jnp.stack(join_units(halves, feed_width, size, 3)),
        )
    kind = rows.dtype
    attention_full, partner_rows, feed_full = scratch_call(
        distribute_kernel,
        (
            jax.ShapeDtypeStruct((size, shard_rows, columns), kind),
            jax.ShapeDtypeStruct(rows.shape, kind),
            jax.ShapeDtypeStruct((3, size, shard_rows, UNITS), kind),
        ),
        [
            pltpu.VMEM((shard_rows, columns), kind),
            pltpu.VMEM((3, shard_rows, feed_width), kind),
            pltpu.VMEM((size, shard_rows, REST), kind),
            pltpu.SemaphoreType.DMA((Gather.slots,)),
            pltpu.SemaphoreType.DMA((size,)),
            pltpu.SemaphoreType.DMA((14,)),
            pltpu.SemaphoreType.DMA((2,)),
            pltpu.SemaphoreType.DMA((size,)),
            pltpu.SemaphoreType.DMA((size,)),
            pltpu.SemaphoreType.DMA((4,)),
            pltpu.SemaphoreType.DMA((size,)),
            pltpu.SemaphoreType.DMA((size,)),
            pltpu.SemaphoreType.DMA((size,)),
            pltpu.SemaphoreType.DMA((size,)),
            pltpu.SemaphoreType.DMA((size,)),
        ],
        collective_id,
        rows,
        *attention,
        gain_columns,
        *feed,
    )
    return attention_full, partner_rows, feed_full.reshape(3, size * shard_rows, UNITS)


def collect_kernel(
    parts_ref, projected_ref, output_ref, gain_ref, out_ref, attention_ref,
    held, received, rest_held, rest_received,
    local_sem, pair_send, pair_receive, rest_pair_send, rest_pair_receive, send_sem, receive_sem, rest_send, rest_receive,
    *scatter_refs,
):
    scatter = Scatter(scatter_refs[:6], scatter_refs[6:10])
    blocks = Blocks(scatter, (projected_ref, output_ref, gain_ref), *scatter_refs[10:13])
    blocks.load()
    z, x, c, t = place()
    own = fsdp_index(z, x, c)
    rows = out_ref.shape[1]
    partner = (own, 1 - t)
    parts = [parts_ref.at[i] for i in range(3)]
    order = (2, 3, 1, 0)
    takes_rest = (c == 0) & (x == t)
    gives_rest = (c == 0) & (x != t)

    def plane(dz):
        return pl.ds(peer(z, x, c, 4 * dz) // 4 * 4, 4)

    def half(which):
        return pl.ds(pl.multiple_of(which * MAIN, MAIN), MAIN)

    rest_columns = pl.ds(2 * MAIN, REST)

    def load(dz, i):
        return pltpu.make_async_copy(parts[i].at[plane(dz), :, half(t)], held.at[dz, i], local_sem.at[3 * dz + i])

    def rest_load(dz, i):
        return pltpu.make_async_copy(
            parts[i].at[plane(dz), :, rest_columns], rest_held.at[dz, i], local_sem.at[12 + 3 * dz + i]
        )

    def pair(dz, i):
        slot = 3 * dz + i
        return remote(
            parts[i].at[plane(dz), :, half(1 - t)], received.at[dz, i], pair_send.at[slot], pair_receive.at[slot], partner
        )

    def rest_pair(dz, i):
        slot = 3 * dz + i
        return remote(
            parts[i].at[plane(dz), :, rest_columns],
            rest_received.at[dz, i],
            rest_pair_send.at[slot],
            rest_pair_receive.at[slot],
            partner,
        )

    def spot(k):
        return peer(z, x, c, k) % 4

    def direct(k):
        return remote(
            held.at[k // 4, :, spot(k)], out_ref.at[:, :, main_of(own)], send_sem.at[k], receive_sem.at[k], (peer(z, x, c, k), t)
        )

    def rest_direct(k):
        return remote(
            rest_held.at[k // 4, :, spot(k)],
            out_ref.at[:, :, rest_of(z)],
            rest_send.at[k],
            rest_receive.at[z],
            (peer(z, x, c, k), t),
        )

    def add(target, source):
        def body(j, carry):
            i, at = j // 4, j % 4
            total = target[i, at].astype(jnp.float32) + source[i, at].astype(jnp.float32)
            target[i, at] = total.astype(target.dtype)
            return carry

        lax.fori_loop(0, 12, body, 0)

    for dz in order:
        for i in range(3):
            load(dz, i).start()

    @pl.when(takes_rest)
    def _():
        for dz in order:
            for i in range(3):
                rest_load(dz, i).start()

    greet([(peer(z, x, c, k), t) for k in range(1, 16)] + [partner])
    blocks.send()
    for dz in order:
        for i in range(3):
            pair(dz, i).start()

        @pl.when(gives_rest)
        def _():
            for i in range(3):
                rest_pair(dz, i).start()

    def pass_on(dz):
        for i in range(3):
            load(dz, i).wait()
            pair(dz, i).wait_recv()
        add(held.at[dz], received.at[dz])
        for k in range(4 * dz, 4 * dz + 4):
            if k:
                direct(k).start()

        @pl.when(takes_rest)
        def _():
            for i in range(3):
                rest_load(dz, i).wait()
                rest_pair(dz, i).wait_recv()
            add(rest_held.at[dz], rest_received.at[dz])
            for k in range(4 * dz, 4 * dz + 4):
                if k:
                    rest_direct(k).start()

    def line(i):
        blocks.both(4 + i)
        scatter.line(i)

    def share(i, carry):
        blocks.both(i)
        scatter.side(i)
        return carry

    lax.fori_loop(0, 4, share, 0)
    pass_on(2)
    line(0)
    pass_on(3)
    line(1)
    pass_on(1)
    line(2)
    pass_on(0)
    blocks.both(7)
    scatter.last()
    outward = pltpu.make_async_copy(scatter.total, attention_ref, local_sem.at[26])
    outward.start()
    keep = pltpu.make_async_copy(held.at[0, :, spot(0)], out_ref.at[:, :, main_of(own)], local_sem.at[24])
    keep.start()
    keep_rest = pltpu.make_async_copy(rest_held.at[0, :, spot(0)], out_ref.at[:, :, rest_of(z)], local_sem.at[25])

    @pl.when(takes_rest)
    def _():
        keep_rest.start()

    for k in range(1, 16):
        direct(k).wait_recv()

    for dz in range(4):
        from_z = peer(z, x, c, 4 * dz) // 4

        def arrived():
            remote(
                rest_held.at[0, :, 0], out_ref.at[:, :, rest_of(from_z)], rest_send.at[0], rest_receive.at[from_z], partner
            ).wait_recv()

        if dz:
            arrived()
        else:

            @pl.when(jnp.logical_not(takes_rest))
            def _():
                arrived()

    for k in range(1, 16):
        direct(k).wait_send()
    for dz in order:
        for i in range(3):
            pair(dz, i).wait_send()

    @pl.when(gives_rest)
    def _():
        for dz in order:
            for i in range(3):
                rest_pair(dz, i).wait_send()

    @pl.when(takes_rest)
    def _():
        for k in range(1, 16):
            rest_direct(k).wait_send()
        keep_rest.wait()

    blocks.finish()
    scatter.finish()
    keep.wait()
    outward.wait()


def collect(gradients, feed_width, attention_parts, collective_id):
    size, pairs = lax.axis_size("fsdp"), lax.axis_size("tp")
    shard_rows = gradients.shape[1] // size
    if size != KERNEL_FSDP:
        packed = part_units([gradients[i] for i in range(3)], feed_width, size, pairs)
        mine = lax.psum_scatter(packed, "tp", scatter_dimension=0, tiled=False)
        mine = mine.reshape(size, shard_rows, mine.shape[-1])
        mine = lax.all_to_all(mine, "fsdp", split_axis=0, concat_axis=0, tiled=True)
        feed = [g.astype(jnp.float32) for g in unpack_units(mine, feed_width, 3)]
        return feed, scatter_fsdp(attention_parts)
    kind = gradients.dtype
    main, rest = (4, 3, 4, shard_rows, MAIN), (4, 3, 4, shard_rows, REST)
    block = (shard_rows, sum(part.shape[2] for part in attention_parts))
    out, attention = scratch_call(
        collect_kernel,
        (
            jax.ShapeDtypeStruct((3, shard_rows, feed_width), kind),
            jax.ShapeDtypeStruct(block, jnp.float32),
        ),
        [
            pltpu.VMEM(main, kind),
            pltpu.VMEM(main, kind),
            pltpu.VMEM(rest, kind),
            pltpu.VMEM(rest, kind),
            pltpu.SemaphoreType.DMA((27,)),
            pltpu.SemaphoreType.DMA((12,)),
            pltpu.SemaphoreType.DMA((12,)),
            pltpu.SemaphoreType.DMA((12,)),
            pltpu.SemaphoreType.DMA((12,)),
            pltpu.SemaphoreType.DMA((size,)),
            pltpu.SemaphoreType.DMA((size,)),
            pltpu.SemaphoreType.DMA((size,)),
            pltpu.SemaphoreType.DMA((4,)),
            *Scatter.scratch(block, kind),
            *[pltpu.SemaphoreType.DMA((24,)) for _ in range(3)],
        ],
        collective_id,
        gradients.reshape(3, size, shard_rows, UNITS),
        *attention_parts,
    )
    return [out[i].astype(jnp.float32) for i in range(3)], attention


def contract_last(left_rows, right_rows):
    return lax.dot_general(
        left_rows, right_rows, (((1,), (1,)), ((), ())), preferred_element_type=jnp.float32
    )


def contract_first(left_rows, right_rows):
    return lax.dot_general(
        left_rows, right_rows, (((0,), (0,)), ((), ())), preferred_element_type=jnp.float32
    )


def normalize_parts(value_rows):
    inverse = lax.rsqrt(jnp.mean(value_rows * value_rows, axis=-1, keepdims=True) + EPSILON)
    return (value_rows * inverse, inverse)


def norm_backward(unit_rows, inverse, norm_gain, upstream):
    scaled = upstream * norm_gain
    return inverse * (scaled - unit_rows * jnp.mean(scaled * unit_rows, axis=-1, keepdims=True))


def layout(lengths_row, row_index):
    segment_ends = jnp.cumsum(lengths_row)
    segment_starts = segment_ends - lengths_row
    segment = jnp.sum((row_index[:, None] >= segment_ends[None, :]).astype(jnp.int32), axis=1)
    onehot = segment[:, None] == jnp.arange(lengths_row.shape[0], dtype=jnp.int32)[None, :]
    segment_begin = jnp.sum(jnp.where(onehot, segment_starts[None, :], 0), axis=1)
    prompt_shift = jnp.where(segment > 0, lengths_row[0], 0)
    return (segment, row_index - segment_begin + prompt_shift)


def rotary_tables(position):
    frequency = jnp.exp(
        jnp.arange(HEAD_SIZE // 2, dtype=jnp.float32) * (-2.0 * math.log(10000.0) / HEAD_SIZE)
    )
    angles = position.astype(jnp.float32)[:, None] * frequency[None, :]
    return (jnp.cos(angles), jnp.sin(angles))


def apply_rotary(value_rows, cosine_lookup, sine_lookup):
    half_width = value_rows.shape[-1] // 2
    first_half = value_rows[..., :half_width]
    second_half = value_rows[..., half_width:]
    cosine_part = cosine_lookup[:, None, :]
    sine_part = sine_lookup[:, None, :]
    return jnp.concatenate(
        [
            first_half * cosine_part - second_half * sine_part,
            second_half * cosine_part + first_half * sine_part,
        ],
        axis=-1,
    )


def unrotate(value_rows, cosine_lookup, sine_lookup):
    half_width = value_rows.shape[-1] // 2
    first_half = value_rows[..., :half_width]
    second_half = value_rows[..., half_width:]
    cosine_part = cosine_lookup[:, None, :]
    sine_part = sine_lookup[:, None, :]
    return jnp.concatenate(
        [
            first_half * cosine_part + second_half * sine_part,
            second_half * cosine_part - first_half * sine_part,
        ],
        axis=-1,
    )


def visible(segment, row_index):
    same_segment = (segment[:, None] == segment[None, :]) & (
        row_index[None, :] <= row_index[:, None]
    )
    from_prompt = (segment[None, :] == 0) & (segment[:, None] > 0)
    return same_segment | from_prompt


def masked_scores(rotated_query, rotated_key, visible_mask):
    raw_scores = jnp.einsum(
        "qgrd,kgd->grqk", rotated_query, rotated_key, preferred_element_type=jnp.float32
    )
    tanh_value = jnp.tanh(raw_scores * HEAD_SIZE ** (-0.5) / SOFTCAP)
    return (jnp.where(visible_mask[None, None], SOFTCAP * tanh_value, NEGATIVE), tanh_value)


def gelu_product(gate_value, up_value):
    return jax.nn.gelu(gate_value, approximate=True) * up_value


def split_columns(width, size):
    main = width // size // LANES * LANES
    return main, width // size - main


def pack_units(weights, size):
    rows, width = weights[0].shape
    main, rest = split_columns(width, size)
    pieces = []
    if main:
        pieces += [
            jnp.transpose(w[:, : main * size].reshape(rows, size, main), (1, 0, 2)) for w in weights
        ]
    if rest:
        pieces += [
            jnp.transpose(w[:, main * size :].reshape(rows, size, rest), (1, 0, 2)) for w in weights
        ]
    packed = jnp.concatenate(pieces, axis=2)
    return jnp.pad(packed, ((0, 0), (0, 0), (0, -packed.shape[2] % LANES)))


def unpack_units(packed, width, amount):
    size, rows, _ = packed.shape
    main, rest = split_columns(width, size)
    arrays = []
    for i in range(amount):
        pieces = []
        if main:
            piece = packed[:, :, i * main : (i + 1) * main]
            pieces.append(jnp.transpose(piece, (1, 0, 2)).reshape(rows, size * main))
        if rest:
            start = amount * main + i * rest
            piece = packed[:, :, start : start + rest]
            pieces.append(jnp.transpose(piece, (1, 0, 2)).reshape(rows, size * rest))
        arrays.append(jnp.concatenate(pieces, axis=1))
    return arrays


def join_units(halves, width, size, amount):
    main, rest = split_columns(width, size)
    arrays = []
    for i in range(amount):
        start = amount * main + i * rest
        pieces = [half[:, i * main : (i + 1) * main] for half in halves]
        pieces += [half[:, start : start + rest] for half in halves]
        joined = jnp.concatenate(pieces, axis=1)
        arrays.append(jnp.pad(joined, ((0, 0), (0, -joined.shape[1] % LANES))))
    return arrays


def part_units(arrays, width, size, pairs):
    main, rest = split_columns(width, size)
    halves = []
    for t in range(pairs):
        pieces = [array[:, t * main : (t + 1) * main] for array in arrays]
        start = pairs * main + t * rest
        pieces += [array[:, start : start + rest] for array in arrays]
        packed = jnp.concatenate(pieces, axis=1)
        halves.append(jnp.pad(packed, ((0, 0), (0, -packed.shape[1] % LANES))))
    return jnp.stack(halves)


def shards(
    block_input,
    lengths,
    attention_norm_gain,
    attention_post_gain,
    feedforward_norm_gain,
    feedforward_post_gain,
    query_weight,
    key_weight,
    value_weight,
    output_weight,
    gate_weight,
    up_weight,
    down_weight,
    output_cotangent,
):
    low = jnp.bfloat16
    size, pairs = lax.axis_size("fsdp"), lax.axis_size("tp")
    rows_local, width = block_input.shape
    shard_rows, feed_width = gate_weight.shape
    query_width, key_width = query_weight.shape[1], key_weight.shape[1]
    output_start = query_width + 2 * key_width
    gain_start = output_start + query_width
    grouped_rows = rows_local * pairs

    gain_columns = jnp.stack(
        [attention_norm_gain, attention_post_gain, feedforward_norm_gain, feedforward_post_gain],
        axis=1,
    )
    attention_full, other_input, feed_full = distribute(
        block_input,
        (query_weight, key_weight, value_weight, output_weight),
        jnp.pad(gain_columns, ((0, 0), (0, LANES - 4))),
        (gate_weight, up_weight, down_weight),
        1,
    )
    attention_full = attention_full.reshape(size * shard_rows, gain_start + LANES)
    gains = jnp.transpose(attention_full[:, gain_start : gain_start + 4]).astype(jnp.float32)
    gain_one, gain_two, gain_three, gain_four = gains[0], gains[1], gains[2], gains[3]

    row_index = (
        jnp.arange(grouped_rows, dtype=jnp.int32) + lax.axis_index("tp") * rows_local
    ) % grouped_rows
    segment, position = layout(lengths[0], row_index)
    cosine_lookup, sine_lookup = rotary_tables(position)
    visible_mask = visible(segment, row_index)
    residual_both = jnp.concatenate([block_input, other_input], axis=0).astype(jnp.float32)
    unit_one_both, inverse_one_both = normalize_parts(residual_both)
    residual = residual_both[:rows_local]
    unit_one, inverse_one = unit_one_both[:rows_local], inverse_one_both[:rows_local]
    normed = (unit_one_both * gain_one).astype(low)
    projected = jnp.dot(
        normed, attention_full[:, :output_start], preferred_element_type=jnp.float32
    )
    query_raw = projected[:, :query_width]
    key_raw = projected[:, query_width : query_width + key_width]
    value_raw = projected[:, query_width + key_width :]
    heads_local = query_width // HEAD_SIZE
    kv_local = key_width // HEAD_SIZE
    repeat_heads = heads_local // kv_local
    rotated_query = apply_rotary(
        query_raw.reshape(grouped_rows, heads_local, HEAD_SIZE), cosine_lookup, sine_lookup
    ).astype(low)
    rotated_query = rotated_query.reshape(grouped_rows, kv_local, repeat_heads, HEAD_SIZE)
    rotated_key = apply_rotary(
        key_raw.reshape(grouped_rows, kv_local, HEAD_SIZE), cosine_lookup, sine_lookup
    ).astype(low)
    value_reduced = value_raw.astype(low).reshape(grouped_rows, kv_local, HEAD_SIZE)
    capped, tanh_value = masked_scores(rotated_query, rotated_key, visible_mask)
    row_peak = jnp.max(capped, axis=-1, keepdims=True)
    exponentials = jnp.exp(capped - row_peak)
    softmax_probs = exponentials / jnp.sum(exponentials, axis=-1, keepdims=True)
    probs_low = softmax_probs.astype(low)
    mixed_heads = jnp.einsum(
        "grqk,kgd->qgrd", probs_low, value_reduced, preferred_element_type=jnp.float32
    )
    attended = mixed_heads.reshape(grouped_rows, heads_local * HEAD_SIZE).astype(low)
    output_full = attention_full[:, output_start:gain_start]
    branch_parts = contract_last(attended, output_full)
    branch_one = branch_parts[:rows_local] + exchange_tp(
        branch_parts[rows_local:].astype(low), 4
    ).astype(jnp.float32)
    unit_two, inverse_two = normalize_parts(branch_one)
    middle = residual + unit_two * gain_two
    unit_three, inverse_three = normalize_parts(middle)

    feed_input, gate_up, hidden = feed_first((unit_three * gain_three).astype(low), feed_full, 5)
    branch_two = feed_last(hidden, feed_full, 6)
    unit_four, inverse_four = normalize_parts(branch_two)
    block_output = (middle + unit_four * gain_four).astype(low)
    upstream = output_cotangent.astype(jnp.float32)
    gain_four_grad = jnp.sum(upstream * unit_four, axis=0)
    branch_two_grad = norm_backward(unit_four, inverse_four, gain_four, upstream).astype(low)
    feed_grad_rows, unit_grads = hidden_back(branch_two_grad, feed_full, gate_up, 7)
    normed_three_grad, feed_grads = feed_backward(
        unit_grads, feed_full, feed_input, feed_grad_rows, hidden, 8
    )
    gain_three_grad = jnp.sum(normed_three_grad * unit_three, axis=0)
    middle_grad = upstream + norm_backward(unit_three, inverse_three, gain_three, normed_three_grad)
    gain_two_grad = jnp.sum(middle_grad * unit_two, axis=0)
    branch_one_grad = norm_backward(unit_two, inverse_two, gain_two, middle_grad).astype(low)
    attention_grad_rows = jnp.concatenate(
        [branch_one_grad, exchange_tp(branch_one_grad, 10)], axis=0
    )
    mixed_grad = jnp.dot(
        attention_grad_rows, output_full, preferred_element_type=jnp.float32
    ).astype(low)
    mixed_grad = mixed_grad.reshape(grouped_rows, kv_local, repeat_heads, HEAD_SIZE)
    value_grad = jnp.einsum(
        "grqk,qgrd->kgd", probs_low, mixed_grad, preferred_element_type=jnp.float32
    )
    probs_grad = jnp.einsum(
        "qgrd,kgd->grqk", mixed_grad, value_reduced, preferred_element_type=jnp.float32
    )
    score_grad = softmax_probs * (
        probs_grad - jnp.sum(softmax_probs * probs_grad, axis=-1, keepdims=True)
    )
    raw_grad = (score_grad * (1.0 - tanh_value * tanh_value) * HEAD_SIZE ** (-0.5)).astype(low)
    query_grad = jnp.einsum(
        "grqk,kgd->qgrd", raw_grad, rotated_key, preferred_element_type=jnp.float32
    )
    key_grad = jnp.einsum(
        "grqk,qgrd->kgd", raw_grad, rotated_query, preferred_element_type=jnp.float32
    )
    query_grad = unrotate(
        query_grad.reshape(grouped_rows, heads_local, HEAD_SIZE), cosine_lookup, sine_lookup
    )
    key_grad = unrotate(key_grad, cosine_lookup, sine_lookup)
    projected_grad = jnp.concatenate(
        [
            query_grad.reshape(grouped_rows, heads_local * HEAD_SIZE).astype(low),
            key_grad.reshape(grouped_rows, kv_local * HEAD_SIZE).astype(low),
            value_grad.reshape(grouped_rows, kv_local * HEAD_SIZE).astype(low),
        ],
        axis=1,
    )
    input_parts = lax.optimization_barrier(
        contract_last(projected_grad, attention_full[:, :output_start])
    )

    gain_grads = jnp.stack(
        [
            jnp.sum(input_parts * unit_one_both, axis=0),
            gain_two_grad,
            gain_three_grad,
            gain_four_grad,
        ]
    )
    sent = jnp.concatenate(
        [input_parts[rows_local:].astype(low), jnp.pad(gain_grads, ((0, 12), (0, 0))).astype(low)]
    )
    received = exchange_tp(sent, 11).astype(jnp.float32)
    normed_one_grad = input_parts[:rows_local] + received[:rows_local]
    gain_grads = gain_grads + received[rows_local : rows_local + 4]
    input_gradient = middle_grad + norm_backward(unit_one, inverse_one, gain_one, normed_one_grad)

    (gate_weight_grad, up_weight_grad, down_weight_grad), attention_grads = collect(
        feed_grads,
        feed_width,
        [
            part.astype(low).reshape(size, shard_rows, part.shape[1])
            for part in (
                contract_first(normed, projected_grad),
                contract_first(attention_grad_rows, attended),
                jnp.pad(jnp.transpose(gain_grads), ((0, 0), (0, LANES - 4))),
            )
        ],
        9,
    )
    gain_shards = jnp.transpose(attention_grads[:, gain_start : gain_start + 4])
    return (
        block_output,
        input_gradient,
        gain_shards[0],
        gain_shards[1],
        gain_shards[2],
        gain_shards[3],
        attention_grads[:, :query_width],
        attention_grads[:, query_width : query_width + key_width],
        attention_grads[:, query_width + key_width : output_start],
        attention_grads[:, output_start:gain_start],
        gate_weight_grad,
        up_weight_grad,
        down_weight_grad,
    )


def solution(mesh):
    placed = (
        P(("fsdp", "tp"), None),
        P("fsdp", None),
        P("fsdp"),
        P("fsdp"),
        P("fsdp"),
        P("fsdp"),
        P("fsdp", "tp"),
        P("fsdp", "tp"),
        P("fsdp", "tp"),
        P("fsdp", "tp"),
        P("fsdp", "tp"),
        P("fsdp", "tp"),
        P("fsdp", "tp"),
        P(("fsdp", "tp"), None),
    )
    return jax.shard_map(
        shards,
        mesh=mesh,
        in_specs=placed,
        out_specs=(
            P(("fsdp", "tp"), None),
            P(("fsdp", "tp"), None),
            P("fsdp"),
            P("fsdp"),
            P("fsdp"),
            P("fsdp"),
            P("fsdp", "tp"),
            P("fsdp", "tp"),
            P("fsdp", "tp"),
            P("fsdp", "tp"),
            P("fsdp", "tp"),
            P("fsdp", "tp"),
            P("fsdp", "tp"),
        ),
        check_vma=False,
    )
```

```python
import functools
import math

import jax
import jax.numpy as jnp
from jax import lax
from jax.experimental import pallas as pl
from jax.experimental.pallas import tpu as pltpu
from jax.sharding import PartitionSpec as P

HEAD_SIZE = 256
MESH = pl.DeviceIdType.MESH
ANY = pl.BlockSpec(memory_space=pl.ANY)
LANES = 128

EPSILON = 1e-06
SOFTCAP = 50.0
NEGATIVE = -1e30

KERNEL_FSDP = 16


def place():
    index = lax.axis_index("fsdp")
    return index // 4, (index // 2) % 2, index % 2, lax.axis_index("tp")


def fsdp_index(z, x, c):
    return (z * 2 + x) * 2 + c


def remote(source, target, send_sem, receive_sem, device):
    return pltpu.make_async_remote_copy(
        src_ref=source,
        dst_ref=target,
        send_sem=send_sem,
        recv_sem=receive_sem,
        device_id=device,
        device_id_type=MESH,
    )


def greet(devices):
    barrier = pltpu.get_barrier_semaphore()
    for device in devices:
        pl.semaphore_signal(barrier, inc=1, device_id=device, device_id_type=MESH)
    pl.semaphore_wait(barrier, len(devices))


def greet_line(z, devices, down, up):
    barrier = pltpu.get_barrier_semaphore()
    for device in devices:
        pl.semaphore_signal(barrier, inc=1, device_id=device, device_id_type=MESH)

    @pl.when(z > 0)
    def _():
        pl.semaphore_signal(barrier, inc=1, device_id=down, device_id_type=MESH)

    @pl.when(z < 3)
    def _():
        pl.semaphore_signal(barrier, inc=1, device_id=up, device_id_type=MESH)

    pl.semaphore_wait(barrier, len(devices) + (z + 2) // 3 + (5 - z) // 3)


class Gather:
    slots = 29

    def __init__(self, block, out_ref, send_sem, receive_sem):
        self.block, self.out, self.send_sem, self.receive_sem = block, out_ref, send_sem, receive_sem
        self.z, self.x, self.c, t = place()
        z, x, c = self.z, self.x, self.c
        self.own = fsdp_index(z, x, c)
        self.down, self.up = (fsdp_index(z - 1, x, c), t), (fsdp_index(z + 1, x, c), t)
        self.across, self.other = (fsdp_index(z, 1 - x, c), t), (fsdp_index(z, x, 1 - c), t)

    def copy(self, source, index, slot, device):
        return remote(source, self.out.at[index], self.send_sem.at[slot], self.receive_sem.at[index], device)

    def relay(self, index, slot, device):
        self.copy(self.out.at[index], index, slot, device).start()

    def arrived(self, index):
        self.copy(self.block, index, 0, self.other).wait_recv()

    def sent(self, slot):
        self.copy(self.block, self.own, slot, self.other).wait_send()

    def start(self):
        @pl.when(self.z < 3)
        def _():
            self.copy(self.block, self.own, 0, self.up).start()

        @pl.when(self.z > 0)
        def _():
            self.copy(self.block, self.own, 1, self.down).start()

        self.copy(self.block, self.own, 2, self.across).start()
        self.copy(self.block, self.own, 3, self.other).start()

    def line(self, d):
        z, x, c = self.z, self.x, self.c

        @pl.when(z >= d)
        def _():
            index = fsdp_index(z - d, x, c)
            base = 4 + 3 * (d - 1)
            self.arrived(index)

            @pl.when(z < 3)
            def _():
                self.relay(index, base, self.up)

            self.relay(index, base + 1, self.across)
            self.relay(index, base + 2, self.other)

        @pl.when(z + d <= 3)
        def _():
            index = fsdp_index(z + d, x, c)
            base = 13 + 3 * (d - 1)
            self.arrived(index)

            @pl.when(z > 0)
            def _():
                self.relay(index, base, self.down)

            self.relay(index, base + 1, self.across)
            self.relay(index, base + 2, self.other)

    def side(self, d):
        z, x, c = self.z, self.x, self.c
        if d == 0:
            index = fsdp_index(z, 1 - x, c)
            self.arrived(index)
            self.relay(index, 22, self.other)
            return

        @pl.when(z >= d)
        def _():
            index = fsdp_index(z - d, 1 - x, c)
            self.arrived(index)
            self.relay(index, 22 + d, self.other)

        @pl.when(z + d <= 3)
        def _():
            index = fsdp_index(z + d, 1 - x, c)
            self.arrived(index)
            self.relay(index, 25 + d, self.other)

    def finish(self, waits=True):
        z = self.z
        if waits:
            for zi in range(4):
                for xi in range(2):
                    self.arrived(fsdp_index(zi, xi, 1 - self.c))

        @pl.when(z < 3)
        def _():
            self.sent(0)

        @pl.when(z > 0)
        def _():
            self.sent(1)

        for slot in (2, 3, 22):
            self.sent(slot)
        for d in (1, 2, 3):

            @pl.when(z >= d)
            def _():
                base = 4 + 3 * (d - 1)

                @pl.when(z < 3)
                def _():
                    self.sent(base)

                for slot in (base + 1, base + 2, 22 + d):
                    self.sent(slot)

            @pl.when(z + d <= 3)
            def _():
                base = 13 + 3 * (d - 1)

                @pl.when(z > 0)
                def _():
                    self.sent(base)

                for slot in (base + 1, base + 2, 25 + d):
                    self.sent(slot)


def scratch_call(kernel, outputs, scratch, collective_id, *operands):
    return pl.pallas_call(
        kernel,
        out_shape=outputs,
        in_specs=[ANY] * len(operands),
        out_specs=jax.tree.map(lambda _: ANY, outputs),
        scratch_shapes=scratch,
        compiler_params=pltpu.CompilerParams(
            collective_id=collective_id, has_side_effects=True, vmem_limit_bytes=60 * 1024 * 1024
        ),
    )(*operands)


def add_rows(rows, step, target, *sources):
    def body(i, carry):
        at = pl.ds(pl.multiple_of(i * step, step), step)
        total = sources[0][at, :].astype(jnp.float32)
        for source in sources[1:]:
            total = total + source[at, :].astype(jnp.float32)
        target[at, :] = total.astype(target.dtype)
        return carry

    lax.fori_loop(0, rows // step, body, 0)


class Scatter:
    def __init__(self, buffers, semaphores):
        self.held, self.from_core, self.from_across, self.from_below, self.from_above, self.total = buffers
        self.send_sem, self.across_sem, self.below_sem, self.above_sem = semaphores
        self.z, self.x, self.c, t = place()
        z, x, c = self.z, self.x, self.c
        self.rows = self.total.shape[0]
        self.down, self.up = (fsdp_index(z - 1, x, c), t), (fsdp_index(z + 1, x, c), t)
        self.across, self.other = (fsdp_index(z, 1 - x, c), t), (fsdp_index(z, x, 1 - c), t)

    def target(self, i):
        half = self.z // 2
        mirrored = self.z + half * (3 - 2 * self.z)
        base = 3 - i + mirrored * (i // 2) * (2 * (i % 2) - 1)
        return base + half * (3 - 2 * base)

    def index(self, k, core):
        return fsdp_index(self.target(k % 4), (self.x + 1 - k // 4) % 2, core)

    def add(self, target, *sources):
        add_rows(self.rows, 16, target, *sources)

    def over(self, i):
        return remote(
            self.held.at[i], self.from_across.at[i], self.send_sem.at[3 + i], self.across_sem.at[i], self.across
        )

    def going_up(self, i, target):
        return remote(
            self.held.at[4 + i], self.from_below.at[target], self.send_sem.at[i], self.below_sem.at[target], self.up
        )

    def going_down(self, i, target):
        return remote(
            self.held.at[4 + i], self.from_above.at[target], self.send_sem.at[i], self.above_sem.at[target], self.down
        )

    def side(self, i):
        self.add(self.held.at[i], self.held.at[i], self.from_core.at[i])
        self.over(i).start()

    def line(self, i):
        z, target = self.z, self.target(i)
        held = self.held.at[4 + i]
        sources = (held, self.from_core.at[4 + i], self.from_across.at[i])
        self.over(i).wait_recv()

        @pl.when(target > z)
        def _():
            @pl.when(z > 0)
            def _():
                self.going_up(i, target).wait_recv()
                self.add(held, *sources, self.from_below.at[target])

            @pl.when(z == 0)
            def _():
                self.add(held, *sources)

            self.going_up(i, target).start()

        @pl.when(target < z)
        def _():
            @pl.when(z < 3)
            def _():
                self.going_down(i, target).wait_recv()
                self.add(held, *sources, self.from_above.at[target])

            @pl.when(z == 3)
            def _():
                self.add(held, *sources)

            self.going_down(i, target).start()

    def last(self):
        z = self.z
        self.over(3).wait_recv()
        self.add(self.total, self.held.at[7], self.from_core.at[7], self.from_across.at[3])

        @pl.when(z > 0)
        def _():
            self.going_up(0, z).wait_recv()
            self.add(self.total, self.total, self.from_below.at[z])

        @pl.when(z < 3)
        def _():
            self.going_down(0, z).wait_recv()
            self.add(self.total, self.total, self.from_above.at[z])

    def finish(self):
        for i in range(4):
            self.over(i).wait_send()
        for i in range(3):
            self.going_up(i, 0).wait_send()

    @staticmethod
    def scratch(block, kind):
        return [
            *[pltpu.VMEM((amount,) + block, kind) for amount in (8, 8, 4, 4, 4)],
            pltpu.VMEM(block, jnp.float32),
            *[pltpu.SemaphoreType.DMA((amount,)) for amount in (7, 4, 4, 4)],
        ]


def contract(left, right, left_dim, right_dim):
    return lax.dot_general(
        left, right, (((left_dim,), (right_dim,)), ((), ())), preferred_element_type=jnp.float32
    )


def backward_kernel(
    unit_grads_ref, weights_ref, rows_ref, hidden_ref, out_ref, weight_grads_ref,
    held, from_core, from_across, from_below, from_above, total, send_sem, across_sem, below_sem, above_sem,
    core_send_sem, core_sem, local_sem, for_core, unit_grads, weights, rows, tile, tile_sem,
):
    scatter = Scatter(
        (held, from_core, from_across, from_below, from_above, total), (send_sem, across_sem, below_sem, above_sem)
    )
    block_rows, width = out_ref.shape
    loads = [
        pltpu.make_async_copy(unit_grads_ref, unit_grads.at[pl.ds(0, 2)], local_sem.at[0]),
        pltpu.make_async_copy(weights_ref.at[pl.ds(0, 2)], weights, local_sem.at[1]),
        pltpu.make_async_copy(hidden_ref, unit_grads.at[2], local_sem.at[2]),
        pltpu.make_async_copy(rows_ref[0], rows.at[0], local_sem.at[3]),
        pltpu.make_async_copy(rows_ref[1], rows.at[1], local_sem.at[4]),
    ]
    for copy in loads:
        copy.start()
    greet_line(scatter.z, (scatter.across, scatter.other), scatter.down, scatter.up)
    loads[0].wait()
    loads[1].wait()

    def to_core(k):
        return remote(for_core.at[k], from_core.at[k], core_send_sem.at[k], core_sem.at[k], scatter.other)

    tile_rows = tile.shape[2]

    def tile_out(u, i):
        at = pl.ds(pl.multiple_of(u * tile_rows, tile_rows), tile_rows)
        return pltpu.make_async_copy(tile.at[u % 2, i], weight_grads_ref.at[i, at, :], tile_sem.at[u % 2, i])

    def weight_tile(u):
        @pl.when(u == 0)
        def _():
            for copy in loads[2:]:
                copy.wait()

        @pl.when(u >= 2)
        def _():
            for i in range(3):
                tile_out(u - 2, i).wait()

        def body(i, carry):
            left = rows[i // 2, :, pl.ds(pl.multiple_of(u * tile_rows, tile_rows), tile_rows)]
            tile[u % 2, i] = contract(left, unit_grads[i], 0, 0).astype(tile.dtype)
            return carry

        lax.fori_loop(0, 3, body, 0)
        for i in range(3):
            tile_out(u, i).start()

    def step(n, carry):
        @pl.when(n < 4)
        def _():
            partial_pair(scatter, unit_grads, weights, block_rows, n, 1 - scatter.c, for_core)
            to_core(n).start()
            to_core(4 + n).start()
            partial_pair(scatter, unit_grads, weights, block_rows, n, scatter.c, held)
            to_core(n).wait_recv()
            scatter.side(n)

        @pl.when(n >= 4)
        def _():
            to_core(n).wait_recv()
            scatter.line(n - 4)

        @pl.when(n >= 4)
        def _():
            weight_tile(2 * n - 8)
            weight_tile(2 * n - 7)

        return carry

    lax.fori_loop(0, 7, step, 0)
    to_core(7).wait_recv()
    scatter.last()
    outward = pltpu.make_async_copy(total, out_ref, local_sem.at[5])
    outward.start()
    for k in range(8):
        to_core(k).wait_send()
    scatter.finish()
    for u in (4, 5):
        for i in range(3):
            tile_out(u, i).wait()
    outward.wait()


def scatter_fsdp(parts):
    return lax.psum_scatter(jnp.concatenate(parts, axis=2), "fsdp", scatter_dimension=0, tiled=False).astype(jnp.float32)


def gather_through(block_ref, gathered, gathered_ref, send_sem, receive_sem, out_sem, prepare, compute):
    gather = Gather(block_ref, gathered, send_sem, receive_sem)
    z, x, c = gather.z, gather.x, gather.c
    _, block_rows, width = gathered.shape
    own = pltpu.make_async_copy(block_ref, gathered.at[gather.own], out_sem.at[8])
    own.start()
    greet_line(z, (gather.across, gather.other), gather.down, gather.up)
    gather.start()

    def out(number):
        at = pl.ds(number * 2, 2)
        return pltpu.make_async_copy(gathered.at[at], gathered_ref.at[at], out_sem.at[number])

    def step(n, carry):
        @pl.when(n == 2)
        def _():
            gather.line(2)
            gather.side(1)

        @pl.when(n == 4)
        def _():
            gather.line(3)
            gather.side(2)

        @pl.when(n == 6)
        def _():
            gather.side(3)

        dz = n // 4 * 2 + n % 2
        side = (x + n // 2) % 2
        zi = (z // 2 + dz // 2) % 2 * 2 + (z + dz) % 2
        number = zi * 2 + side
        gather.arrived(fsdp_index(zi, side, 1 - c))
        out(number).start()
        left = gathered[pl.ds(number * 2, 2)].reshape(2 * block_rows, width)
        compute(number, pl.ds(pl.multiple_of(number * 2 * block_rows, 2 * block_rows), 2 * block_rows), left)
        return carry

    gather.line(1)
    gather.side(0)
    own.wait()
    prepare()
    lax.fori_loop(0, 8, step, 0)
    gather.finish(waits=False)
    for number in range(8):
        out(number).wait()


GELU_SCALE = math.sqrt(2.0 / math.pi)
GELU_CUBE = 0.044715


def feed_first_kernel(
    block_ref, weights_ref, gathered_ref, gate_up_ref, hidden_ref,
    gathered, send_sem, receive_sem, out_sem, weights, gate_up, hidden, load_sem, gate_up_sem, hidden_sem,
):
    load = pltpu.make_async_copy(weights_ref.at[pl.ds(0, 2)], weights, load_sem.at[0])
    load.start()

    def outs(number, rows):
        return (
            pltpu.make_async_copy(gate_up.at[:, rows, :], gate_up_ref.at[:, rows, :], gate_up_sem.at[number]),
            pltpu.make_async_copy(hidden.at[rows, :], hidden_ref.at[rows, :], hidden_sem.at[number]),
        )

    def compute(number, rows, left):
        gate = contract(left, weights[0], 1, 0)
        gate_up[0, rows, :] = gate
        up = contract(left, weights[1], 1, 0)
        gate_up[1, rows, :] = up
        gate = gate_up[0, rows, :]
        curve = jnp.tanh(GELU_SCALE * (gate + GELU_CUBE * (gate * gate * gate)))
        hidden[rows, :] = (0.5 * gate * (1.0 + curve) * up).astype(hidden.dtype)
        for copy in outs(number, rows):
            copy.start()

    gather_through(block_ref, gathered, gathered_ref, send_sem, receive_sem, out_sem, load.wait, compute)
    pair_rows = hidden.shape[0] // 8
    for number in range(8):
        for copy in outs(number, pl.ds(number * pair_rows, pair_rows)):
            copy.wait()


def hidden_back_kernel(
    block_ref, weights_ref, gate_up_ref, gathered_ref, unit_grads_ref,
    gathered, send_sem, receive_sem, out_sem, weights, gate_up, unit_grads, load_sem, grads_sem,
):
    loads = [
        pltpu.make_async_copy(weights_ref.at[2], weights, load_sem.at[0]),
        pltpu.make_async_copy(gate_up_ref, gate_up, load_sem.at[1]),
    ]
    for copy in loads:
        copy.start()

    def prepare():
        for copy in loads:
            copy.wait()

    def out(number, rows):
        return pltpu.make_async_copy(unit_grads.at[:, rows, :], unit_grads_ref.at[:, rows, :], grads_sem.at[number])

    def compute(number, rows, left):
        hidden_grad = contract(left, weights[...], 1, 0)
        gate, up = gate_up[0, rows, :], gate_up[1, rows, :]
        square = gate * gate
        curve = jnp.tanh(GELU_SCALE * (gate + GELU_CUBE * (square * gate)))
        inner = GELU_SCALE * (1.0 + 3.0 * GELU_CUBE * square)
        slope = 0.5 * (1.0 + curve) + 0.5 * gate * (1.0 - curve * curve) * inner
        unit_grads[0, rows, :] = (hidden_grad * up * slope).astype(unit_grads.dtype)
        unit_grads[1, rows, :] = (hidden_grad * (0.5 * gate * (1.0 + curve))).astype(unit_grads.dtype)
        out(number, rows).start()

    gather_through(block_ref, gathered, gathered_ref, send_sem, receive_sem, out_sem, prepare, compute)
    pair_rows = unit_grads.shape[1] // 8
    for number in range(8):
        out(number, pl.ds(number * pair_rows, pair_rows)).wait()


def gather_scratch(size, block, kind):
    return [
        pltpu.VMEM((size,) + block, kind),
        pltpu.SemaphoreType.DMA((Gather.slots,)),
        pltpu.SemaphoreType.DMA((size,)),
        pltpu.SemaphoreType.DMA((9,)),
    ]


def feed_first(block, feed_full, collective_id):
    size = lax.axis_size("fsdp")
    tokens, width, units, kind = size * block.shape[0], block.shape[1], feed_full.shape[2], block.dtype
    if size != KERNEL_FSDP:
        rows = lax.all_gather(block, "fsdp", axis=0, tiled=True)
        gate, up = contract(rows, feed_full[0], 1, 0), contract(rows, feed_full[1], 1, 0)
        return rows, jnp.stack([gate, up]), gelu_product(gate, up).astype(kind)
    rows, gate_up, hidden = scratch_call(
        feed_first_kernel,
        (
            jax.ShapeDtypeStruct((size,) + block.shape, kind),
            jax.ShapeDtypeStruct((2, tokens, units), jnp.float32),
            jax.ShapeDtypeStruct((tokens, units), kind),
        ),
        [
            *gather_scratch(size, block.shape, kind),
            pltpu.VMEM((2, width, units), kind),
            pltpu.VMEM((2, tokens, units), jnp.float32),
            pltpu.VMEM((tokens, units), kind),
            pltpu.SemaphoreType.DMA((1,)),
            pltpu.SemaphoreType.DMA((8,)),
            pltpu.SemaphoreType.DMA((8,)),
        ],
        collective_id,
        block,
        feed_full,
    )
    return rows.reshape(tokens, width), gate_up, hidden


def hidden_back(block, feed_full, gate_up, collective_id):
    size = lax.axis_size("fsdp")
    tokens, width, units, kind = size * block.shape[0], block.shape[1], feed_full.shape[2], block.dtype
    if size != KERNEL_FSDP:
        rows = lax.all_gather(block, "fsdp", axis=0, tiled=True)
        unused_out, pullback = jax.vjp(gelu_product, gate_up[0], gate_up[1])
        gradients = pullback(contract(rows, feed_full[2], 1, 0))
        return rows, jnp.stack(gradients).astype(kind)
    rows, unit_grads = scratch_call(
        hidden_back_kernel,
        (
            jax.ShapeDtypeStruct((size,) + block.shape, kind),
            jax.ShapeDtypeStruct((2, tokens, units), kind),
        ),
        [
            *gather_scratch(size, block.shape, kind),
            pltpu.VMEM((width, units), kind),
            pltpu.VMEM((2, tokens, units), jnp.float32),
            pltpu.VMEM((2, tokens, units), kind),
            pltpu.SemaphoreType.DMA((2,)),
            pltpu.SemaphoreType.DMA((8,)),
        ],
        collective_id,
        block,
        feed_full,
        gate_up,
    )
    return rows.reshape(tokens, width), unit_grads


def partial_pair(scatter, units, weights, block_rows, j, core, target):
    amount, width, _ = weights.shape
    step = 3 * 256
    spots = [pl.ds(pl.multiple_of(scatter.index(k, core) * block_rows, block_rows), block_rows) for k in (j, 4 + j)]

    def body(d, carry):
        at = pl.ds(pl.multiple_of(d * step, step), step)
        sums = None
        for i in range(amount):
            left = jnp.concatenate([units[i, spot, :] for spot in spots], axis=0)
            part = contract(left, weights[i, at, :], 1, 1)
            sums = part if sums is None else sums + part
        sums = sums.astype(target.dtype)
        target[j, :, at] = sums[:block_rows]
        target[4 + j, :, at] = sums[block_rows:]
        return carry

    lax.fori_loop(0, width // step, body, 0)


def feed_last_kernel(
    hidden_ref, weights_ref, out_ref,
    held, from_core, from_across, from_below, from_above, total, send_sem, across_sem, below_sem, above_sem,
    core_send_sem, core_sem, local_sem, for_core, hidden, weights,
):
    scatter = Scatter(
        (held, from_core, from_across, from_below, from_above, total), (send_sem, across_sem, below_sem, above_sem)
    )
    loads = [
        pltpu.make_async_copy(hidden_ref, hidden.at[0], local_sem.at[0]),
        pltpu.make_async_copy(weights_ref.at[pl.ds(2, 1)], weights, local_sem.at[1]),
    ]
    for copy in loads:
        copy.start()
    greet_line(scatter.z, (scatter.across, scatter.other), scatter.down, scatter.up)
    for copy in loads:
        copy.wait()

    def to_core(k):
        return remote(for_core.at[k], from_core.at[k], core_send_sem.at[k], core_sem.at[k], scatter.other)

    def share(j, carry):
        partial_pair(scatter, hidden, weights, out_ref.shape[0], j, 1 - scatter.c, for_core)
        to_core(j).start()
        to_core(4 + j).start()
        partial_pair(scatter, hidden, weights, out_ref.shape[0], j, scatter.c, held)
        to_core(j).wait_recv()
        scatter.side(j)
        return carry

    def along(i, carry):
        to_core(4 + i).wait_recv()
        scatter.line(i)
        return carry

    lax.fori_loop(0, 4, share, 0)
    lax.fori_loop(0, 3, along, 0)
    to_core(7).wait_recv()
    scatter.last()
    outward = pltpu.make_async_copy(total, out_ref, local_sem.at[2])
    outward.start()
    for k in range(8):
        to_core(k).wait_send()
    scatter.finish()
    outward.wait()


def feed_last(hidden, feed_full, collective_id):
    size = lax.axis_size("fsdp")
    tokens, width, kind = hidden.shape[0], feed_full.shape[1], hidden.dtype
    block = (tokens // size, width)
    if size != KERNEL_FSDP:
        sums = contract(hidden, feed_full[2], 1, 1).astype(kind)
        return scatter_fsdp((sums.reshape((size,) + block),))
    return scratch_call(
        feed_last_kernel,
        jax.ShapeDtypeStruct(block, jnp.float32),
        [
            *Scatter.scratch(block, kind),
            pltpu.SemaphoreType.DMA((8,)),
            pltpu.SemaphoreType.DMA((8,)),
            pltpu.SemaphoreType.DMA((3,)),
            pltpu.VMEM((8,) + block, kind),
            pltpu.VMEM((1,) + hidden.shape, kind),
            pltpu.VMEM((1,) + feed_full.shape[1:], kind),
        ],
        collective_id,
        hidden,
        feed_full,
    )


def feed_backward(unit_grads, feed_full, feed_input, feed_grad_rows, hidden, collective_id):
    size = lax.axis_size("fsdp")
    kind = hidden.dtype
    tokens, width = feed_input.shape
    if size != KERNEL_FSDP:
        gate_grad, up_grad = unit_grads[0], unit_grads[1]
        sums = contract(gate_grad, feed_full[0], 1, 1) + contract(up_grad, feed_full[1], 1, 1)
        return (
            scatter_fsdp((sums.astype(kind).reshape(size, tokens // size, width),)),
            jnp.stack(
                [
                    contract(left, right, 0, 0).astype(kind)
                    for left, right in ((feed_input, gate_grad), (feed_input, up_grad), (feed_grad_rows, hidden))
                ]
            ),
        )
    block, units = (tokens // size, width), hidden.shape[1]
    tile_rows = width // 6

    def kernel(unit_grads_ref, weights_ref, input_ref, grad_ref, hidden_ref, *refs):
        backward_kernel(unit_grads_ref, weights_ref, (input_ref, grad_ref), hidden_ref, *refs)

    rows_grad, weight_grads = scratch_call(
        kernel,
        (jax.ShapeDtypeStruct(block, jnp.float32), jax.ShapeDtypeStruct((3, width, units), kind)),
        [
            *Scatter.scratch(block, kind),
            pltpu.SemaphoreType.DMA((8,)),
            pltpu.SemaphoreType.DMA((8,)),
            pltpu.SemaphoreType.DMA((6,)),
            pltpu.VMEM((8,) + block, kind),
            pltpu.VMEM((3, tokens, units), kind),
            pltpu.VMEM((2, width, units), kind),
            pltpu.VMEM((2, tokens, width), kind),
            pltpu.VMEM((2, 3, tile_rows, units), kind),
            pltpu.SemaphoreType.DMA((2, 3)),
        ],
        collective_id,
        unit_grads,
        feed_full,
        feed_input,
        feed_grad_rows,
        hidden,
    )
    return rows_grad, weight_grads


def exchange_kernel(block_ref, out_ref, send_sem, receive_sem):
    index, t = lax.axis_index("fsdp"), lax.axis_index("tp")
    partner = (index, 1 - t)
    greet((partner,))
    copy = remote(block_ref, out_ref, send_sem.at[0], receive_sem.at[0], partner)
    copy.start()
    copy.wait()


def exchange_tp(block, collective_id):
    if lax.axis_size("fsdp") != KERNEL_FSDP:
        return lax.ppermute(block, "tp", [(0, 1), (1, 0)])
    return scratch_call(
        exchange_kernel,
        jax.ShapeDtypeStruct(block.shape, block.dtype),
        [pltpu.SemaphoreType.DMA((1,)), pltpu.SemaphoreType.DMA((1,))],
        collective_id,
        block,
    )


def peer(z, x, c, k):
    kz, kx, kc = k // 4, (k // 2) % 2, k % 2
    high, low = z // 2, z % 2
    high = 1 - high if kz // 2 else high
    low = 1 - low if kz % 2 else low
    return fsdp_index(high * 2 + low, 1 - x if kx else x, 1 - c if kc else c)


MAIN = 2 * LANES
REST = LANES
FIRST_REST = KERNEL_FSDP * MAIN
UNITS = 2 * MAIN + REST


def main_of(owner):
    return pl.ds(pl.multiple_of(owner * MAIN, MAIN), MAIN)


def rest_of(z):
    return pl.ds(pl.multiple_of(FIRST_REST + z * REST, REST), REST)


def distribute_kernel(
    rows_ref, query_ref, key_ref, value_ref, output_ref, gain_ref, gate_ref, up_ref, down_ref,
    attention_ref, partner_ref, feed_ref,
    stage, feed, zeros,
    gather_send, gather_receive, local_sem, pair_rows_sem, send_sem, receive_sem, rest_send, rest_receive,
    on_send, on_receive, rest_on_send, rest_on_receive,
):
    z, x, c, t = place()
    own = fsdp_index(z, x, c)
    partner = (own, 1 - t)
    greet([(peer(z, x, c, k), t) for k in range(1, 16)] + [partner])
    rows_copy = remote(rows_ref, partner_ref, pair_rows_sem.at[0], pair_rows_sem.at[1], partner)
    rows_copy.start()
    loads, start = [], 0
    for i, ref in enumerate((query_ref, key_ref, value_ref, output_ref, gain_ref)):
        loads.append(pltpu.make_async_copy(ref, stage.at[:, pl.ds(start, ref.shape[1])], local_sem.at[i]))
        start += ref.shape[1]
    feed_loads = [
        pltpu.make_async_copy(ref, feed.at[i], local_sem.at[5 + i])
        for i, ref in enumerate((gate_ref, up_ref, down_ref))
    ]
    for copy in loads + feed_loads:
        copy.start()
    for copy in loads:
        copy.wait()
    gather = Gather(stage, attention_ref, gather_send, gather_receive)
    gather.start()
    keep = pltpu.make_async_copy(stage, attention_ref.at[own], local_sem.at[8])
    keep.start()
    for copy in feed_loads:
        copy.wait()

    def main_at(half, source):
        return feed_ref.at[:, source, :, pl.ds(pl.multiple_of(half * MAIN, MAIN), MAIN)]

    def rest_at(source):
        return feed_ref.at[:, source, :, pl.ds(2 * MAIN, REST)]

    takes_rest = (c == 0) & (x == t)

    def direct(k):
        to = peer(z, x, c, k)
        return remote(feed.at[:, :, main_of(to)], main_at(t, own), send_sem.at[k], receive_sem.at[k], (to, t))

    def rest(dz):
        to_z = peer(z, x, c, 4 * dz) // 4
        slot = 4 * dz + 2 * ((x + t) % 2) + c
        return remote(
            feed.at[:, :, rest_of(to_z)], rest_at(own), rest_send.at[dz], rest_receive.at[slot], (fsdp_index(to_z, t, 0), t)
        )

    def onward(k):
        at = main_at(t, peer(z, x, c, k))
        return remote(at if k else feed.at[:, :, main_of(own)], at, on_send.at[k], on_receive.at[k], partner)

    def rest_onward(k):
        at = rest_at(peer(z, x, c, k))
        return remote(at if k else feed.at[:, :, rest_of(z)], at, rest_on_send.at[k], rest_on_receive.at[k], partner)

    def send(dz):
        for k in range(4 * dz, 4 * dz + 4):
            if k:
                direct(k).start()
        if dz:
            rest(dz).start()
        else:

            @pl.when(jnp.logical_not(takes_rest))
            def _():
                rest(0).start()

    def pass_on(dz):
        for k in range(4 * dz, 4 * dz + 4):
            if k:
                direct(k).wait_recv()
            onward(k).start()

        @pl.when(takes_rest)
        def _():
            for k in range(4 * dz, 4 * dz + 4):
                if k:
                    remote(
                        feed.at[:, :, rest_of(0)], rest_at(own), rest_send.at[0], rest_receive.at[k], partner
                    ).wait_recv()
                rest_onward(k).start()

    send(0)
    send(1)
    keep_main = pltpu.make_async_copy(feed.at[:, :, main_of(own)], main_at(t, own), local_sem.at[9])
    keep_main.start()
    keep_rest = pltpu.make_async_copy(feed.at[:, :, rest_of(z)], rest_at(own), local_sem.at[10])

    @pl.when(takes_rest)
    def _():
        keep_rest.start()

    fills = [
        pltpu.make_async_copy(zeros, feed_ref.at[i, :, :, pl.ds(2 * MAIN, REST)], local_sem.at[11 + i])
        for i in range(3)
    ]

    @pl.when(c == 1)
    def _():
        zeros[...] = jnp.zeros_like(zeros)
        for copy in fills:
            copy.start()

    send(2)
    pass_on(0)
    pass_on(1)
    gather.line(1)
    gather.side(0)
    send(3)
    gather.line(2)
    gather.side(1)
    pass_on(2)
    gather.line(3)
    pass_on(3)
    gather.side(2)
    gather.side(3)
    gather.finish()
    rows_copy.wait()
    for k in range(16):
        onward(k).wait_recv()
        onward(k).wait_send()
        if k:
            direct(k).wait_send()

    @pl.when(jnp.logical_not(takes_rest))
    def _():
        rest(0).wait_send()

    for dz in (1, 2, 3):
        rest(dz).wait_send()

    @pl.when(takes_rest)
    def _():
        for k in range(16):
            rest_onward(k).wait_send()
        keep_rest.wait()

    @pl.when((c == 0) & (x != t))
    def _():
        for k in range(16):
            rest_onward(k).wait_recv()

    @pl.when(c == 1)
    def _():
        for copy in fills:
            copy.wait()

    keep.wait()
    keep_main.wait()


def distribute(rows, attention, gain_columns, feed, collective_id):
    size = lax.axis_size("fsdp")
    shard_rows, feed_width = feed[0].shape
    columns = sum(w.shape[1] for w in attention) + gain_columns.shape[1]
    if size != KERNEL_FSDP:
        halves = lax.all_to_all(pack_units(feed, size), "fsdp", split_axis=0, concat_axis=0, tiled=True)
        halves = lax.all_gather(halves, "tp", axis=0)
        halves = halves.reshape(halves.shape[0], size * shard_rows, halves.shape[-1])
        return (
            lax.all_gather(jnp.concatenate((*attention, gain_columns), axis=1), "fsdp", axis=0),
            lax.ppermute(rows, "tp", [(0, 1), (1, 0)]),
            jnp.stack(join_units(halves, feed_width, size, 3)),
        )
    kind = rows.dtype
    attention_full, partner_rows, feed_full = scratch_call(
        distribute_kernel,
        (
            jax.ShapeDtypeStruct((size, shard_rows, columns), kind),
            jax.ShapeDtypeStruct(rows.shape, kind),
            jax.ShapeDtypeStruct((3, size, shard_rows, UNITS), kind),
        ),
        [
            pltpu.VMEM((shard_rows, columns), kind),
            pltpu.VMEM((3, shard_rows, feed_width), kind),
            pltpu.VMEM((size, shard_rows, REST), kind),
            pltpu.SemaphoreType.DMA((Gather.slots,)),
            pltpu.SemaphoreType.DMA((size,)),
            pltpu.SemaphoreType.DMA((14,)),
            pltpu.SemaphoreType.DMA((2,)),
            pltpu.SemaphoreType.DMA((size,)),
            pltpu.SemaphoreType.DMA((size,)),
            pltpu.SemaphoreType.DMA((4,)),
            pltpu.SemaphoreType.DMA((size,)),
            pltpu.SemaphoreType.DMA((size,)),
            pltpu.SemaphoreType.DMA((size,)),
            pltpu.SemaphoreType.DMA((size,)),
            pltpu.SemaphoreType.DMA((size,)),
        ],
        collective_id,
        rows,
        *attention,
        gain_columns,
        *feed,
    )
    return attention_full, partner_rows, feed_full.reshape(3, size * shard_rows, UNITS)


def collect_kernel(
    parts_ref, rows_ref, grad_rows_ref, projected_ref, attended_ref, gain_ref, out_ref, attention_ref,
    held, received, rest_held, rest_received,
    local_sem, pair_send, pair_receive, rest_pair_send, rest_pair_receive, send_sem, receive_sem, rest_send, rest_receive,
    *scatter_refs,
):
    scatter = Scatter(scatter_refs[:6], scatter_refs[6:10])
    for_core, left, projected, attended, core_send_sem, core_sem, operand_sem, gain_sem = scatter_refs[10:]
    operands = [
        pltpu.make_async_copy(source, target, operand_sem.at[i])
        for i, (source, target) in enumerate(
            ((rows_ref, left.at[0]), (grad_rows_ref, left.at[1]), (projected_ref, projected), (attended_ref, attended))
        )
    ]
    for copy in operands:
        copy.start()
    split, gain_start = projected.shape[1], projected.shape[1] + attended.shape[1]

    def gains(k, core, target, slot):
        return pltpu.make_async_copy(
            gain_ref.at[scatter.index(k, core)],
            target.at[k, :, pl.ds(gain_start, gain_ref.shape[2])],
            gain_sem.at[slot],
        )

    def weight_block(k, core, target):
        index = scatter.index(k, core)
        target[k, :, :split] = contract(left[0, index], projected[...], 1, 0).astype(target.dtype)
        target[k, :, split:gain_start] = contract(left[1, index], attended[...], 1, 0).astype(target.dtype)

    def to_core(k):
        return remote(
            for_core.at[k], scatter.from_core.at[k], core_send_sem.at[k], core_sem.at[k], scatter.other
        )

    def share(k, carry):
        weight_block(k, 1 - scatter.c, for_core)
        gains(k, 1 - scatter.c, for_core, k).wait()
        to_core(k).start()
        weight_block(k, scatter.c, scatter.held)
        gains(k, scatter.c, scatter.held, 8 + k).wait()

        @pl.when(k < 4)
        def _():
            to_core(k).wait_recv()
            scatter.side(k)

        return carry

    for k in range(8):
        gains(k, 1 - scatter.c, for_core, k).start()
        gains(k, scatter.c, scatter.held, 8 + k).start()
    z, x, c, t = place()
    own = fsdp_index(z, x, c)
    rows = out_ref.shape[1]
    partner = (own, 1 - t)
    parts = [parts_ref.at[i] for i in range(3)]
    order = (2, 3, 1, 0)
    takes_rest = (c == 0) & (x == t)
    gives_rest = (c == 0) & (x != t)

    def plane(dz):
        return pl.ds(peer(z, x, c, 4 * dz) // 4 * 4, 4)

    def half(which):
        return pl.ds(pl.multiple_of(which * MAIN, MAIN), MAIN)

    rest_columns = pl.ds(2 * MAIN, REST)

    def load(dz, i):
        return pltpu.make_async_copy(parts[i].at[plane(dz), :, half(t)], held.at[dz, i], local_sem.at[3 * dz + i])

    def rest_load(dz, i):
        return pltpu.make_async_copy(
            parts[i].at[plane(dz), :, rest_columns], rest_held.at[dz, i], local_sem.at[12 + 3 * dz + i]
        )

    def pair(dz, i):
        slot = 3 * dz + i
        return remote(
            parts[i].at[plane(dz), :, half(1 - t)], received.at[dz, i], pair_send.at[slot], pair_receive.at[slot], partner
        )

    def rest_pair(dz, i):
        slot = 3 * dz + i
        return remote(
            parts[i].at[plane(dz), :, rest_columns],
            rest_received.at[dz, i],
            rest_pair_send.at[slot],
            rest_pair_receive.at[slot],
            partner,
        )

    def spot(k):
        return peer(z, x, c, k) % 4

    def direct(k):
        return remote(
            held.at[k // 4, :, spot(k)], out_ref.at[:, :, main_of(own)], send_sem.at[k], receive_sem.at[k], (peer(z, x, c, k), t)
        )

    def rest_direct(k):
        return remote(
            rest_held.at[k // 4, :, spot(k)],
            out_ref.at[:, :, rest_of(z)],
            rest_send.at[k],
            rest_receive.at[z],
            (peer(z, x, c, k), t),
        )

    def add(target, source):
        def body(j, carry):
            i, at = j // 4, j % 4
            total = target[i, at].astype(jnp.float32) + source[i, at].astype(jnp.float32)
            target[i, at] = total.astype(target.dtype)
            return carry

        lax.fori_loop(0, 12, body, 0)

    for dz in order:
        for i in range(3):
            load(dz, i).start()

    @pl.when(takes_rest)
    def _():
        for dz in order:
            for i in range(3):
                rest_load(dz, i).start()

    greet([(peer(z, x, c, k), t) for k in range(1, 16)] + [partner])
    for dz in order:
        for i in range(3):
            pair(dz, i).start()

        @pl.when(gives_rest)
        def _():
            for i in range(3):
                rest_pair(dz, i).start()

    def pass_on(dz):
        for i in range(3):
            load(dz, i).wait()
            pair(dz, i).wait_recv()
        add(held.at[dz], received.at[dz])
        for k in range(4 * dz, 4 * dz + 4):
            if k:
                direct(k).start()

        @pl.when(takes_rest)
        def _():
            for i in range(3):
                rest_load(dz, i).wait()
                rest_pair(dz, i).wait_recv()
            add(rest_held.at[dz], rest_received.at[dz])
            for k in range(4 * dz, 4 * dz + 4):
                if k:
                    rest_direct(k).start()

    def line(i):
        to_core(4 + i).wait_recv()
        scatter.line(i)

    for copy in operands:
        copy.wait()
    lax.fori_loop(0, 8, share, 0)
    pass_on(2)
    line(0)
    pass_on(3)
    line(1)
    pass_on(1)
    line(2)
    pass_on(0)
    to_core(7).wait_recv()
    scatter.last()
    outward = pltpu.make_async_copy(scatter.total, attention_ref, local_sem.at[26])
    outward.start()
    keep = pltpu.make_async_copy(held.at[0, :, spot(0)], out_ref.at[:, :, main_of(own)], local_sem.at[24])
    keep.start()
    keep_rest = pltpu.make_async_copy(rest_held.at[0, :, spot(0)], out_ref.at[:, :, rest_of(z)], local_sem.at[25])

    @pl.when(takes_rest)
    def _():
        keep_rest.start()

    for k in range(1, 16):
        direct(k).wait_recv()

    for dz in range(4):
        from_z = peer(z, x, c, 4 * dz) // 4

        def arrived():
            remote(
                rest_held.at[0, :, 0], out_ref.at[:, :, rest_of(from_z)], rest_send.at[0], rest_receive.at[from_z], partner
            ).wait_recv()

        if dz:
            arrived()
        else:

            @pl.when(jnp.logical_not(takes_rest))
            def _():
                arrived()

    for k in range(1, 16):
        direct(k).wait_send()
    for dz in order:
        for i in range(3):
            pair(dz, i).wait_send()

    @pl.when(gives_rest)
    def _():
        for dz in order:
            for i in range(3):
                rest_pair(dz, i).wait_send()

    @pl.when(takes_rest)
    def _():
        for k in range(1, 16):
            rest_direct(k).wait_send()
        keep_rest.wait()

    for k in range(8):
        to_core(k).wait_send()
    scatter.finish()
    keep.wait()
    outward.wait()


def collect(gradients, feed_width, rows, projected, grad_rows, attended, gain_parts, collective_id):
    size, pairs = lax.axis_size("fsdp"), lax.axis_size("tp")
    shard_rows = gradients.shape[1] // size
    if size != KERNEL_FSDP:
        packed = part_units([gradients[i] for i in range(3)], feed_width, size, pairs)
        mine = lax.psum_scatter(packed, "tp", scatter_dimension=0, tiled=False)
        mine = mine.reshape(size, shard_rows, mine.shape[-1])
        mine = lax.all_to_all(mine, "fsdp", split_axis=0, concat_axis=0, tiled=True)
        feed = [g.astype(jnp.float32) for g in unpack_units(mine, feed_width, 3)]
        parts = (contract(rows, projected, 0, 0), contract(grad_rows, attended, 0, 0), gain_parts)
        return feed, scatter_fsdp([part.astype(rows.dtype).reshape(size, shard_rows, -1) for part in parts])
    kind = gradients.dtype
    main, rest = (4, 3, 4, shard_rows, MAIN), (4, 3, 4, shard_rows, REST)
    columns = projected.shape[1] + attended.shape[1] + gain_parts.shape[1]
    block, by_block = (shard_rows, columns), (size, shard_rows, rows.shape[0])
    out, attention = scratch_call(
        collect_kernel,
        (
            jax.ShapeDtypeStruct((3, shard_rows, feed_width), kind),
            jax.ShapeDtypeStruct(block, jnp.float32),
        ),
        [
            pltpu.VMEM(main, kind),
            pltpu.VMEM(main, kind),
            pltpu.VMEM(rest, kind),
            pltpu.VMEM(rest, kind),
            pltpu.SemaphoreType.DMA((27,)),
            pltpu.SemaphoreType.DMA((12,)),
            pltpu.SemaphoreType.DMA((12,)),
            pltpu.SemaphoreType.DMA((12,)),
            pltpu.SemaphoreType.DMA((12,)),
            pltpu.SemaphoreType.DMA((size,)),
            pltpu.SemaphoreType.DMA((size,)),
            pltpu.SemaphoreType.DMA((size,)),
            pltpu.SemaphoreType.DMA((4,)),
            *Scatter.scratch(block, kind),
            pltpu.VMEM((8,) + block, kind),
            pltpu.VMEM((2,) + by_block, kind),
            pltpu.VMEM(projected.shape, kind),
            pltpu.VMEM(attended.shape, kind),
            pltpu.SemaphoreType.DMA((8,)),
            pltpu.SemaphoreType.DMA((8,)),
            pltpu.SemaphoreType.DMA((4,)),
            pltpu.SemaphoreType.DMA((16,)),
        ],
        collective_id,
        gradients.reshape(3, size, shard_rows, UNITS),
        jnp.transpose(rows).reshape(by_block),
        jnp.transpose(grad_rows).reshape(by_block),
        projected,
        attended,
        gain_parts.astype(kind).reshape(size, shard_rows, -1),
    )
    return [out[i].astype(jnp.float32) for i in range(3)], attention


def contract_last(left_rows, right_rows):
    return lax.dot_general(
        left_rows, right_rows, (((1,), (1,)), ((), ())), preferred_element_type=jnp.float32
    )


def contract_first(left_rows, right_rows):
    return lax.dot_general(
        left_rows, right_rows, (((0,), (0,)), ((), ())), preferred_element_type=jnp.float32
    )


def normalize_parts(value_rows):
    inverse = lax.rsqrt(jnp.mean(value_rows * value_rows, axis=-1, keepdims=True) + EPSILON)
    return (value_rows * inverse, inverse)


def norm_backward(unit_rows, inverse, norm_gain, upstream):
    scaled = upstream * norm_gain
    return inverse * (scaled - unit_rows * jnp.mean(scaled * unit_rows, axis=-1, keepdims=True))


def layout(lengths_row, row_index):
    segment_ends = jnp.cumsum(lengths_row)
    segment_starts = segment_ends - lengths_row
    segment = jnp.sum((row_index[:, None] >= segment_ends[None, :]).astype(jnp.int32), axis=1)
    onehot = segment[:, None] == jnp.arange(lengths_row.shape[0], dtype=jnp.int32)[None, :]
    segment_begin = jnp.sum(jnp.where(onehot, segment_starts[None, :], 0), axis=1)
    prompt_shift = jnp.where(segment > 0, lengths_row[0], 0)
    return (segment, row_index - segment_begin + prompt_shift)


def rotary_tables(position):
    frequency = jnp.exp(
        jnp.arange(HEAD_SIZE // 2, dtype=jnp.float32) * (-2.0 * math.log(10000.0) / HEAD_SIZE)
    )
    angles = position.astype(jnp.float32)[:, None] * frequency[None, :]
    return (jnp.cos(angles), jnp.sin(angles))


def apply_rotary(value_rows, cosine_lookup, sine_lookup):
    half_width = value_rows.shape[-1] // 2
    first_half = value_rows[..., :half_width]
    second_half = value_rows[..., half_width:]
    cosine_part = cosine_lookup[:, None, :]
    sine_part = sine_lookup[:, None, :]
    return jnp.concatenate(
        [
            first_half * cosine_part - second_half * sine_part,
            second_half * cosine_part + first_half * sine_part,
        ],
        axis=-1,
    )


def unrotate(value_rows, cosine_lookup, sine_lookup):
    half_width = value_rows.shape[-1] // 2
    first_half = value_rows[..., :half_width]
    second_half = value_rows[..., half_width:]
    cosine_part = cosine_lookup[:, None, :]
    sine_part = sine_lookup[:, None, :]
    return jnp.concatenate(
        [
            first_half * cosine_part + second_half * sine_part,
            second_half * cosine_part - first_half * sine_part,
        ],
        axis=-1,
    )


def visible(segment, row_index):
    same_segment = (segment[:, None] == segment[None, :]) & (
        row_index[None, :] <= row_index[:, None]
    )
    from_prompt = (segment[None, :] == 0) & (segment[:, None] > 0)
    return same_segment | from_prompt


def masked_scores(rotated_query, rotated_key, visible_mask):
    raw_scores = jnp.einsum(
        "qgrd,kgd->grqk", rotated_query, rotated_key, preferred_element_type=jnp.float32
    )
    tanh_value = jnp.tanh(raw_scores * HEAD_SIZE ** (-0.5) / SOFTCAP)
    return (jnp.where(visible_mask[None, None], SOFTCAP * tanh_value, NEGATIVE), tanh_value)


def gelu_product(gate_value, up_value):
    return jax.nn.gelu(gate_value, approximate=True) * up_value


def split_columns(width, size):
    main = width // size // LANES * LANES
    return main, width // size - main


def pack_units(weights, size):
    rows, width = weights[0].shape
    main, rest = split_columns(width, size)
    pieces = []
    if main:
        pieces += [
            jnp.transpose(w[:, : main * size].reshape(rows, size, main), (1, 0, 2)) for w in weights
        ]
    if rest:
        pieces += [
            jnp.transpose(w[:, main * size :].reshape(rows, size, rest), (1, 0, 2)) for w in weights
        ]
    packed = jnp.concatenate(pieces, axis=2)
    return jnp.pad(packed, ((0, 0), (0, 0), (0, -packed.shape[2] % LANES)))


def unpack_units(packed, width, amount):
    size, rows, _ = packed.shape
    main, rest = split_columns(width, size)
    arrays = []
    for i in range(amount):
        pieces = []
        if main:
            piece = packed[:, :, i * main : (i + 1) * main]
            pieces.append(jnp.transpose(piece, (1, 0, 2)).reshape(rows, size * main))
        if rest:
            start = amount * main + i * rest
            piece = packed[:, :, start : start + rest]
            pieces.append(jnp.transpose(piece, (1, 0, 2)).reshape(rows, size * rest))
        arrays.append(jnp.concatenate(pieces, axis=1))
    return arrays


def join_units(halves, width, size, amount):
    main, rest = split_columns(width, size)
    arrays = []
    for i in range(amount):
        start = amount * main + i * rest
        pieces = [half[:, i * main : (i + 1) * main] for half in halves]
        pieces += [half[:, start : start + rest] for half in halves]
        joined = jnp.concatenate(pieces, axis=1)
        arrays.append(jnp.pad(joined, ((0, 0), (0, -joined.shape[1] % LANES))))
    return arrays


def part_units(arrays, width, size, pairs):
    main, rest = split_columns(width, size)
    halves = []
    for t in range(pairs):
        pieces = [array[:, t * main : (t + 1) * main] for array in arrays]
        start = pairs * main + t * rest
        pieces += [array[:, start : start + rest] for array in arrays]
        packed = jnp.concatenate(pieces, axis=1)
        halves.append(jnp.pad(packed, ((0, 0), (0, -packed.shape[1] % LANES))))
    return jnp.stack(halves)


def shards(
    block_input,
    lengths,
    attention_norm_gain,
    attention_post_gain,
    feedforward_norm_gain,
    feedforward_post_gain,
    query_weight,
    key_weight,
    value_weight,
    output_weight,
    gate_weight,
    up_weight,
    down_weight,
    output_cotangent,
):
    low = jnp.bfloat16
    size, pairs = lax.axis_size("fsdp"), lax.axis_size("tp")
    rows_local, width = block_input.shape
    shard_rows, feed_width = gate_weight.shape
    query_width, key_width = query_weight.shape[1], key_weight.shape[1]
    output_start = query_width + 2 * key_width
    gain_start = output_start + query_width
    grouped_rows = rows_local * pairs

    gain_columns = jnp.stack(
        [attention_norm_gain, attention_post_gain, feedforward_norm_gain, feedforward_post_gain],
        axis=1,
    )
    attention_full, other_input, feed_full = distribute(
        block_input,
        (query_weight, key_weight, value_weight, output_weight),
        jnp.pad(gain_columns, ((0, 0), (0, LANES - 4))),
        (gate_weight, up_weight, down_weight),
        1,
    )
    attention_full = attention_full.reshape(size * shard_rows, gain_start + LANES)
    gains = jnp.transpose(attention_full[:, gain_start : gain_start + 4]).astype(jnp.float32)
    gain_one, gain_two, gain_three, gain_four = gains[0], gains[1], gains[2], gains[3]

    row_index = (
        jnp.arange(grouped_rows, dtype=jnp.int32) + lax.axis_index("tp") * rows_local
    ) % grouped_rows
    segment, position = layout(lengths[0], row_index)
    cosine_lookup, sine_lookup = rotary_tables(position)
    visible_mask = visible(segment, row_index)
    residual_both = jnp.concatenate([block_input, other_input], axis=0).astype(jnp.float32)
    unit_one_both, inverse_one_both = normalize_parts(residual_both)
    residual = residual_both[:rows_local]
    unit_one, inverse_one = unit_one_both[:rows_local], inverse_one_both[:rows_local]
    normed = lax.optimization_barrier((unit_one_both * gain_one).astype(low))
    projected = jnp.dot(
        normed, attention_full[:, :output_start], preferred_element_type=jnp.float32
    )
    query_raw = projected[:, :query_width]
    key_raw = projected[:, query_width : query_width + key_width]
    value_raw = projected[:, query_width + key_width :]
    heads_local = query_width // HEAD_SIZE
    kv_local = key_width // HEAD_SIZE
    repeat_heads = heads_local // kv_local
    rotated_query = apply_rotary(
        query_raw.reshape(grouped_rows, heads_local, HEAD_SIZE), cosine_lookup, sine_lookup
    ).astype(low)
    rotated_query = rotated_query.reshape(grouped_rows, kv_local, repeat_heads, HEAD_SIZE)
    rotated_key = apply_rotary(
        key_raw.reshape(grouped_rows, kv_local, HEAD_SIZE), cosine_lookup, sine_lookup
    ).astype(low)
    value_reduced = value_raw.astype(low).reshape(grouped_rows, kv_local, HEAD_SIZE)
    capped, tanh_value = masked_scores(rotated_query, rotated_key, visible_mask)
    row_peak = jnp.max(capped, axis=-1, keepdims=True)
    exponentials = jnp.exp(capped - row_peak)
    softmax_probs = exponentials / jnp.sum(exponentials, axis=-1, keepdims=True)
    probs_low = softmax_probs.astype(low)
    mixed_heads = jnp.einsum(
        "grqk,kgd->qgrd", probs_low, value_reduced, preferred_element_type=jnp.float32
    )
    attended = mixed_heads.reshape(grouped_rows, heads_local * HEAD_SIZE).astype(low)
    output_full = attention_full[:, output_start:gain_start]
    branch_parts = contract_last(attended, output_full)
    branch_one = branch_parts[:rows_local] + exchange_tp(
        branch_parts[rows_local:].astype(low), 4
    ).astype(jnp.float32)
    unit_two, inverse_two = normalize_parts(branch_one)
    middle = residual + unit_two * gain_two
    unit_three, inverse_three = normalize_parts(middle)

    feed_input, gate_up, hidden = feed_first((unit_three * gain_three).astype(low), feed_full, 5)
    branch_two = feed_last(hidden, feed_full, 6)
    unit_four, inverse_four = normalize_parts(branch_two)
    block_output = (middle + unit_four * gain_four).astype(low)
    upstream = output_cotangent.astype(jnp.float32)
    gain_four_grad = jnp.sum(upstream * unit_four, axis=0)
    branch_two_grad = norm_backward(unit_four, inverse_four, gain_four, upstream).astype(low)
    feed_grad_rows, unit_grads = hidden_back(branch_two_grad, feed_full, gate_up, 7)
    normed_three_grad, feed_grads = feed_backward(
        unit_grads, feed_full, feed_input, feed_grad_rows, hidden, 8
    )
    gain_three_grad = jnp.sum(normed_three_grad * unit_three, axis=0)
    middle_grad = upstream + norm_backward(unit_three, inverse_three, gain_three, normed_three_grad)
    gain_two_grad = jnp.sum(middle_grad * unit_two, axis=0)
    branch_one_grad = norm_backward(unit_two, inverse_two, gain_two, middle_grad).astype(low)
    attention_grad_rows = jnp.concatenate(
        [branch_one_grad, exchange_tp(branch_one_grad, 10)], axis=0
    )
    mixed_grad = jnp.dot(
        attention_grad_rows, output_full, preferred_element_type=jnp.float32
    ).astype(low)
    mixed_grad = mixed_grad.reshape(grouped_rows, kv_local, repeat_heads, HEAD_SIZE)
    value_grad = jnp.einsum(
        "grqk,qgrd->kgd", probs_low, mixed_grad, preferred_element_type=jnp.float32
    )
    probs_grad = jnp.einsum(
        "qgrd,kgd->grqk", mixed_grad, value_reduced, preferred_element_type=jnp.float32
    )
    score_grad = softmax_probs * (
        probs_grad - jnp.sum(softmax_probs * probs_grad, axis=-1, keepdims=True)
    )
    raw_grad = (score_grad * (1.0 - tanh_value * tanh_value) * HEAD_SIZE ** (-0.5)).astype(low)
    query_grad = jnp.einsum(
        "grqk,kgd->qgrd", raw_grad, rotated_key, preferred_element_type=jnp.float32
    )
    key_grad = jnp.einsum(
        "grqk,qgrd->kgd", raw_grad, rotated_query, preferred_element_type=jnp.float32
    )
    query_grad = unrotate(
        query_grad.reshape(grouped_rows, heads_local, HEAD_SIZE), cosine_lookup, sine_lookup
    )
    key_grad = unrotate(key_grad, cosine_lookup, sine_lookup)
    projected_grad = jnp.concatenate(
        [
            query_grad.reshape(grouped_rows, heads_local * HEAD_SIZE).astype(low),
            key_grad.reshape(grouped_rows, kv_local * HEAD_SIZE).astype(low),
            value_grad.reshape(grouped_rows, kv_local * HEAD_SIZE).astype(low),
        ],
        axis=1,
    )
    input_parts = lax.optimization_barrier(
        contract_last(projected_grad, attention_full[:, :output_start])
    )

    gain_grads = jnp.stack(
        [
            jnp.sum(input_parts * unit_one_both, axis=0),
            gain_two_grad,
            gain_three_grad,
            gain_four_grad,
        ]
    )
    sent = jnp.concatenate(
        [input_parts[rows_local:].astype(low), jnp.pad(gain_grads, ((0, 12), (0, 0))).astype(low)]
    )
    received = exchange_tp(sent, 11).astype(jnp.float32)
    normed_one_grad = input_parts[:rows_local] + received[:rows_local]
    gain_grads = gain_grads + received[rows_local : rows_local + 4]
    input_gradient = middle_grad + norm_backward(unit_one, inverse_one, gain_one, normed_one_grad)

    (gate_weight_grad, up_weight_grad, down_weight_grad), attention_grads = collect(
        feed_grads,
        feed_width,
        normed,
        projected_grad,
        attention_grad_rows,
        attended,
        jnp.pad(jnp.transpose(gain_grads), ((0, 0), (0, LANES - 4))),
        9,
    )
    gain_shards = jnp.transpose(attention_grads[:, gain_start : gain_start + 4])
    return (
        block_output,
        input_gradient,
        gain_shards[0],
        gain_shards[1],
        gain_shards[2],
        gain_shards[3],
        attention_grads[:, :query_width],
        attention_grads[:, query_width : query_width + key_width],
        attention_grads[:, query_width + key_width : output_start],
        attention_grads[:, output_start:gain_start],
        gate_weight_grad,
        up_weight_grad,
        down_weight_grad,
    )


def solution(mesh):
    placed = (
        P(("fsdp", "tp"), None),
        P("fsdp", None),
        P("fsdp"),
        P("fsdp"),
        P("fsdp"),
        P("fsdp"),
        P("fsdp", "tp"),
        P("fsdp", "tp"),
        P("fsdp", "tp"),
        P("fsdp", "tp"),
        P("fsdp", "tp"),
        P("fsdp", "tp"),
        P("fsdp", "tp"),
        P(("fsdp", "tp"), None),
    )
    return jax.shard_map(
        shards,
        mesh=mesh,
        in_specs=placed,
        out_specs=(
            P(("fsdp", "tp"), None),
            P(("fsdp", "tp"), None),
            P("fsdp"),
            P("fsdp"),
            P("fsdp"),
            P("fsdp"),
            P("fsdp", "tp"),
            P("fsdp", "tp"),
            P("fsdp", "tp"),
            P("fsdp", "tp"),
            P("fsdp", "tp"),
            P("fsdp", "tp"),
            P("fsdp", "tp"),
        ),
        check_vma=False,
    )
```

```python
import functools
import math

import jax
import jax.numpy as jnp
from jax import lax
from jax.experimental import pallas as pl
from jax.experimental.pallas import tpu as pltpu
from jax.sharding import PartitionSpec as P

HEAD_SIZE = 256
MESH = pl.DeviceIdType.MESH
ANY = pl.BlockSpec(memory_space=pl.ANY)
LANES = 128

EPSILON = 1e-06
SOFTCAP = 50.0
NEGATIVE = -1e30

KERNEL_FSDP = 16


def place():
    index = lax.axis_index("fsdp")
    return index // 4, (index // 2) % 2, index % 2, lax.axis_index("tp")


def fsdp_index(z, x, c):
    return (z * 2 + x) * 2 + c


def remote(source, target, send_sem, receive_sem, device):
    return pltpu.make_async_remote_copy(
        src_ref=source,
        dst_ref=target,
        send_sem=send_sem,
        recv_sem=receive_sem,
        device_id=device,
        device_id_type=MESH,
    )


def greet(devices):
    barrier = pltpu.get_barrier_semaphore()
    for device in devices:
        pl.semaphore_signal(barrier, inc=1, device_id=device, device_id_type=MESH)
    pl.semaphore_wait(barrier, len(devices))


def greet_line(z, devices, down, up):
    barrier = pltpu.get_barrier_semaphore()
    for device in devices:
        pl.semaphore_signal(barrier, inc=1, device_id=device, device_id_type=MESH)

    @pl.when(z > 0)
    def _():
        pl.semaphore_signal(barrier, inc=1, device_id=down, device_id_type=MESH)

    @pl.when(z < 3)
    def _():
        pl.semaphore_signal(barrier, inc=1, device_id=up, device_id_type=MESH)

    pl.semaphore_wait(barrier, len(devices) + (z + 2) // 3 + (5 - z) // 3)


class Gather:
    slots = 29

    def __init__(self, block, out_ref, send_sem, receive_sem):
        self.block, self.out, self.send_sem, self.receive_sem = block, out_ref, send_sem, receive_sem
        self.z, self.x, self.c, t = place()
        z, x, c = self.z, self.x, self.c
        self.own = fsdp_index(z, x, c)
        self.down, self.up = (fsdp_index(z - 1, x, c), t), (fsdp_index(z + 1, x, c), t)
        self.across, self.other = (fsdp_index(z, 1 - x, c), t), (fsdp_index(z, x, 1 - c), t)

    def copy(self, source, index, slot, device):
        return remote(source, self.out.at[index], self.send_sem.at[slot], self.receive_sem.at[index], device)

    def relay(self, index, slot, device):
        self.copy(self.out.at[index], index, slot, device).start()

    def arrived(self, index):
        self.copy(self.block, index, 0, self.other).wait_recv()

    def sent(self, slot):
        self.copy(self.block, self.own, slot, self.other).wait_send()

    def start(self):
        @pl.when(self.z < 3)
        def _():
            self.copy(self.block, self.own, 0, self.up).start()

        @pl.when(self.z > 0)
        def _():
            self.copy(self.block, self.own, 1, self.down).start()

        self.copy(self.block, self.own, 2, self.across).start()
        self.copy(self.block, self.own, 3, self.other).start()

    def line(self, d):
        z, x, c = self.z, self.x, self.c

        @pl.when(z >= d)
        def _():
            index = fsdp_index(z - d, x, c)
            base = 4 + 3 * (d - 1)
            self.arrived(index)

            @pl.when(z < 3)
            def _():
                self.relay(index, base, self.up)

            self.relay(index, base + 1, self.across)
            self.relay(index, base + 2, self.other)

        @pl.when(z + d <= 3)
        def _():
            index = fsdp_index(z + d, x, c)
            base = 13 + 3 * (d - 1)
            self.arrived(index)

            @pl.when(z > 0)
            def _():
                self.relay(index, base, self.down)

            self.relay(index, base + 1, self.across)
            self.relay(index, base + 2, self.other)

    def side(self, d):
        z, x, c = self.z, self.x, self.c
        if d == 0:
            index = fsdp_index(z, 1 - x, c)
            self.arrived(index)
            self.relay(index, 22, self.other)
            return

        @pl.when(z >= d)
        def _():
            index = fsdp_index(z - d, 1 - x, c)
            self.arrived(index)
            self.relay(index, 22 + d, self.other)

        @pl.when(z + d <= 3)
        def _():
            index = fsdp_index(z + d, 1 - x, c)
            self.arrived(index)
            self.relay(index, 25 + d, self.other)

    def finish(self, waits=True):
        z = self.z
        if waits:
            for zi in range(4):
                for xi in range(2):
                    self.arrived(fsdp_index(zi, xi, 1 - self.c))

        @pl.when(z < 3)
        def _():
            self.sent(0)

        @pl.when(z > 0)
        def _():
            self.sent(1)

        for slot in (2, 3, 22):
            self.sent(slot)
        for d in (1, 2, 3):

            @pl.when(z >= d)
            def _():
                base = 4 + 3 * (d - 1)

                @pl.when(z < 3)
                def _():
                    self.sent(base)

                for slot in (base + 1, base + 2, 22 + d):
                    self.sent(slot)

            @pl.when(z + d <= 3)
            def _():
                base = 13 + 3 * (d - 1)

                @pl.when(z > 0)
                def _():
                    self.sent(base)

                for slot in (base + 1, base + 2, 25 + d):
                    self.sent(slot)


def scratch_call(kernel, outputs, scratch, collective_id, *operands):
    return pl.pallas_call(
        kernel,
        out_shape=outputs,
        in_specs=[ANY] * len(operands),
        out_specs=jax.tree.map(lambda _: ANY, outputs),
        scratch_shapes=scratch,
        compiler_params=pltpu.CompilerParams(
            collective_id=collective_id, has_side_effects=True, vmem_limit_bytes=60 * 1024 * 1024
        ),
    )(*operands)


def add_rows(rows, step, target, *sources):
    def body(i, carry):
        at = pl.ds(pl.multiple_of(i * step, step), step)
        total = sources[0][at, :].astype(jnp.float32)
        for source in sources[1:]:
            total = total + source[at, :].astype(jnp.float32)
        target[at, :] = total.astype(target.dtype)
        return carry

    lax.fori_loop(0, rows // step, body, 0)


class Scatter:
    def __init__(self, buffers, semaphores):
        self.held, self.from_core, self.from_across, self.from_below, self.from_above, self.total = buffers
        self.send_sem, self.across_sem, self.below_sem, self.above_sem = semaphores
        self.z, self.x, self.c, t = place()
        z, x, c = self.z, self.x, self.c
        self.rows = self.total.shape[0]
        self.down, self.up = (fsdp_index(z - 1, x, c), t), (fsdp_index(z + 1, x, c), t)
        self.across, self.other = (fsdp_index(z, 1 - x, c), t), (fsdp_index(z, x, 1 - c), t)

    def target(self, i):
        half = self.z // 2
        mirrored = self.z + half * (3 - 2 * self.z)
        base = 3 - i + mirrored * (i // 2) * (2 * (i % 2) - 1)
        return base + half * (3 - 2 * base)

    def index(self, k, core):
        return fsdp_index(self.target(k % 4), (self.x + 1 - k // 4) % 2, core)

    def add(self, target, *sources):
        add_rows(self.rows, 16, target, *sources)

    def over(self, i):
        return remote(
            self.held.at[i], self.from_across.at[i], self.send_sem.at[3 + i], self.across_sem.at[i], self.across
        )

    def going_up(self, i, target):
        return remote(
            self.held.at[4 + i], self.from_below.at[target], self.send_sem.at[i], self.below_sem.at[target], self.up
        )

    def going_down(self, i, target):
        return remote(
            self.held.at[4 + i], self.from_above.at[target], self.send_sem.at[i], self.above_sem.at[target], self.down
        )

    def side(self, i):
        self.add(self.held.at[i], self.held.at[i], self.from_core.at[i])
        self.over(i).start()

    def line(self, i):
        z, target = self.z, self.target(i)
        held = self.held.at[4 + i]
        sources = (held, self.from_core.at[4 + i], self.from_across.at[i])
        self.over(i).wait_recv()

        @pl.when(target > z)
        def _():
            @pl.when(z > 0)
            def _():
                self.going_up(i, target).wait_recv()
                self.add(held, *sources, self.from_below.at[target])

            @pl.when(z == 0)
            def _():
                self.add(held, *sources)

            self.going_up(i, target).start()

        @pl.when(target < z)
        def _():
            @pl.when(z < 3)
            def _():
                self.going_down(i, target).wait_recv()
                self.add(held, *sources, self.from_above.at[target])

            @pl.when(z == 3)
            def _():
                self.add(held, *sources)

            self.going_down(i, target).start()

    def last(self):
        z = self.z
        self.over(3).wait_recv()
        self.add(self.total, self.held.at[7], self.from_core.at[7], self.from_across.at[3])

        @pl.when(z > 0)
        def _():
            self.going_up(0, z).wait_recv()
            self.add(self.total, self.total, self.from_below.at[z])

        @pl.when(z < 3)
        def _():
            self.going_down(0, z).wait_recv()
            self.add(self.total, self.total, self.from_above.at[z])

    def finish(self):
        for i in range(4):
            self.over(i).wait_send()
        for i in range(3):
            self.going_up(i, 0).wait_send()

    @staticmethod
    def scratch(block, kind):
        return [
            *[pltpu.VMEM((amount,) + block, kind) for amount in (8, 8, 4, 4, 4)],
            pltpu.VMEM(block, jnp.float32),
            *[pltpu.SemaphoreType.DMA((amount,)) for amount in (7, 4, 4, 4)],
        ]


def contract(left, right, left_dim, right_dim):
    return lax.dot_general(
        left, right, (((left_dim,), (right_dim,)), ((), ())), preferred_element_type=jnp.float32
    )


def backward_kernel(
    unit_grads_ref, weights_ref, rows_ref, hidden_ref, out_ref, weight_grads_ref,
    held, from_core, from_across, from_below, from_above, total, send_sem, across_sem, below_sem, above_sem,
    core_send_sem, core_sem, local_sem, for_core, unit_grads, weights, rows, tile, tile_sem,
):
    scatter = Scatter(
        (held, from_core, from_across, from_below, from_above, total), (send_sem, across_sem, below_sem, above_sem)
    )
    block_rows, width = out_ref.shape
    loads = [
        pltpu.make_async_copy(unit_grads_ref, unit_grads.at[pl.ds(0, 2)], local_sem.at[0]),
        pltpu.make_async_copy(weights_ref.at[pl.ds(0, 2)], weights, local_sem.at[1]),
        pltpu.make_async_copy(hidden_ref, unit_grads.at[2], local_sem.at[2]),
        pltpu.make_async_copy(rows_ref[0], rows.at[0], local_sem.at[3]),
        pltpu.make_async_copy(rows_ref[1], rows.at[1], local_sem.at[4]),
    ]
    for copy in loads:
        copy.start()
    greet_line(scatter.z, (scatter.across, scatter.other), scatter.down, scatter.up)
    loads[0].wait()
    loads[1].wait()

    def to_core(k):
        return remote(for_core.at[k], from_core.at[k], core_send_sem.at[k], core_sem.at[k], scatter.other)

    tile_rows = tile.shape[2]

    def tile_out(u, i):
        at = pl.ds(pl.multiple_of(u * tile_rows, tile_rows), tile_rows)
        return pltpu.make_async_copy(tile.at[u % 2, i], weight_grads_ref.at[i, at, :], tile_sem.at[u % 2, i])

    def weight_tile(u):
        @pl.when(u == 0)
        def _():
            for copy in loads[2:]:
                copy.wait()

        @pl.when(u >= 2)
        def _():
            for i in range(3):
                tile_out(u - 2, i).wait()

        def body(i, carry):
            left = rows[i // 2, :, pl.ds(pl.multiple_of(u * tile_rows, tile_rows), tile_rows)]
            tile[u % 2, i] = contract(left, unit_grads[i], 0, 0).astype(tile.dtype)
            return carry

        lax.fori_loop(0, 3, body, 0)
        for i in range(3):
            tile_out(u, i).start()

    def step(n, carry):
        @pl.when(n < 4)
        def _():
            partial_pair(scatter, unit_grads, weights, block_rows, n, 1 - scatter.c, for_core)
            to_core(n).start()
            to_core(4 + n).start()
            partial_pair(scatter, unit_grads, weights, block_rows, n, scatter.c, held)
            to_core(n).wait_recv()
            scatter.side(n)

        @pl.when(n >= 4)
        def _():
            to_core(n).wait_recv()
            scatter.line(n - 4)

        @pl.when(n >= 4)
        def _():
            weight_tile(2 * n - 8)
            weight_tile(2 * n - 7)

        return carry

    lax.fori_loop(0, 7, step, 0)
    to_core(7).wait_recv()
    scatter.last()
    outward = pltpu.make_async_copy(total, out_ref, local_sem.at[5])
    outward.start()
    for k in range(8):
        to_core(k).wait_send()
    scatter.finish()
    for u in (4, 5):
        for i in range(3):
            tile_out(u, i).wait()
    outward.wait()


def scatter_fsdp(parts):
    return lax.psum_scatter(jnp.concatenate(parts, axis=2), "fsdp", scatter_dimension=0, tiled=False).astype(jnp.float32)


def gather_through(block_ref, gathered, gathered_ref, send_sem, receive_sem, out_sem, prepare, compute):
    gather = Gather(block_ref, gathered, send_sem, receive_sem)
    z, x, c = gather.z, gather.x, gather.c
    _, block_rows, width = gathered.shape
    own = pltpu.make_async_copy(block_ref, gathered.at[gather.own], out_sem.at[8])
    own.start()
    greet_line(z, (gather.across, gather.other), gather.down, gather.up)
    gather.start()

    def out(number):
        at = pl.ds(number * 2, 2)
        return pltpu.make_async_copy(gathered.at[at], gathered_ref.at[at], out_sem.at[number])

    def step(n, carry):
        @pl.when(n == 2)
        def _():
            gather.line(2)
            gather.side(1)

        @pl.when(n == 4)
        def _():
            gather.line(3)
            gather.side(2)

        @pl.when(n == 6)
        def _():
            gather.side(3)

        dz = n // 4 * 2 + n % 2
        side = (x + n // 2) % 2
        zi = (z // 2 + dz // 2) % 2 * 2 + (z + dz) % 2
        number = zi * 2 + side
        gather.arrived(fsdp_index(zi, side, 1 - c))
        out(number).start()
        left = gathered[pl.ds(number * 2, 2)].reshape(2 * block_rows, width)
        compute(number, pl.ds(pl.multiple_of(number * 2 * block_rows, 2 * block_rows), 2 * block_rows), left)
        return carry

    gather.line(1)
    gather.side(0)
    own.wait()
    prepare()
    lax.fori_loop(0, 8, step, 0)
    gather.finish(waits=False)
    for number in range(8):
        out(number).wait()


GELU_SCALE = math.sqrt(2.0 / math.pi)
GELU_CUBE = 0.044715


def feed_first_kernel(
    block_ref, weights_ref, gathered_ref, gate_up_ref, hidden_ref,
    gathered, send_sem, receive_sem, out_sem, weights, gate_up, hidden, load_sem, gate_up_sem, hidden_sem,
):
    load = pltpu.make_async_copy(weights_ref.at[pl.ds(0, 2)], weights, load_sem.at[0])
    load.start()

    def outs(number, rows):
        return (
            pltpu.make_async_copy(gate_up.at[:, rows, :], gate_up_ref.at[:, rows, :], gate_up_sem.at[number]),
            pltpu.make_async_copy(hidden.at[rows, :], hidden_ref.at[rows, :], hidden_sem.at[number]),
        )

    def compute(number, rows, left):
        gate = contract(left, weights[0], 1, 0)
        gate_up[0, rows, :] = gate
        up = contract(left, weights[1], 1, 0)
        gate_up[1, rows, :] = up
        gate = gate_up[0, rows, :]
        curve = jnp.tanh(GELU_SCALE * (gate + GELU_CUBE * (gate * gate * gate)))
        hidden[rows, :] = (0.5 * gate * (1.0 + curve) * up).astype(hidden.dtype)
        for copy in outs(number, rows):
            copy.start()

    gather_through(block_ref, gathered, gathered_ref, send_sem, receive_sem, out_sem, load.wait, compute)
    pair_rows = hidden.shape[0] // 8
    for number in range(8):
        for copy in outs(number, pl.ds(number * pair_rows, pair_rows)):
            copy.wait()


def hidden_back_kernel(
    block_ref, weights_ref, gate_up_ref, gathered_ref, unit_grads_ref,
    gathered, send_sem, receive_sem, out_sem, weights, gate_up, unit_grads, load_sem, grads_sem,
):
    loads = [
        pltpu.make_async_copy(weights_ref.at[2], weights, load_sem.at[0]),
        pltpu.make_async_copy(gate_up_ref, gate_up, load_sem.at[1]),
    ]
    for copy in loads:
        copy.start()

    def prepare():
        for copy in loads:
            copy.wait()

    def out(number, rows):
        return pltpu.make_async_copy(unit_grads.at[:, rows, :], unit_grads_ref.at[:, rows, :], grads_sem.at[number])

    def compute(number, rows, left):
        hidden_grad = contract(left, weights[...], 1, 0)
        gate, up = gate_up[0, rows, :], gate_up[1, rows, :]
        square = gate * gate
        curve = jnp.tanh(GELU_SCALE * (gate + GELU_CUBE * (square * gate)))
        inner = GELU_SCALE * (1.0 + 3.0 * GELU_CUBE * square)
        slope = 0.5 * (1.0 + curve) + 0.5 * gate * (1.0 - curve * curve) * inner
        unit_grads[0, rows, :] = (hidden_grad * up * slope).astype(unit_grads.dtype)
        unit_grads[1, rows, :] = (hidden_grad * (0.5 * gate * (1.0 + curve))).astype(unit_grads.dtype)
        out(number, rows).start()

    gather_through(block_ref, gathered, gathered_ref, send_sem, receive_sem, out_sem, prepare, compute)
    pair_rows = unit_grads.shape[1] // 8
    for number in range(8):
        out(number, pl.ds(number * pair_rows, pair_rows)).wait()


def gather_scratch(size, block, kind):
    return [
        pltpu.VMEM((size,) + block, kind),
        pltpu.SemaphoreType.DMA((Gather.slots,)),
        pltpu.SemaphoreType.DMA((size,)),
        pltpu.SemaphoreType.DMA((9,)),
    ]


def feed_first(block, feed_full, collective_id):
    size = lax.axis_size("fsdp")
    tokens, width, units, kind = size * block.shape[0], block.shape[1], feed_full.shape[2], block.dtype
    if size != KERNEL_FSDP:
        rows = lax.all_gather(block, "fsdp", axis=0, tiled=True)
        gate, up = contract(rows, feed_full[0], 1, 0), contract(rows, feed_full[1], 1, 0)
        return rows, jnp.stack([gate, up]), gelu_product(gate, up).astype(kind)
    rows, gate_up, hidden = scratch_call(
        feed_first_kernel,
        (
            jax.ShapeDtypeStruct((size,) + block.shape, kind),
            jax.ShapeDtypeStruct((2, tokens, units), jnp.float32),
            jax.ShapeDtypeStruct((tokens, units), kind),
        ),
        [
            *gather_scratch(size, block.shape, kind),
            pltpu.VMEM((2, width, units), kind),
            pltpu.VMEM((2, tokens, units), jnp.float32),
            pltpu.VMEM((tokens, units), kind),
            pltpu.SemaphoreType.DMA((1,)),
            pltpu.SemaphoreType.DMA((8,)),
            pltpu.SemaphoreType.DMA((8,)),
        ],
        collective_id,
        block,
        feed_full,
    )
    return rows.reshape(tokens, width), gate_up, hidden


def hidden_back(block, feed_full, gate_up, collective_id):
    size = lax.axis_size("fsdp")
    tokens, width, units, kind = size * block.shape[0], block.shape[1], feed_full.shape[2], block.dtype
    if size != KERNEL_FSDP:
        rows = lax.all_gather(block, "fsdp", axis=0, tiled=True)
        unused_out, pullback = jax.vjp(gelu_product, gate_up[0], gate_up[1])
        gradients = pullback(contract(rows, feed_full[2], 1, 0))
        return rows, jnp.stack(gradients).astype(kind)
    rows, unit_grads = scratch_call(
        hidden_back_kernel,
        (
            jax.ShapeDtypeStruct((size,) + block.shape, kind),
            jax.ShapeDtypeStruct((2, tokens, units), kind),
        ),
        [
            *gather_scratch(size, block.shape, kind),
            pltpu.VMEM((width, units), kind),
            pltpu.VMEM((2, tokens, units), jnp.float32),
            pltpu.VMEM((2, tokens, units), kind),
            pltpu.SemaphoreType.DMA((2,)),
            pltpu.SemaphoreType.DMA((8,)),
        ],
        collective_id,
        block,
        feed_full,
        gate_up,
    )
    return rows.reshape(tokens, width), unit_grads


def partial_pair(scatter, units, weights, block_rows, j, core, target):
    amount, width, _ = weights.shape
    step = 6 * 192
    spots = [pl.ds(pl.multiple_of(scatter.index(k, core) * block_rows, block_rows), block_rows) for k in (j, 4 + j)]

    def body(d, carry):
        at = pl.ds(pl.multiple_of(d * step, step), step)
        sums = None
        for i in range(amount):
            left = jnp.concatenate([units[i, spot, :] for spot in spots], axis=0)
            part = contract(left, weights[i, at, :], 1, 1)
            sums = part if sums is None else sums + part
        sums = sums.astype(target.dtype)
        target[j, :, at] = sums[:block_rows]
        target[4 + j, :, at] = sums[block_rows:]
        return carry

    lax.fori_loop(0, width // step, body, 0)


def feed_last_kernel(
    hidden_ref, weights_ref, out_ref,
    held, from_core, from_across, from_below, from_above, total, send_sem, across_sem, below_sem, above_sem,
    core_send_sem, core_sem, local_sem, for_core, hidden, weights,
):
    scatter = Scatter(
        (held, from_core, from_across, from_below, from_above, total), (send_sem, across_sem, below_sem, above_sem)
    )
    loads = [
        pltpu.make_async_copy(hidden_ref, hidden.at[0], local_sem.at[0]),
        pltpu.make_async_copy(weights_ref.at[pl.ds(2, 1)], weights, local_sem.at[1]),
    ]
    for copy in loads:
        copy.start()
    greet_line(scatter.z, (scatter.across, scatter.other), scatter.down, scatter.up)
    for copy in loads:
        copy.wait()

    def to_core(k):
        return remote(for_core.at[k], from_core.at[k], core_send_sem.at[k], core_sem.at[k], scatter.other)

    def share(j, carry):
        partial_pair(scatter, hidden, weights, out_ref.shape[0], j, 1 - scatter.c, for_core)
        to_core(j).start()
        to_core(4 + j).start()
        partial_pair(scatter, hidden, weights, out_ref.shape[0], j, scatter.c, held)
        to_core(j).wait_recv()
        scatter.side(j)
        return carry

    def along(i, carry):
        to_core(4 + i).wait_recv()
        scatter.line(i)
        return carry

    lax.fori_loop(0, 4, share, 0)
    lax.fori_loop(0, 3, along, 0)
    to_core(7).wait_recv()
    scatter.last()
    outward = pltpu.make_async_copy(total, out_ref, local_sem.at[2])
    outward.start()
    for k in range(8):
        to_core(k).wait_send()
    scatter.finish()
    outward.wait()


def feed_last(hidden, feed_full, collective_id):
    size = lax.axis_size("fsdp")
    tokens, width, kind = hidden.shape[0], feed_full.shape[1], hidden.dtype
    block = (tokens // size, width)
    if size != KERNEL_FSDP:
        sums = contract(hidden, feed_full[2], 1, 1).astype(kind)
        return scatter_fsdp((sums.reshape((size,) + block),))
    return scratch_call(
        feed_last_kernel,
        jax.ShapeDtypeStruct(block, jnp.float32),
        [
            *Scatter.scratch(block, kind),
            pltpu.SemaphoreType.DMA((8,)),
            pltpu.SemaphoreType.DMA((8,)),
            pltpu.SemaphoreType.DMA((3,)),
            pltpu.VMEM((8,) + block, kind),
            pltpu.VMEM((1,) + hidden.shape, kind),
            pltpu.VMEM((1,) + feed_full.shape[1:], kind),
        ],
        collective_id,
        hidden,
        feed_full,
    )


def feed_backward(unit_grads, feed_full, feed_input, feed_grad_rows, hidden, collective_id):
    size = lax.axis_size("fsdp")
    kind = hidden.dtype
    tokens, width = feed_input.shape
    if size != KERNEL_FSDP:
        gate_grad, up_grad = unit_grads[0], unit_grads[1]
        sums = contract(gate_grad, feed_full[0], 1, 1) + contract(up_grad, feed_full[1], 1, 1)
        return (
            scatter_fsdp((sums.astype(kind).reshape(size, tokens // size, width),)),
            jnp.stack(
                [
                    contract(left, right, 0, 0).astype(kind)
                    for left, right in ((feed_input, gate_grad), (feed_input, up_grad), (feed_grad_rows, hidden))
                ]
            ),
        )
    block, units = (tokens // size, width), hidden.shape[1]
    tile_rows = width // 6

    def kernel(unit_grads_ref, weights_ref, input_ref, grad_ref, hidden_ref, *refs):
        backward_kernel(unit_grads_ref, weights_ref, (input_ref, grad_ref), hidden_ref, *refs)

    rows_grad, weight_grads = scratch_call(
        kernel,
        (jax.ShapeDtypeStruct(block, jnp.float32), jax.ShapeDtypeStruct((3, width, units), kind)),
        [
            *Scatter.scratch(block, kind),
            pltpu.SemaphoreType.DMA((8,)),
            pltpu.SemaphoreType.DMA((8,)),
            pltpu.SemaphoreType.DMA((6,)),
            pltpu.VMEM((8,) + block, kind),
            pltpu.VMEM((3, tokens, units), kind),
            pltpu.VMEM((2, width, units), kind),
            pltpu.VMEM((2, tokens, width), kind),
            pltpu.VMEM((2, 3, tile_rows, units), kind),
            pltpu.SemaphoreType.DMA((2, 3)),
        ],
        collective_id,
        unit_grads,
        feed_full,
        feed_input,
        feed_grad_rows,
        hidden,
    )
    return rows_grad, weight_grads


def exchange_kernel(block_ref, out_ref, send_sem, receive_sem):
    index, t = lax.axis_index("fsdp"), lax.axis_index("tp")
    partner = (index, 1 - t)
    greet((partner,))
    copy = remote(block_ref, out_ref, send_sem.at[0], receive_sem.at[0], partner)
    copy.start()
    copy.wait()


def exchange_tp(block, collective_id):
    if lax.axis_size("fsdp") != KERNEL_FSDP:
        return lax.ppermute(block, "tp", [(0, 1), (1, 0)])
    return scratch_call(
        exchange_kernel,
        jax.ShapeDtypeStruct(block.shape, block.dtype),
        [pltpu.SemaphoreType.DMA((1,)), pltpu.SemaphoreType.DMA((1,))],
        collective_id,
        block,
    )


def peer(z, x, c, k):
    kz, kx, kc = k // 4, (k // 2) % 2, k % 2
    high, low = z // 2, z % 2
    high = 1 - high if kz // 2 else high
    low = 1 - low if kz % 2 else low
    return fsdp_index(high * 2 + low, 1 - x if kx else x, 1 - c if kc else c)


MAIN = 2 * LANES
REST = LANES
FIRST_REST = KERNEL_FSDP * MAIN
UNITS = 2 * MAIN + REST


def main_of(owner):
    return pl.ds(pl.multiple_of(owner * MAIN, MAIN), MAIN)


def rest_of(z):
    return pl.ds(pl.multiple_of(FIRST_REST + z * REST, REST), REST)


def distribute_kernel(
    rows_ref, query_ref, key_ref, value_ref, output_ref, gain_ref, gate_ref, up_ref, down_ref,
    attention_ref, partner_ref, feed_ref,
    stage, feed, zeros,
    gather_send, gather_receive, local_sem, pair_rows_sem, send_sem, receive_sem, rest_send, rest_receive,
    on_send, on_receive, rest_on_send, rest_on_receive,
):
    z, x, c, t = place()
    own = fsdp_index(z, x, c)
    partner = (own, 1 - t)
    greet([(peer(z, x, c, k), t) for k in range(1, 16)] + [partner])
    rows_copy = remote(rows_ref, partner_ref, pair_rows_sem.at[0], pair_rows_sem.at[1], partner)
    rows_copy.start()
    loads, start = [], 0
    for i, ref in enumerate((query_ref, key_ref, value_ref, output_ref, gain_ref)):
        loads.append(pltpu.make_async_copy(ref, stage.at[:, pl.ds(start, ref.shape[1])], local_sem.at[i]))
        start += ref.shape[1]
    feed_loads = [
        pltpu.make_async_copy(ref, feed.at[i], local_sem.at[5 + i])
        for i, ref in enumerate((gate_ref, up_ref, down_ref))
    ]
    for copy in loads + feed_loads:
        copy.start()
    for copy in loads:
        copy.wait()
    gather = Gather(stage, attention_ref, gather_send, gather_receive)
    gather.start()
    keep = pltpu.make_async_copy(stage, attention_ref.at[own], local_sem.at[8])
    keep.start()
    for copy in feed_loads:
        copy.wait()

    def main_at(half, source):
        return feed_ref.at[:, source, :, pl.ds(pl.multiple_of(half * MAIN, MAIN), MAIN)]

    def rest_at(source):
        return feed_ref.at[:, source, :, pl.ds(2 * MAIN, REST)]

    takes_rest = (c == 0) & (x == t)

    def direct(k):
        to = peer(z, x, c, k)
        return remote(feed.at[:, :, main_of(to)], main_at(t, own), send_sem.at[k], receive_sem.at[k], (to, t))

    def rest(dz):
        to_z = peer(z, x, c, 4 * dz) // 4
        slot = 4 * dz + 2 * ((x + t) % 2) + c
        return remote(
            feed.at[:, :, rest_of(to_z)], rest_at(own), rest_send.at[dz], rest_receive.at[slot], (fsdp_index(to_z, t, 0), t)
        )

    def onward(k):
        at = main_at(t, peer(z, x, c, k))
        return remote(at if k else feed.at[:, :, main_of(own)], at, on_send.at[k], on_receive.at[k], partner)

    def rest_onward(k):
        at = rest_at(peer(z, x, c, k))
        return remote(at if k else feed.at[:, :, rest_of(z)], at, rest_on_send.at[k], rest_on_receive.at[k], partner)

    def send(dz):
        for k in range(4 * dz, 4 * dz + 4):
            if k:
                direct(k).start()
        if dz:
            rest(dz).start()
        else:

            @pl.when(jnp.logical_not(takes_rest))
            def _():
                rest(0).start()

    def pass_on(dz):
        for k in range(4 * dz, 4 * dz + 4):
            if k:
                direct(k).wait_recv()
            onward(k).start()

        @pl.when(takes_rest)
        def _():
            for k in range(4 * dz, 4 * dz + 4):
                if k:
                    remote(
                        feed.at[:, :, rest_of(0)], rest_at(own), rest_send.at[0], rest_receive.at[k], partner
                    ).wait_recv()
                rest_onward(k).start()

    send(0)
    send(1)
    keep_main = pltpu.make_async_copy(feed.at[:, :, main_of(own)], main_at(t, own), local_sem.at[9])
    keep_main.start()
    keep_rest = pltpu.make_async_copy(feed.at[:, :, rest_of(z)], rest_at(own), local_sem.at[10])

    @pl.when(takes_rest)
    def _():
        keep_rest.start()

    fills = [
        pltpu.make_async_copy(zeros, feed_ref.at[i, :, :, pl.ds(2 * MAIN, REST)], local_sem.at[11 + i])
        for i in range(3)
    ]

    @pl.when(c == 1)
    def _():
        zeros[...] = jnp.zeros_like(zeros)
        for copy in fills:
            copy.start()

    send(2)
    pass_on(0)
    pass_on(1)
    gather.line(1)
    gather.side(0)
    send(3)
    gather.line(2)
    gather.side(1)
    pass_on(2)
    gather.line(3)
    pass_on(3)
    gather.side(2)
    gather.side(3)
    gather.finish()
    rows_copy.wait()
    for k in range(16):
        onward(k).wait_recv()
        onward(k).wait_send()
        if k:
            direct(k).wait_send()

    @pl.when(jnp.logical_not(takes_rest))
    def _():
        rest(0).wait_send()

    for dz in (1, 2, 3):
        rest(dz).wait_send()

    @pl.when(takes_rest)
    def _():
        for k in range(16):
            rest_onward(k).wait_send()
        keep_rest.wait()

    @pl.when((c == 0) & (x != t))
    def _():
        for k in range(16):
            rest_onward(k).wait_recv()

    @pl.when(c == 1)
    def _():
        for copy in fills:
            copy.wait()

    keep.wait()
    keep_main.wait()


def distribute(rows, attention, gain_columns, feed, collective_id):
    size = lax.axis_size("fsdp")
    shard_rows, feed_width = feed[0].shape
    columns = sum(w.shape[1] for w in attention) + gain_columns.shape[1]
    if size != KERNEL_FSDP:
        halves = lax.all_to_all(pack_units(feed, size), "fsdp", split_axis=0, concat_axis=0, tiled=True)
        halves = lax.all_gather(halves, "tp", axis=0)
        halves = halves.reshape(halves.shape[0], size * shard_rows, halves.shape[-1])
        return (
            lax.all_gather(jnp.concatenate((*attention, gain_columns), axis=1), "fsdp", axis=0),
            lax.ppermute(rows, "tp", [(0, 1), (1, 0)]),
            jnp.stack(join_units(halves, feed_width, size, 3)),
        )
    kind = rows.dtype
    attention_full, partner_rows, feed_full = scratch_call(
        distribute_kernel,
        (
            jax.ShapeDtypeStruct((size, shard_rows, columns), kind),
            jax.ShapeDtypeStruct(rows.shape, kind),
            jax.ShapeDtypeStruct((3, size, shard_rows, UNITS), kind),
        ),
        [
            pltpu.VMEM((shard_rows, columns), kind),
            pltpu.VMEM((3, shard_rows, feed_width), kind),
            pltpu.VMEM((size, shard_rows, REST), kind),
            pltpu.SemaphoreType.DMA((Gather.slots,)),
            pltpu.SemaphoreType.DMA((size,)),
            pltpu.SemaphoreType.DMA((14,)),
            pltpu.SemaphoreType.DMA((2,)),
            pltpu.SemaphoreType.DMA((size,)),
            pltpu.SemaphoreType.DMA((size,)),
            pltpu.SemaphoreType.DMA((4,)),
            pltpu.SemaphoreType.DMA((size,)),
            pltpu.SemaphoreType.DMA((size,)),
            pltpu.SemaphoreType.DMA((size,)),
            pltpu.SemaphoreType.DMA((size,)),
            pltpu.SemaphoreType.DMA((size,)),
        ],
        collective_id,
        rows,
        *attention,
        gain_columns,
        *feed,
    )
    return attention_full, partner_rows, feed_full.reshape(3, size * shard_rows, UNITS)


def collect_kernel(
    parts_ref, rows_ref, grad_rows_ref, projected_ref, attended_ref, gain_ref, out_ref, attention_ref,
    held, received, rest_held, rest_received,
    local_sem, pair_send, pair_receive, rest_pair_send, rest_pair_receive, send_sem, receive_sem, rest_send, rest_receive,
    *scatter_refs,
):
    scatter = Scatter(scatter_refs[:6], scatter_refs[6:10])
    for_core, left, projected, attended, core_send_sem, core_sem, operand_sem, gain_sem = scatter_refs[10:]
    operands = [
        pltpu.make_async_copy(source, target, operand_sem.at[i])
        for i, (source, target) in enumerate(
            ((rows_ref, left.at[0]), (grad_rows_ref, left.at[1]), (projected_ref, projected), (attended_ref, attended))
        )
    ]
    for copy in operands:
        copy.start()
    split, gain_start = projected.shape[1], projected.shape[1] + attended.shape[1]

    def gains(k, core, target, slot):
        return pltpu.make_async_copy(
            gain_ref.at[scatter.index(k, core)],
            target.at[k, :, pl.ds(gain_start, gain_ref.shape[2])],
            gain_sem.at[slot],
        )

    def weight_block(k, core, target):
        index = scatter.index(k, core)
        target[k, :, :split] = contract(left[0, index], projected[...], 1, 0).astype(target.dtype)
        target[k, :, split:gain_start] = contract(left[1, index], attended[...], 1, 0).astype(target.dtype)

    def to_core(k):
        return remote(
            for_core.at[k], scatter.from_core.at[k], core_send_sem.at[k], core_sem.at[k], scatter.other
        )

    def share(k, carry):
        weight_block(k, 1 - scatter.c, for_core)
        gains(k, 1 - scatter.c, for_core, k).wait()
        to_core(k).start()
        weight_block(k, scatter.c, scatter.held)
        gains(k, scatter.c, scatter.held, 8 + k).wait()

        @pl.when(k < 4)
        def _():
            to_core(k).wait_recv()
            scatter.side(k)

        return carry

    for k in range(8):
        gains(k, 1 - scatter.c, for_core, k).start()
        gains(k, scatter.c, scatter.held, 8 + k).start()
    z, x, c, t = place()
    own = fsdp_index(z, x, c)
    rows = out_ref.shape[1]
    partner = (own, 1 - t)
    parts = [parts_ref.at[i] for i in range(3)]
    order = (2, 3, 1, 0)
    takes_rest = (c == 0) & (x == t)
    gives_rest = (c == 0) & (x != t)

    def plane(dz):
        return pl.ds(peer(z, x, c, 4 * dz) // 4 * 4, 4)

    def half(which):
        return pl.ds(pl.multiple_of(which * MAIN, MAIN), MAIN)

    rest_columns = pl.ds(2 * MAIN, REST)

    def load(dz, i):
        return pltpu.make_async_copy(parts[i].at[plane(dz), :, half(t)], held.at[dz, i], local_sem.at[3 * dz + i])

    def rest_load(dz, i):
        return pltpu.make_async_copy(
            parts[i].at[plane(dz), :, rest_columns], rest_held.at[dz, i], local_sem.at[12 + 3 * dz + i]
        )

    def pair(dz, i):
        slot = 3 * dz + i
        return remote(
            parts[i].at[plane(dz), :, half(1 - t)], received.at[dz, i], pair_send.at[slot], pair_receive.at[slot], partner
        )

    def rest_pair(dz, i):
        slot = 3 * dz + i
        return remote(
            parts[i].at[plane(dz), :, rest_columns],
            rest_received.at[dz, i],
            rest_pair_send.at[slot],
            rest_pair_receive.at[slot],
            partner,
        )

    def spot(k):
        return peer(z, x, c, k) % 4

    def direct(k):
        return remote(
            held.at[k // 4, :, spot(k)], out_ref.at[:, :, main_of(own)], send_sem.at[k], receive_sem.at[k], (peer(z, x, c, k), t)
        )

    def rest_direct(k):
        return remote(
            rest_held.at[k // 4, :, spot(k)],
            out_ref.at[:, :, rest_of(z)],
            rest_send.at[k],
            rest_receive.at[z],
            (peer(z, x, c, k), t),
        )

    def add(target, source):
        def body(j, carry):
            i, at = j // 4, j % 4
            total = target[i, at].astype(jnp.float32) + source[i, at].astype(jnp.float32)
            target[i, at] = total.astype(target.dtype)
            return carry

        lax.fori_loop(0, 12, body, 0)

    for dz in order:
        for i in range(3):
            load(dz, i).start()

    @pl.when(takes_rest)
    def _():
        for dz in order:
            for i in range(3):
                rest_load(dz, i).start()

    greet([(peer(z, x, c, k), t) for k in range(1, 16)] + [partner])
    for dz in order:
        for i in range(3):
            pair(dz, i).start()

        @pl.when(gives_rest)
        def _():
            for i in range(3):
                rest_pair(dz, i).start()

    def pass_on(dz):
        for i in range(3):
            load(dz, i).wait()
            pair(dz, i).wait_recv()
        add(held.at[dz], received.at[dz])
        for k in range(4 * dz, 4 * dz + 4):
            if k:
                direct(k).start()

        @pl.when(takes_rest)
        def _():
            for i in range(3):
                rest_load(dz, i).wait()
                rest_pair(dz, i).wait_recv()
            add(rest_held.at[dz], rest_received.at[dz])
            for k in range(4 * dz, 4 * dz + 4):
                if k:
                    rest_direct(k).start()

    def line(i):
        to_core(4 + i).wait_recv()
        scatter.line(i)

    for copy in operands:
        copy.wait()
    lax.fori_loop(0, 8, share, 0)
    pass_on(2)
    line(0)
    pass_on(3)
    line(1)
    pass_on(1)
    line(2)
    pass_on(0)
    to_core(7).wait_recv()
    scatter.last()
    outward = pltpu.make_async_copy(scatter.total, attention_ref, local_sem.at[26])
    outward.start()
    keep = pltpu.make_async_copy(held.at[0, :, spot(0)], out_ref.at[:, :, main_of(own)], local_sem.at[24])
    keep.start()
    keep_rest = pltpu.make_async_copy(rest_held.at[0, :, spot(0)], out_ref.at[:, :, rest_of(z)], local_sem.at[25])

    @pl.when(takes_rest)
    def _():
        keep_rest.start()

    for k in range(1, 16):
        direct(k).wait_recv()

    for dz in range(4):
        from_z = peer(z, x, c, 4 * dz) // 4

        def arrived():
            remote(
                rest_held.at[0, :, 0], out_ref.at[:, :, rest_of(from_z)], rest_send.at[0], rest_receive.at[from_z], partner
            ).wait_recv()

        if dz:
            arrived()
        else:

            @pl.when(jnp.logical_not(takes_rest))
            def _():
                arrived()

    for k in range(1, 16):
        direct(k).wait_send()
    for dz in order:
        for i in range(3):
            pair(dz, i).wait_send()

    @pl.when(gives_rest)
    def _():
        for dz in order:
            for i in range(3):
                rest_pair(dz, i).wait_send()

    @pl.when(takes_rest)
    def _():
        for k in range(1, 16):
            rest_direct(k).wait_send()
        keep_rest.wait()

    for k in range(8):
        to_core(k).wait_send()
    scatter.finish()
    keep.wait()
    outward.wait()


def collect(gradients, feed_width, rows, projected, grad_rows, attended, gain_parts, collective_id):
    size, pairs = lax.axis_size("fsdp"), lax.axis_size("tp")
    shard_rows = gradients.shape[1] // size
    if size != KERNEL_FSDP:
        packed = part_units([gradients[i] for i in range(3)], feed_width, size, pairs)
        mine = lax.psum_scatter(packed, "tp", scatter_dimension=0, tiled=False)
        mine = mine.reshape(size, shard_rows, mine.shape[-1])
        mine = lax.all_to_all(mine, "fsdp", split_axis=0, concat_axis=0, tiled=True)
        feed = [g.astype(jnp.float32) for g in unpack_units(mine, feed_width, 3)]
        parts = (contract(rows, projected, 0, 0), contract(grad_rows, attended, 0, 0), gain_parts)
        return feed, scatter_fsdp([part.astype(rows.dtype).reshape(size, shard_rows, -1) for part in parts])
    kind = gradients.dtype
    main, rest = (4, 3, 4, shard_rows, MAIN), (4, 3, 4, shard_rows, REST)
    columns = projected.shape[1] + attended.shape[1] + gain_parts.shape[1]
    block, by_block = (shard_rows, columns), (size, shard_rows, rows.shape[0])
    out, attention = scratch_call(
        collect_kernel,
        (
            jax.ShapeDtypeStruct((3, shard_rows, feed_width), kind),
            jax.ShapeDtypeStruct(block, jnp.float32),
        ),
        [
            pltpu.VMEM(main, kind),
            pltpu.VMEM(main, kind),
            pltpu.VMEM(rest, kind),
            pltpu.VMEM(rest, kind),
            pltpu.SemaphoreType.DMA((27,)),
            pltpu.SemaphoreType.DMA((12,)),
            pltpu.SemaphoreType.DMA((12,)),
            pltpu.SemaphoreType.DMA((12,)),
            pltpu.SemaphoreType.DMA((12,)),
            pltpu.SemaphoreType.DMA((size,)),
            pltpu.SemaphoreType.DMA((size,)),
            pltpu.SemaphoreType.DMA((size,)),
            pltpu.SemaphoreType.DMA((4,)),
            *Scatter.scratch(block, kind),
            pltpu.VMEM((8,) + block, kind),
            pltpu.VMEM((2,) + by_block, kind),
            pltpu.VMEM(projected.shape, kind),
            pltpu.VMEM(attended.shape, kind),
            pltpu.SemaphoreType.DMA((8,)),
            pltpu.SemaphoreType.DMA((8,)),
            pltpu.SemaphoreType.DMA((4,)),
            pltpu.SemaphoreType.DMA((16,)),
        ],
        collective_id,
        gradients.reshape(3, size, shard_rows, UNITS),
        jnp.transpose(rows).reshape(by_block),
        jnp.transpose(grad_rows).reshape(by_block),
        projected,
        attended,
        gain_parts.astype(kind).reshape(size, shard_rows, -1),
    )
    return [out[i].astype(jnp.float32) for i in range(3)], attention


def contract_last(left_rows, right_rows):
    return lax.dot_general(
        left_rows, right_rows, (((1,), (1,)), ((), ())), preferred_element_type=jnp.float32
    )


def contract_first(left_rows, right_rows):
    return lax.dot_general(
        left_rows, right_rows, (((0,), (0,)), ((), ())), preferred_element_type=jnp.float32
    )


def normalize_parts(value_rows):
    inverse = lax.rsqrt(jnp.mean(value_rows * value_rows, axis=-1, keepdims=True) + EPSILON)
    return (value_rows * inverse, inverse)


def norm_backward(unit_rows, inverse, norm_gain, upstream):
    scaled = upstream * norm_gain
    return inverse * (scaled - unit_rows * jnp.mean(scaled * unit_rows, axis=-1, keepdims=True))


def layout(lengths_row, row_index):
    segment_ends = jnp.cumsum(lengths_row)
    segment_starts = segment_ends - lengths_row
    segment = jnp.sum((row_index[:, None] >= segment_ends[None, :]).astype(jnp.int32), axis=1)
    onehot = segment[:, None] == jnp.arange(lengths_row.shape[0], dtype=jnp.int32)[None, :]
    segment_begin = jnp.sum(jnp.where(onehot, segment_starts[None, :], 0), axis=1)
    prompt_shift = jnp.where(segment > 0, lengths_row[0], 0)
    return (segment, row_index - segment_begin + prompt_shift)


def rotary_tables(position):
    frequency = jnp.exp(
        jnp.arange(HEAD_SIZE // 2, dtype=jnp.float32) * (-2.0 * math.log(10000.0) / HEAD_SIZE)
    )
    angles = position.astype(jnp.float32)[:, None] * frequency[None, :]
    return (jnp.cos(angles), jnp.sin(angles))


def apply_rotary(value_rows, cosine_lookup, sine_lookup):
    half_width = value_rows.shape[-1] // 2
    first_half = value_rows[..., :half_width]
    second_half = value_rows[..., half_width:]
    cosine_part = cosine_lookup[:, None, :]
    sine_part = sine_lookup[:, None, :]
    return jnp.concatenate(
        [
            first_half * cosine_part - second_half * sine_part,
            second_half * cosine_part + first_half * sine_part,
        ],
        axis=-1,
    )


def unrotate(value_rows, cosine_lookup, sine_lookup):
    half_width = value_rows.shape[-1] // 2
    first_half = value_rows[..., :half_width]
    second_half = value_rows[..., half_width:]
    cosine_part = cosine_lookup[:, None, :]
    sine_part = sine_lookup[:, None, :]
    return jnp.concatenate(
        [
            first_half * cosine_part + second_half * sine_part,
            second_half * cosine_part - first_half * sine_part,
        ],
        axis=-1,
    )


def visible(segment, row_index):
    same_segment = (segment[:, None] == segment[None, :]) & (
        row_index[None, :] <= row_index[:, None]
    )
    from_prompt = (segment[None, :] == 0) & (segment[:, None] > 0)
    return same_segment | from_prompt


def masked_scores(rotated_query, rotated_key, visible_mask):
    raw_scores = jnp.einsum(
        "qgrd,kgd->grqk", rotated_query, rotated_key, preferred_element_type=jnp.float32
    )
    tanh_value = jnp.tanh(raw_scores * HEAD_SIZE ** (-0.5) / SOFTCAP)
    return (jnp.where(visible_mask[None, None], SOFTCAP * tanh_value, NEGATIVE), tanh_value)


def gelu_product(gate_value, up_value):
    return jax.nn.gelu(gate_value, approximate=True) * up_value


def split_columns(width, size):
    main = width // size // LANES * LANES
    return main, width // size - main


def pack_units(weights, size):
    rows, width = weights[0].shape
    main, rest = split_columns(width, size)
    pieces = []
    if main:
        pieces += [
            jnp.transpose(w[:, : main * size].reshape(rows, size, main), (1, 0, 2)) for w in weights
        ]
    if rest:
        pieces += [
            jnp.transpose(w[:, main * size :].reshape(rows, size, rest), (1, 0, 2)) for w in weights
        ]
    packed = jnp.concatenate(pieces, axis=2)
    return jnp.pad(packed, ((0, 0), (0, 0), (0, -packed.shape[2] % LANES)))


def unpack_units(packed, width, amount):
    size, rows, _ = packed.shape
    main, rest = split_columns(width, size)
    arrays = []
    for i in range(amount):
        pieces = []
        if main:
            piece = packed[:, :, i * main : (i + 1) * main]
            pieces.append(jnp.transpose(piece, (1, 0, 2)).reshape(rows, size * main))
        if rest:
            start = amount * main + i * rest
            piece = packed[:, :, start : start + rest]
            pieces.append(jnp.transpose(piece, (1, 0, 2)).reshape(rows, size * rest))
        arrays.append(jnp.concatenate(pieces, axis=1))
    return arrays


def join_units(halves, width, size, amount):
    main, rest = split_columns(width, size)
    arrays = []
    for i in range(amount):
        start = amount * main + i * rest
        pieces = [half[:, i * main : (i + 1) * main] for half in halves]
        pieces += [half[:, start : start + rest] for half in halves]
        joined = jnp.concatenate(pieces, axis=1)
        arrays.append(jnp.pad(joined, ((0, 0), (0, -joined.shape[1] % LANES))))
    return arrays


def part_units(arrays, width, size, pairs):
    main, rest = split_columns(width, size)
    halves = []
    for t in range(pairs):
        pieces = [array[:, t * main : (t + 1) * main] for array in arrays]
        start = pairs * main + t * rest
        pieces += [array[:, start : start + rest] for array in arrays]
        packed = jnp.concatenate(pieces, axis=1)
        halves.append(jnp.pad(packed, ((0, 0), (0, -packed.shape[1] % LANES))))
    return jnp.stack(halves)


def shards(
    block_input,
    lengths,
    attention_norm_gain,
    attention_post_gain,
    feedforward_norm_gain,
    feedforward_post_gain,
    query_weight,
    key_weight,
    value_weight,
    output_weight,
    gate_weight,
    up_weight,
    down_weight,
    output_cotangent,
):
    low = jnp.bfloat16
    size, pairs = lax.axis_size("fsdp"), lax.axis_size("tp")
    rows_local, width = block_input.shape
    shard_rows, feed_width = gate_weight.shape
    query_width, key_width = query_weight.shape[1], key_weight.shape[1]
    output_start = query_width + 2 * key_width
    gain_start = output_start + query_width
    grouped_rows = rows_local * pairs

    gain_columns = jnp.stack(
        [attention_norm_gain, attention_post_gain, feedforward_norm_gain, feedforward_post_gain],
        axis=1,
    )
    attention_full, other_input, feed_full = distribute(
        block_input,
        (query_weight, key_weight, value_weight, output_weight),
        jnp.pad(gain_columns, ((0, 0), (0, LANES - 4))),
        (gate_weight, up_weight, down_weight),
        1,
    )
    attention_full = attention_full.reshape(size * shard_rows, gain_start + LANES)
    gains = jnp.transpose(attention_full[:, gain_start : gain_start + 4]).astype(jnp.float32)
    gain_one, gain_two, gain_three, gain_four = gains[0], gains[1], gains[2], gains[3]

    row_index = (
        jnp.arange(grouped_rows, dtype=jnp.int32) + lax.axis_index("tp") * rows_local
    ) % grouped_rows
    segment, position = layout(lengths[0], row_index)
    cosine_lookup, sine_lookup = rotary_tables(position)
    visible_mask = visible(segment, row_index)
    residual_both = jnp.concatenate([block_input, other_input], axis=0).astype(jnp.float32)
    unit_one_both, inverse_one_both = normalize_parts(residual_both)
    residual = residual_both[:rows_local]
    unit_one, inverse_one = unit_one_both[:rows_local], inverse_one_both[:rows_local]
    normed = lax.optimization_barrier((unit_one_both * gain_one).astype(low))
    projected = jnp.dot(
        normed, attention_full[:, :output_start], preferred_element_type=jnp.float32
    )
    query_raw = projected[:, :query_width]
    key_raw = projected[:, query_width : query_width + key_width]
    value_raw = projected[:, query_width + key_width :]
    heads_local = query_width // HEAD_SIZE
    kv_local = key_width // HEAD_SIZE
    repeat_heads = heads_local // kv_local
    rotated_query = apply_rotary(
        query_raw.reshape(grouped_rows, heads_local, HEAD_SIZE), cosine_lookup, sine_lookup
    ).astype(low)
    rotated_query = rotated_query.reshape(grouped_rows, kv_local, repeat_heads, HEAD_SIZE)
    rotated_key = apply_rotary(
        key_raw.reshape(grouped_rows, kv_local, HEAD_SIZE), cosine_lookup, sine_lookup
    ).astype(low)
    value_reduced = value_raw.astype(low).reshape(grouped_rows, kv_local, HEAD_SIZE)
    capped, tanh_value = masked_scores(rotated_query, rotated_key, visible_mask)
    row_peak = jnp.max(capped, axis=-1, keepdims=True)
    exponentials = jnp.exp(capped - row_peak)
    softmax_probs = exponentials / jnp.sum(exponentials, axis=-1, keepdims=True)
    probs_low = softmax_probs.astype(low)
    mixed_heads = jnp.einsum(
        "grqk,kgd->qgrd", probs_low, value_reduced, preferred_element_type=jnp.float32
    )
    attended = mixed_heads.reshape(grouped_rows, heads_local * HEAD_SIZE).astype(low)
    output_full = attention_full[:, output_start:gain_start]
    branch_parts = contract_last(attended, output_full)
    branch_one = branch_parts[:rows_local] + exchange_tp(
        branch_parts[rows_local:].astype(low), 4
    ).astype(jnp.float32)
    unit_two, inverse_two = normalize_parts(branch_one)
    middle = residual + unit_two * gain_two
    unit_three, inverse_three = normalize_parts(middle)

    feed_input, gate_up, hidden = feed_first((unit_three * gain_three).astype(low), feed_full, 5)
    branch_two = feed_last(hidden, feed_full, 6)
    unit_four, inverse_four = normalize_parts(branch_two)
    block_output = (middle + unit_four * gain_four).astype(low)
    upstream = output_cotangent.astype(jnp.float32)
    gain_four_grad = jnp.sum(upstream * unit_four, axis=0)
    branch_two_grad = norm_backward(unit_four, inverse_four, gain_four, upstream).astype(low)
    feed_grad_rows, unit_grads = hidden_back(branch_two_grad, feed_full, gate_up, 7)
    normed_three_grad, feed_grads = feed_backward(
        unit_grads, feed_full, feed_input, feed_grad_rows, hidden, 8
    )
    gain_three_grad = jnp.sum(normed_three_grad * unit_three, axis=0)
    middle_grad = upstream + norm_backward(unit_three, inverse_three, gain_three, normed_three_grad)
    gain_two_grad = jnp.sum(middle_grad * unit_two, axis=0)
    branch_one_grad = norm_backward(unit_two, inverse_two, gain_two, middle_grad).astype(low)
    attention_grad_rows = jnp.concatenate(
        [branch_one_grad, exchange_tp(branch_one_grad, 10)], axis=0
    )
    mixed_grad = jnp.dot(
        attention_grad_rows, output_full, preferred_element_type=jnp.float32
    ).astype(low)
    mixed_grad = mixed_grad.reshape(grouped_rows, kv_local, repeat_heads, HEAD_SIZE)
    value_grad = jnp.einsum(
        "grqk,qgrd->kgd", probs_low, mixed_grad, preferred_element_type=jnp.float32
    )
    probs_grad = jnp.einsum(
        "qgrd,kgd->grqk", mixed_grad, value_reduced, preferred_element_type=jnp.float32
    )
    score_grad = softmax_probs * (
        probs_grad - jnp.sum(softmax_probs * probs_grad, axis=-1, keepdims=True)
    )
    raw_grad = (score_grad * (1.0 - tanh_value * tanh_value) * HEAD_SIZE ** (-0.5)).astype(low)
    query_grad = jnp.einsum(
        "grqk,kgd->qgrd", raw_grad, rotated_key, preferred_element_type=jnp.float32
    )
    key_grad = jnp.einsum(
        "grqk,qgrd->kgd", raw_grad, rotated_query, preferred_element_type=jnp.float32
    )
    query_grad = unrotate(
        query_grad.reshape(grouped_rows, heads_local, HEAD_SIZE), cosine_lookup, sine_lookup
    )
    key_grad = unrotate(key_grad, cosine_lookup, sine_lookup)
    projected_grad = jnp.concatenate(
        [
            query_grad.reshape(grouped_rows, heads_local * HEAD_SIZE).astype(low),
            key_grad.reshape(grouped_rows, kv_local * HEAD_SIZE).astype(low),
            value_grad.reshape(grouped_rows, kv_local * HEAD_SIZE).astype(low),
        ],
        axis=1,
    )
    input_parts = lax.optimization_barrier(
        contract_last(projected_grad, attention_full[:, :output_start])
    )

    gain_grads = jnp.stack(
        [
            jnp.sum(input_parts * unit_one_both, axis=0),
            gain_two_grad,
            gain_three_grad,
            gain_four_grad,
        ]
    )
    sent = jnp.concatenate(
        [input_parts[rows_local:].astype(low), jnp.pad(gain_grads, ((0, 12), (0, 0))).astype(low)]
    )
    received = exchange_tp(sent, 11).astype(jnp.float32)
    normed_one_grad = input_parts[:rows_local] + received[:rows_local]
    gain_grads = gain_grads + received[rows_local : rows_local + 4]
    input_gradient = middle_grad + norm_backward(unit_one, inverse_one, gain_one, normed_one_grad)

    (gate_weight_grad, up_weight_grad, down_weight_grad), attention_grads = collect(
        feed_grads,
        feed_width,
        normed,
        projected_grad,
        attention_grad_rows,
        attended,
        jnp.pad(jnp.transpose(gain_grads), ((0, 0), (0, LANES - 4))),
        9,
    )
    gain_shards = jnp.transpose(attention_grads[:, gain_start : gain_start + 4])
    return (
        block_output,
        input_gradient,
        gain_shards[0],
        gain_shards[1],
        gain_shards[2],
        gain_shards[3],
        attention_grads[:, :query_width],
        attention_grads[:, query_width : query_width + key_width],
        attention_grads[:, query_width + key_width : output_start],
        attention_grads[:, output_start:gain_start],
        gate_weight_grad,
        up_weight_grad,
        down_weight_grad,
    )


def solution(mesh):
    placed = (
        P(("fsdp", "tp"), None),
        P("fsdp", None),
        P("fsdp"),
        P("fsdp"),
        P("fsdp"),
        P("fsdp"),
        P("fsdp", "tp"),
        P("fsdp", "tp"),
        P("fsdp", "tp"),
        P("fsdp", "tp"),
        P("fsdp", "tp"),
        P("fsdp", "tp"),
        P("fsdp", "tp"),
        P(("fsdp", "tp"), None),
    )
    return jax.shard_map(
        shards,
        mesh=mesh,
        in_specs=placed,
        out_specs=(
            P(("fsdp", "tp"), None),
            P(("fsdp", "tp"), None),
            P("fsdp"),
            P("fsdp"),
            P("fsdp"),
            P("fsdp"),
            P("fsdp", "tp"),
            P("fsdp", "tp"),
            P("fsdp", "tp"),
            P("fsdp", "tp"),
            P("fsdp", "tp"),
            P("fsdp", "tp"),
            P("fsdp", "tp"),
        ),
        check_vma=False,
    )
```
